32 devices in a mesh: seq: 4 (over y, x), batch: 8 (over z, core).
Axes of the slice: x: 2, y: 2, z: 4, core: 2. Of those that a mesh axis runs over, the one named last changes fastest.
Arguments:
- layer_input: bfloat16 [8, 1024, 2048], P('batch', 'seq'), may hold values from -6 to 6
- segments: int32 [8, 1024], P('batch', 'seq'), may hold values from 0 to 128, as said below
- mixer_gain: bfloat16 [2048], P(('seq', 'batch')), may hold values from 0.5 to 1.5
- query_weight: bfloat16 [2048, 2048], P(('seq', 'batch')), may hold values from -0.125 to 0.125
- key_weight: bfloat16 [2048, 2048], P(('seq', 'batch')), may hold values from -0.125 to 0.125
- value_weight: bfloat16 [2048, 2048], P(('seq', 'batch')), may hold values from -0.125 to 0.125
- squeeze: bfloat16 [2048, 16], P(('seq', 'batch')), may hold values from -0.125 to 0.125
- expand: bfloat16 [16, 256], P(None, ('seq', 'batch')), may hold values from -1.5 to 1.5
- forget_bias: bfloat16 [256], P(('seq', 'batch')), may hold values from 1 to 9
- swish_weight: bfloat16 [2048, 2048], P(('seq', 'batch')), may hold values from -0.125 to 0.125
- head_gain: bfloat16 [2048], P(('seq', 'batch')), may hold values from 0.5 to 1.5
- output_weight: bfloat16 [2048, 2048], P(('seq', 'batch')), may hold values from -0.125 to 0.125
- feed_gain: bfloat16 [2048], P(('seq', 'batch')), may hold values from 0.5 to 1.5
- gate_weight: bfloat16 [2048, 5632], P(('seq', 'batch')), may hold values from -0.125 to 0.125
- up_weight: bfloat16 [2048, 5632], P(('seq', 'batch')), may hold values from -0.125 to 0.125
- down_weight: bfloat16 [5632, 2048], P(('seq', 'batch')), may hold values from -0.078125 to 0.078125
- cotangent: bfloat16 [8, 1024, 2048], P('batch', 'seq'), may hold values from -6 to 6
Outputs:
- layer_output: bfloat16 [8, 1024, 2048], P('batch', 'seq')
- grad_input: bfloat16 [8, 1024, 2048], P('batch', 'seq')
- grad_mixer: float32 [2048], P(('seq', 'batch'))
- grad_query: float32 [2048, 2048], P(('seq', 'batch'))
- grad_key: float32 [2048, 2048], P(('seq', 'batch'))
- grad_value: float32 [2048, 2048], P(('seq', 'batch'))
- grad_squeeze: float32 [2048, 16], P(('seq', 'batch'))
- grad_expand: float32 [16, 256], P(None, ('seq', 'batch'))
- grad_bias: float32 [256], P(('seq', 'batch'))
- grad_swish: float32 [2048, 2048], P(('seq', 'batch'))
- grad_head: float32 [2048], P(('seq', 'batch'))
- grad_output: float32 [2048, 2048], P(('seq', 'batch'))
- grad_feed: float32 [2048], P(('seq', 'batch'))
- grad_gate: float32 [2048, 5632], P(('seq', 'batch'))
- grad_up: float32 [2048, 5632], P(('seq', 'batch'))
- grad_down: float32 [5632, 2048], P(('seq', 'batch'))
The draws below stay inside these ranges and needn't reach their ends.
Inputs may be any that keep to these rules, and one draw needn't show every extreme that they name: `segments`: document numbers start at 0 in each sequence, never fall and rise by one where a document starts; each sequence holds exactly 129 documents. In every sequence one document begins within the first 128 positions and ends within the last 128; all other documents lie there too.
All inputs are finite; a program needn't handle non-finite values.
Results may differ from the reference program's by a relative error of at most 0.025.
Values may be sent and summed in bfloat16 or wider, within the bound.
A program may use at most 512 MiB of HBM per device.

```python
import jax
import jax.numpy as jnp
from jax import lax

D = 2048
HEADS = 4
SLOTS = 64
FF = 5632
RANK = 16
TOK_DEV = 256
SEQS = 8
LEN = 1024


def draw_segments(key, part):
    half = TOK_DEV // 2
    count = half
    candidates = jnp.concatenate([jnp.arange(1, half, dtype=jnp.int32), jnp.arange(LEN - half + 1, LEN, dtype=jnp.int32)])
    width = candidates.shape[0]
    scores = jax.random.randint(key, (SEQS, width), 0, 1 << 20) * width + jnp.arange(width, dtype=jnp.int32)[None, :]
    order = jnp.argsort(scores, axis=1, stable=True)[:, :count]
    chosen = candidates[order]
    position = jnp.arange(LEN, dtype=jnp.int32)[None, None, :]
    starts = jnp.any(position == chosen[:, :, None], axis=1)
    return jnp.cumsum(starts.astype(jnp.int32), axis=1).astype(jnp.int32)


def draw_forget_bias(key, part):
    count_all = HEADS * SLOTS
    return jax.random.uniform(key, (count_all,), jnp.float32, 1.0, 8.5).astype(jnp.bfloat16)


def shard_levels(rng, shape, pieces, smallest, top_value):
    gain = 1.0
    for axis_at, shards_of in pieces:
        steps = jax.random.uniform(jax.random.fold_in(jax.random.fold_in(rng, 6), axis_at), (shards_of,), jnp.float32, smallest / len(pieces), top_value / len(pieces))
        gain = gain * jnp.repeat(jnp.exp(steps), shape[axis_at] // shards_of).reshape((-1,) + (1,) * (len(shape) - 1 - axis_at))
    return gain


def bell_draw(rng, dims, deviation, bound, cuts=(), kind=jnp.bfloat16):
    gain = shard_levels(rng, dims, cuts, -0.22, 0.18) if cuts else 1.0
    entries = jax.random.normal(rng, dims, jnp.float32) * deviation * gain
    return jnp.minimum(jnp.maximum(entries, -bound), bound).astype(kind)


def setup_inputs(seed: int = 0) -> dict:
    key_of = jax.random.split(jax.random.key(seed), 18)
    return {
        "layer_input": bell_draw(key_of[0], (SEQS, LEN, D), 1.0, 6.0, ((0, 8), (1, 4))),
        "segments": draw_segments(jax.random.fold_in(key_of[17], 71), 0),
        "mixer_gain": jnp.clip(1.0 + 0.1 * jax.random.normal(key_of[2], (D,), jnp.float32), 0.5, 1.5).astype(jnp.bfloat16),
        "query_weight": bell_draw(key_of[3], (D, D), D ** -0.5, 0.125, ((0, 32),)),
        "key_weight": bell_draw(key_of[4], (D, D), D ** -0.5, 0.125, ((0, 32),)),
        "value_weight": bell_draw(key_of[5], (D, D), D ** -0.5, 0.125, ((0, 32),)),
        "squeeze": bell_draw(key_of[6], (D, RANK), D ** -0.5, 0.125, ((0, 32),)),
        "expand": bell_draw(key_of[7], (RANK, HEADS * SLOTS), RANK ** -0.5, 1.5, ((1, 32),)),
        "forget_bias": draw_forget_bias(jax.random.fold_in(key_of[17], 71), 0),
        "swish_weight": bell_draw(key_of[9], (D, D), D ** -0.5, 0.125, ((0, 32),)),
        "head_gain": jnp.clip(1.0 + 0.1 * jax.random.normal(key_of[10], (D,), jnp.float32), 0.5, 1.5).astype(jnp.bfloat16),
        "output_weight": bell_draw(key_of[11], (D, D), D ** -0.5, 0.125, ((0, 32),)),
        "feed_gain": jnp.clip(1.0 + 0.1 * jax.random.normal(key_of[12], (D,), jnp.float32), 0.5, 1.5).astype(jnp.bfloat16),
        "gate_weight": bell_draw(key_of[13], (D, FF), D ** -0.5, 0.125, ((0, 32),)),
        "up_weight": bell_draw(key_of[14], (D, FF), D ** -0.5, 0.125, ((0, 32),)),
        "down_weight": bell_draw(key_of[15], (FF, D), FF ** -0.5, 0.078125, ((0, 32),)),
        "cotangent": bell_draw(key_of[16], (SEQS, LEN, D), 1.0, 6.0, ((0, 8), (1, 4))),
    }


EPS = 1e-06
TAU_GATE = 8.0

@jax.custom_vjp
def low(v):
    return lax.optimization_barrier(v.astype(jnp.bfloat16)).astype(jnp.float32)

@jax.custom_vjp
def low_back(v):
    return v

def low_keep(v):
    return (low(v), None)

def low_pass(kept, grad):
    return (grad,)

def back_keep(v):
    return (v, None)

def back_low(kept, grad):
    return (low(grad),)
low.defvjp(low_keep, low_pass)
low_back.defvjp(back_keep, back_low)

def highest(left, right):
    return jnp.dot(left, right, precision=lax.Precision.HIGHEST, preferred_element_type=jnp.float32)

def rms_scale(features):
    return lax.rsqrt(lax.optimization_barrier(jnp.mean(features * features, axis=-1, keepdims=True)) + EPS)

def head_block(query_rows, key_rows, value_rows, log_rate, segment, last_prev, key_state, value_state):
    positions = jnp.arange(query_rows.shape[0])
    factor = query_rows.shape[1] ** (-0.25)
    cumulative = jnp.cumsum(log_rate, axis=0)
    inflow = -jnp.expm1(log_rate)
    visible = (segment[:, None] == segment[None, :]) & (positions[None, :] <= positions[:, None])
    spread = jnp.where(visible[:, :, None], cumulative[:, None, :] - cumulative[None, :, :], 0.0)
    weight = jnp.exp(spread) * visible.astype(jnp.float32)[:, :, None] * inflow[None, :, :]
    carried = (segment == last_prev).astype(jnp.float32)[:, None] * jnp.exp(cumulative)
    scores = highest(query_rows, key_rows.T) * factor
    logits = jnp.einsum('tsm,ts->tm', weight, scores, precision=lax.Precision.HIGHEST)
    logits = logits + carried * highest(query_rows, key_state.T) * factor
    attention = jax.nn.softmax(logits, axis=-1)
    mixing = jnp.einsum('tm,tsm->ts', attention, weight, precision=lax.Precision.HIGHEST)
    output = highest(mixing, value_rows) + highest(attention * carried, value_state)
    key_end = highest(weight[-1].T, key_rows) + carried[-1][:, None] * key_state
    value_end = highest(weight[-1].T, value_rows) + carried[-1][:, None] * value_state
    return (output, key_end, value_end)

def sequence_forward(inputs_seq, segment, weights):
    mixer_gain, query_weight, key_weight, value_weight, squeeze, expand, forget_bias, swish_weight, head_gain, output_weight, feed_gain, gate_weight, up_weight, down_weight = weights
    length = inputs_seq.shape[0]
    model_width = inputs_seq.shape[1]
    head_size = model_width // HEADS
    blocks = length // TOK_DEV
    normed = low(inputs_seq * rms_scale(inputs_seq) * mixer_gain)
    query_rows = low(low_back(highest(normed, query_weight)))
    key_rows = low(low_back(highest(normed, key_weight)))
    value_rows = low(low_back(highest(normed, value_weight)))
    reduced = low(low_back(highest(normed, squeeze)))
    forget_logit = low_back(highest(reduced, expand) + forget_bias)
    log_rate = jax.nn.log_sigmoid(forget_logit) / TAU_GATE
    swish_pre = low_back(highest(normed, swish_weight))

    def split_heads(rows_in, inner):
        return rows_in.reshape(blocks, TOK_DEV, HEADS, inner).transpose(0, 2, 1, 3)
    items = (split_heads(query_rows, head_size), split_heads(key_rows, head_size), split_heads(value_rows, head_size), split_heads(log_rate, SLOTS), segment.reshape(blocks, TOK_DEV))

    def block_step(carried, per_block):
        key_state, value_state, last_prev = carried
        query_block, key_block, value_block, rate_block, segment_block = per_block
        outputs, key_end, value_end = jax.vmap(head_block, in_axes=(0, 0, 0, 0, None, None, 0, 0))(query_block, key_block, value_block, rate_block, segment_block, last_prev, key_state, value_state)
        return ((key_end, value_end, segment_block[-1]), outputs)
    zero_state = jnp.zeros((HEADS, SLOTS, head_size), jnp.float32)
    initial = (zero_state, zero_state, jnp.asarray(-1.0, dtype=jnp.float32))
    _, mixed = lax.scan(jax.checkpoint(block_step), initial, items)
    per_head = mixed.transpose(0, 2, 1, 3).reshape(length, HEADS, head_size)
    head_normed = (per_head * rms_scale(per_head)).reshape(length, model_width) * head_gain
    gated = low(head_normed * jax.nn.silu(swish_pre))
    hidden = inputs_seq + low_back(highest(gated, output_weight))
    feed_in = low(hidden * rms_scale(hidden) * feed_gain)
    gate_pre = low_back(highest(feed_in, gate_weight))
    up_pre = low_back(highest(feed_in, up_weight))
    inner = low(jax.nn.silu(gate_pre) * up_pre)
    return hidden + low_back(highest(inner, down_weight))

def reference(layer_input, segments, mixer_gain, query_weight, key_weight, value_weight, squeeze, expand, forget_bias, swish_weight, head_gain, output_weight, feed_gain, gate_weight, up_weight, down_weight, cotangent):
    weights = tuple((tensor.astype(jnp.float32) for tensor in (mixer_gain, query_weight, key_weight, value_weight, squeeze, expand, forget_bias, swish_weight, head_gain, output_weight, feed_gain, gate_weight, up_weight, down_weight)))
    inputs_all = layer_input.astype(jnp.float32)
    segment_all = segments.astype(jnp.float32)

    def forward(inputs_now, weights_now):
        return lax.map(lambda pair: sequence_forward(pair[0], pair[1], weights_now), (inputs_now, segment_all))
    result, pullback = jax.vjp(forward, inputs_all, weights)
    grad_inputs, grads = pullback(cotangent.astype(jnp.float32))
    return (result.astype(jnp.bfloat16), grad_inputs.astype(jnp.bfloat16), grads[0], grads[1], grads[2], grads[3], grads[4], grads[5], grads[6], grads[7], grads[8], grads[9], grads[10], grads[11], grads[12], grads[13])
```

```python
import functools

import jax
import jax.numpy as jnp
import numpy as np
from jax import lax
from jax.experimental import pallas as pl
from jax.experimental.pallas import tpu as pltpu
from jax.sharding import PartitionSpec as P

HEADS = 4
SLOTS = 64
RANK = 16
EPS = 1e-06
TAU_GATE = 8.0
CHUNK = 128
SUB = 16
BOTH = ("seq", "batch")
F32 = jnp.float32
BF16 = jnp.bfloat16
HIGHEST = lax.Precision.HIGHEST


def dot_nn(left, right):
    return lax.dot_general(left, right, (((1,), (0,)), ((), ())), preferred_element_type=F32)


def dot_nt(left, right):
    return lax.dot_general(left, right, (((1,), (1,)), ((), ())), preferred_element_type=F32)


def dot_tn(left, right):
    return lax.dot_general(left, right, (((0,), (0,)), ((), ())), preferred_element_type=F32)


def exact_nn(left, right):
    return lax.dot_general(
        left, right, (((1,), (0,)), ((), ())), precision=HIGHEST, preferred_element_type=F32
    )


def exact_nt(left, right):
    return lax.dot_general(
        left, right, (((1,), (1,)), ((), ())), precision=HIGHEST, preferred_element_type=F32
    )


def halves(value):
    high = value.astype(BF16)
    return high, (value - high.astype(F32)).astype(BF16)


def split_nn(left, right):
    high, rest = halves(left)
    return dot_nn(high, right) + dot_nn(rest, right)


def split_nt(left, right):
    high, rest = halves(left)
    return dot_nt(high, right) + dot_nt(rest, right)


def chunk_tables():
    at = np.arange(CHUNK)
    sums, covers = [], []
    half = SUB
    while half < CHUNK:
        right = (at // half) % 2 == 1
        edge = (at // (2 * half)) * 2 * half + half - 1
        low = np.where(right, edge, at)
        high = np.where(right, at, edge)
        sums.append((at[:, None] > low[None, :]) & (at[:, None] <= high[None, :]))
        same = (at[:, None] // (2 * half)) == (at[None, :] // (2 * half))
        covers.append(same & ~right[:, None] & right[None, :])
        half *= 2
    sums.append(at[:, None] <= at[None, :])
    sums.append(at[:, None] > at[None, :])
    apart = at[None, :] - at[:, None]
    apart = np.where(at[None, :] // SUB == at[:, None] // SUB, apart, -1)
    return (
        np.concatenate(sums, axis=1).astype(np.float32),
        np.stack(covers).astype(np.float32),
        np.maximum(apart, -1).astype(np.int32),
    )


def rolled(value, by):
    return value if by % CHUNK == 0 else pltpu.roll(value, by % CHUNK, 1)


def exponents(rate, sums):
    return jnp.exp(exact_nn(rate, sums))


def piece(value, at):
    return value[:, at * CHUNK : (at + 1) * CHUNK]


def mixer_forward_kernel(
    levels,
    factor,
    mine,
    query,
    key,
    value,
    rate,
    inflow,
    rows,
    segment_col,
    sums,
    covers,
    apart,
    output,
    attention_out,
    logits_out,
    key_start,
    value_start,
    key_state,
    value_state,
):
    @pl.when(pl.program_id(0) == 0)
    def _():
        key_state[...] = jnp.zeros_like(key_state)
        value_state[...] = jnp.zeros_like(value_state)

    key_in, value_in = key_state[...], value_state[...]
    key_start[0] = key_in
    value_start[0] = value_in
    q, k, v = query[...], key[...], value[...]
    a, g = rate[...], inflow[...]
    decay = exponents(a, sums[...])
    before, after = piece(decay, levels), piece(decay, levels + 1)
    carried = before * rows[1:2, :]
    visible = segment_col[...] == rows[0:1, :]
    scores = jnp.where(visible, dot_nt(k, q) * factor, 0.0)
    logits = carried * (split_nt(key_in, q) * factor)
    for level in range(levels):
        part = piece(decay, level)
        logits = logits + part * exact_nn(part * g, scores * covers[level])
    gap = apart[...]
    total = jnp.zeros_like(a)
    weights = []
    for by in range(SUB):
        if by:
            total = total + rolled(a, by - 1)
        weight = jnp.exp(total) * rolled(g, by)
        weights.append(weight)
        logits = logits + weight * jnp.sum(
            jnp.where(gap == by, scores, 0.0), axis=0, keepdims=True
        )
    attention = jnp.exp(logits - jnp.max(logits, axis=0, keepdims=True))
    attention = attention / jnp.sum(attention, axis=0, keepdims=True)
    attention_out[...] = attention
    logits_out[...] = logits
    mixing = jnp.zeros((CHUNK, CHUNK), F32)
    for level in range(levels):
        part = piece(decay, level)
        mixing = mixing + covers[level] * dot_tn(
            (part * g).astype(BF16), (part * attention).astype(BF16)
        )
    for by in range(SUB):
        row = jnp.sum(weights[by] * attention, axis=0, keepdims=True)
        mixing = jnp.where(gap == by, row, mixing)
    mixing = jnp.where(visible, mixing, 0.0).astype(BF16)
    output[...] = dot_tn(mixing, v) + dot_tn(
        (carried * attention).astype(BF16), value_in.astype(BF16)
    )
    ends = after * g * rows[2:3, :]
    keep = carried[:, CHUNK - 1 : CHUNK]
    key_state[...] = keep * key_in + split_nn(ends, k)
    value_state[...] = keep * value_in + split_nn(ends, v)


def mixer_backward_kernel(
    levels,
    factor,
    mine,
    query,
    key,
    value,
    grad_output,
    rate,
    inflow,
    rows,
    segment_col,
    sums,
    covers,
    apart,
    later,
    attention_in,
    logits_in,
    key_start,
    value_start,
    grad_query,
    grad_key,
    grad_value,
    grad_rate,
    key_grad,
    value_grad,
    flow,
):
    @pl.when(pl.program_id(0) == 0)
    def _():
        key_grad[...] = jnp.zeros_like(key_grad)
        value_grad[...] = jnp.zeros_like(value_grad)
        flow[...] = jnp.zeros_like(flow)

    key_in, value_in = key_start[0], value_start[0]
    key_after, value_after = key_grad[...], value_grad[...]
    q, k, v, d = query[...], key[...], value[...], grad_output[...]
    a, g = rate[...], inflow[...]
    attention, logits = attention_in[...], logits_in[...]
    decay = exponents(a, sums[...])
    before, after = piece(decay, levels), piece(decay, levels + 1)
    carried = before * rows[1:2, :]
    visible = segment_col[...] == rows[0:1, :]
    scores = jnp.where(visible, dot_nt(k, q) * factor, 0.0)
    reads = jnp.where(visible, dot_nt(v, d), 0.0)
    gap = apart[...]
    grad_att = carried * split_nt(value_in, d)
    for level in range(levels):
        part = piece(decay, level)
        grad_att = grad_att + part * exact_nn(part * g, reads * covers[level])
    total = jnp.zeros_like(a)
    bare, weights, score_rows, read_rows = [], [], [], []
    for by in range(SUB):
        if by:
            total = total + rolled(a, by - 1)
        bare.append(jnp.exp(total))
        weights.append(bare[by] * rolled(g, by))
        score_rows.append(jnp.sum(jnp.where(gap == by, scores, 0.0), axis=0, keepdims=True))
        read_rows.append(jnp.sum(jnp.where(gap == by, reads, 0.0), axis=0, keepdims=True))
        grad_att = grad_att + weights[by] * read_rows[by]
    grad_logits = attention * (
        grad_att - jnp.sum(attention * grad_att, axis=0, keepdims=True)
    )
    mixing = jnp.zeros((CHUNK, CHUNK), F32)
    spread = jnp.zeros((CHUNK, CHUNK), F32)
    ends = after * rows[2:3, :]
    grad_inflow = ends * (split_nt(key_after, k) + split_nt(value_after, v))
    for level in range(levels):
        part = piece(decay, level)
        left = (part * g).astype(BF16)
        att_part, log_part = part * attention, part * grad_logits
        mixing = mixing + covers[level] * dot_tn(left, att_part.astype(BF16))
        spread = spread + covers[level] * dot_tn(left, log_part.astype(BF16))
        grad_inflow = grad_inflow + part * (
            exact_nt(log_part, scores * covers[level]) + exact_nt(att_part, reads * covers[level])
        )
    for by in range(SUB):
        row = jnp.sum(weights[by] * attention, axis=0, keepdims=True)
        mixing = jnp.where(gap == by, row, mixing)
        row = jnp.sum(weights[by] * grad_logits, axis=0, keepdims=True)
        spread = jnp.where(gap == by, row, spread)
        terms = bare[by] * (grad_logits * score_rows[by] + attention * read_rows[by])
        grad_inflow = grad_inflow + rolled(terms, -by)
    mixing = jnp.where(visible, mixing, 0.0).astype(BF16)
    spread = (jnp.where(visible, spread, 0.0) * factor).astype(BF16)
    log_carried = carried * grad_logits * factor
    att_carried = carried * attention
    ends = (ends * g).astype(BF16)
    grad_query[...] = (
        dot_tn(spread, k) + dot_tn(log_carried.astype(BF16), key_in.astype(BF16))
    ).astype(BF16)
    grad_key[...] = (dot_nn(spread, q) + dot_tn(ends, key_after.astype(BF16))).astype(BF16)
    grad_value[...] = (dot_nn(mixing, d) + dot_tn(ends, value_after.astype(BF16))).astype(BF16)
    change = grad_logits * logits + attention * grad_att - g * grad_inflow
    same = jnp.where(visible, later[...], 0.0)
    flows = exact_nn(change, same) + rows[2:3, :] * flow[:, 0:1]
    grad_rate[...] = rows[3:4, :] * flows - jnp.exp(a) * grad_inflow
    keep = carried[:, CHUNK - 1 : CHUNK]
    key_before = keep * key_after + split_nn(log_carried, q)
    value_before = keep * value_after + split_nn(att_carried, d)
    key_grad[...] = key_before
    value_grad[...] = value_before
    flow[...] = jnp.broadcast_to(
        jnp.sum(key_before * key_in + value_before * value_in, axis=1, keepdims=True), flow.shape
    )


def mixer_specs(length, size, ring, backward):
    count = length // CHUNK
    per = count // ring

    def natural(step):
        return count - 1 - step if backward else step

    def moved(step, mine):
        at = natural(step)
        return lax.bitwise_xor(at // per, mine[0]) * per + at % per

    wide = pl.BlockSpec((CHUNK, size), lambda step, mine: (moved(step, mine), 0))
    slim = pl.BlockSpec((SLOTS, CHUNK), lambda step, mine: (0, moved(step, mine)))
    plain = pl.BlockSpec((SLOTS, CHUNK), lambda step, mine: (0, natural(step)))
    rows = pl.BlockSpec((8, CHUNK), lambda step, mine: (0, natural(step)))
    column = pl.BlockSpec((CHUNK, 1), lambda step, mine: (natural(step), 0))
    state = pl.BlockSpec((1, SLOTS, size), lambda step, mine: (natural(step), 0, 0))
    return count, wide, slim, plain, rows, column, state


def whole(array):
    rank = array.ndim
    return pl.BlockSpec(array.shape, lambda step, mine: (0,) * rank)


def mixer_forward(mine, ring, query, key, value, rate, inflow, rows, column):
    length, size = query.shape
    sums, covers, apart = (jnp.asarray(table) for table in chunk_tables())
    count, wide, slim, plain, row_spec, col_spec, state = mixer_specs(length, size, ring, False)
    kernel = functools.partial(mixer_forward_kernel, covers.shape[0], size ** (-0.25))
    return pl.pallas_call(
        kernel,
        out_shape=(
            jax.ShapeDtypeStruct((length, size), F32),
            jax.ShapeDtypeStruct((SLOTS, length), F32),
            jax.ShapeDtypeStruct((SLOTS, length), F32),
            jax.ShapeDtypeStruct((count, SLOTS, size), F32),
            jax.ShapeDtypeStruct((count, SLOTS, size), F32),
        ),
        grid_spec=pltpu.PrefetchScalarGridSpec(
            num_scalar_prefetch=1,
            grid=(count,),
            in_specs=[
                wide, wide, wide, slim, slim, row_spec, col_spec,
                whole(sums), whole(covers), whole(apart),
            ],
            out_specs=[wide, plain, plain, state, state],
            scratch_shapes=[pltpu.VMEM((SLOTS, size), F32)] * 2,
        ),
        compiler_params=pltpu.CompilerParams(vmem_limit_bytes=32 << 20),
        cost_estimate=pl.CostEstimate(
            flops=length * size * 2000, bytes_accessed=length * size * 12, transcendentals=length * 4096
        ),
        name="mixer_forward",
    )(mine, query, key, value, rate, inflow, rows, column, sums, covers, apart)


def mixer_backward(
    mine, ring, query, key, value, grad, rate, inflow, rows, column, attention, logits, starts
):
    length, size = query.shape
    sums, covers, apart = (jnp.asarray(table) for table in chunk_tables())
    later = jnp.asarray(np.tril(np.ones((CHUNK, CHUNK), np.float32)))
    count, wide, slim, plain, row_spec, col_spec, state = mixer_specs(length, size, ring, True)
    kernel = functools.partial(mixer_backward_kernel, covers.shape[0], size ** (-0.25))
    return pl.pallas_call(
        kernel,
        out_shape=(
            jax.ShapeDtypeStruct((length, size), BF16),
            jax.ShapeDtypeStruct((length, size), BF16),
            jax.ShapeDtypeStruct((length, size), BF16),
            jax.ShapeDtypeStruct((SLOTS, length), F32),
        ),
        grid_spec=pltpu.PrefetchScalarGridSpec(
            num_scalar_prefetch=1,
            grid=(count,),
            in_specs=[
                wide, wide, wide, wide, slim, slim, row_spec, col_spec,
                whole(sums), whole(covers), whole(apart), whole(later),
                plain, plain, state, state,
            ],
            out_specs=[wide, wide, wide, slim],
            scratch_shapes=[pltpu.VMEM((SLOTS, size), F32)] * 2 + [pltpu.VMEM((SLOTS, 128), F32)],
        ),
        compiler_params=pltpu.CompilerParams(vmem_limit_bytes=32 << 20),
        cost_estimate=pl.CostEstimate(
            flops=length * size * 4000, bytes_accessed=length * size * 20, transcendentals=length * 4096
        ),
        name="mixer_backward",
    )(
        mine, query, key, value, grad, rate, inflow, rows, column,
        sums, covers, apart, later, attention, logits, *starts,
    )


def rms_scale(features):
    return lax.rsqrt(jnp.mean(features * features, axis=-1, keepdims=True) + EPS)


def swapped(block, by, ring):
    return lax.ppermute(block, "seq", [(i, i ^ by) for i in range(ring)])


def gathered(block, ring):
    return jnp.concatenate([block] + [swapped(block, by, ring) for by in range(1, ring)], axis=0)


def scattered(terms, ring):
    rows = terms.shape[0] // ring
    total = terms[:rows].astype(F32)
    for by in range(1, ring):
        total = total + swapped(terms[by * rows : (by + 1) * rows].astype(BF16), by, ring).astype(F32)
    return total


def exchanged(blocks, mine, ring):
    parts = [
        swapped(lax.dynamic_index_in_dim(blocks, mine ^ by, 0, keepdims=False), by, ring)
        if by
        else lax.dynamic_index_in_dim(blocks, mine, 0, keepdims=False)
        for by in range(ring)
    ]
    made = jnp.stack(parts)
    return jnp.concatenate(
        [lax.dynamic_index_in_dim(made, mine ^ j, 0, keepdims=True) for j in range(ring)], axis=0
    )


def local(
    layer_input,
    segments,
    mixer_gain,
    query_weight,
    key_weight,
    value_weight,
    squeeze,
    expand,
    forget_bias,
    swish_weight,
    head_gain,
    output_weight,
    feed_gain,
    gate_weight,
    up_weight,
    down_weight,
    cotangent,
):
    ring, lines = lax.axis_size("seq"), lax.axis_size("batch")
    devices = ring * lines
    mine = lax.axis_index("seq")
    rows, width = layer_input.shape[1], layer_input.shape[2]
    length = rows * ring
    own = width // devices
    head_size = width // HEADS
    copies = ring // HEADS
    part = width // ring
    head = mine // copies
    hidden_part = gate_weight.shape[1] // ring
    slots_all = HEADS * SLOTS

    def permuted(array):
        shape = array.shape[:-1]
        array = array.reshape(shape + (ring, lines, own))
        return jnp.swapaxes(array, -3, -2).reshape(shape + (width,))

    def restored(array):
        shape = array.shape[:-1]
        array = array.reshape(shape + (lines, ring, own))
        return jnp.swapaxes(array, -3, -2).reshape(shape + (width,))

    def to_order(array):
        if copies == 1:
            return array
        blocks = array.reshape((ring, rows) + array.shape[1:])
        moved = [lax.dynamic_index_in_dim(blocks, mine ^ by, 0, keepdims=False) for by in range(ring)]
        return jnp.concatenate(moved, axis=0)

    def whole_head(array):
        if copies == 1:
            return array
        full = lax.all_gather(to_order(array), "seq", axis=1, tiled=True)
        return to_order(lax.dynamic_slice_in_dim(full, head * head_size, head_size, 1))

    def own_part(array):
        if copies == 1:
            return array
        return lax.dynamic_slice_in_dim(array, (mine % copies) * part, part, 1)

    small = jnp.concatenate(
        [
            mixer_gain,
            head_gain,
            feed_gain,
            forget_bias,
            expand.T.reshape(-1),
            squeeze.reshape(-1),
        ]
    )
    small = lax.all_gather(small, BOTH, axis=0, tiled=False)
    cuts = np.cumsum([own, own, own, slots_all // devices, RANK * slots_all // devices])
    gain_one, gain_head, gain_two, bias_full, expand_t, w_squeeze = jnp.split(small, cuts, axis=1)
    gain_one = permuted(gain_one.reshape(width)).astype(F32)
    gain_head = lax.dynamic_slice_in_dim(gain_head.reshape(width), head * head_size, head_size, 0)
    gain_head = gain_head.astype(F32)
    gain_two = gain_two.reshape(width).astype(F32)
    bias_head = lax.dynamic_slice_in_dim(bias_full.reshape(slots_all), head * SLOTS, SLOTS, 0)
    expand_head = lax.dynamic_slice_in_dim(
        expand_t.reshape(slots_all, RANK), head * SLOTS, SLOTS, 0
    )
    w_squeeze = permuted(w_squeeze.reshape(width, RANK).T)

    def columns(*arrays):
        blocks = [a.reshape(own, ring, a.shape[1] // ring) for a in arrays]
        return jnp.concatenate(blocks, axis=2).transpose(1, 0, 2)

    mixer_columns = exchanged(
        columns(query_weight, key_weight, value_weight, swish_weight), mine, ring
    )
    w_mixer = lax.all_gather(mixer_columns, "batch", axis=0, tiled=False).reshape(width, 4 * part)
    w_output = lax.all_gather(output_weight, "batch", axis=0, tiled=True)
    feed_columns = exchanged(columns(gate_weight, up_weight), mine, ring)
    w_feed = lax.all_gather(feed_columns, "batch", axis=0, tiled=False).reshape(
        width, 2 * hidden_part
    )
    w_down = lax.all_gather(down_weight, "batch", axis=0, tiled=True)

    segment = lax.all_gather(segments.reshape(rows), "seq", axis=0, tiled=True).astype(F32)
    chunked = segment.reshape(-1, CHUNK)
    before = jnp.concatenate([jnp.full((1,), -1.0, F32), chunked[:-1, -1]])
    previous = jnp.concatenate([jnp.full((1,), -1.0, F32), segment[:-1]])
    mask_rows = jnp.stack(
        [
            segment,
            (chunked == before[:, None]).astype(F32).reshape(-1),
            (chunked == chunked[:, -1:]).astype(F32).reshape(-1),
            (segment == previous).astype(F32),
        ]
        + [jnp.zeros_like(segment)] * 4
    )
    segment_col = segment[:, None]

    input_own = layer_input.reshape(rows, width)
    inputs = gathered(permuted(input_own), ring).astype(F32)
    scale_one = rms_scale(inputs)
    plain_one = inputs * scale_one
    normed = (plain_one * gain_one).astype(BF16)
    mixer_pre = dot_nn(normed, w_mixer)
    query = whole_head(mixer_pre[:, :part].astype(BF16))
    key = whole_head(mixer_pre[:, part : 2 * part].astype(BF16))
    value = whole_head(mixer_pre[:, 2 * part : 3 * part].astype(BF16))
    swish_pre = whole_head(mixer_pre[:, 3 * part :])
    reduced = dot_nt(normed, w_squeeze).astype(BF16)
    forget_logit = dot_nt(expand_head, reduced) + bias_head.astype(F32)[:, None]
    log_rate = jax.nn.log_sigmoid(forget_logit) / TAU_GATE
    inflow = -jnp.expm1(log_rate)
    order = mine.reshape(1).astype(jnp.int32)
    mixed, attention, logits, key_start, value_start = mixer_forward(
        order, ring, query, key, value, log_rate, inflow, mask_rows, segment_col
    )
    head_factor = rms_scale(mixed)
    head_plain = mixed * head_factor
    head_normed = head_plain * gain_head
    swish_sig = jax.nn.sigmoid(swish_pre)
    swish_act = swish_pre * swish_sig
    gated = own_part((head_normed * swish_act).astype(BF16))
    hidden = input_own.astype(F32) + scattered(dot_nn(gated, w_output), ring)

    scale_two = rms_scale(hidden)
    feed_in = gathered(permuted((hidden * scale_two * gain_two).astype(BF16)), ring)
    feed_pre = dot_nn(feed_in, w_feed)
    gate_pre, up_pre = feed_pre[:, :hidden_part], feed_pre[:, hidden_part:]
    gate_sig = jax.nn.sigmoid(gate_pre)
    gate_act = gate_pre * gate_sig
    inner = (gate_act * up_pre).astype(BF16)
    result = hidden + scattered(dot_nn(inner, w_down), ring)
    layer_output = result.astype(BF16).reshape(1, rows, width)

    grad_own = cotangent.reshape(rows, width)
    grad_out = gathered(grad_own, ring)
    grad_inner = dot_nt(grad_out, w_down)
    grad_gatepre = grad_inner * up_pre * (gate_sig * (1.0 + gate_pre * (1.0 - gate_sig)))
    grad_feedpre = jnp.concatenate(
        [grad_gatepre.astype(BF16), (grad_inner * gate_act).astype(BF16)], axis=1
    )
    grad_feedin = restored(scattered(dot_nt(grad_feedpre, w_feed), ring))
    term_down = dot_tn(inner, grad_out).astype(BF16)
    term_feedpre = dot_tn(feed_in, grad_feedpre).astype(BF16)
    down_share = lax.psum_scatter(term_down, "batch", scatter_dimension=0, tiled=True)
    feed_share = lax.psum_scatter(term_feedpre, "batch", scatter_dimension=0, tiled=True)
    feed_share = exchanged(feed_share.reshape(ring, own, 2 * hidden_part), mine, ring)
    gate_share = feed_share[:, :, :hidden_part].transpose(1, 0, 2).reshape(own, -1)
    up_share = feed_share[:, :, hidden_part:].transpose(1, 0, 2).reshape(own, -1)
    term_feed = jnp.sum(grad_feedin * hidden * scale_two, axis=0)
    scaled_two = grad_feedin * gain_two
    grad_hidden = (
        grad_own.astype(F32)
        + scale_two * scaled_two
        - hidden * scale_two**3 * jnp.mean(scaled_two * hidden, axis=-1, keepdims=True)
    )

    grad_branch = gathered(grad_hidden.astype(BF16), ring)
    grad_gated = whole_head(dot_nt(grad_branch, w_output))
    term_output = dot_tn(gated, grad_branch).astype(BF16)
    output_share = lax.psum_scatter(term_output, "batch", scatter_dimension=0, tiled=True)
    slope = swish_sig * (1.0 + swish_pre * (1.0 - swish_sig))
    grad_swishpre = own_part((grad_gated * head_normed * slope).astype(BF16))
    grad_normed_head = grad_gated * swish_act
    term_head = jnp.sum(grad_normed_head * head_plain, axis=0) / copies
    scaled_head = grad_normed_head * gain_head
    grad_mixed = head_factor * scaled_head - mixed * head_factor**3 * jnp.mean(
        scaled_head * mixed, axis=-1, keepdims=True
    )
    grad_query, grad_key, grad_value, grad_rate = mixer_backward(
        order,
        ring,
        query,
        key,
        value,
        grad_mixed.astype(BF16),
        log_rate,
        inflow,
        mask_rows,
        segment_col,
        attention,
        logits,
        (key_start, value_start),
    )
    grad_logit = (grad_rate * jax.nn.sigmoid(-forget_logit) / TAU_GATE).astype(BF16)
    term_bias = jnp.sum(grad_logit.astype(F32), axis=1) / copies
    term_expand = dot_nn(grad_logit, reduced) / copies
    grad_reduced = (dot_tn(grad_logit, expand_head) / copies).astype(BF16)
    grad_pre = jnp.concatenate(
        [own_part(grad_query), own_part(grad_key), own_part(grad_value), grad_swishpre], axis=1
    )
    grad_normed = dot_nt(grad_pre, w_mixer) + dot_nn(grad_reduced, w_squeeze)
    term_mixer = restored(jnp.sum(grad_normed * plain_one, axis=0))
    term_squeeze = restored(dot_tn(grad_reduced, normed))
    grad_normed = restored(scattered(grad_normed, ring))
    term_pre = dot_tn(normed, grad_pre).astype(BF16)
    pre_share = lax.psum_scatter(term_pre, "batch", scatter_dimension=0, tiled=True)
    pre_share = exchanged(pre_share.reshape(ring, own, 4 * part), mine, ring)
    pre_share = pre_share.reshape(ring, own, 4, part).transpose(2, 1, 0, 3).reshape(4, own, width)
    pre_share = pre_share.astype(F32)
    inputs_own = input_own.astype(F32)
    scale_own = rms_scale(inputs_own)
    scaled_one = grad_normed * restored(gain_one)
    grad_inputs = (
        grad_hidden
        + scale_own * scaled_one
        - inputs_own * scale_own**3 * jnp.mean(scaled_one * inputs_own, axis=-1, keepdims=True)
    )
    grad_input = grad_inputs.astype(BF16).reshape(1, rows, width)

    def placed(array, size):
        full = jnp.zeros((HEADS, size) + array.shape[1:], F32)
        return lax.dynamic_update_slice_in_dim(full, array[None], head, 0)

    terms = jnp.concatenate(
        [
            term_mixer.reshape(devices, -1),
            placed(term_head, head_size).reshape(devices, -1),
            term_feed.reshape(devices, -1),
            placed(term_bias, SLOTS).reshape(devices, -1),
            placed(term_expand, SLOTS).reshape(devices, -1),
            term_squeeze.T.reshape(devices, -1),
        ],
        axis=1,
    )
    share = lax.psum_scatter(terms, BOTH, scatter_dimension=0, tiled=True)[0]
    mixer_share, head_share, feedgain_share, bias_share, expand_share, squeeze_share = jnp.split(
        share, cuts
    )
    return (
        layer_output,
        grad_input,
        mixer_share,
        pre_share[0],
        pre_share[1],
        pre_share[2],
        squeeze_share.reshape(own, RANK),
        expand_share.reshape(-1, RANK).T,
        bias_share,
        pre_share[3],
        head_share,
        output_share.astype(F32),
        feedgain_share,
        gate_share.astype(F32),
        up_share.astype(F32),
        down_share.astype(F32),
    )


def solution(mesh):
    rows = P(BOTH, None)
    spread = P(BOTH)
    in_specs = (
        P("batch", "seq", None),
        P("batch", "seq"),
        spread,
        rows,
        rows,
        rows,
        rows,
        P(None, BOTH),
        spread,
        rows,
        spread,
        rows,
        spread,
        rows,
        rows,
        rows,
        P("batch", "seq", None),
    )
    out_specs = (
        P("batch", "seq", None),
        P("batch", "seq", None),
        spread,
        rows,
        rows,
        rows,
        rows,
        P(None, BOTH),
        spread,
        rows,
        spread,
        rows,
        spread,
        rows,
        rows,
        rows,
    )
    return jax.shard_map(local, mesh=mesh, in_specs=in_specs, out_specs=out_specs, check_vma=False)
```

```python
import functools

import jax
import jax.numpy as jnp
import numpy as np
from jax import lax
from jax.experimental import pallas as pl
from jax.experimental.pallas import tpu as pltpu
from jax.sharding import PartitionSpec as P

HEADS = 4
SLOTS = 64
RANK = 16
EPS = 1e-06
TAU_GATE = 8.0
CHUNK = 128
SUB = 16
BOTH = ("seq", "batch")
F32 = jnp.float32
BF16 = jnp.bfloat16
HIGHEST = lax.Precision.HIGHEST


def dot_nn(left, right):
    return lax.dot_general(left, right, (((1,), (0,)), ((), ())), preferred_element_type=F32)


def dot_nt(left, right):
    return lax.dot_general(left, right, (((1,), (1,)), ((), ())), preferred_element_type=F32)


def dot_tn(left, right):
    return lax.dot_general(left, right, (((0,), (0,)), ((), ())), preferred_element_type=F32)


def exact_nn(left, right):
    return lax.dot_general(
        left, right, (((1,), (0,)), ((), ())), precision=HIGHEST, preferred_element_type=F32
    )


def exact_nt(left, right):
    return lax.dot_general(
        left, right, (((1,), (1,)), ((), ())), precision=HIGHEST, preferred_element_type=F32
    )


def halves(value):
    high = value.astype(BF16)
    return high, (value - high.astype(F32)).astype(BF16)


def split_nn(left, right):
    high, rest = halves(left)
    return dot_nn(high, right) + dot_nn(rest, right)


def split_nt(left, right):
    high, rest = halves(left)
    return dot_nt(high, right) + dot_nt(rest, right)


def chunk_tables():
    at = np.arange(CHUNK)
    sums, covers = [], []
    half = SUB
    while half < CHUNK:
        right = (at // half) % 2 == 1
        edge = (at // (2 * half)) * 2 * half + half - 1
        low = np.where(right, edge, at)
        high = np.where(right, at, edge)
        sums.append((at[:, None] > low[None, :]) & (at[:, None] <= high[None, :]))
        same = (at[:, None] // (2 * half)) == (at[None, :] // (2 * half))
        covers.append(same & ~right[:, None] & right[None, :])
        half *= 2
    sums.append(at[:, None] <= at[None, :])
    sums.append(at[:, None] > at[None, :])
    apart = at[None, :] - at[:, None]
    apart = np.where(at[None, :] // SUB == at[:, None] // SUB, apart, -1)
    return (
        np.concatenate(sums, axis=1).astype(np.float32),
        np.stack(covers).astype(np.float32),
        np.maximum(apart, -1).astype(np.int32),
    )


def rolled(value, by):
    return value if by % CHUNK == 0 else pltpu.roll(value, by % CHUNK, 1)


def exponents(rate, sums):
    return jnp.exp(exact_nn(rate, sums))


def piece(value, at):
    return value[:, at * CHUNK : (at + 1) * CHUNK]


def mixer_forward_kernel(
    levels,
    factor,
    mine,
    query,
    key,
    value,
    rate,
    inflow,
    rows,
    segment_col,
    sums,
    covers,
    apart,
    output,
    attention_out,
    logits_out,
    key_start,
    value_start,
    key_state,
    value_state,
):
    @pl.when(pl.program_id(0) == 0)
    def _():
        key_state[...] = jnp.zeros_like(key_state)
        value_state[...] = jnp.zeros_like(value_state)

    key_in, value_in = key_state[...], value_state[...]
    key_start[0] = key_in
    value_start[0] = value_in
    q, k, v = query[...], key[...], value[...]
    a, g = rate[...], inflow[...]
    decay = exponents(a, sums[...])
    before, after = piece(decay, levels), piece(decay, levels + 1)
    carried = before * rows[1:2, :]
    visible = segment_col[...] == rows[0:1, :]
    scores = jnp.where(visible, dot_nt(k, q) * factor, 0.0)
    logits = carried * (split_nt(key_in, q) * factor)
    for level in range(levels):
        part = piece(decay, level)
        logits = logits + part * exact_nn(part * g, scores * covers[level])
    gap = apart[...]
    total = jnp.zeros_like(a)
    weights = []
    for by in range(SUB):
        if by:
            total = total + rolled(a, by - 1)
        weight = jnp.exp(total) * rolled(g, by)
        weights.append(weight)
        logits = logits + weight * jnp.sum(
            jnp.where(gap == by, scores, 0.0), axis=0, keepdims=True
        )
    attention = jnp.exp(logits - jnp.max(logits, axis=0, keepdims=True))
    attention = attention / jnp.sum(attention, axis=0, keepdims=True)
    attention_out[...] = attention
    logits_out[...] = logits
    mixing = jnp.zeros((CHUNK, CHUNK), F32)
    for level in range(levels):
        part = piece(decay, level)
        mixing = mixing + covers[level] * dot_tn(
            (part * g).astype(BF16), (part * attention).astype(BF16)
        )
    for by in range(SUB):
        row = jnp.sum(weights[by] * attention, axis=0, keepdims=True)
        mixing = jnp.where(gap == by, row, mixing)
    mixing = jnp.where(visible, mixing, 0.0).astype(BF16)
    output[...] = dot_tn(mixing, v) + dot_tn(
        (carried * attention).astype(BF16), value_in.astype(BF16)
    )
    ends = after * g * rows[2:3, :]
    keep = carried[:, CHUNK - 1 : CHUNK]
    key_state[...] = keep * key_in + split_nn(ends, k)
    value_state[...] = keep * value_in + split_nn(ends, v)


def mixer_backward_kernel(
    levels,
    factor,
    mine,
    query,
    key,
    value,
    grad_output,
    rate,
    inflow,
    rows,
    segment_col,
    sums,
    covers,
    apart,
    later,
    attention_in,
    logits_in,
    key_start,
    value_start,
    grad_query,
    grad_key,
    grad_value,
    grad_rate,
    key_grad,
    value_grad,
    flow,
):
    @pl.when(pl.program_id(0) == 0)
    def _():
        key_grad[...] = jnp.zeros_like(key_grad)
        value_grad[...] = jnp.zeros_like(value_grad)
        flow[...] = jnp.zeros_like(flow)

    key_in, value_in = key_start[0], value_start[0]
    key_after, value_after = key_grad[...], value_grad[...]
    q, k, v, d = query[...], key[...], value[...], grad_output[...]
    a, g = rate[...], inflow[...]
    attention, logits = attention_in[...], logits_in[...]
    decay = exponents(a, sums[...])
    before, after = piece(decay, levels), piece(decay, levels + 1)
    carried = before * rows[1:2, :]
    visible = segment_col[...] == rows[0:1, :]
    scores = jnp.where(visible, dot_nt(k, q) * factor, 0.0)
    reads = jnp.where(visible, dot_nt(v, d), 0.0)
    gap = apart[...]
    grad_att = carried * split_nt(value_in, d)
    for level in range(levels):
        part = piece(decay, level)
        grad_att = grad_att + part * exact_nn(part * g, reads * covers[level])
    total = jnp.zeros_like(a)
    bare, weights, score_rows, read_rows = [], [], [], []
    for by in range(SUB):
        if by:
            total = total + rolled(a, by - 1)
        bare.append(jnp.exp(total))
        weights.append(bare[by] * rolled(g, by))
        score_rows.append(jnp.sum(jnp.where(gap == by, scores, 0.0), axis=0, keepdims=True))
        read_rows.append(jnp.sum(jnp.where(gap == by, reads, 0.0), axis=0, keepdims=True))
        grad_att = grad_att + weights[by] * read_rows[by]
    grad_logits = attention * (
        grad_att - jnp.sum(attention * grad_att, axis=0, keepdims=True)
    )
    mixing = jnp.zeros((CHUNK, CHUNK), F32)
    spread = jnp.zeros((CHUNK, CHUNK), F32)
    ends = after * rows[2:3, :]
    grad_inflow = ends * (split_nt(key_after, k) + split_nt(value_after, v))
    for level in range(levels):
        part = piece(decay, level)
        left = (part * g).astype(BF16)
        att_part, log_part = part * attention, part * grad_logits
        mixing = mixing + covers[level] * dot_tn(left, att_part.astype(BF16))
        spread = spread + covers[level] * dot_tn(left, log_part.astype(BF16))
        grad_inflow = grad_inflow + part * (
            exact_nt(log_part, scores * covers[level]) + exact_nt(att_part, reads * covers[level])
        )
    for by in range(SUB):
        row = jnp.sum(weights[by] * attention, axis=0, keepdims=True)
        mixing = jnp.where(gap == by, row, mixing)
        row = jnp.sum(weights[by] * grad_logits, axis=0, keepdims=True)
        spread = jnp.where(gap == by, row, spread)
        terms = bare[by] * (grad_logits * score_rows[by] + attention * read_rows[by])
        grad_inflow = grad_inflow + rolled(terms, -by)
    mixing = jnp.where(visible, mixing, 0.0).astype(BF16)
    spread = (jnp.where(visible, spread, 0.0) * factor).astype(BF16)
    log_carried = carried * grad_logits * factor
    att_carried = carried * attention
    ends = (ends * g).astype(BF16)
    grad_query[...] = (
        dot_tn(spread, k) + dot_tn(log_carried.astype(BF16), key_in.astype(BF16))
    ).astype(BF16)
    grad_key[...] = (dot_nn(spread, q) + dot_tn(ends, key_after.astype(BF16))).astype(BF16)
    grad_value[...] = (dot_nn(mixing, d) + dot_tn(ends, value_after.astype(BF16))).astype(BF16)
    change = grad_logits * logits + attention * grad_att - g * grad_inflow
    same = jnp.where(visible, later[...], 0.0)
    flows = exact_nn(change, same) + rows[2:3, :] * flow[:, 0:1]
    grad_rate[...] = rows[3:4, :] * flows - jnp.exp(a) * grad_inflow
    keep = carried[:, CHUNK - 1 : CHUNK]
    key_before = keep * key_after + split_nn(log_carried, q)
    value_before = keep * value_after + split_nn(att_carried, d)
    key_grad[...] = key_before
    value_grad[...] = value_before
    flow[...] = jnp.broadcast_to(
        jnp.sum(key_before * key_in + value_before * value_in, axis=1, keepdims=True), flow.shape
    )


def mixer_specs(length, size, ring, backward):
    count = length // CHUNK
    per = count // ring

    def natural(step):
        return count - 1 - step if backward else step

    def moved(step, mine):
        at = natural(step)
        return lax.bitwise_xor(at // per, mine[0]) * per + at % per

    wide = pl.BlockSpec((CHUNK, size), lambda step, mine: (moved(step, mine), 0))
    slim = pl.BlockSpec((SLOTS, CHUNK), lambda step, mine: (0, moved(step, mine)))
    plain = pl.BlockSpec((SLOTS, CHUNK), lambda step, mine: (0, natural(step)))
    rows = pl.BlockSpec((8, CHUNK), lambda step, mine: (0, natural(step)))
    column = pl.BlockSpec((CHUNK, 1), lambda step, mine: (natural(step), 0))
    state = pl.BlockSpec((1, SLOTS, size), lambda step, mine: (natural(step), 0, 0))
    return count, wide, slim, plain, rows, column, state


def whole(array):
    rank = array.ndim
    return pl.BlockSpec(array.shape, lambda step, mine: (0,) * rank)


def mixer_forward(mine, ring, query, key, value, rate, inflow, rows, column):
    length, size = query.shape
    sums, covers, apart = (jnp.asarray(table) for table in chunk_tables())
    count, wide, slim, plain, row_spec, col_spec, state = mixer_specs(length, size, ring, False)
    kernel = functools.partial(mixer_forward_kernel, covers.shape[0], size ** (-0.25))
    return pl.pallas_call(
        kernel,
        out_shape=(
            jax.ShapeDtypeStruct((length, size), F32),
            jax.ShapeDtypeStruct((SLOTS, length), F32),
            jax.ShapeDtypeStruct((SLOTS, length), F32),
            jax.ShapeDtypeStruct((count, SLOTS, size), F32),
            jax.ShapeDtypeStruct((count, SLOTS, size), F32),
        ),
        grid_spec=pltpu.PrefetchScalarGridSpec(
            num_scalar_prefetch=1,
            grid=(count,),
            in_specs=[
                wide, wide, wide, slim, slim, row_spec, col_spec,
                whole(sums), whole(covers), whole(apart),
            ],
            out_specs=[wide, plain, plain, state, state],
            scratch_shapes=[pltpu.VMEM((SLOTS, size), F32)] * 2,
        ),
        compiler_params=pltpu.CompilerParams(vmem_limit_bytes=32 << 20),
        cost_estimate=pl.CostEstimate(
            flops=length * size * 2000, bytes_accessed=length * size * 12, transcendentals=length * 4096
        ),
        name="mixer_forward",
    )(mine, query, key, value, rate, inflow, rows, column, sums, covers, apart)


def mixer_backward(
    mine, ring, query, key, value, grad, rate, inflow, rows, column, attention, logits, starts
):
    length, size = query.shape
    sums, covers, apart = (jnp.asarray(table) for table in chunk_tables())
    later = jnp.asarray(np.tril(np.ones((CHUNK, CHUNK), np.float32)))
    count, wide, slim, plain, row_spec, col_spec, state = mixer_specs(length, size, ring, True)
    kernel = functools.partial(mixer_backward_kernel, covers.shape[0], size ** (-0.25))
    return pl.pallas_call(
        kernel,
        out_shape=(
            jax.ShapeDtypeStruct((length, size), BF16),
            jax.ShapeDtypeStruct((length, size), BF16),
            jax.ShapeDtypeStruct((length, size), BF16),
            jax.ShapeDtypeStruct((SLOTS, length), F32),
        ),
        grid_spec=pltpu.PrefetchScalarGridSpec(
            num_scalar_prefetch=1,
            grid=(count,),
            in_specs=[
                wide, wide, wide, wide, slim, slim, row_spec, col_spec,
                whole(sums), whole(covers), whole(apart), whole(later),
                plain, plain, state, state,
            ],
            out_specs=[wide, wide, wide, slim],
            scratch_shapes=[pltpu.VMEM((SLOTS, size), F32)] * 2 + [pltpu.VMEM((SLOTS, 128), F32)],
        ),
        compiler_params=pltpu.CompilerParams(vmem_limit_bytes=32 << 20),
        cost_estimate=pl.CostEstimate(
            flops=length * size * 4000, bytes_accessed=length * size * 20, transcendentals=length * 4096
        ),
        name="mixer_backward",
    )(
        mine, query, key, value, grad, rate, inflow, rows, column,
        sums, covers, apart, later, attention, logits, *starts,
    )


def rms_scale(features):
    return lax.rsqrt(jnp.mean(features * features, axis=-1, keepdims=True) + EPS)


def swapped(block, by, ring):
    return lax.ppermute(block, "seq", [(i, i ^ by) for i in range(ring)])


def gathered(block, ring):
    if ring != 4:
        return jnp.concatenate([block] + [swapped(block, by, ring) for by in range(1, ring)], axis=0)
    half = block.shape[0] // 2
    one, two = swapped(block, 1, ring), swapped(block, 2, ring)
    low, high = swapped(two[:half], 1, ring), swapped(one[half:], 2, ring)
    return jnp.concatenate([block, one, two, low, high], axis=0)


def scattered(terms, ring):
    rows = terms.shape[0] // ring
    parts = [terms[by * rows : (by + 1) * rows] for by in range(ring)]
    total = parts[0].astype(F32)
    if ring != 4:
        for by in range(1, ring):
            total = total + swapped(parts[by], by, ring).astype(F32)
        return total
    half = rows // 2
    low, high = swapped(parts[3][:half], 1, ring), swapped(parts[3][half:], 2, ring)
    two = jnp.concatenate([added(parts[2][:half], low), parts[2][half:]], axis=0)
    one = jnp.concatenate([parts[1][:half], added(parts[1][half:], high)], axis=0)
    return total + swapped(one, 1, ring).astype(F32) + swapped(two, 2, ring).astype(F32)


def added(left, right):
    return (left.astype(F32) + right.astype(F32)).astype(BF16)


def flipped(block, axis, by):
    return lax.ppermute(block, axis, [(i, i ^ by) for i in range(lax.axis_size(axis))])


def doubled(block, axis):
    by, mine = 1, lax.axis_index(axis)
    while by < lax.axis_size(axis):
        other = flipped(block, axis, by)
        first = (mine & by) == 0
        block = jnp.concatenate(
            [jnp.where(first, block, other), jnp.where(first, other, block)], axis=0
        )
        by *= 2
    return block


def halved(block, axis):
    by, mine = lax.axis_size(axis) // 2, lax.axis_index(axis)
    while by:
        low, high = jnp.split(block, 2, axis=0)
        first = (mine & by) == 0
        block = jnp.where(first, low, high) + flipped(jnp.where(first, high, low), axis, by)
        by //= 2
    return block


def after(value, *others):
    return lax.optimization_barrier((value,) + others)[0]


def exchanged(blocks, mine, ring):
    parts = [
        swapped(lax.dynamic_index_in_dim(blocks, mine ^ by, 0, keepdims=False), by, ring)
        if by
        else lax.dynamic_index_in_dim(blocks, mine, 0, keepdims=False)
        for by in range(ring)
    ]
    made = jnp.stack(parts)
    return jnp.concatenate(
        [lax.dynamic_index_in_dim(made, mine ^ j, 0, keepdims=True) for j in range(ring)], axis=0
    )


def local(
    layer_input,
    segments,
    mixer_gain,
    query_weight,
    key_weight,
    value_weight,
    squeeze,
    expand,
    forget_bias,
    swish_weight,
    head_gain,
    output_weight,
    feed_gain,
    gate_weight,
    up_weight,
    down_weight,
    cotangent,
):
    ring, lines = lax.axis_size("seq"), lax.axis_size("batch")
    devices = ring * lines
    mine = lax.axis_index("seq")
    rows, width = layer_input.shape[1], layer_input.shape[2]
    length = rows * ring
    own = width // devices
    head_size = width // HEADS
    copies = ring // HEADS
    part = width // ring
    head = mine // copies
    hidden_part = gate_weight.shape[1] // ring
    slots_all = HEADS * SLOTS

    def permuted(array):
        shape = array.shape[:-1]
        array = array.reshape(shape + (ring, lines, own))
        return jnp.swapaxes(array, -3, -2).reshape(shape + (width,))

    def restored(array):
        shape = array.shape[:-1]
        array = array.reshape(shape + (lines, ring, own))
        return jnp.swapaxes(array, -3, -2).reshape(shape + (width,))

    def to_order(array):
        if copies == 1:
            return array
        blocks = array.reshape((ring, rows) + array.shape[1:])
        moved = [lax.dynamic_index_in_dim(blocks, mine ^ by, 0, keepdims=False) for by in range(ring)]
        return jnp.concatenate(moved, axis=0)

    def whole_head(array):
        if copies == 1:
            return array
        full = lax.all_gather(to_order(array), "seq", axis=1, tiled=True)
        return to_order(lax.dynamic_slice_in_dim(full, head * head_size, head_size, 1))

    def own_part(array):
        if copies == 1:
            return array
        return lax.dynamic_slice_in_dim(array, (mine % copies) * part, part, 1)

    small = jnp.concatenate(
        [
            mixer_gain,
            head_gain,
            feed_gain,
            forget_bias,
            expand.T.reshape(-1),
            squeeze.reshape(-1),
        ]
    )
    small = doubled(doubled(small[None], "batch"), "seq")
    cuts = np.cumsum([own, own, own, slots_all // devices, RANK * slots_all // devices])
    gain_one, gain_head, gain_two, bias_full, expand_t, w_squeeze = jnp.split(small, cuts, axis=1)
    gain_one = permuted(gain_one.reshape(width)).astype(F32)
    gain_head = lax.dynamic_slice_in_dim(gain_head.reshape(width), head * head_size, head_size, 0)
    gain_head = gain_head.astype(F32)
    gain_two = gain_two.reshape(width).astype(F32)
    bias_head = lax.dynamic_slice_in_dim(bias_full.reshape(slots_all), head * SLOTS, SLOTS, 0)
    expand_head = lax.dynamic_slice_in_dim(
        expand_t.reshape(slots_all, RANK), head * SLOTS, SLOTS, 0
    )
    w_squeeze = permuted(w_squeeze.reshape(width, RANK).T)

    def columns(*arrays):
        blocks = [a.reshape(own, ring, a.shape[1] // ring) for a in arrays]
        return jnp.concatenate(blocks, axis=2).transpose(1, 0, 2)

    mixer_columns = exchanged(
        columns(query_weight, key_weight, value_weight, swish_weight), mine, ring
    )
    w_mixer = lax.all_gather(mixer_columns, "batch", axis=0, tiled=False).reshape(width, 4 * part)
    w_output = lax.all_gather(output_weight, "batch", axis=0, tiled=True)
    feed_columns = exchanged(columns(gate_weight, up_weight), mine, ring)
    w_feed = lax.all_gather(feed_columns, "batch", axis=0, tiled=False).reshape(
        width, 2 * hidden_part
    )
    w_down = lax.all_gather(down_weight, "batch", axis=0, tiled=True)

    segment = doubled(segments.reshape(1, rows), "seq").reshape(length).astype(F32)
    chunked = segment.reshape(-1, CHUNK)
    before = jnp.concatenate([jnp.full((1,), -1.0, F32), chunked[:-1, -1]])
    previous = jnp.concatenate([jnp.full((1,), -1.0, F32), segment[:-1]])
    mask_rows = jnp.stack(
        [
            segment,
            (chunked == before[:, None]).astype(F32).reshape(-1),
            (chunked == chunked[:, -1:]).astype(F32).reshape(-1),
            (segment == previous).astype(F32),
        ]
        + [jnp.zeros_like(segment)] * 4
    )
    segment_col = segment[:, None]

    input_own = layer_input.reshape(rows, width)
    inputs = gathered(permuted(input_own), ring)
    grad_own = cotangent.reshape(rows, width)
    grad_out = gathered(after(grad_own, inputs), ring)
    inputs = inputs.astype(F32)
    scale_one = rms_scale(inputs)
    plain_one = inputs * scale_one
    normed = (plain_one * gain_one).astype(BF16)
    mixer_pre = dot_nn(normed, w_mixer)
    query = whole_head(mixer_pre[:, :part].astype(BF16))
    key = whole_head(mixer_pre[:, part : 2 * part].astype(BF16))
    value = whole_head(mixer_pre[:, 2 * part : 3 * part].astype(BF16))
    swish_pre = whole_head(mixer_pre[:, 3 * part :])
    reduced = dot_nt(normed, w_squeeze).astype(BF16)
    forget_logit = dot_nt(expand_head, reduced) + bias_head.astype(F32)[:, None]
    log_rate = jax.nn.log_sigmoid(forget_logit) / TAU_GATE
    inflow = -jnp.expm1(log_rate)
    order = mine.reshape(1).astype(jnp.int32)
    mixed, attention, logits, key_start, value_start = mixer_forward(
        order, ring, query, key, value, log_rate, inflow, mask_rows, segment_col
    )
    head_factor = rms_scale(mixed)
    head_plain = mixed * head_factor
    head_normed = head_plain * gain_head
    swish_sig = jax.nn.sigmoid(swish_pre)
    swish_act = swish_pre * swish_sig
    gated = own_part((head_normed * swish_act).astype(BF16))
    hidden = input_own.astype(F32) + scattered(dot_nn(gated, w_output).astype(BF16), ring)

    scale_two = rms_scale(hidden)
    feed_in = gathered(permuted((hidden * scale_two * gain_two).astype(BF16)), ring)
    feed_pre = dot_nn(feed_in, w_feed)
    gate_pre, up_pre = feed_pre[:, :hidden_part], feed_pre[:, hidden_part:]
    gate_sig = jax.nn.sigmoid(gate_pre)
    gate_act = gate_pre * gate_sig
    inner = (gate_act * up_pre).astype(BF16)

    term_down = dot_tn(inner, grad_out).astype(BF16)
    grad_inner = dot_nt(after(grad_out, term_down), w_down)
    grad_gatepre = grad_inner * up_pre * (gate_sig * (1.0 + gate_pre * (1.0 - gate_sig)))
    grad_feedpre = jnp.concatenate(
        [grad_gatepre.astype(BF16), (grad_inner * gate_act).astype(BF16)], axis=1
    )
    back_feedin = dot_nt(grad_feedpre, w_feed).astype(BF16)
    grad_feedin = restored(scattered(back_feedin, ring))
    term_feedpre = dot_tn(feed_in, after(grad_feedpre, back_feedin)).astype(BF16)
    result = hidden + scattered(dot_nn(after(inner, term_feedpre), w_down).astype(BF16), ring)
    layer_output = result.astype(BF16).reshape(1, rows, width)
    down_share = lax.psum_scatter(term_down, "batch", scatter_dimension=0, tiled=True)
    feed_share = lax.psum_scatter(after(term_feedpre, down_share), "batch", scatter_dimension=0, tiled=True)
    feed_sum = feed_share
    feed_share = exchanged(feed_share.reshape(ring, own, 2 * hidden_part), mine, ring)
    gate_share = feed_share[:, :, :hidden_part].transpose(1, 0, 2).reshape(own, -1)
    up_share = feed_share[:, :, hidden_part:].transpose(1, 0, 2).reshape(own, -1)
    term_feed = jnp.sum(grad_feedin * hidden * scale_two, axis=0)
    scaled_two = grad_feedin * gain_two
    grad_hidden = (
        grad_own.astype(F32)
        + scale_two * scaled_two
        - hidden * scale_two**3 * jnp.mean(scaled_two * hidden, axis=-1, keepdims=True)
    )

    grad_branch = after(gathered(grad_hidden.astype(BF16), ring), term_feedpre)
    grad_gated = whole_head(dot_nt(grad_branch, w_output))
    term_output = dot_tn(gated, grad_branch).astype(BF16)
    slope = swish_sig * (1.0 + swish_pre * (1.0 - swish_sig))
    grad_swishpre = own_part((grad_gated * head_normed * slope).astype(BF16))
    grad_normed_head = grad_gated * swish_act
    term_head = jnp.sum(grad_normed_head * head_plain, axis=0) / copies
    scaled_head = grad_normed_head * gain_head
    grad_mixed = head_factor * scaled_head - mixed * head_factor**3 * jnp.mean(
        scaled_head * mixed, axis=-1, keepdims=True
    )
    grad_query, grad_key, grad_value, grad_rate = mixer_backward(
        order,
        ring,
        query,
        key,
        value,
        grad_mixed.astype(BF16),
        log_rate,
        inflow,
        mask_rows,
        segment_col,
        attention,
        logits,
        (key_start, value_start),
    )
    grad_logit = (grad_rate * jax.nn.sigmoid(-forget_logit) / TAU_GATE).astype(BF16)
    term_bias = jnp.sum(grad_logit.astype(F32), axis=1) / copies
    term_expand = dot_nn(grad_logit, reduced) / copies
    grad_reduced = (dot_tn(grad_logit, expand_head) / copies).astype(BF16)
    grad_pre = jnp.concatenate(
        [own_part(grad_query), own_part(grad_key), own_part(grad_value), grad_swishpre], axis=1
    )
    grad_normed = dot_nt(grad_pre, w_mixer) + dot_nn(grad_reduced, w_squeeze)
    term_mixer = restored(jnp.sum(grad_normed * plain_one, axis=0))
    term_squeeze = restored(dot_tn(grad_reduced, normed))
    term_pre = dot_tn(normed, grad_pre).astype(BF16)
    grad_normed = restored(scattered(after(grad_normed.astype(BF16), term_pre), ring))
    pre_share = lax.psum_scatter(after(term_pre, feed_sum), "batch", scatter_dimension=0, tiled=True)
    output_share = lax.psum_scatter(
        after(term_output, pre_share), "batch", scatter_dimension=0, tiled=True
    )
    pre_share = exchanged(pre_share.reshape(ring, own, 4 * part), mine, ring)
    pre_share = pre_share.reshape(ring, own, 4, part).transpose(2, 1, 0, 3).reshape(4, own, width)
    pre_share = pre_share.astype(F32)
    inputs_own = input_own.astype(F32)
    scale_own = rms_scale(inputs_own)
    scaled_one = grad_normed * restored(gain_one)
    grad_inputs = (
        grad_hidden
        + scale_own * scaled_one
        - inputs_own * scale_own**3 * jnp.mean(scaled_one * inputs_own, axis=-1, keepdims=True)
    )
    grad_input = grad_inputs.astype(BF16).reshape(1, rows, width)

    def placed(array, size):
        full = jnp.zeros((HEADS, size) + array.shape[1:], F32)
        return lax.dynamic_update_slice_in_dim(full, array[None], head, 0)

    terms = jnp.concatenate(
        [
            term_mixer.reshape(devices, -1),
            placed(term_head, head_size).reshape(devices, -1),
            term_feed.reshape(devices, -1),
            placed(term_bias, SLOTS).reshape(devices, -1),
            placed(term_expand, SLOTS).reshape(devices, -1),
            term_squeeze.T.reshape(devices, -1),
        ],
        axis=1,
    )
    share = halved(halved(terms, "seq"), "batch")[0]
    mixer_share, head_share, feedgain_share, bias_share, expand_share, squeeze_share = jnp.split(
        share, cuts
    )
    return (
        layer_output,
        grad_input,
        mixer_share,
        pre_share[0],
        pre_share[1],
        pre_share[2],
        squeeze_share.reshape(own, RANK),
        expand_share.reshape(-1, RANK).T,
        bias_share,
        pre_share[3],
        head_share,
        output_share.astype(F32),
        feedgain_share,
        gate_share.astype(F32),
        up_share.astype(F32),
        down_share.astype(F32),
    )


def solution(mesh):
    rows = P(BOTH, None)
    spread = P(BOTH)
    in_specs = (
        P("batch", "seq", None),
        P("batch", "seq"),
        spread,
        rows,
        rows,
        rows,
        rows,
        P(None, BOTH),
        spread,
        rows,
        spread,
        rows,
        spread,
        rows,
        rows,
        rows,
        P("batch", "seq", None),
    )
    out_specs = (
        P("batch", "seq", None),
        P("batch", "seq", None),
        spread,
        rows,
        rows,
        rows,
        rows,
        P(None, BOTH),
        spread,
        rows,
        spread,
        rows,
        spread,
        rows,
        rows,
        rows,
    )
    return jax.shard_map(local, mesh=mesh, in_specs=in_specs, out_specs=out_specs, check_vma=False)
```

```python
import functools

import jax
import jax.numpy as jnp
import numpy as np
from jax import lax
from jax.experimental import pallas as pl
from jax.experimental.pallas import tpu as pltpu
from jax.sharding import PartitionSpec as P

HEADS = 4
SLOTS = 64
RANK = 16
EPS = 1e-06
TAU_GATE = 8.0
CHUNK = 128
SUB = 16
BOTH = ("seq", "batch")
F32 = jnp.float32
BF16 = jnp.bfloat16
HIGHEST = lax.Precision.HIGHEST


def dot_nn(left, right):
    return lax.dot_general(left, right, (((1,), (0,)), ((), ())), preferred_element_type=F32)


def dot_nt(left, right):
    return lax.dot_general(left, right, (((1,), (1,)), ((), ())), preferred_element_type=F32)


def dot_tn(left, right):
    return lax.dot_general(left, right, (((0,), (0,)), ((), ())), preferred_element_type=F32)


def exact_nn(left, right):
    return lax.dot_general(
        left, right, (((1,), (0,)), ((), ())), precision=HIGHEST, preferred_element_type=F32
    )


def exact_nt(left, right):
    return lax.dot_general(
        left, right, (((1,), (1,)), ((), ())), precision=HIGHEST, preferred_element_type=F32
    )


def halves(value):
    high = value.astype(BF16)
    return high, (value - high.astype(F32)).astype(BF16)


def split_nn(left, right):
    high, rest = halves(left)
    return dot_nn(high, right) + dot_nn(rest, right)


def split_nt(left, right):
    high, rest = halves(left)
    return dot_nt(high, right) + dot_nt(rest, right)


def chunk_tables():
    at = np.arange(CHUNK)
    sums, covers = [], []
    half = SUB
    while half < CHUNK:
        right = (at // half) % 2 == 1
        edge = (at // (2 * half)) * 2 * half + half - 1
        low = np.where(right, edge, at)
        high = np.where(right, at, edge)
        sums.append((at[:, None] > low[None, :]) & (at[:, None] <= high[None, :]))
        same = (at[:, None] // (2 * half)) == (at[None, :] // (2 * half))
        covers.append(same & ~right[:, None] & right[None, :])
        half *= 2
    sums.append(at[:, None] <= at[None, :])
    sums.append(at[:, None] > at[None, :])
    apart = at[None, :] - at[:, None]
    apart = np.where(at[None, :] // SUB == at[:, None] // SUB, apart, -1)
    return (
        np.concatenate(sums, axis=1).astype(np.float32),
        np.stack(covers).astype(np.float32),
        np.maximum(apart, -1).astype(np.int32),
    )


def rolled(value, by):
    return value if by % CHUNK == 0 else pltpu.roll(value, by % CHUNK, 1)


def exponents(rate, sums):
    return jnp.exp(exact_nn(rate, sums))


def piece(value, at):
    return value[:, at * CHUNK : (at + 1) * CHUNK]


def mixer_forward_kernel(
    levels,
    factor,
    mine,
    query,
    key,
    value,
    rate,
    inflow,
    rows,
    segment_col,
    sums,
    covers,
    apart,
    output,
    attention_out,
    logits_out,
    key_start,
    value_start,
    key_state,
    value_state,
):
    @pl.when(pl.program_id(0) == 0)
    def _():
        key_state[...] = jnp.zeros_like(key_state)
        value_state[...] = jnp.zeros_like(value_state)

    key_in, value_in = key_state[...], value_state[...]
    key_start[0] = key_in
    value_start[0] = value_in
    q, k, v = query[...], key[...], value[...]
    a, g = rate[...], inflow[...]
    decay = exponents(a, sums[...])
    before, after = piece(decay, levels), piece(decay, levels + 1)
    carried = before * rows[1:2, :]
    visible = segment_col[...] == rows[0:1, :]
    scores = jnp.where(visible, dot_nt(k, q) * factor, 0.0)
    logits = carried * (split_nt(key_in, q) * factor)
    for level in range(levels):
        part = piece(decay, level)
        logits = logits + part * exact_nn(part * g, scores * covers[level])
    gap = apart[...]
    total = jnp.zeros_like(a)
    weights = []
    for by in range(SUB):
        if by:
            total = total + rolled(a, by - 1)
        weight = jnp.exp(total) * rolled(g, by)
        weights.append(weight)
        logits = logits + weight * jnp.sum(
            jnp.where(gap == by, scores, 0.0), axis=0, keepdims=True
        )
    attention = jnp.exp(logits - jnp.max(logits, axis=0, keepdims=True))
    attention = attention / jnp.sum(attention, axis=0, keepdims=True)
    attention_out[...] = attention
    logits_out[...] = logits
    mixing = jnp.zeros((CHUNK, CHUNK), F32)
    for level in range(levels):
        part = piece(decay, level)
        mixing = mixing + covers[level] * dot_tn(
            (part * g).astype(BF16), (part * attention).astype(BF16)
        )
    for by in range(SUB):
        row = jnp.sum(weights[by] * attention, axis=0, keepdims=True)
        mixing = jnp.where(gap == by, row, mixing)
    mixing = jnp.where(visible, mixing, 0.0).astype(BF16)
    output[...] = dot_tn(mixing, v) + dot_tn(
        (carried * attention).astype(BF16), value_in.astype(BF16)
    )
    ends = after * g * rows[2:3, :]
    keep = carried[:, CHUNK - 1 : CHUNK]
    key_state[...] = keep * key_in + split_nn(ends, k)
    value_state[...] = keep * value_in + split_nn(ends, v)


def mixer_backward_kernel(
    levels,
    factor,
    mine,
    query,
    key,
    value,
    grad_output,
    rate,
    inflow,
    rows,
    segment_col,
    sums,
    covers,
    apart,
    later,
    attention_in,
    logits_in,
    key_start,
    value_start,
    grad_query,
    grad_key,
    grad_value,
    grad_rate,
    key_grad,
    value_grad,
    flow,
):
    @pl.when(pl.program_id(0) == 0)
    def _():
        key_grad[...] = jnp.zeros_like(key_grad)
        value_grad[...] = jnp.zeros_like(value_grad)
        flow[...] = jnp.zeros_like(flow)

    key_in, value_in = key_start[0], value_start[0]
    key_after, value_after = key_grad[...], value_grad[...]
    q, k, v, d = query[...], key[...], value[...], grad_output[...]
    a, g = rate[...], inflow[...]
    attention, logits = attention_in[...], logits_in[...]
    decay = exponents(a, sums[...])
    before, after = piece(decay, levels), piece(decay, levels + 1)
    carried = before * rows[1:2, :]
    visible = segment_col[...] == rows[0:1, :]
    scores = jnp.where(visible, dot_nt(k, q) * factor, 0.0)
    reads = jnp.where(visible, dot_nt(v, d), 0.0)
    gap = apart[...]
    grad_att = carried * split_nt(value_in, d)
    for level in range(levels):
        part = piece(decay, level)
        grad_att = grad_att + part * exact_nn(part * g, reads * covers[level])
    total = jnp.zeros_like(a)
    bare, weights, score_rows, read_rows = [], [], [], []
    for by in range(SUB):
        if by:
            total = total + rolled(a, by - 1)
        bare.append(jnp.exp(total))
        weights.append(bare[by] * rolled(g, by))
        score_rows.append(jnp.sum(jnp.where(gap == by, scores, 0.0), axis=0, keepdims=True))
        read_rows.append(jnp.sum(jnp.where(gap == by, reads, 0.0), axis=0, keepdims=True))
        grad_att = grad_att + weights[by] * read_rows[by]
    grad_logits = attention * (
        grad_att - jnp.sum(attention * grad_att, axis=0, keepdims=True)
    )
    mixing = jnp.zeros((CHUNK, CHUNK), F32)
    spread = jnp.zeros((CHUNK, CHUNK), F32)
    ends = after * rows[2:3, :]
    grad_inflow = ends * (split_nt(key_after, k) + split_nt(value_after, v))
    for level in range(levels):
        part = piece(decay, level)
        left = (part * g).astype(BF16)
        att_part, log_part = part * attention, part * grad_logits
        mixing = mixing + covers[level] * dot_tn(left, att_part.astype(BF16))
        spread = spread + covers[level] * dot_tn(left, log_part.astype(BF16))
        grad_inflow = grad_inflow + part * (
            exact_nt(log_part, scores * covers[level]) + exact_nt(att_part, reads * covers[level])
        )
    for by in range(SUB):
        row = jnp.sum(weights[by] * attention, axis=0, keepdims=True)
        mixing = jnp.where(gap == by, row, mixing)
        row = jnp.sum(weights[by] * grad_logits, axis=0, keepdims=True)
        spread = jnp.where(gap == by, row, spread)
        terms = bare[by] * (grad_logits * score_rows[by] + attention * read_rows[by])
        grad_inflow = grad_inflow + rolled(terms, -by)
    mixing = jnp.where(visible, mixing, 0.0).astype(BF16)
    spread = (jnp.where(visible, spread, 0.0) * factor).astype(BF16)
    log_carried = carried * grad_logits * factor
    att_carried = carried * attention
    ends = (ends * g).astype(BF16)
    grad_query[...] = (
        dot_tn(spread, k) + dot_tn(log_carried.astype(BF16), key_in.astype(BF16))
    ).astype(BF16)
    grad_key[...] = (dot_nn(spread, q) + dot_tn(ends, key_after.astype(BF16))).astype(BF16)
    grad_value[...] = (dot_nn(mixing, d) + dot_tn(ends, value_after.astype(BF16))).astype(BF16)
    change = grad_logits * logits + attention * grad_att - g * grad_inflow
    same = jnp.where(visible, later[...], 0.0)
    flows = exact_nn(change, same) + rows[2:3, :] * flow[:, 0:1]
    grad_rate[...] = rows[3:4, :] * flows - jnp.exp(a) * grad_inflow
    keep = carried[:, CHUNK - 1 : CHUNK]
    key_before = keep * key_after + split_nn(log_carried, q)
    value_before = keep * value_after + split_nn(att_carried, d)
    key_grad[...] = key_before
    value_grad[...] = value_before
    flow[...] = jnp.broadcast_to(
        jnp.sum(key_before * key_in + value_before * value_in, axis=1, keepdims=True), flow.shape
    )


def mixer_specs(length, size, ring, backward):
    count = length // CHUNK
    per = count // ring

    def natural(step):
        return count - 1 - step if backward else step

    def moved(step, mine):
        at = natural(step)
        return lax.bitwise_xor(at // per, mine[0]) * per + at % per

    wide = pl.BlockSpec((CHUNK, size), lambda step, mine: (moved(step, mine), 0))
    slim = pl.BlockSpec((SLOTS, CHUNK), lambda step, mine: (0, moved(step, mine)))
    plain = pl.BlockSpec((SLOTS, CHUNK), lambda step, mine: (0, natural(step)))
    rows = pl.BlockSpec((8, CHUNK), lambda step, mine: (0, natural(step)))
    column = pl.BlockSpec((CHUNK, 1), lambda step, mine: (natural(step), 0))
    state = pl.BlockSpec((1, SLOTS, size), lambda step, mine: (natural(step), 0, 0))
    return count, wide, slim, plain, rows, column, state


def whole(array):
    rank = array.ndim
    return pl.BlockSpec(array.shape, lambda step, mine: (0,) * rank)


def mixer_forward(mine, ring, query, key, value, rate, inflow, rows, column):
    length, size = query.shape
    sums, covers, apart = (jnp.asarray(table) for table in chunk_tables())
    count, wide, slim, plain, row_spec, col_spec, state = mixer_specs(length, size, ring, False)
    kernel = functools.partial(mixer_forward_kernel, covers.shape[0], size ** (-0.25))
    return pl.pallas_call(
        kernel,
        out_shape=(
            jax.ShapeDtypeStruct((length, size), F32),
            jax.ShapeDtypeStruct((SLOTS, length), F32),
            jax.ShapeDtypeStruct((SLOTS, length), F32),
            jax.ShapeDtypeStruct((count, SLOTS, size), F32),
            jax.ShapeDtypeStruct((count, SLOTS, size), F32),
        ),
        grid_spec=pltpu.PrefetchScalarGridSpec(
            num_scalar_prefetch=1,
            grid=(count,),
            in_specs=[
                wide, wide, wide, slim, slim, row_spec, col_spec,
                whole(sums), whole(covers), whole(apart),
            ],
            out_specs=[wide, plain, plain, state, state],
            scratch_shapes=[pltpu.VMEM((SLOTS, size), F32)] * 2,
        ),
        compiler_params=pltpu.CompilerParams(vmem_limit_bytes=32 << 20),
        cost_estimate=pl.CostEstimate(
            flops=length * size * 2000, bytes_accessed=length * size * 12, transcendentals=length * 4096
        ),
        name="mixer_forward",
    )(mine, query, key, value, rate, inflow, rows, column, sums, covers, apart)


def mixer_backward(
    mine, ring, query, key, value, grad, rate, inflow, rows, column, attention, logits, starts
):
    length, size = query.shape
    sums, covers, apart = (jnp.asarray(table) for table in chunk_tables())
    later = jnp.asarray(np.tril(np.ones((CHUNK, CHUNK), np.float32)))
    count, wide, slim, plain, row_spec, col_spec, state = mixer_specs(length, size, ring, True)
    kernel = functools.partial(mixer_backward_kernel, covers.shape[0], size ** (-0.25))
    return pl.pallas_call(
        kernel,
        out_shape=(
            jax.ShapeDtypeStruct((length, size), BF16),
            jax.ShapeDtypeStruct((length, size), BF16),
            jax.ShapeDtypeStruct((length, size), BF16),
            jax.ShapeDtypeStruct((SLOTS, length), F32),
        ),
        grid_spec=pltpu.PrefetchScalarGridSpec(
            num_scalar_prefetch=1,
            grid=(count,),
            in_specs=[
                wide, wide, wide, wide, slim, slim, row_spec, col_spec,
                whole(sums), whole(covers), whole(apart), whole(later),
                plain, plain, state, state,
            ],
            out_specs=[wide, wide, wide, slim],
            scratch_shapes=[pltpu.VMEM((SLOTS, size), F32)] * 2 + [pltpu.VMEM((SLOTS, 128), F32)],
        ),
        compiler_params=pltpu.CompilerParams(vmem_limit_bytes=32 << 20),
        cost_estimate=pl.CostEstimate(
            flops=length * size * 4000, bytes_accessed=length * size * 20, transcendentals=length * 4096
        ),
        name="mixer_backward",
    )(
        mine, query, key, value, grad, rate, inflow, rows, column,
        sums, covers, apart, later, attention, logits, *starts,
    )


def peers(ring, mine):
    found = []
    for by in range(1, ring):
        at, bit = mine, 1
        while bit <= by:
            if by & bit:
                at = at + bit * (1 - 2 * ((at // bit) % 2))
            bit *= 2
        found.append(at)
    return found


class Copies:
    def __init__(self, local, send, recv):
        self.local, self.send, self.recv = local, send, recv
        self.here, self.away = 0, 0
        self.open = []

    def near(self, source, target):
        copy = pltpu.make_async_copy(source, target, self.local.at[self.here])
        self.here += 1
        copy.start()
        return copy

    def far(self, source, target, landed, device, when=None):
        at = self.away
        self.away += 1
        copy = pltpu.make_async_remote_copy(
            source, target, self.send.at[at], self.recv.at[at], device_id=device,
            device_id_type=pl.DeviceIdType.MESH,
        )
        if when is None:
            copy.start()
        else:
            pl.when(when)(copy.start)
        self.open.append((copy, when))
        return pltpu.make_async_remote_copy(
            landed, landed, self.send.at[at], self.recv.at[at], device_id=device,
            device_id_type=pl.DeviceIdType.MESH,
        ).wait_recv

    def close(self):
        for copy, when in self.open:
            if when is None:
                copy.wait_send()
            else:
                pl.when(when)(copy.wait_send)


def slab_chain(copies, chips, place):
    mine, batch = lax.axis_index("seq"), lax.axis_index("batch")
    chip, core = batch // 2, batch % 2
    other = (mine, chip * 2 + (1 - core))

    def at(where):
        return jnp.clip(where, 0, chips - 1) * 2 + core

    def send(step, way):
        block, come = chip - way * (step - 1), chip - way * step
        when = (block >= 0) & (block < chips) & (chip + way >= 0) & (chip + way < chips)
        came = (come >= 0) & (come < chips)
        wait = copies.far(
            place(at(block)), place(at(block)), place(at(come)), (mine, at(chip + way)), when
        )
        return wait, came, at(come)

    crossing = [(copies.far(place(batch), place(batch), place(other[1]), other), None)]
    flying = [send(1, 1), send(1, -1)] if chips > 1 else []
    yield
    for step in range(1, chips):
        coming = []
        for way, (wait, came, landed) in zip((1, -1), flying):
            pl.when(came)(wait)
            if step + 1 < chips:
                coming.append(send(step + 1, way))
            there = landed + 1 - 2 * core
            crossing.append(
                (copies.far(place(landed), place(landed), place(there), other, came), came)
            )
        flying = coming
        yield
    for wait, came in crossing:
        if came is None:
            wait()
        else:
            pl.when(came)(wait)
    yield


def start_kernel(
    ring, lines, inputs, w_query, w_key, w_value, w_swish, w_out, gate, up, small,
    inputs_all, w_mixer, w_output, feed_columns, small_all, local_sem, send_sem, recv_sem,
):
    mine, batch = lax.axis_index("seq"), lax.axis_index("batch")
    chips = lines // 2
    copies = Copies(local_sem, send_sem, recv_sem)
    part = w_mixer.shape[3] // 4
    half = inputs.shape[0] // 2
    others = peers(ring, mine)
    pieces = (w_query, w_key, w_value, w_swish)

    def column(ref, at):
        if len(ref.shape) == 3:
            return ref.at[at]
        size = ref.shape[1] // ring
        return ref.at[:, pl.ds(pl.multiple_of(at * size, 128), size)]

    def slot(source, piece):
        return w_mixer.at[source, batch, :, pl.ds(piece * part, part)]

    near = [copies.near(column(ref, mine), slot(mine, at)) for at, ref in enumerate(pieces)]
    near += [copies.near(w_out, w_output.at[batch]), copies.near(small, small_all.at[mine, batch])]
    column_waits, small_waits = [], []
    for to in others:
        column_waits.append(
            [
                copies.far(column(ref, to), slot(mine, at), slot(to, at), (to, batch))
                for at, ref in enumerate(pieces)
            ]
        )
        small_waits.append(
            copies.far(small, small_all.at[mine, batch], small_all.at[to, batch], (to, batch))
        )
    own_input = copies.near(inputs, inputs_all.at[0])
    direct = 2 if ring == 4 else ring - 1
    input_waits = [
        copies.far(inputs, inputs_all.at[by + 1], inputs_all.at[by + 1], (others[by], batch))
        for by in range(direct)
    ]
    for copy in near:
        copy.wait()

    def started(place):
        chain = slab_chain(copies, chips, place)
        next(chain)
        chains.append(chain)

    chains = []
    started(lambda at: w_mixer.at[mine, at])
    for waits, source in zip(column_waits, others):
        for wait in waits:
            wait()
        started(lambda at, source=source: w_mixer.at[source, at])
    for wait, source in zip(small_waits, others):
        wait()
        started(lambda at, source=source: small_all.at[source, at])
    started(lambda at: small_all.at[mine, at])
    started(lambda at: w_output.at[at])
    own_feed = [copies.near(column(ref, mine), feed_columns.at[at, mine]) for at, ref in enumerate((gate, up))]
    for chain in chains:
        if chips > 1:
            next(chain)
    if ring == 4:
        for wait in input_waits:
            wait()
        low, high = pl.ds(0, half), pl.ds(half, half)
        input_waits = [
            copies.far(
                inputs_all.at[have, rows], inputs_all.at[3, rows], inputs_all.at[3, rows], (to, batch)
            )
            for have, rows, to in ((2, low, others[0]), (1, high, others[1]))
        ]
    feed_waits = [
        copies.far(
            column(ref, to), feed_columns.at[at, mine], feed_columns.at[at, to], (to, batch)
        )
        for to in others
        for at, ref in enumerate((gate, up))
    ]
    for _ in range(chips - 1 if chips > 1 else 1):
        for chain in chains:
            next(chain)
    for wait in input_waits + feed_waits:
        wait()
    for copy in [own_input] + own_feed:
        copy.wait()
    copies.close()


def start(ring, lines, inputs, columns, w_out, gate, up, small):
    own, width = columns[0].shape
    part, hidden = width // ring, gate.shape[1] // ring
    if hidden % 128:
        gate, up = (a.reshape(own, ring, hidden).transpose(1, 0, 2) for a in (gate, up))
    chains = 2 * ring + 1
    away = (ring - 1) * 8 + 4 + chains * (4 * (lines // 2 - 1) + 1)
    anywhere = pl.BlockSpec(memory_space=pl.ANY)
    return pl.pallas_call(
        functools.partial(start_kernel, ring, lines),
        out_shape=(
            jax.ShapeDtypeStruct((ring,) + inputs.shape, BF16),
            jax.ShapeDtypeStruct((ring, lines, own, 4 * part), BF16),
            jax.ShapeDtypeStruct((lines,) + w_out.shape, BF16),
            jax.ShapeDtypeStruct((2, ring, own, hidden), BF16),
            jax.ShapeDtypeStruct((ring, lines) + small.shape, BF16),
        ),
        in_specs=[anywhere] * 9,
        out_specs=[anywhere] * 5,
        scratch_shapes=[
            pltpu.SemaphoreType.DMA((12,)),
            pltpu.SemaphoreType.DMA((away,)),
            pltpu.SemaphoreType.DMA((away,)),
        ],
        compiler_params=pltpu.CompilerParams(has_side_effects=True),
        name="start",
    )(inputs, *columns, w_out, gate, up, small)


def rms_scale(features):
    return lax.rsqrt(jnp.mean(features * features, axis=-1, keepdims=True) + EPS)


def swapped(block, by, ring):
    return lax.ppermute(block, "seq", [(i, i ^ by) for i in range(ring)])


def gathered(block, ring):
    if ring != 4:
        return jnp.concatenate([block] + [swapped(block, by, ring) for by in range(1, ring)], axis=0)
    half = block.shape[0] // 2
    one, two = swapped(block, 1, ring), swapped(block, 2, ring)
    low, high = swapped(two[:half], 1, ring), swapped(one[half:], 2, ring)
    return jnp.concatenate([block, one, two, low, high], axis=0)


def scattered(terms, ring):
    rows = terms.shape[0] // ring
    parts = [terms[by * rows : (by + 1) * rows] for by in range(ring)]
    total = parts[0].astype(F32)
    if ring != 4:
        for by in range(1, ring):
            total = total + swapped(parts[by], by, ring).astype(F32)
        return total
    half = rows // 2
    low, high = swapped(parts[3][:half], 1, ring), swapped(parts[3][half:], 2, ring)
    two = jnp.concatenate([added(parts[2][:half], low), parts[2][half:]], axis=0)
    one = jnp.concatenate([parts[1][:half], added(parts[1][half:], high)], axis=0)
    return total + swapped(one, 1, ring).astype(F32) + swapped(two, 2, ring).astype(F32)


def added(left, right):
    return (left.astype(F32) + right.astype(F32)).astype(BF16)


def flipped(block, axis, by):
    return lax.ppermute(block, axis, [(i, i ^ by) for i in range(lax.axis_size(axis))])


def doubled(block, axis):
    by, mine = 1, lax.axis_index(axis)
    while by < lax.axis_size(axis):
        other = flipped(block, axis, by)
        first = (mine & by) == 0
        block = jnp.concatenate(
            [jnp.where(first, block, other), jnp.where(first, other, block)], axis=0
        )
        by *= 2
    return block


def halved(block, axis):
    by, mine = lax.axis_size(axis) // 2, lax.axis_index(axis)
    while by:
        low, high = jnp.split(block, 2, axis=0)
        first = (mine & by) == 0
        block = jnp.where(first, low, high) + flipped(jnp.where(first, high, low), axis, by)
        by //= 2
    return block


def after(value, *others):
    return lax.optimization_barrier((value,) + others)[0]


def exchanged(blocks, mine, ring):
    parts = [
        swapped(lax.dynamic_index_in_dim(blocks, mine ^ by, 0, keepdims=False), by, ring)
        if by
        else lax.dynamic_index_in_dim(blocks, mine, 0, keepdims=False)
        for by in range(ring)
    ]
    made = jnp.stack(parts)
    return jnp.concatenate(
        [lax.dynamic_index_in_dim(made, mine ^ j, 0, keepdims=True) for j in range(ring)], axis=0
    )


def local(
    layer_input,
    segments,
    mixer_gain,
    query_weight,
    key_weight,
    value_weight,
    squeeze,
    expand,
    forget_bias,
    swish_weight,
    head_gain,
    output_weight,
    feed_gain,
    gate_weight,
    up_weight,
    down_weight,
    cotangent,
):
    ring, lines = lax.axis_size("seq"), lax.axis_size("batch")
    devices = ring * lines
    mine = lax.axis_index("seq")
    rows, width = layer_input.shape[1], layer_input.shape[2]
    length = rows * ring
    own = width // devices
    head_size = width // HEADS
    copies = ring // HEADS
    part = width // ring
    head = mine // copies
    hidden_part = gate_weight.shape[1] // ring
    slots_all = HEADS * SLOTS

    def to_order(array):
        if copies == 1:
            return array
        blocks = array.reshape((ring, rows) + array.shape[1:])
        moved = [lax.dynamic_index_in_dim(blocks, mine ^ by, 0, keepdims=False) for by in range(ring)]
        return jnp.concatenate(moved, axis=0)

    def whole_head(array):
        if copies == 1:
            return array
        full = lax.all_gather(to_order(array), "seq", axis=1, tiled=True)
        return to_order(lax.dynamic_slice_in_dim(full, head * head_size, head_size, 1))

    def own_part(array):
        if copies == 1:
            return array
        return lax.dynamic_slice_in_dim(array, (mine % copies) * part, part, 1)

    params = jnp.concatenate(
        [
            mixer_gain,
            head_gain,
            feed_gain,
            forget_bias,
            expand.T.reshape(-1),
            squeeze.reshape(-1),
        ]
    )
    count = params.shape[0]
    params = jnp.concatenate([params, segments.reshape(rows).astype(BF16)])
    params = jnp.pad(params, (0, -params.shape[0] % 2048)).reshape(-1, 128)
    input_own = layer_input.reshape(rows, width)
    inputs, w_mixer, w_output, feed_columns, small = start(
        ring,
        lines,
        input_own,
        (query_weight, key_weight, value_weight, swish_weight),
        output_weight,
        gate_weight,
        up_weight,
        params,
    )
    inputs = inputs.reshape(length, width)
    w_mixer = w_mixer.reshape(width, 4 * part)
    w_output = w_output.reshape(part, width)
    small = small.reshape(devices, -1)
    segment = lax.dynamic_index_in_dim(
        small.reshape(ring, lines, -1), lax.axis_index("batch"), 1, keepdims=False
    )[:, count : count + rows].reshape(length).astype(F32)
    cuts = np.cumsum([own, own, own, slots_all // devices, RANK * slots_all // devices])
    gain_one, gain_head, gain_two, bias_full, expand_t, w_squeeze = jnp.split(
        small[:, :count], cuts, axis=1
    )
    gain_one = gain_one.reshape(width).astype(F32)
    gain_head = lax.dynamic_slice_in_dim(gain_head.reshape(width), head * head_size, head_size, 0)
    gain_head = gain_head.astype(F32)
    gain_two = gain_two.reshape(width).astype(F32)
    bias_head = lax.dynamic_slice_in_dim(bias_full.reshape(slots_all), head * SLOTS, SLOTS, 0)
    expand_head = lax.dynamic_slice_in_dim(
        expand_t.reshape(slots_all, RANK), head * SLOTS, SLOTS, 0
    )
    w_squeeze = w_squeeze.reshape(width, RANK).T

    feed_blocks = lax.all_gather(
        feed_columns.reshape(2 * ring * own, hidden_part), "batch", axis=0, tiled=False
    )
    feed_blocks = feed_blocks.reshape(lines, 2, ring, own, hidden_part)
    feed_blocks = feed_blocks.transpose(1, 2, 0, 3, 4).reshape(2, width, hidden_part)
    w_gate, w_up = feed_blocks[0], feed_blocks[1]
    w_down = lax.all_gather(after(down_weight, inputs), "batch", axis=0, tiled=True)

    chunked = segment.reshape(-1, CHUNK)
    before = jnp.concatenate([jnp.full((1,), -1.0, F32), chunked[:-1, -1]])
    previous = jnp.concatenate([jnp.full((1,), -1.0, F32), segment[:-1]])
    mask_rows = jnp.stack(
        [
            segment,
            (chunked == before[:, None]).astype(F32).reshape(-1),
            (chunked == chunked[:, -1:]).astype(F32).reshape(-1),
            (segment == previous).astype(F32),
        ]
        + [jnp.zeros_like(segment)] * 4
    )
    segment_col = segment[:, None]

    grad_own = cotangent.reshape(rows, width)
    grad_out = gathered(after(grad_own, inputs), ring)
    inputs = inputs.astype(F32)
    scale_one = rms_scale(inputs)
    plain_one = inputs * scale_one
    normed = (plain_one * gain_one).astype(BF16)
    mixer_pre = dot_nn(normed, w_mixer)
    query = whole_head(mixer_pre[:, :part].astype(BF16))
    key = whole_head(mixer_pre[:, part : 2 * part].astype(BF16))
    value = whole_head(mixer_pre[:, 2 * part : 3 * part].astype(BF16))
    swish_pre = whole_head(mixer_pre[:, 3 * part :])
    reduced = dot_nt(normed, w_squeeze).astype(BF16)
    forget_logit = dot_nt(expand_head, reduced) + bias_head.astype(F32)[:, None]
    log_rate = jax.nn.log_sigmoid(forget_logit) / TAU_GATE
    inflow = -jnp.expm1(log_rate)
    order = mine.reshape(1).astype(jnp.int32)
    query, grad_out = lax.optimization_barrier((query, grad_out))
    mixed, attention, logits, key_start, value_start = mixer_forward(
        order, ring, query, key, value, log_rate, inflow, mask_rows, segment_col
    )
    head_factor = rms_scale(mixed)
    head_plain = mixed * head_factor
    head_normed = head_plain * gain_head
    swish_sig = jax.nn.sigmoid(swish_pre)
    swish_act = swish_pre * swish_sig
    gated = own_part((head_normed * swish_act).astype(BF16))
    hidden = input_own.astype(F32) + scattered(dot_nn(gated, w_output).astype(BF16), ring)

    scale_two = rms_scale(hidden)
    feed_in = gathered(((hidden * scale_two * gain_two).astype(BF16)), ring)
    gate_pre, up_pre = dot_nn(feed_in, w_gate), dot_nn(feed_in, w_up)
    gate_sig = jax.nn.sigmoid(gate_pre)
    gate_act = gate_pre * gate_sig
    inner = (gate_act * up_pre).astype(BF16)

    term_down = dot_tn(inner, grad_out).astype(BF16)
    grad_inner = dot_nt(after(grad_out, term_down), w_down)
    grad_gatepre = grad_inner * up_pre * (gate_sig * (1.0 + gate_pre * (1.0 - gate_sig)))
    grad_gatepre = grad_gatepre.astype(BF16)
    grad_uppre = (grad_inner * gate_act).astype(BF16)
    back_feedin = (dot_nt(grad_gatepre, w_gate) + dot_nt(grad_uppre, w_up)).astype(BF16)
    grad_feedin = scattered(back_feedin, ring)
    feed_rows = after(feed_in, back_feedin)
    term_gate = dot_tn(feed_rows, grad_gatepre).astype(BF16)
    term_up = dot_tn(feed_rows, grad_uppre).astype(BF16)
    result = hidden + scattered(dot_nn(after(inner, term_gate, term_up), w_down).astype(BF16), ring)
    layer_output = result.astype(BF16).reshape(1, rows, width)
    down_share = lax.psum_scatter(term_down, "batch", scatter_dimension=0, tiled=True)
    term_feedpre = jnp.stack([term_gate, term_up]).reshape(2, ring, lines, own, hidden_part)
    term_feedpre = term_feedpre.transpose(2, 0, 1, 3, 4).reshape(-1, hidden_part)
    feed_sum = lax.psum_scatter(
        after(term_feedpre, down_share), "batch", scatter_dimension=0, tiled=True
    )
    feed_share = feed_sum.reshape(2, ring, own, hidden_part).transpose(1, 0, 2, 3)
    feed_share = exchanged(feed_share, mine, ring)
    gate_share = feed_share[:, 0].transpose(1, 0, 2).reshape(own, -1)
    up_share = feed_share[:, 1].transpose(1, 0, 2).reshape(own, -1)
    term_feed = jnp.sum(grad_feedin * hidden * scale_two, axis=0)
    scaled_two = grad_feedin * gain_two
    grad_hidden = (
        grad_own.astype(F32)
        + scale_two * scaled_two
        - hidden * scale_two**3 * jnp.mean(scaled_two * hidden, axis=-1, keepdims=True)
    )

    grad_branch = after(gathered(grad_hidden.astype(BF16), ring), term_gate, term_up)
    grad_gated = whole_head(dot_nt(grad_branch, w_output))
    term_output = dot_tn(gated, grad_branch).astype(BF16)
    slope = swish_sig * (1.0 + swish_pre * (1.0 - swish_sig))
    grad_swishpre = own_part((grad_gated * head_normed * slope).astype(BF16))
    grad_normed_head = grad_gated * swish_act
    term_head = jnp.sum(grad_normed_head * head_plain, axis=0) / copies
    scaled_head = grad_normed_head * gain_head
    grad_mixed = head_factor * scaled_head - mixed * head_factor**3 * jnp.mean(
        scaled_head * mixed, axis=-1, keepdims=True
    )
    grad_query, grad_key, grad_value, grad_rate = mixer_backward(
        order,
        ring,
        query,
        key,
        value,
        grad_mixed.astype(BF16),
        log_rate,
        inflow,
        mask_rows,
        segment_col,
        attention,
        logits,
        (key_start, value_start),
    )
    grad_logit = (grad_rate * jax.nn.sigmoid(-forget_logit) / TAU_GATE).astype(BF16)
    term_bias = jnp.sum(grad_logit.astype(F32), axis=1) / copies
    term_expand = dot_nn(grad_logit, reduced) / copies
    grad_reduced = (dot_tn(grad_logit, expand_head) / copies).astype(BF16)
    grad_pre = jnp.concatenate(
        [own_part(grad_query), own_part(grad_key), own_part(grad_value), grad_swishpre], axis=1
    )
    grad_normed = dot_nt(grad_pre, w_mixer) + dot_nn(grad_reduced, w_squeeze)
    term_mixer = (jnp.sum(grad_normed * plain_one, axis=0))
    term_squeeze = (dot_tn(grad_reduced, normed))
    term_pre = dot_tn(normed, grad_pre).astype(BF16)
    term_pre = term_pre.reshape(ring, lines, own, 4 * part).transpose(1, 0, 2, 3)
    term_pre = term_pre.reshape(width, 4 * part)
    grad_normed = (scattered(after(grad_normed.astype(BF16), term_pre), ring))
    pre_share = lax.psum_scatter(after(term_pre, feed_sum), "batch", scatter_dimension=0, tiled=True)
    output_share = lax.psum_scatter(
        after(term_output, pre_share), "batch", scatter_dimension=0, tiled=True
    )
    pre_share = exchanged(pre_share.reshape(ring, own, 4 * part), mine, ring)
    pre_share = pre_share.reshape(ring, own, 4, part).transpose(2, 1, 0, 3).reshape(4, own, width)
    pre_share = pre_share.astype(F32)
    inputs_own = input_own.astype(F32)
    scale_own = rms_scale(inputs_own)
    scaled_one = grad_normed * (gain_one)
    grad_inputs = (
        grad_hidden
        + scale_own * scaled_one
        - inputs_own * scale_own**3 * jnp.mean(scaled_one * inputs_own, axis=-1, keepdims=True)
    )
    grad_input = grad_inputs.astype(BF16).reshape(1, rows, width)

    def placed(array, size):
        full = jnp.zeros((HEADS, size) + array.shape[1:], F32)
        return lax.dynamic_update_slice_in_dim(full, array[None], head, 0)

    terms = jnp.concatenate(
        [
            term_mixer.reshape(devices, -1),
            placed(term_head, head_size).reshape(devices, -1),
            term_feed.reshape(devices, -1),
            placed(term_bias, SLOTS).reshape(devices, -1),
            placed(term_expand, SLOTS).reshape(devices, -1),
            term_squeeze.T.reshape(devices, -1),
        ],
        axis=1,
    )
    share = halved(halved(terms, "seq"), "batch")[0]
    mixer_share, head_share, feedgain_share, bias_share, expand_share, squeeze_share = jnp.split(
        share, cuts
    )
    return (
        layer_output,
        grad_input,
        mixer_share,
        pre_share[0],
        pre_share[1],
        pre_share[2],
        squeeze_share.reshape(own, RANK),
        expand_share.reshape(-1, RANK).T,
        bias_share,
        pre_share[3],
        head_share,
        output_share.astype(F32),
        feedgain_share,
        gate_share.astype(F32),
        up_share.astype(F32),
        down_share.astype(F32),
    )


def solution(mesh):
    rows = P(BOTH, None)
    spread = P(BOTH)
    in_specs = (
        P("batch", "seq", None),
        P("batch", "seq"),
        spread,
        rows,
        rows,
        rows,
        rows,
        P(None, BOTH),
        spread,
        rows,
        spread,
        rows,
        spread,
        rows,
        rows,
        rows,
        P("batch", "seq", None),
    )
    out_specs = (
        P("batch", "seq", None),
        P("batch", "seq", None),
        spread,
        rows,
        rows,
        rows,
        rows,
        P(None, BOTH),
        spread,
        rows,
        spread,
        rows,
        spread,
        rows,
        rows,
        rows,
    )
    return jax.shard_map(local, mesh=mesh, in_specs=in_specs, out_specs=out_specs, check_vma=False)
```

```python
import functools

import jax
import jax.numpy as jnp
import numpy as np
from jax import lax
from jax.experimental import pallas as pl
from jax.experimental.pallas import tpu as pltpu
from jax.sharding import PartitionSpec as P

HEADS = 4
SLOTS = 64
RANK = 16
EPS = 1e-06
TAU_GATE = 8.0
CHUNK = 128
SUB = 16
BOTH = ("seq", "batch")
F32 = jnp.float32
BF16 = jnp.bfloat16
HIGHEST = lax.Precision.HIGHEST


def dot_nn(left, right):
    return lax.dot_general(left, right, (((1,), (0,)), ((), ())), preferred_element_type=F32)


def dot_nt(left, right):
    return lax.dot_general(left, right, (((1,), (1,)), ((), ())), preferred_element_type=F32)


def dot_tn(left, right):
    return lax.dot_general(left, right, (((0,), (0,)), ((), ())), preferred_element_type=F32)


def exact_nn(left, right):
    return lax.dot_general(
        left, right, (((1,), (0,)), ((), ())), precision=HIGHEST, preferred_element_type=F32
    )


def exact_nt(left, right):
    return lax.dot_general(
        left, right, (((1,), (1,)), ((), ())), precision=HIGHEST, preferred_element_type=F32
    )


def halves(value):
    high = value.astype(BF16)
    return high, (value - high.astype(F32)).astype(BF16)


def split_nn(left, right):
    high, rest = halves(left)
    return dot_nn(high, right) + dot_nn(rest, right)


def split_nt(left, right):
    high, rest = halves(left)
    return dot_nt(high, right) + dot_nt(rest, right)


def chunk_tables():
    at = np.arange(CHUNK)
    sums, covers = [], []
    half = SUB
    while half < CHUNK:
        right = (at // half) % 2 == 1
        edge = (at // (2 * half)) * 2 * half + half - 1
        low = np.where(right, edge, at)
        high = np.where(right, at, edge)
        sums.append((at[:, None] > low[None, :]) & (at[:, None] <= high[None, :]))
        same = (at[:, None] // (2 * half)) == (at[None, :] // (2 * half))
        covers.append(same & ~right[:, None] & right[None, :])
        half *= 2
    sums.append(at[:, None] <= at[None, :])
    sums.append(at[:, None] > at[None, :])
    apart = at[None, :] - at[:, None]
    apart = np.where(at[None, :] // SUB == at[:, None] // SUB, apart, -1)
    return (
        np.concatenate(sums, axis=1).astype(np.float32),
        np.stack(covers).astype(np.float32),
        np.maximum(apart, -1).astype(np.int32),
    )


def rolled(value, by):
    return value if by % CHUNK == 0 else pltpu.roll(value, by % CHUNK, 1)


def exponents(rate, sums):
    return jnp.exp(exact_nn(rate, sums))


def piece(value, at):
    return value[:, at * CHUNK : (at + 1) * CHUNK]


def mixer_forward_kernel(
    levels,
    factor,
    mine,
    query,
    key,
    value,
    rate,
    inflow,
    rows,
    segment_col,
    sums,
    covers,
    apart,
    output,
    attention_out,
    logits_out,
    key_start,
    value_start,
    key_state,
    value_state,
):
    @pl.when(pl.program_id(0) == 0)
    def _():
        key_state[...] = jnp.zeros_like(key_state)
        value_state[...] = jnp.zeros_like(value_state)

    key_in, value_in = key_state[...], value_state[...]
    key_start[0] = key_in
    value_start[0] = value_in
    q, k, v = query[...], key[...], value[...]
    a, g = rate[...], inflow[...]
    decay = exponents(a, sums[...])
    before, after = piece(decay, levels), piece(decay, levels + 1)
    carried = before * rows[1:2, :]
    visible = segment_col[...] == rows[0:1, :]
    scores = jnp.where(visible, dot_nt(k, q) * factor, 0.0)
    logits = carried * (split_nt(key_in, q) * factor)
    for level in range(levels):
        part = piece(decay, level)
        logits = logits + part * exact_nn(part * g, scores * covers[level])
    gap = apart[...]
    total = jnp.zeros_like(a)
    weights = []
    for by in range(SUB):
        if by:
            total = total + rolled(a, by - 1)
        weight = jnp.exp(total) * rolled(g, by)
        weights.append(weight)
        logits = logits + weight * jnp.sum(
            jnp.where(gap == by, scores, 0.0), axis=0, keepdims=True
        )
    attention = jnp.exp(logits - jnp.max(logits, axis=0, keepdims=True))
    attention = attention / jnp.sum(attention, axis=0, keepdims=True)
    attention_out[...] = attention
    logits_out[...] = logits
    mixing = jnp.zeros((CHUNK, CHUNK), F32)
    for level in range(levels):
        part = piece(decay, level)
        mixing = mixing + covers[level] * dot_tn(
            (part * g).astype(BF16), (part * attention).astype(BF16)
        )
    for by in range(SUB):
        row = jnp.sum(weights[by] * attention, axis=0, keepdims=True)
        mixing = jnp.where(gap == by, row, mixing)
    mixing = jnp.where(visible, mixing, 0.0).astype(BF16)
    output[...] = dot_tn(mixing, v) + dot_tn(
        (carried * attention).astype(BF16), value_in.astype(BF16)
    )
    ends = after * g * rows[2:3, :]
    keep = carried[:, CHUNK - 1 : CHUNK]
    key_state[...] = keep * key_in + split_nn(ends, k)
    value_state[...] = keep * value_in + split_nn(ends, v)


def mixer_backward_kernel(
    levels,
    factor,
    mine,
    query,
    key,
    value,
    grad_output,
    rate,
    inflow,
    rows,
    segment_col,
    sums,
    covers,
    apart,
    later,
    attention_in,
    logits_in,
    key_start,
    value_start,
    grad_query,
    grad_key,
    grad_value,
    grad_rate,
    key_grad,
    value_grad,
    flow,
):
    @pl.when(pl.program_id(0) == 0)
    def _():
        key_grad[...] = jnp.zeros_like(key_grad)
        value_grad[...] = jnp.zeros_like(value_grad)
        flow[...] = jnp.zeros_like(flow)

    key_in, value_in = key_start[0], value_start[0]
    key_after, value_after = key_grad[...], value_grad[...]
    q, k, v, d = query[...], key[...], value[...], grad_output[...]
    a, g = rate[...], inflow[...]
    attention, logits = attention_in[...], logits_in[...]
    decay = exponents(a, sums[...])
    before, after = piece(decay, levels), piece(decay, levels + 1)
    carried = before * rows[1:2, :]
    visible = segment_col[...] == rows[0:1, :]
    scores = jnp.where(visible, dot_nt(k, q) * factor, 0.0)
    reads = jnp.where(visible, dot_nt(v, d), 0.0)
    gap = apart[...]
    grad_att = carried * split_nt(value_in, d)
    for level in range(levels):
        part = piece(decay, level)
        grad_att = grad_att + part * exact_nn(part * g, reads * covers[level])
    total = jnp.zeros_like(a)
    bare, weights, score_rows, read_rows = [], [], [], []
    for by in range(SUB):
        if by:
            total = total + rolled(a, by - 1)
        bare.append(jnp.exp(total))
        weights.append(bare[by] * rolled(g, by))
        score_rows.append(jnp.sum(jnp.where(gap == by, scores, 0.0), axis=0, keepdims=True))
        read_rows.append(jnp.sum(jnp.where(gap == by, reads, 0.0), axis=0, keepdims=True))
        grad_att = grad_att + weights[by] * read_rows[by]
    grad_logits = attention * (
        grad_att - jnp.sum(attention * grad_att, axis=0, keepdims=True)
    )
    mixing = jnp.zeros((CHUNK, CHUNK), F32)
    spread = jnp.zeros((CHUNK, CHUNK), F32)
    ends = after * rows[2:3, :]
    grad_inflow = ends * (split_nt(key_after, k) + split_nt(value_after, v))
    for level in range(levels):
        part = piece(decay, level)
        left = (part * g).astype(BF16)
        att_part, log_part = part * attention, part * grad_logits
        mixing = mixing + covers[level] * dot_tn(left, att_part.astype(BF16))
        spread = spread + covers[level] * dot_tn(left, log_part.astype(BF16))
        grad_inflow = grad_inflow + part * (
            exact_nt(log_part, scores * covers[level]) + exact_nt(att_part, reads * covers[level])
        )
    for by in range(SUB):
        row = jnp.sum(weights[by] * attention, axis=0, keepdims=True)
        mixing = jnp.where(gap == by, row, mixing)
        row = jnp.sum(weights[by] * grad_logits, axis=0, keepdims=True)
        spread = jnp.where(gap == by, row, spread)
        terms = bare[by] * (grad_logits * score_rows[by] + attention * read_rows[by])
        grad_inflow = grad_inflow + rolled(terms, -by)
    mixing = jnp.where(visible, mixing, 0.0).astype(BF16)
    spread = (jnp.where(visible, spread, 0.0) * factor).astype(BF16)
    log_carried = carried * grad_logits * factor
    att_carried = carried * attention
    ends = (ends * g).astype(BF16)
    grad_query[...] = (
        dot_tn(spread, k) + dot_tn(log_carried.astype(BF16), key_in.astype(BF16))
    ).astype(BF16)
    grad_key[...] = (dot_nn(spread, q) + dot_tn(ends, key_after.astype(BF16))).astype(BF16)
    grad_value[...] = (dot_nn(mixing, d) + dot_tn(ends, value_after.astype(BF16))).astype(BF16)
    change = grad_logits * logits + attention * grad_att - g * grad_inflow
    same = jnp.where(visible, later[...], 0.0)
    flows = exact_nn(change, same) + rows[2:3, :] * flow[:, 0:1]
    grad_rate[...] = rows[3:4, :] * flows - jnp.exp(a) * grad_inflow
    keep = carried[:, CHUNK - 1 : CHUNK]
    key_before = keep * key_after + split_nn(log_carried, q)
    value_before = keep * value_after + split_nn(att_carried, d)
    key_grad[...] = key_before
    value_grad[...] = value_before
    flow[...] = jnp.broadcast_to(
        jnp.sum(key_before * key_in + value_before * value_in, axis=1, keepdims=True), flow.shape
    )


def mixer_specs(length, size, ring, backward):
    count = length // CHUNK
    per = count // ring

    def natural(step):
        return count - 1 - step if backward else step

    def moved(step, mine):
        at = natural(step)
        return lax.bitwise_xor(at // per, mine[0]) * per + at % per

    wide = pl.BlockSpec((CHUNK, size), lambda step, mine: (moved(step, mine), 0))
    slim = pl.BlockSpec((SLOTS, CHUNK), lambda step, mine: (0, moved(step, mine)))
    plain = pl.BlockSpec((SLOTS, CHUNK), lambda step, mine: (0, natural(step)))
    rows = pl.BlockSpec((8, CHUNK), lambda step, mine: (0, natural(step)))
    column = pl.BlockSpec((CHUNK, 1), lambda step, mine: (natural(step), 0))
    state = pl.BlockSpec((1, SLOTS, size), lambda step, mine: (natural(step), 0, 0))
    return count, wide, slim, plain, rows, column, state


def whole(array):
    rank = array.ndim
    return pl.BlockSpec(array.shape, lambda step, mine: (0,) * rank)


def mixer_forward(mine, ring, query, key, value, rate, inflow, rows, column):
    length, size = query.shape
    sums, covers, apart = (jnp.asarray(table) for table in chunk_tables())
    count, wide, slim, plain, row_spec, col_spec, state = mixer_specs(length, size, ring, False)
    kernel = functools.partial(mixer_forward_kernel, covers.shape[0], size ** (-0.25))
    return pl.pallas_call(
        kernel,
        out_shape=(
            jax.ShapeDtypeStruct((length, size), F32),
            jax.ShapeDtypeStruct((SLOTS, length), F32),
            jax.ShapeDtypeStruct((SLOTS, length), F32),
            jax.ShapeDtypeStruct((count, SLOTS, size), F32),
            jax.ShapeDtypeStruct((count, SLOTS, size), F32),
        ),
        grid_spec=pltpu.PrefetchScalarGridSpec(
            num_scalar_prefetch=1,
            grid=(count,),
            in_specs=[
                wide, wide, wide, slim, slim, row_spec, col_spec,
                whole(sums), whole(covers), whole(apart),
            ],
            out_specs=[wide, plain, plain, state, state],
            scratch_shapes=[pltpu.VMEM((SLOTS, size), F32)] * 2,
        ),
        compiler_params=pltpu.CompilerParams(vmem_limit_bytes=32 << 20),
        cost_estimate=pl.CostEstimate(
            flops=length * size * 2000, bytes_accessed=length * size * 12, transcendentals=length * 4096
        ),
        name="mixer_forward",
    )(mine, query, key, value, rate, inflow, rows, column, sums, covers, apart)


def mixer_backward(
    mine, ring, query, key, value, grad, rate, inflow, rows, column, attention, logits, starts
):
    length, size = query.shape
    sums, covers, apart = (jnp.asarray(table) for table in chunk_tables())
    later = jnp.asarray(np.tril(np.ones((CHUNK, CHUNK), np.float32)))
    count, wide, slim, plain, row_spec, col_spec, state = mixer_specs(length, size, ring, True)
    kernel = functools.partial(mixer_backward_kernel, covers.shape[0], size ** (-0.25))
    return pl.pallas_call(
        kernel,
        out_shape=(
            jax.ShapeDtypeStruct((length, size), BF16),
            jax.ShapeDtypeStruct((length, size), BF16),
            jax.ShapeDtypeStruct((length, size), BF16),
            jax.ShapeDtypeStruct((SLOTS, length), F32),
        ),
        grid_spec=pltpu.PrefetchScalarGridSpec(
            num_scalar_prefetch=1,
            grid=(count,),
            in_specs=[
                wide, wide, wide, wide, slim, slim, row_spec, col_spec,
                whole(sums), whole(covers), whole(apart), whole(later),
                plain, plain, state, state,
            ],
            out_specs=[wide, wide, wide, slim],
            scratch_shapes=[pltpu.VMEM((SLOTS, size), F32)] * 2 + [pltpu.VMEM((SLOTS, 128), F32)],
        ),
        compiler_params=pltpu.CompilerParams(vmem_limit_bytes=32 << 20),
        cost_estimate=pl.CostEstimate(
            flops=length * size * 4000, bytes_accessed=length * size * 20, transcendentals=length * 4096
        ),
        name="mixer_backward",
    )(
        mine, query, key, value, grad, rate, inflow, rows, column,
        sums, covers, apart, later, attention, logits, *starts,
    )


def peers(ring, mine):
    found = []
    for by in range(1, ring):
        at, bit = mine, 1
        while bit <= by:
            if by & bit:
                at = at + bit * (1 - 2 * ((at // bit) % 2))
            bit *= 2
        found.append(at)
    return found


class Copies:
    def __init__(self, local, send, recv):
        self.local, self.send, self.recv = local, send, recv
        self.here, self.away = 0, 0
        self.open = []

    def near(self, source, target):
        copy = pltpu.make_async_copy(source, target, self.local.at[self.here])
        self.here += 1
        copy.start()
        return copy

    def far(self, source, target, landed, device, when=None):
        at = self.away
        self.away += 1
        copy = pltpu.make_async_remote_copy(
            source, target, self.send.at[at], self.recv.at[at], device_id=device,
            device_id_type=pl.DeviceIdType.MESH,
        )
        if when is None:
            copy.start()
        else:
            pl.when(when)(copy.start)
        self.open.append((copy, when))
        return pltpu.make_async_remote_copy(
            landed, landed, self.send.at[at], self.recv.at[at], device_id=device,
            device_id_type=pl.DeviceIdType.MESH,
        ).wait_recv

    def close(self):
        for copy, when in self.open:
            if when is None:
                copy.wait_send()
            else:
                pl.when(when)(copy.wait_send)


def slab_chain(copies, chips, place):
    mine, batch = lax.axis_index("seq"), lax.axis_index("batch")
    chip, core = batch // 2, batch % 2
    other = (mine, chip * 2 + (1 - core))

    def at(where):
        return jnp.clip(where, 0, chips - 1) * 2 + core

    def send(step, way):
        block, come = chip - way * (step - 1), chip - way * step
        when = (block >= 0) & (block < chips) & (chip + way >= 0) & (chip + way < chips)
        came = (come >= 0) & (come < chips)
        wait = copies.far(
            place(at(block)), place(at(block)), place(at(come)), (mine, at(chip + way)), when
        )
        return wait, came, at(come)

    crossing = [(copies.far(place(batch), place(batch), place(other[1]), other), None)]
    flying = [send(1, 1), send(1, -1)] if chips > 1 else []
    yield
    for step in range(1, chips):
        coming = []
        for way, (wait, came, landed) in zip((1, -1), flying):
            pl.when(came)(wait)
            if step + 1 < chips:
                coming.append(send(step + 1, way))
            there = landed + 1 - 2 * core
            crossing.append(
                (copies.far(place(landed), place(landed), place(there), other, came), came)
            )
        flying = coming
        yield
    for wait, came in crossing:
        if came is None:
            wait()
        else:
            pl.when(came)(wait)
    yield


def start_kernel(
    ring, lines, inputs, cotangent, w_query, w_key, w_value, w_swish, w_out, gate, up, small,
    inputs_all, cotangent_all, w_mixer, swish_columns, out_rows, feed_columns, small_all,
    local_sem, send_sem, recv_sem,
):
    mine, batch = lax.axis_index("seq"), lax.axis_index("batch")
    chips = lines // 2
    copies = Copies(local_sem, send_sem, recv_sem)
    part = swish_columns.shape[2]
    half = inputs.shape[0] // 2
    others = peers(ring, mine)
    pieces = (w_query, w_key, w_value)

    def column(ref, at):
        if len(ref.shape) == 3:
            return ref.at[at]
        size = ref.shape[1] // ring
        return ref.at[:, pl.ds(pl.multiple_of(at * size, 128), size)]

    def slot(source, piece):
        return w_mixer.at[source, batch, :, pl.ds(piece * part, part)]

    near = [copies.near(column(ref, mine), slot(mine, at)) for at, ref in enumerate(pieces)]
    near += [copies.near(small, small_all.at[mine, batch])]
    column_waits, small_waits = [], []
    for to in others:
        column_waits.append(
            [
                copies.far(column(ref, to), slot(mine, at), slot(to, at), (to, batch))
                for at, ref in enumerate(pieces)
            ]
        )
        small_waits.append(
            copies.far(small, small_all.at[mine, batch], small_all.at[to, batch], (to, batch))
        )
    direct = 2 if ring == 4 else ring - 1

    def sent(block, blocks):
        return copies.near(block, blocks.at[0]), [
            copies.far(block, blocks.at[by + 1], blocks.at[by + 1], (others[by], batch))
            for by in range(direct)
        ]

    def passed_on(blocks, waits):
        for wait in waits:
            wait()
        if ring != 4:
            return []
        low, high = pl.ds(0, half), pl.ds(half, half)
        return [
            copies.far(blocks.at[have, rows], blocks.at[3, rows], blocks.at[3, rows], (to, batch))
            for have, rows, to in ((2, low, others[0]), (1, high, others[1]))
        ]

    own_input, input_waits = sent(inputs, inputs_all)
    for copy in near:
        copy.wait()

    def started(place):
        chain = slab_chain(copies, chips, place)
        next(chain)
        chains.append(chain)

    chains = []
    started(lambda at: w_mixer.at[mine, at])
    for waits, source in zip(column_waits, others):
        for wait in waits:
            wait()
        started(lambda at, source=source: w_mixer.at[source, at])
    for wait, source in zip(small_waits, others):
        wait()
        started(lambda at, source=source: small_all.at[source, at])
    started(lambda at: small_all.at[mine, at])
    input_waits = passed_on(inputs_all, input_waits)
    own_columns = [
        copies.near(column(w_swish, mine), swish_columns.at[mine]),
        copies.near(w_out, out_rows),
    ]
    own_columns += [
        copies.near(column(ref, mine), feed_columns.at[at, mine]) for at, ref in enumerate((gate, up))
    ]
    other_waits = [
        copies.far(column(w_swish, to), swish_columns.at[mine], swish_columns.at[to], (to, batch))
        for to in others
    ]
    other_waits += [
        copies.far(
            column(ref, to), feed_columns.at[at, mine], feed_columns.at[at, to], (to, batch)
        )
        for to in others
        for at, ref in enumerate((gate, up))
    ]
    own_cotangent, cotangent_waits = sent(cotangent, cotangent_all)
    for step in range(1, chips + 1):
        for chain in chains:
            if chips > 1 or step > 1:
                next(chain)
        if step == min(2, chips):
            cotangent_waits = passed_on(cotangent_all, cotangent_waits)
    if chips == 1:
        for chain in chains:
            next(chain)
    for wait in input_waits + cotangent_waits + other_waits:
        wait()
    for copy in [own_input, own_cotangent] + own_columns:
        copy.wait()
    copies.close()


def start(ring, lines, inputs, cotangent, columns, w_out, gate, up, small):
    own, width = columns[0].shape
    part, hidden = width // ring, gate.shape[1] // ring
    if hidden % 128:
        gate, up = (a.reshape(own, ring, hidden).transpose(1, 0, 2) for a in (gate, up))
    chains = 2 * ring
    away = (ring - 1) * 9 + 4 + chains * (4 * (lines // 2 - 1) + 1)
    gathered_shape = jax.ShapeDtypeStruct((ring,) + inputs.shape, BF16)
    return pl.pallas_call(
        functools.partial(start_kernel, ring, lines),
        out_shape=(
            gathered_shape,
            gathered_shape,
            jax.ShapeDtypeStruct((ring, lines, own, 3 * part), BF16),
            jax.ShapeDtypeStruct((ring, own, part), BF16),
            jax.ShapeDtypeStruct(w_out.shape, BF16),
            jax.ShapeDtypeStruct((2, ring, own, hidden), BF16),
            jax.ShapeDtypeStruct((ring, lines) + small.shape, BF16),
        ),
        in_specs=[pl.BlockSpec(memory_space=pltpu.VMEM)] * 10,
        out_specs=[pl.BlockSpec(memory_space=pl.ANY)] * 7,
        scratch_shapes=[
            pltpu.SemaphoreType.DMA((12,)),
            pltpu.SemaphoreType.DMA((away,)),
            pltpu.SemaphoreType.DMA((away,)),
        ],
        compiler_params=pltpu.CompilerParams(has_side_effects=True, vmem_limit_bytes=32 << 20),
        name="start",
    )(inputs, cotangent, *columns, w_out, gate, up, small)


PARTS = 4


def fold_kernel(finish, extras, *refs):
    terms, given = refs[0], refs[1 : 1 + extras]
    blocks = refs[1 + extras]
    made = refs[2 + extras : -9]
    first, second, third, two_low, one_high, own, local_sem, send_sem, recv_sem = refs[-9:]
    mine, batch = lax.axis_index("seq"), lax.axis_index("batch")
    others = peers(4, mine)
    row, col = (others[0], batch), (others[1], batch)
    copies = Copies(local_sem, send_sem, recv_sem)
    size = terms.shape[1] // PARTS

    def span(at):
        low = pl.ds(at * size, size // 2)
        return pl.ds(at * size, size), low, pl.ds(at * size + size // 2, size // 2)

    opening, direct = [], []

    def open_part(at):
        _, low, high = span(at)
        opening.append(
            (
                copies.far(terms.at[3, low], first.at[low], first.at[low], row),
                copies.far(terms.at[3, high], first.at[high], first.at[high], col),
            )
        )

    def pass_part(at):
        _, low, high = span(at)
        waits = [
            copies.far(terms.at[2, high], second.at[high], second.at[high], col),
            copies.far(terms.at[1, low], third.at[low], third.at[low], row),
        ]
        opening[at][0]()
        two_low[low, :] = added(terms[2, low, :], first[low, :])
        waits.append(copies.far(two_low.at[low], second.at[low], second.at[low], col))
        opening[at][1]()
        one_high[high, :] = added(terms[1, high, :], first[high, :])
        waits.append(copies.far(one_high.at[high], third.at[high], third.at[high], row))
        direct.append(waits)

    spread, local, passed = [], [], []

    def close_part(at):
        full, _, _ = span(at)
        for wait in direct[at]:
            wait()
        total = terms[0, full, :].astype(F32) + second[full, :].astype(F32) + third[full, :].astype(F32)
        own[full, :] = finish(total, full, at, given, made)
        spread.append(
            (
                copies.far(own.at[full], blocks.at[1, full], blocks.at[1, full], row),
                copies.far(own.at[full], blocks.at[2, full], blocks.at[2, full], col),
            )
        )
        local.append(copies.near(own.at[full], blocks.at[0, full]))

    def forward_part(at):
        _, low, high = span(at)
        for wait in spread[at]:
            wait()
        passed.append(copies.far(blocks.at[2, low], blocks.at[3, low], blocks.at[3, low], row))
        passed.append(copies.far(blocks.at[1, high], blocks.at[3, high], blocks.at[3, high], col))

    open_part(0)
    for at in range(PARTS + 2):
        if at + 1 < PARTS:
            open_part(at + 1)
        if at < PARTS:
            pass_part(at)
        if 1 <= at <= PARTS:
            close_part(at - 1)
        if at >= 2:
            forward_part(at - 2)
    for wait in passed:
        wait()
    for copy in local:
        copy.wait()
    copies.close()


def finish_forward(total, full, at, given, made):
    inputs, gain = given
    hidden = inputs[full, :].astype(F32) + total
    made[0][full, :] = hidden
    return (hidden * rms_scale(hidden) * gain[...]).astype(BF16)


def finish_backward(total, full, at, given, made):
    cotangent, hidden_ref, gain = given
    hidden = hidden_ref[full, :]
    scale = rms_scale(hidden)
    plain = hidden * scale
    term = jnp.sum(total * plain, axis=0, keepdims=True)
    made[1][...] = term if at == 0 else made[1][...] + term
    scaled = total * gain[...]
    grad = (
        cotangent[full, :].astype(F32)
        + scale * scaled
        - plain * (scale * jnp.mean(scaled * plain, axis=-1, keepdims=True))
    )
    made[0][full, :] = grad
    return grad.astype(BF16)


def fold(finish, terms, given, made, name):
    ring, rows, width = terms.shape
    inside = pl.BlockSpec(memory_space=pltpu.VMEM)
    block = pltpu.VMEM((rows, width), BF16)
    return pl.pallas_call(
        functools.partial(fold_kernel, finish, len(given)),
        out_shape=(jax.ShapeDtypeStruct((ring, rows, width), BF16),) + made,
        in_specs=[inside] * (1 + len(given)),
        out_specs=[pl.BlockSpec(memory_space=pl.ANY)] + [inside] * len(made),
        scratch_shapes=[block] * 6
        + [
            pltpu.SemaphoreType.DMA((PARTS,)),
            pltpu.SemaphoreType.DMA((PARTS * 10,)),
            pltpu.SemaphoreType.DMA((PARTS * 10,)),
        ],
        compiler_params=pltpu.CompilerParams(has_side_effects=True, vmem_limit_bytes=40 << 20),
        name=name,
    )(terms, *given)


def rms_scale(features):
    return lax.rsqrt(jnp.mean(features * features, axis=-1, keepdims=True) + EPS)


def swapped(block, by, ring):
    return lax.ppermute(block, "seq", [(i, i ^ by) for i in range(ring)])


def gathered(block, ring):
    if ring != 4:
        return jnp.concatenate([block] + [swapped(block, by, ring) for by in range(1, ring)], axis=0)
    half = block.shape[0] // 2
    one, two = swapped(block, 1, ring), swapped(block, 2, ring)
    low, high = swapped(two[:half], 1, ring), swapped(one[half:], 2, ring)
    return jnp.concatenate([block, one, two, low, high], axis=0)


def scattered(terms, ring):
    rows = terms.shape[0] // ring
    parts = [terms[by * rows : (by + 1) * rows] for by in range(ring)]
    total = parts[0].astype(F32)
    if ring != 4:
        for by in range(1, ring):
            total = total + swapped(parts[by], by, ring).astype(F32)
        return total
    half = rows // 2
    low, high = swapped(parts[3][:half], 1, ring), swapped(parts[3][half:], 2, ring)
    two = jnp.concatenate([added(parts[2][:half], low), parts[2][half:]], axis=0)
    one = jnp.concatenate([parts[1][:half], added(parts[1][half:], high)], axis=0)
    return total + swapped(one, 1, ring).astype(F32) + swapped(two, 2, ring).astype(F32)


def added(left, right):
    return (left.astype(F32) + right.astype(F32)).astype(BF16)


def flipped(block, axis, by):
    return lax.ppermute(block, axis, [(i, i ^ by) for i in range(lax.axis_size(axis))])


def doubled(block, axis):
    by, mine = 1, lax.axis_index(axis)
    while by < lax.axis_size(axis):
        other = flipped(block, axis, by)
        first = (mine & by) == 0
        block = jnp.concatenate(
            [jnp.where(first, block, other), jnp.where(first, other, block)], axis=0
        )
        by *= 2
    return block


def halved(block, axis):
    by, mine = lax.axis_size(axis) // 2, lax.axis_index(axis)
    while by:
        low, high = jnp.split(block, 2, axis=0)
        first = (mine & by) == 0
        block = jnp.where(first, low, high) + flipped(jnp.where(first, high, low), axis, by)
        by //= 2
    return block


def after(value, *others):
    return lax.optimization_barrier((value,) + others)[0]


def exchanged(blocks, mine, ring):
    parts = [
        swapped(lax.dynamic_index_in_dim(blocks, mine ^ by, 0, keepdims=False), by, ring)
        if by
        else lax.dynamic_index_in_dim(blocks, mine, 0, keepdims=False)
        for by in range(ring)
    ]
    made = jnp.stack(parts)
    return jnp.concatenate(
        [lax.dynamic_index_in_dim(made, mine ^ j, 0, keepdims=True) for j in range(ring)], axis=0
    )


def local(
    layer_input,
    segments,
    mixer_gain,
    query_weight,
    key_weight,
    value_weight,
    squeeze,
    expand,
    forget_bias,
    swish_weight,
    head_gain,
    output_weight,
    feed_gain,
    gate_weight,
    up_weight,
    down_weight,
    cotangent,
):
    ring, lines = lax.axis_size("seq"), lax.axis_size("batch")
    devices = ring * lines
    mine = lax.axis_index("seq")
    rows, width = layer_input.shape[1], layer_input.shape[2]
    length = rows * ring
    own = width // devices
    head_size = width // HEADS
    copies = ring // HEADS
    part = width // ring
    head = mine // copies
    hidden_part = gate_weight.shape[1] // ring
    slots_all = HEADS * SLOTS

    def to_order(array):
        if copies == 1:
            return array
        blocks = array.reshape((ring, rows) + array.shape[1:])
        moved = [lax.dynamic_index_in_dim(blocks, mine ^ by, 0, keepdims=False) for by in range(ring)]
        return jnp.concatenate(moved, axis=0)

    def whole_head(array):
        if copies == 1:
            return array
        full = lax.all_gather(to_order(array), "seq", axis=1, tiled=True)
        return to_order(lax.dynamic_slice_in_dim(full, head * head_size, head_size, 1))

    def own_part(array):
        if copies == 1:
            return array
        return lax.dynamic_slice_in_dim(array, (mine % copies) * part, part, 1)

    params = jnp.concatenate(
        [
            mixer_gain,
            head_gain,
            feed_gain,
            forget_bias,
            expand.T.reshape(-1),
            squeeze.reshape(-1),
        ]
    )
    count = params.shape[0]
    params = jnp.concatenate([params, segments.reshape(rows).astype(BF16)])
    params = jnp.pad(params, (0, -params.shape[0] % 2048)).reshape(-1, 128)
    input_own = layer_input.reshape(rows, width)
    grad_own = cotangent.reshape(rows, width)
    inputs, grad_out, w_mixer, swish_columns, out_rows, feed_columns, small = start(
        ring,
        lines,
        input_own,
        grad_own,
        (query_weight, key_weight, value_weight, swish_weight),
        output_weight,
        gate_weight,
        up_weight,
        params,
    )
    inputs = inputs.reshape(length, width)
    grad_out = grad_out.reshape(length, width)
    w_mixer = w_mixer.reshape(width, 3 * part)
    small = small.reshape(devices, -1)
    segment = lax.dynamic_index_in_dim(
        small.reshape(ring, lines, -1), lax.axis_index("batch"), 1, keepdims=False
    )[:, count : count + rows].reshape(length).astype(F32)
    cuts = np.cumsum([own, own, own, slots_all // devices, RANK * slots_all // devices])
    gain_one, gain_head, gain_two, bias_full, expand_t, w_squeeze = jnp.split(
        small[:, :count], cuts, axis=1
    )
    gain_one = gain_one.reshape(width).astype(F32)
    gain_head = lax.dynamic_slice_in_dim(gain_head.reshape(width), head * head_size, head_size, 0)
    gain_head = gain_head.astype(F32)
    gain_two = gain_two.reshape(width).astype(F32)
    bias_head = lax.dynamic_slice_in_dim(bias_full.reshape(slots_all), head * SLOTS, SLOTS, 0)
    expand_head = lax.dynamic_slice_in_dim(
        expand_t.reshape(slots_all, RANK), head * SLOTS, SLOTS, 0
    )
    w_squeeze = w_squeeze.reshape(width, RANK).T

    def over_batch(blocks):
        kinds, columns = blocks.shape[0], blocks.shape[-1]
        full = lax.all_gather(blocks.reshape(-1, columns), "batch", axis=0, tiled=False)
        full = full.reshape(lines, kinds, ring, own, columns)
        return full.transpose(1, 2, 0, 3, 4).reshape(kinds, width, columns)

    w_swish = over_batch(swish_columns[None])[0]
    w_output = lax.all_gather(after(out_rows, w_swish), "batch", axis=0, tiled=True)
    w_gate, w_up = over_batch(after(feed_columns, w_output))
    w_down = lax.all_gather(after(down_weight, w_output), "batch", axis=0, tiled=True)

    chunked = segment.reshape(-1, CHUNK)
    before = jnp.concatenate([jnp.full((1,), -1.0, F32), chunked[:-1, -1]])
    previous = jnp.concatenate([jnp.full((1,), -1.0, F32), segment[:-1]])
    mask_rows = jnp.stack(
        [
            segment,
            (chunked == before[:, None]).astype(F32).reshape(-1),
            (chunked == chunked[:, -1:]).astype(F32).reshape(-1),
            (segment == previous).astype(F32),
        ]
        + [jnp.zeros_like(segment)] * 4
    )
    segment_col = segment[:, None]

    inputs = inputs.astype(F32)
    scale_one = rms_scale(inputs)
    plain_one = inputs * scale_one
    normed = (plain_one * gain_one).astype(BF16)
    mixer_pre = dot_nn(normed, w_mixer)
    query = whole_head(mixer_pre[:, :part].astype(BF16))
    key = whole_head(mixer_pre[:, part : 2 * part].astype(BF16))
    value = whole_head(mixer_pre[:, 2 * part : 3 * part].astype(BF16))
    swish_pre = whole_head(dot_nn(normed, w_swish))
    reduced = dot_nt(normed, w_squeeze).astype(BF16)
    forget_logit = dot_nt(expand_head, reduced) + bias_head.astype(F32)[:, None]
    log_rate = jax.nn.log_sigmoid(forget_logit) / TAU_GATE
    inflow = -jnp.expm1(log_rate)
    order = mine.reshape(1).astype(jnp.int32)
    mixed, attention, logits, key_start, value_start = mixer_forward(
        order, ring, query, key, value, log_rate, inflow, mask_rows, segment_col
    )
    head_factor = rms_scale(mixed)
    head_plain = mixed * head_factor
    head_normed = head_plain * gain_head
    swish_sig = jax.nn.sigmoid(swish_pre)
    swish_act = swish_pre * swish_sig
    gated = own_part((head_normed * swish_act).astype(BF16))
    terms = dot_nn(gated, w_output).astype(BF16)
    if ring == 4:
        feed_in, hidden = fold(
            finish_forward,
            terms.reshape(ring, rows, width),
            (input_own, gain_two[None]),
            (jax.ShapeDtypeStruct((rows, width), F32),),
            "fold_forward",
        )
        feed_in = feed_in.reshape(length, width)
    else:
        hidden = input_own.astype(F32) + scattered(terms, ring)
        feed_in = gathered((hidden * rms_scale(hidden) * gain_two).astype(BF16), ring)

    gate_pre, up_pre = dot_nn(feed_in, w_gate), dot_nn(feed_in, w_up)
    gate_sig = jax.nn.sigmoid(gate_pre)
    gate_act = gate_pre * gate_sig
    inner = (gate_act * up_pre).astype(BF16)

    term_down = dot_tn(inner, grad_out).astype(BF16)
    grad_inner = dot_nt(after(grad_out, term_down), w_down)
    grad_gatepre = grad_inner * up_pre * (gate_sig * (1.0 + gate_pre * (1.0 - gate_sig)))
    grad_gatepre = grad_gatepre.astype(BF16)
    grad_uppre = (grad_inner * gate_act).astype(BF16)
    back_feedin = (dot_nt(grad_gatepre, w_gate) + dot_nt(grad_uppre, w_up)).astype(BF16)
    term_gate = dot_tn(feed_in, grad_gatepre).astype(BF16)
    term_up = dot_tn(feed_in, grad_uppre).astype(BF16)
    result_terms = dot_nn(inner, w_down).astype(BF16)
    result = hidden + scattered(result_terms, ring)
    layer_output = result.astype(BF16).reshape(1, rows, width)
    down_share = lax.psum_scatter(term_down, "batch", scatter_dimension=0, tiled=True)
    term_feedpre = jnp.stack([term_gate, term_up]).reshape(2, ring, lines, own, hidden_part)
    term_feedpre = term_feedpre.transpose(2, 0, 1, 3, 4).reshape(-1, hidden_part)
    feed_sum_start = term_feedpre
    feed_sum = lax.psum_scatter(
        after(term_feedpre, down_share), "batch", scatter_dimension=0, tiled=True
    )
    feed_share = feed_sum.reshape(2, ring, own, hidden_part).transpose(1, 0, 2, 3)
    feed_share = exchanged(feed_share, mine, ring)
    gate_share = feed_share[:, 0].transpose(1, 0, 2).reshape(own, -1)
    up_share = feed_share[:, 1].transpose(1, 0, 2).reshape(own, -1)
    if ring == 4:
        grad_branch, grad_hidden, term_feed = fold(
            finish_backward,
            after(back_feedin, feed_sum_start).reshape(ring, rows, width),
            (grad_own, hidden, gain_two[None]),
            (
                jax.ShapeDtypeStruct((rows, width), F32),
                jax.ShapeDtypeStruct((1, width), F32),
            ),
            "fold_backward",
        )
        grad_branch, term_feed = grad_branch.reshape(length, width), term_feed[0]
    else:
        grad_feedin = scattered(back_feedin, ring)
        scale_two = rms_scale(hidden)
        term_feed = jnp.sum(grad_feedin * hidden * scale_two, axis=0)
        scaled_two = grad_feedin * gain_two
        grad_hidden = (
            grad_own.astype(F32)
            + scale_two * scaled_two
            - hidden * scale_two**3 * jnp.mean(scaled_two * hidden, axis=-1, keepdims=True)
        )
        grad_branch = gathered(grad_hidden.astype(BF16), ring)

    grad_gated = whole_head(dot_nt(grad_branch, w_output))
    term_output = dot_tn(gated, grad_branch).astype(BF16)

    def line_major(term):
        return term.reshape(ring, lines, own, -1).transpose(1, 0, 2, 3).reshape(width, -1)

    slope = swish_sig * (1.0 + swish_pre * (1.0 - swish_sig))
    grad_swishpre = own_part((grad_gated * head_normed * slope).astype(BF16))
    term_swish = line_major(dot_tn(normed, grad_swishpre).astype(BF16))
    swish_sum = lax.psum_scatter(
        after(term_swish, feed_sum), "batch", scatter_dimension=0, tiled=True
    )
    output_share = lax.psum_scatter(
        after(term_output, swish_sum), "batch", scatter_dimension=0, tiled=True
    )
    grad_normed_head = grad_gated * swish_act
    term_head = jnp.sum(grad_normed_head * head_plain, axis=0) / copies
    scaled_head = grad_normed_head * gain_head
    grad_mixed = head_factor * scaled_head - mixed * head_factor**3 * jnp.mean(
        scaled_head * mixed, axis=-1, keepdims=True
    )
    grad_query, grad_key, grad_value, grad_rate = mixer_backward(
        order,
        ring,
        query,
        key,
        value,
        grad_mixed.astype(BF16),
        log_rate,
        inflow,
        mask_rows,
        segment_col,
        attention,
        logits,
        (key_start, value_start),
    )
    grad_logit = (grad_rate * jax.nn.sigmoid(-forget_logit) / TAU_GATE).astype(BF16)
    term_bias = jnp.sum(grad_logit.astype(F32), axis=1) / copies
    term_expand = dot_nn(grad_logit, reduced) / copies
    grad_reduced = (dot_tn(grad_logit, expand_head) / copies).astype(BF16)
    grad_pre = jnp.concatenate(
        [own_part(grad_query), own_part(grad_key), own_part(grad_value)], axis=1
    )
    grad_normed = (
        dot_nt(grad_pre, w_mixer) + dot_nt(grad_swishpre, w_swish) + dot_nn(grad_reduced, w_squeeze)
    )
    term_mixer = (jnp.sum(grad_normed * plain_one, axis=0))
    term_squeeze = (dot_tn(grad_reduced, normed))
    term_pre = line_major(dot_tn(normed, grad_pre).astype(BF16))
    grad_normed = scattered(after(grad_normed.astype(BF16), term_pre), ring)
    pre_sum = lax.psum_scatter(
        after(term_pre, output_share), "batch", scatter_dimension=0, tiled=True
    )
    pre_share = exchanged(pre_sum.reshape(ring, own, 3 * part), mine, ring)
    pre_share = pre_share.reshape(ring, own, 3, part).transpose(2, 1, 0, 3).reshape(3, own, width)
    pre_share = pre_share.astype(F32)
    swish_share = exchanged(swish_sum.reshape(ring, own, part), mine, ring)
    swish_share = swish_share.transpose(1, 0, 2).reshape(own, width).astype(F32)
    inputs_own = input_own.astype(F32)
    scale_own = rms_scale(inputs_own)
    scaled_one = grad_normed * (gain_one)
    grad_inputs = (
        grad_hidden
        + scale_own * scaled_one
        - inputs_own * scale_own**3 * jnp.mean(scaled_one * inputs_own, axis=-1, keepdims=True)
    )
    grad_input = grad_inputs.astype(BF16).reshape(1, rows, width)

    def placed(array, size):
        full = jnp.zeros((HEADS, size) + array.shape[1:], F32)
        return lax.dynamic_update_slice_in_dim(full, array[None], head, 0)

    terms = jnp.concatenate(
        [
            term_mixer.reshape(devices, -1),
            placed(term_head, head_size).reshape(devices, -1),
            term_feed.reshape(devices, -1),
            placed(term_bias, SLOTS).reshape(devices, -1),
            placed(term_expand, SLOTS).reshape(devices, -1),
            term_squeeze.T.reshape(devices, -1),
        ],
        axis=1,
    )
    share = halved(halved(terms, "seq"), "batch")[0]
    mixer_share, head_share, feedgain_share, bias_share, expand_share, squeeze_share = jnp.split(
        share, cuts
    )
    return (
        layer_output,
        grad_input,
        mixer_share,
        pre_share[0],
        pre_share[1],
        pre_share[2],
        squeeze_share.reshape(own, RANK),
        expand_share.reshape(-1, RANK).T,
        bias_share,
        swish_share,
        head_share,
        output_share.astype(F32),
        feedgain_share,
        gate_share.astype(F32),
        up_share.astype(F32),
        down_share.astype(F32),
    )


def solution(mesh):
    rows = P(BOTH, None)
    spread = P(BOTH)
    in_specs = (
        P("batch", "seq", None),
        P("batch", "seq"),
        spread,
        rows,
        rows,
        rows,
        rows,
        P(None, BOTH),
        spread,
        rows,
        spread,
        rows,
        spread,
        rows,
        rows,
        rows,
        P("batch", "seq", None),
    )
    out_specs = (
        P("batch", "seq", None),
        P("batch", "seq", None),
        spread,
        rows,
        rows,
        rows,
        rows,
        P(None, BOTH),
        spread,
        rows,
        spread,
        rows,
        spread,
        rows,
        rows,
        rows,
    )
    return jax.shard_map(local, mesh=mesh, in_specs=in_specs, out_specs=out_specs, check_vma=False)
```

```python
import functools

import jax
import jax.numpy as jnp
import numpy as np
from jax import lax
from jax.experimental import pallas as pl
from jax.experimental.pallas import tpu as pltpu
from jax.sharding import PartitionSpec as P

HEADS = 4
SLOTS = 64
RANK = 16
EPS = 1e-06
TAU_GATE = 8.0
CHUNK = 128
SUB = 16
BOTH = ("seq", "batch")
F32 = jnp.float32
BF16 = jnp.bfloat16
HIGHEST = lax.Precision.HIGHEST


def dot_nn(left, right):
    return lax.dot_general(left, right, (((1,), (0,)), ((), ())), preferred_element_type=F32)


def dot_nt(left, right):
    return lax.dot_general(left, right, (((1,), (1,)), ((), ())), preferred_element_type=F32)


def dot_tn(left, right):
    return lax.dot_general(left, right, (((0,), (0,)), ((), ())), preferred_element_type=F32)


def exact_nn(left, right):
    return lax.dot_general(
        left, right, (((1,), (0,)), ((), ())), precision=HIGHEST, preferred_element_type=F32
    )


def exact_nt(left, right):
    return lax.dot_general(
        left, right, (((1,), (1,)), ((), ())), precision=HIGHEST, preferred_element_type=F32
    )


def halves(value):
    high = value.astype(BF16)
    return high, (value - high.astype(F32)).astype(BF16)


def split_nn(left, right):
    high, rest = halves(left)
    return dot_nn(high, right) + dot_nn(rest, right)


def split_nt(left, right):
    high, rest = halves(left)
    return dot_nt(high, right) + dot_nt(rest, right)


def chunk_tables():
    at = np.arange(CHUNK)
    sums, covers = [], []
    half = SUB
    while half < CHUNK:
        right = (at // half) % 2 == 1
        edge = (at // (2 * half)) * 2 * half + half - 1
        low = np.where(right, edge, at)
        high = np.where(right, at, edge)
        sums.append((at[:, None] > low[None, :]) & (at[:, None] <= high[None, :]))
        same = (at[:, None] // (2 * half)) == (at[None, :] // (2 * half))
        covers.append(same & ~right[:, None] & right[None, :])
        half *= 2
    sums.append(at[:, None] <= at[None, :])
    sums.append(at[:, None] > at[None, :])
    apart = at[None, :] - at[:, None]
    apart = np.where(at[None, :] // SUB == at[:, None] // SUB, apart, -1)
    return (
        np.concatenate(sums, axis=1).astype(np.float32),
        np.stack(covers).astype(np.float32),
        np.maximum(apart, -1).astype(np.int32),
    )


def rolled(value, by):
    return value if by % CHUNK == 0 else pltpu.roll(value, by % CHUNK, 1)


def exponents(rate, sums):
    return jnp.exp(exact_nn(rate, sums))


def piece(value, at):
    return value[:, at * CHUNK : (at + 1) * CHUNK]


def mixer_forward_kernel(
    levels,
    factor,
    mine,
    query,
    key,
    value,
    rate,
    inflow,
    rows,
    segment_col,
    sums,
    covers,
    apart,
    output,
    attention_out,
    logits_out,
    key_start,
    value_start,
    key_state,
    value_state,
):
    @pl.when(pl.program_id(0) == 0)
    def _():
        key_state[...] = jnp.zeros_like(key_state)
        value_state[...] = jnp.zeros_like(value_state)

    key_in, value_in = key_state[...], value_state[...]
    key_start[0] = key_in
    value_start[0] = value_in
    q, k, v = query[...], key[...], value[...]
    a, g = rate[...], inflow[...]
    decay = exponents(a, sums[...])
    before, after = piece(decay, levels), piece(decay, levels + 1)
    carried = before * rows[1:2, :]
    visible = segment_col[...] == rows[0:1, :]
    scores = jnp.where(visible, dot_nt(k, q) * factor, 0.0)
    logits = carried * (split_nt(key_in, q) * factor)
    for level in range(levels):
        part = piece(decay, level)
        logits = logits + part * exact_nn(part * g, scores * covers[level])
    gap = apart[...]
    total = jnp.zeros_like(a)
    weights = []
    for by in range(SUB):
        if by:
            total = total + rolled(a, by - 1)
        weight = jnp.exp(total) * rolled(g, by)
        weights.append(weight)
        logits = logits + weight * jnp.sum(
            jnp.where(gap == by, scores, 0.0), axis=0, keepdims=True
        )
    attention = jnp.exp(logits - jnp.max(logits, axis=0, keepdims=True))
    attention = attention / jnp.sum(attention, axis=0, keepdims=True)
    attention_out[...] = attention
    logits_out[...] = logits
    mixing = jnp.zeros((CHUNK, CHUNK), F32)
    for level in range(levels):
        part = piece(decay, level)
        mixing = mixing + covers[level] * dot_tn(
            (part * g).astype(BF16), (part * attention).astype(BF16)
        )
    for by in range(SUB):
        row = jnp.sum(weights[by] * attention, axis=0, keepdims=True)
        mixing = jnp.where(gap == by, row, mixing)
    mixing = jnp.where(visible, mixing, 0.0).astype(BF16)
    output[...] = dot_tn(mixing, v) + dot_tn(
        (carried * attention).astype(BF16), value_in.astype(BF16)
    )
    ends = after * g * rows[2:3, :]
    keep = carried[:, CHUNK - 1 : CHUNK]
    key_state[...] = keep * key_in + split_nn(ends, k)
    value_state[...] = keep * value_in + split_nn(ends, v)


def mixer_backward_kernel(
    levels,
    factor,
    mine,
    query,
    key,
    value,
    grad_output,
    rate,
    inflow,
    rows,
    segment_col,
    sums,
    covers,
    apart,
    later,
    attention_in,
    logits_in,
    key_start,
    value_start,
    grad_query,
    grad_key,
    grad_value,
    grad_rate,
    key_grad,
    value_grad,
    flow,
):
    @pl.when(pl.program_id(0) == 0)
    def _():
        key_grad[...] = jnp.zeros_like(key_grad)
        value_grad[...] = jnp.zeros_like(value_grad)
        flow[...] = jnp.zeros_like(flow)

    key_in, value_in = key_start[0], value_start[0]
    key_after, value_after = key_grad[...], value_grad[...]
    q, k, v, d = query[...], key[...], value[...], grad_output[...]
    a, g = rate[...], inflow[...]
    attention, logits = attention_in[...], logits_in[...]
    decay = exponents(a, sums[...])
    before, after = piece(decay, levels), piece(decay, levels + 1)
    carried = before * rows[1:2, :]
    visible = segment_col[...] == rows[0:1, :]
    scores = jnp.where(visible, dot_nt(k, q) * factor, 0.0)
    reads = jnp.where(visible, dot_nt(v, d), 0.0)
    gap = apart[...]
    grad_att = carried * split_nt(value_in, d)
    for level in range(levels):
        part = piece(decay, level)
        grad_att = grad_att + part * exact_nn(part * g, reads * covers[level])
    total = jnp.zeros_like(a)
    bare, weights, score_rows, read_rows = [], [], [], []
    for by in range(SUB):
        if by:
            total = total + rolled(a, by - 1)
        bare.append(jnp.exp(total))
        weights.append(bare[by] * rolled(g, by))
        score_rows.append(jnp.sum(jnp.where(gap == by, scores, 0.0), axis=0, keepdims=True))
        read_rows.append(jnp.sum(jnp.where(gap == by, reads, 0.0), axis=0, keepdims=True))
        grad_att = grad_att + weights[by] * read_rows[by]
    grad_logits = attention * (
        grad_att - jnp.sum(attention * grad_att, axis=0, keepdims=True)
    )
    mixing = jnp.zeros((CHUNK, CHUNK), F32)
    spread = jnp.zeros((CHUNK, CHUNK), F32)
    ends = after * rows[2:3, :]
    grad_inflow = ends * (split_nt(key_after, k) + split_nt(value_after, v))
    for level in range(levels):
        part = piece(decay, level)
        left = (part * g).astype(BF16)
        att_part, log_part = part * attention, part * grad_logits
        mixing = mixing + covers[level] * dot_tn(left, att_part.astype(BF16))
        spread = spread + covers[level] * dot_tn(left, log_part.astype(BF16))
        grad_inflow = grad_inflow + part * (
            exact_nt(log_part, scores * covers[level]) + exact_nt(att_part, reads * covers[level])
        )
    for by in range(SUB):
        row = jnp.sum(weights[by] * attention, axis=0, keepdims=True)
        mixing = jnp.where(gap == by, row, mixing)
        row = jnp.sum(weights[by] * grad_logits, axis=0, keepdims=True)
        spread = jnp.where(gap == by, row, spread)
        terms = bare[by] * (grad_logits * score_rows[by] + attention * read_rows[by])
        grad_inflow = grad_inflow + rolled(terms, -by)
    mixing = jnp.where(visible, mixing, 0.0).astype(BF16)
    spread = (jnp.where(visible, spread, 0.0) * factor).astype(BF16)
    log_carried = carried * grad_logits * factor
    att_carried = carried * attention
    ends = (ends * g).astype(BF16)
    grad_query[...] = (
        dot_tn(spread, k) + dot_tn(log_carried.astype(BF16), key_in.astype(BF16))
    ).astype(BF16)
    grad_key[...] = (dot_nn(spread, q) + dot_tn(ends, key_after.astype(BF16))).astype(BF16)
    grad_value[...] = (dot_nn(mixing, d) + dot_tn(ends, value_after.astype(BF16))).astype(BF16)
    change = grad_logits * logits + attention * grad_att - g * grad_inflow
    same = jnp.where(visible, later[...], 0.0)
    flows = exact_nn(change, same) + rows[2:3, :] * flow[:, 0:1]
    grad_rate[...] = rows[3:4, :] * flows - jnp.exp(a) * grad_inflow
    keep = carried[:, CHUNK - 1 : CHUNK]
    key_before = keep * key_after + split_nn(log_carried, q)
    value_before = keep * value_after + split_nn(att_carried, d)
    key_grad[...] = key_before
    value_grad[...] = value_before
    flow[...] = jnp.broadcast_to(
        jnp.sum(key_before * key_in + value_before * value_in, axis=1, keepdims=True), flow.shape
    )


def mixer_specs(length, size, ring, backward):
    count = length // CHUNK
    per = count // ring

    def natural(step):
        return count - 1 - step if backward else step

    def moved(step, mine):
        at = natural(step)
        return lax.bitwise_xor(at // per, mine[0]) * per + at % per

    wide = pl.BlockSpec((CHUNK, size), lambda step, mine: (moved(step, mine), 0))
    slim = pl.BlockSpec((SLOTS, CHUNK), lambda step, mine: (0, moved(step, mine)))
    plain = pl.BlockSpec((SLOTS, CHUNK), lambda step, mine: (0, natural(step)))
    rows = pl.BlockSpec((8, CHUNK), lambda step, mine: (0, natural(step)))
    column = pl.BlockSpec((CHUNK, 1), lambda step, mine: (natural(step), 0))
    state = pl.BlockSpec((1, SLOTS, size), lambda step, mine: (natural(step), 0, 0))
    return count, wide, slim, plain, rows, column, state


def whole(array):
    rank = array.ndim
    return pl.BlockSpec(array.shape, lambda step, mine: (0,) * rank)


def mixer_forward(mine, ring, query, key, value, rate, inflow, rows, column):
    length, size = query.shape
    sums, covers, apart = (jnp.asarray(table) for table in chunk_tables())
    count, wide, slim, plain, row_spec, col_spec, state = mixer_specs(length, size, ring, False)
    kernel = functools.partial(mixer_forward_kernel, covers.shape[0], size ** (-0.25))
    return pl.pallas_call(
        kernel,
        out_shape=(
            jax.ShapeDtypeStruct((length, size), F32),
            jax.ShapeDtypeStruct((SLOTS, length), F32),
            jax.ShapeDtypeStruct((SLOTS, length), F32),
            jax.ShapeDtypeStruct((count, SLOTS, size), F32),
            jax.ShapeDtypeStruct((count, SLOTS, size), F32),
        ),
        grid_spec=pltpu.PrefetchScalarGridSpec(
            num_scalar_prefetch=1,
            grid=(count,),
            in_specs=[
                wide, wide, wide, slim, slim, row_spec, col_spec,
                whole(sums), whole(covers), whole(apart),
            ],
            out_specs=[wide, plain, plain, state, state],
            scratch_shapes=[pltpu.VMEM((SLOTS, size), F32)] * 2,
        ),
        compiler_params=pltpu.CompilerParams(vmem_limit_bytes=32 << 20),
        cost_estimate=pl.CostEstimate(
            flops=length * size * 2000, bytes_accessed=length * size * 12, transcendentals=length * 4096
        ),
        name="mixer_forward",
    )(mine, query, key, value, rate, inflow, rows, column, sums, covers, apart)


def mixer_backward(
    mine, ring, query, key, value, grad, rate, inflow, rows, column, attention, logits, starts
):
    length, size = query.shape
    sums, covers, apart = (jnp.asarray(table) for table in chunk_tables())
    later = jnp.asarray(np.tril(np.ones((CHUNK, CHUNK), np.float32)))
    count, wide, slim, plain, row_spec, col_spec, state = mixer_specs(length, size, ring, True)
    kernel = functools.partial(mixer_backward_kernel, covers.shape[0], size ** (-0.25))
    return pl.pallas_call(
        kernel,
        out_shape=(
            jax.ShapeDtypeStruct((length, size), BF16),
            jax.ShapeDtypeStruct((length, size), BF16),
            jax.ShapeDtypeStruct((length, size), BF16),
            jax.ShapeDtypeStruct((SLOTS, length), F32),
        ),
        grid_spec=pltpu.PrefetchScalarGridSpec(
            num_scalar_prefetch=1,
            grid=(count,),
            in_specs=[
                wide, wide, wide, wide, slim, slim, row_spec, col_spec,
                whole(sums), whole(covers), whole(apart), whole(later),
                plain, plain, state, state,
            ],
            out_specs=[wide, wide, wide, slim],
            scratch_shapes=[pltpu.VMEM((SLOTS, size), F32)] * 2 + [pltpu.VMEM((SLOTS, 128), F32)],
        ),
        compiler_params=pltpu.CompilerParams(vmem_limit_bytes=32 << 20),
        cost_estimate=pl.CostEstimate(
            flops=length * size * 4000, bytes_accessed=length * size * 20, transcendentals=length * 4096
        ),
        name="mixer_backward",
    )(
        mine, query, key, value, grad, rate, inflow, rows, column,
        sums, covers, apart, later, attention, logits, *starts,
    )


def peers(ring, mine):
    found = []
    for by in range(1, ring):
        at, bit = mine, 1
        while bit <= by:
            if by & bit:
                at = at + bit * (1 - 2 * ((at // bit) % 2))
            bit *= 2
        found.append(at)
    return found


class Copies:
    def __init__(self, local, send, recv):
        self.local, self.send, self.recv = local, send, recv
        self.here, self.away = 0, 0
        self.open = []

    def near(self, source, target):
        copy = pltpu.make_async_copy(source, target, self.local.at[self.here])
        self.here += 1
        copy.start()
        return copy

    def far(self, source, target, landed, device, when=None):
        at = self.away
        self.away += 1
        copy = pltpu.make_async_remote_copy(
            source, target, self.send.at[at], self.recv.at[at], device_id=device,
            device_id_type=pl.DeviceIdType.MESH,
        )
        if when is None:
            copy.start()
        else:
            pl.when(when)(copy.start)
        self.open.append((copy, when))
        return pltpu.make_async_remote_copy(
            landed, landed, self.send.at[at], self.recv.at[at], device_id=device,
            device_id_type=pl.DeviceIdType.MESH,
        ).wait_recv

    def close(self):
        for copy, when in self.open:
            if when is None:
                copy.wait_send()
            else:
                pl.when(when)(copy.wait_send)


def slab_chain(copies, chips, place):
    mine, batch = lax.axis_index("seq"), lax.axis_index("batch")
    chip, core = batch // 2, batch % 2
    other = (mine, chip * 2 + (1 - core))

    def at(where):
        return jnp.clip(where, 0, chips - 1) * 2 + core

    def send(step, way):
        block, come = chip - way * (step - 1), chip - way * step
        when = (block >= 0) & (block < chips) & (chip + way >= 0) & (chip + way < chips)
        came = (come >= 0) & (come < chips)
        wait = copies.far(
            place(at(block)), place(at(block)), place(at(come)), (mine, at(chip + way)), when
        )
        return wait, came, at(come)

    crossing = [(copies.far(place(batch), place(batch), place(other[1]), other), None)]
    flying = [send(1, 1), send(1, -1)] if chips > 1 else []
    yield
    for step in range(1, chips):
        coming = []
        for way, (wait, came, landed) in zip((1, -1), flying):
            pl.when(came)(wait)
            if step + 1 < chips:
                coming.append(send(step + 1, way))
            there = landed + 1 - 2 * core
            crossing.append(
                (copies.far(place(landed), place(landed), place(there), other, came), came)
            )
        flying = coming
        yield
    for wait, came in crossing:
        if came is None:
            wait()
        else:
            pl.when(came)(wait)
    yield


def start_kernel(
    ring, lines, inputs, w_query, w_key, w_value, w_swish, w_out, gate, up, small,
    inputs_all, w_mixer, swish_columns, out_rows, feed_columns, small_all,
    local_sem, send_sem, recv_sem,
):
    mine, batch = lax.axis_index("seq"), lax.axis_index("batch")
    chips = lines // 2
    copies = Copies(local_sem, send_sem, recv_sem)
    part = swish_columns.shape[2]
    half = inputs.shape[0] // 2
    others = peers(ring, mine)
    pieces = (w_query, w_key, w_value)

    def column(ref, at):
        if len(ref.shape) == 3:
            return ref.at[at]
        size = ref.shape[1] // ring
        return ref.at[:, pl.ds(pl.multiple_of(at * size, 128), size)]

    def slot(source, piece):
        return w_mixer.at[source, batch, :, pl.ds(piece * part, part)]

    near = [copies.near(column(ref, mine), slot(mine, at)) for at, ref in enumerate(pieces)]
    near += [copies.near(small, small_all.at[mine, batch])]
    column_waits, small_waits = [], []
    for to in others:
        column_waits.append(
            [
                copies.far(column(ref, to), slot(mine, at), slot(to, at), (to, batch))
                for at, ref in enumerate(pieces)
            ]
        )
        small_waits.append(
            copies.far(small, small_all.at[mine, batch], small_all.at[to, batch], (to, batch))
        )
    direct = 2 if ring == 4 else ring - 1

    def sent(block, blocks):
        return copies.near(block, blocks.at[0]), [
            copies.far(block, blocks.at[by + 1], blocks.at[by + 1], (others[by], batch))
            for by in range(direct)
        ]

    def passed_on(blocks, waits):
        for wait in waits:
            wait()
        if ring != 4:
            return []
        low, high = pl.ds(0, half), pl.ds(half, half)
        return [
            copies.far(blocks.at[have, rows], blocks.at[3, rows], blocks.at[3, rows], (to, batch))
            for have, rows, to in ((2, low, others[0]), (1, high, others[1]))
        ]

    own_input, input_waits = sent(inputs, inputs_all)
    for copy in near:
        copy.wait()

    def started(place):
        chain = slab_chain(copies, chips, place)
        next(chain)
        chains.append(chain)

    chains = []
    started(lambda at: w_mixer.at[mine, at])
    for waits, source in zip(column_waits, others):
        for wait in waits:
            wait()
        started(lambda at, source=source: w_mixer.at[source, at])
    for wait, source in zip(small_waits, others):
        wait()
        started(lambda at, source=source: small_all.at[source, at])
    started(lambda at: small_all.at[mine, at])
    input_waits = passed_on(inputs_all, input_waits)
    own_columns = [
        copies.near(column(w_swish, mine), swish_columns.at[mine]),
        copies.near(w_out, out_rows),
    ]
    own_columns += [
        copies.near(column(ref, mine), feed_columns.at[at, mine]) for at, ref in enumerate((gate, up))
    ]
    other_waits = [
        copies.far(column(w_swish, to), swish_columns.at[mine], swish_columns.at[to], (to, batch))
        for to in others
    ]
    other_waits += [
        copies.far(
            column(ref, to), feed_columns.at[at, mine], feed_columns.at[at, to], (to, batch)
        )
        for to in others
        for at, ref in enumerate((gate, up))
    ]
    for step in range(1, chips + 1):
        for chain in chains:
            if chips > 1 or step > 1:
                next(chain)
    if chips == 1:
        for chain in chains:
            next(chain)
    for wait in input_waits + other_waits:
        wait()
    for copy in [own_input] + own_columns:
        copy.wait()
    copies.close()


def start(ring, lines, inputs, columns, w_out, gate, up, small):
    own, width = columns[0].shape
    part, hidden = width // ring, gate.shape[1] // ring
    if hidden % 128:
        gate, up = (a.reshape(own, ring, hidden).transpose(1, 0, 2) for a in (gate, up))
    inside, anywhere = (pl.BlockSpec(memory_space=space) for space in (pltpu.VMEM, pl.ANY))
    chains = 2 * ring
    away = (ring - 1) * 9 + 2 + chains * (4 * (lines // 2 - 1) + 1)
    return pl.pallas_call(
        functools.partial(start_kernel, ring, lines),
        out_shape=(
            jax.ShapeDtypeStruct((ring,) + inputs.shape, BF16),
            jax.ShapeDtypeStruct((ring, lines, own, 3 * part), BF16),
            jax.ShapeDtypeStruct((ring, own, part), BF16),
            jax.ShapeDtypeStruct(w_out.shape, BF16),
            jax.ShapeDtypeStruct((2, ring, own, hidden), BF16),
            jax.ShapeDtypeStruct((ring, lines) + small.shape, BF16),
        ),
        in_specs=[inside] * 4 + [anywhere] * 4 + [inside],
        out_specs=[anywhere] * 6,
        scratch_shapes=[
            pltpu.SemaphoreType.DMA((12,)),
            pltpu.SemaphoreType.DMA((away,)),
            pltpu.SemaphoreType.DMA((away,)),
        ],
        compiler_params=pltpu.CompilerParams(has_side_effects=True, vmem_limit_bytes=32 << 20),
        name="start",
    )(inputs, *columns, w_out, gate, up, small)


PARTS = 4


def fold_kernel(finish, extras, *refs):
    terms, given = refs[0], refs[1 : 1 + extras]
    blocks = refs[1 + extras]
    made = refs[2 + extras : -9]
    first, second, third, two_low, one_high, own, local_sem, send_sem, recv_sem = refs[-9:]
    mine, batch = lax.axis_index("seq"), lax.axis_index("batch")
    others = peers(4, mine)
    row, col = (others[0], batch), (others[1], batch)
    copies = Copies(local_sem, send_sem, recv_sem)
    size = terms.shape[1] // PARTS

    def span(at):
        low = pl.ds(at * size, size // 2)
        return pl.ds(at * size, size), low, pl.ds(at * size + size // 2, size // 2)

    opening, direct = [], []

    def open_part(at):
        _, low, high = span(at)
        opening.append(
            (
                copies.far(terms.at[3, low], first.at[low], first.at[low], row),
                copies.far(terms.at[3, high], first.at[high], first.at[high], col),
            )
        )

    def pass_part(at):
        _, low, high = span(at)
        waits = [
            copies.far(terms.at[2, high], second.at[high], second.at[high], col),
            copies.far(terms.at[1, low], third.at[low], third.at[low], row),
        ]
        opening[at][0]()
        two_low[low, :] = added(terms[2, low, :], first[low, :])
        waits.append(copies.far(two_low.at[low], second.at[low], second.at[low], col))
        opening[at][1]()
        one_high[high, :] = added(terms[1, high, :], first[high, :])
        waits.append(copies.far(one_high.at[high], third.at[high], third.at[high], row))
        direct.append(waits)

    spread, local, passed = [], [], []

    def close_part(at):
        full, _, _ = span(at)
        for wait in direct[at]:
            wait()
        total = terms[0, full, :].astype(F32) + second[full, :].astype(F32) + third[full, :].astype(F32)
        own[full, :] = finish(total, full, at, given, made)
        spread.append(
            (
                copies.far(own.at[full], blocks.at[1, full], blocks.at[1, full], row),
                copies.far(own.at[full], blocks.at[2, full], blocks.at[2, full], col),
            )
        )
        local.append(copies.near(own.at[full], blocks.at[0, full]))

    def forward_part(at):
        _, low, high = span(at)
        for wait in spread[at]:
            wait()
        passed.append(copies.far(blocks.at[2, low], blocks.at[3, low], blocks.at[3, low], row))
        passed.append(copies.far(blocks.at[1, high], blocks.at[3, high], blocks.at[3, high], col))

    open_part(0)
    for at in range(PARTS + 2):
        if at + 1 < PARTS:
            open_part(at + 1)
        if at < PARTS:
            pass_part(at)
        if 1 <= at <= PARTS:
            close_part(at - 1)
        if at >= 2:
            forward_part(at - 2)
    for wait in passed:
        wait()
    for copy in local:
        copy.wait()
    copies.close()


def finish_forward(total, full, at, given, made):
    inputs, gain = given
    hidden = inputs[full, :].astype(F32) + total
    made[0][full, :] = hidden
    return (hidden * rms_scale(hidden) * gain[...]).astype(BF16)


def finish_backward(total, full, at, given, made):
    cotangent, hidden_ref, gain = given
    hidden = hidden_ref[full, :]
    scale = rms_scale(hidden)
    plain = hidden * scale
    term = jnp.sum(total * plain, axis=0, keepdims=True)
    made[1][...] = term if at == 0 else made[1][...] + term
    scaled = total * gain[...]
    grad = (
        cotangent[full, :].astype(F32)
        + scale * scaled
        - plain * (scale * jnp.mean(scaled * plain, axis=-1, keepdims=True))
    )
    made[0][full, :] = grad
    return grad.astype(BF16)


def finish_kernel(
    lines, mixer_terms, out_terms, input_terms, feed_sum, small_terms, inputs, gain, grad_hidden,
    grad_query, grad_key, grad_value, grad_swish, grad_out, grad_gate, grad_up, grad_input, small_sum,
    crossed, staged, arrived, summed, outgoing, mixer_blocks, feed_blocks, small_ring, small_mine, small_line,
    first, second, third, two_low, one_high, local_sem, send_sem, recv_sem,
):
    mine, batch = lax.axis_index("seq"), lax.axis_index("batch")
    chips = lines // 2
    chip, core = batch // 2, batch % 2
    sibling = chip * 2 + (1 - core)
    others = peers(4, mine)
    row, col = (others[0], batch), (others[1], batch)
    copies = Copies(local_sem, send_sem, recv_sem)
    slabs = others + [mine, None]

    def term(slab, owner):
        return out_terms.at[owner] if slabs[slab] is None else mixer_terms.at[slabs[slab], owner]

    cross_waits = {}
    for slab in range(len(slabs)):
        for owner in range(chips):
            cross_waits[slab, owner] = copies.far(
                term(slab, owner * 2 + (1 - core)),
                crossed.at[slab, owner],
                crossed.at[slab, owner],
                (mine, sibling),
            )
    small_waits = [
        copies.far(small_terms.at[to], small_ring.at[at], small_ring.at[at], (to, batch))
        for at, to in enumerate(others)
    ]
    feed_waits = [
        copies.far(feed_sum.at[:, to], feed_blocks.at[mine], feed_blocks.at[to], (to, batch))
        for to in others
    ]

    size = input_terms.shape[1] // PARTS
    opening, direct = [], []

    def span(at):
        low = pl.ds(at * size, size // 2)
        return pl.ds(at * size, size), low, pl.ds(at * size + size // 2, size // 2)

    def open_part(at):
        _, low, high = span(at)
        opening.append(
            (
                copies.far(input_terms.at[3, low], first.at[low], first.at[low], row),
                copies.far(input_terms.at[3, high], first.at[high], first.at[high], col),
            )
        )

    def pass_part(at):
        _, low, high = span(at)
        waits = [
            copies.far(input_terms.at[2, high], second.at[high], second.at[high], col),
            copies.far(input_terms.at[1, low], third.at[low], third.at[low], row),
        ]
        opening[at][0]()
        two_low[low, :] = added(input_terms[2, low, :], first[low, :])
        waits.append(copies.far(two_low.at[low], second.at[low], second.at[low], col))
        opening[at][1]()
        one_high[high, :] = added(input_terms[1, high, :], first[high, :])
        waits.append(copies.far(one_high.at[high], third.at[high], third.at[high], row))
        direct.append(waits)

    def close_part(at):
        full, _, _ = span(at)
        for wait in direct[at]:
            wait()
        total = (
            input_terms[0, full, :].astype(F32)
            + second[full, :].astype(F32)
            + third[full, :].astype(F32)
        )
        features = inputs[full, :].astype(F32)
        scale = rms_scale(features)
        plain = features * scale
        scaled = total * gain[...]
        grad = (
            grad_hidden[full, :]
            + scale * scaled
            - plain * (scale * jnp.mean(scaled * plain, axis=-1, keepdims=True))
        )
        grad_input[full, :] = grad.astype(BF16)

    def small_part():
        for wait in small_waits:
            wait()
        small_mine[...] = small_terms[mine] + small_ring[0] + small_ring[1] + small_ring[2]
        for by in range(1, lines):
            to, source = (batch + by) % lines, (batch + lines - by) % lines
            small_waits.append(
                copies.far(small_mine.at[to], small_line.at[by], small_line.at[by], (mine, to))
            )

    def feed_part():
        for wait in feed_waits:
            wait()
        feed_blocks[mine] = feed_sum[:, mine]
        wide = feed_sum.shape[3]
        for source in range(4):
            at = pl.ds(source * wide, wide)
            grad_gate[:, at] = feed_blocks[source, 0].astype(F32)
            grad_up[:, at] = feed_blocks[source, 1].astype(F32)

    beside = [functools.partial(open_part, 1)]
    for at in range(PARTS):
        if at + 2 <= PARTS - 1:
            beside.append(functools.partial(open_part, at + 2))
        beside.append(functools.partial(pass_part, at))
        if at == 0:
            beside.append(small_part)
        if at:
            beside.append(functools.partial(close_part, at - 1))
    beside.append(functools.partial(close_part, PARTS - 1))
    beside.append(feed_part)
    open_part(0)

    def both_cores(slab, owner):
        return term(slab, owner * 2 + core)[...].astype(F32) + crossed[slab, owner].astype(F32)

    crossed_in = set()

    def wait_cross(slab):
        if slab not in crossed_in:
            crossed_in.add(slab)
            for owner in range(chips):
                cross_waits[slab, owner]()

    flying = {}
    for far in range(chips - 1, 0, -1):
        for slab in range(len(slabs)):
            wait_cross(slab)
            for side, way in enumerate((1, -1)):
                owner = chip + way * far
                sends = (owner >= 0) & (owner < chips)
                held = jnp.clip(owner, 0, chips - 1)
                before = chip - way
                gets = sends & (before >= 0) & (before < chips)
                here = staged.at[side, far - 1, slab]
                if far < chips - 1:
                    wait = flying[side, far + 1, slab]

                    @pl.when(gets)
                    def _(wait=wait, slab=slab, held=held, here=here, side=side, far=far):
                        wait()
                        here[...] = (
                            both_cores(slab, held) + arrived[side, far, slab].astype(F32)
                        ).astype(BF16)

                    @pl.when(sends & jnp.logical_not((before >= 0) & (before < chips)))
                    def _(slab=slab, held=held, here=here):
                        here[...] = both_cores(slab, held).astype(BF16)
                else:

                    @pl.when(sends)
                    def _(slab=slab, held=held, here=here):
                        here[...] = both_cores(slab, held).astype(BF16)

                target = jnp.clip(chip + way, 0, chips - 1) * 2 + core
                flying[side, far, slab] = copies.far(
                    here,
                    arrived.at[side, far - 1, slab],
                    arrived.at[side, far - 1, slab],
                    (mine, target),
                    sends,
                )
            if beside:
                beside.pop(0)()
    ring_waits = []
    for slab in range(len(slabs)):
        total = summed.at[slab]
        total[...] = both_cores(slab, chip)
        for side, way in enumerate((1, -1)):
            before = chip - way
            wait = flying[side, 1, slab]

            @pl.when((before >= 0) & (before < chips))
            def _(wait=wait, total=total, slab=slab, side=side):
                wait()
                total[...] += arrived[side, 0, slab].astype(F32)

        if slabs[slab] is None:
            grad_out[...] = total[...]
        elif slab == len(others):
            mixer_blocks[mine] = total[...].astype(BF16)
        else:
            outgoing[slab] = total[...].astype(BF16)
            to = slabs[slab]
            ring_waits.append(
                copies.far(
                    outgoing.at[slab], mixer_blocks.at[mine], mixer_blocks.at[to], (to, batch)
                )
            )
        if beside:
            beside.pop(0)()
    for piece in beside:
        piece()
    for wait in small_waits[3:]:
        wait()
    total = small_mine[batch]
    for by in range(1, lines):
        total = total + small_line[by]
    small_sum[...] = total
    for wait in ring_waits:
        wait()
    part = grad_query.shape[1] // 4
    for source in range(4):
        at = pl.ds(source * part, part)
        for piece, out in enumerate((grad_query, grad_key, grad_value, grad_swish)):
            out[:, at] = mixer_blocks[source, :, piece * part : (piece + 1) * part].astype(F32)
    copies.close()


def finish(lines, mixer_terms, out_terms, input_terms, feed_sum, small_terms, inputs, gain, grad_hidden):
    ring, _, own, width = mixer_terms.shape
    rows, hidden = inputs.shape[0], feed_sum.shape[3]
    chips = lines // 2
    inside = pl.BlockSpec(memory_space=pltpu.VMEM)
    block = pltpu.VMEM((rows, width), BF16)
    small = small_terms.shape[2:]
    away = (ring + 1) * (chips + 2 * (chips - 1)) + 3 * (ring - 1) + PARTS * 6 + lines - 1
    square = jax.ShapeDtypeStruct((own, width), F32)
    wide = jax.ShapeDtypeStruct((own, ring * hidden), F32)
    return pl.pallas_call(
        functools.partial(finish_kernel, lines),
        out_shape=(square,) * 5
        + (wide,) * 2
        + (jax.ShapeDtypeStruct((rows, width), BF16), jax.ShapeDtypeStruct(small, F32)),
        in_specs=[inside] * 8,
        out_specs=[inside] * 9,
        scratch_shapes=[
            pltpu.VMEM((ring + 1, chips, own, width), BF16),
            pltpu.VMEM((2, chips - 1, ring + 1, own, width), BF16),
            pltpu.VMEM((2, chips - 1, ring + 1, own, width), BF16),
            pltpu.VMEM((ring + 1, own, width), F32),
            pltpu.VMEM((ring - 1, own, width), BF16),
            pltpu.VMEM((ring, own, width), BF16),
            pltpu.VMEM((ring, 2, own, hidden), BF16),
            pltpu.VMEM((ring - 1, lines) + small, F32),
            pltpu.VMEM((lines,) + small, F32),
            pltpu.VMEM((lines,) + small, F32),
        ]
        + [block] * 5
        + [
            pltpu.SemaphoreType.DMA((1,)),
            pltpu.SemaphoreType.DMA((away,)),
            pltpu.SemaphoreType.DMA((away,)),
        ],
        compiler_params=pltpu.CompilerParams(has_side_effects=True, vmem_limit_bytes=58 << 20),
        name="finish",
    )(mixer_terms, out_terms, input_terms, feed_sum, small_terms, inputs, gain, grad_hidden)


def fold(finish, terms, given, made, name):
    ring, rows, width = terms.shape
    inside = pl.BlockSpec(memory_space=pltpu.VMEM)
    block = pltpu.VMEM((rows, width), BF16)
    return pl.pallas_call(
        functools.partial(fold_kernel, finish, len(given)),
        out_shape=(jax.ShapeDtypeStruct((ring, rows, width), BF16),) + made,
        in_specs=[inside] * (1 + len(given)),
        out_specs=[pl.BlockSpec(memory_space=pl.ANY)] + [inside] * len(made),
        scratch_shapes=[block] * 6
        + [
            pltpu.SemaphoreType.DMA((PARTS,)),
            pltpu.SemaphoreType.DMA((PARTS * 10,)),
            pltpu.SemaphoreType.DMA((PARTS * 10,)),
        ],
        compiler_params=pltpu.CompilerParams(has_side_effects=True, vmem_limit_bytes=40 << 20),
        name=name,
    )(terms, *given)


def rms_scale(features):
    return lax.rsqrt(jnp.mean(features * features, axis=-1, keepdims=True) + EPS)


def swapped(block, by, ring):
    return lax.ppermute(block, "seq", [(i, i ^ by) for i in range(ring)])


def gathered(block, ring):
    if ring != 4:
        return jnp.concatenate([block] + [swapped(block, by, ring) for by in range(1, ring)], axis=0)
    half = block.shape[0] // 2
    one, two = swapped(block, 1, ring), swapped(block, 2, ring)
    low, high = swapped(two[:half], 1, ring), swapped(one[half:], 2, ring)
    return jnp.concatenate([block, one, two, low, high], axis=0)


def scattered(terms, ring):
    rows = terms.shape[0] // ring
    parts = [terms[by * rows : (by + 1) * rows] for by in range(ring)]
    total = parts[0].astype(F32)
    if ring != 4:
        for by in range(1, ring):
            total = total + swapped(parts[by], by, ring).astype(F32)
        return total
    half = rows // 2
    low, high = swapped(parts[3][:half], 1, ring), swapped(parts[3][half:], 2, ring)
    two = jnp.concatenate([added(parts[2][:half], low), parts[2][half:]], axis=0)
    one = jnp.concatenate([parts[1][:half], added(parts[1][half:], high)], axis=0)
    return total + swapped(one, 1, ring).astype(F32) + swapped(two, 2, ring).astype(F32)


def added(left, right):
    return (left.astype(F32) + right.astype(F32)).astype(BF16)


def flipped(block, axis, by):
    return lax.ppermute(block, axis, [(i, i ^ by) for i in range(lax.axis_size(axis))])


def doubled(block, axis):
    by, mine = 1, lax.axis_index(axis)
    while by < lax.axis_size(axis):
        other = flipped(block, axis, by)
        first = (mine & by) == 0
        block = jnp.concatenate(
            [jnp.where(first, block, other), jnp.where(first, other, block)], axis=0
        )
        by *= 2
    return block


def halved(block, axis):
    by, mine = lax.axis_size(axis) // 2, lax.axis_index(axis)
    while by:
        low, high = jnp.split(block, 2, axis=0)
        first = (mine & by) == 0
        block = jnp.where(first, low, high) + flipped(jnp.where(first, high, low), axis, by)
        by //= 2
    return block


def after(value, *others):
    return lax.optimization_barrier((value,) + others)[0]


def exchanged(blocks, mine, ring):
    parts = [
        swapped(lax.dynamic_index_in_dim(blocks, mine ^ by, 0, keepdims=False), by, ring)
        if by
        else lax.dynamic_index_in_dim(blocks, mine, 0, keepdims=False)
        for by in range(ring)
    ]
    made = jnp.stack(parts)
    return jnp.concatenate(
        [lax.dynamic_index_in_dim(made, mine ^ j, 0, keepdims=True) for j in range(ring)], axis=0
    )


def local(
    layer_input,
    segments,
    mixer_gain,
    query_weight,
    key_weight,
    value_weight,
    squeeze,
    expand,
    forget_bias,
    swish_weight,
    head_gain,
    output_weight,
    feed_gain,
    gate_weight,
    up_weight,
    down_weight,
    cotangent,
):
    ring, lines = lax.axis_size("seq"), lax.axis_size("batch")
    devices = ring * lines
    mine = lax.axis_index("seq")
    rows, width = layer_input.shape[1], layer_input.shape[2]
    length = rows * ring
    own = width // devices
    head_size = width // HEADS
    copies = ring // HEADS
    part = width // ring
    head = mine // copies
    hidden_part = gate_weight.shape[1] // ring
    slots_all = HEADS * SLOTS

    def to_order(array):
        if copies == 1:
            return array
        blocks = array.reshape((ring, rows) + array.shape[1:])
        moved = [lax.dynamic_index_in_dim(blocks, mine ^ by, 0, keepdims=False) for by in range(ring)]
        return jnp.concatenate(moved, axis=0)

    def whole_head(array):
        if copies == 1:
            return array
        full = lax.all_gather(to_order(array), "seq", axis=1, tiled=True)
        return to_order(lax.dynamic_slice_in_dim(full, head * head_size, head_size, 1))

    def own_part(array):
        if copies == 1:
            return array
        return lax.dynamic_slice_in_dim(array, (mine % copies) * part, part, 1)

    params = jnp.concatenate(
        [
            mixer_gain,
            head_gain,
            feed_gain,
            forget_bias,
            expand.T.reshape(-1),
            squeeze.reshape(-1),
        ]
    )
    count = params.shape[0]
    params = jnp.concatenate([params, segments.reshape(rows).astype(BF16)])
    params = jnp.pad(params, (0, -params.shape[0] % 2048)).reshape(-1, 128)
    input_own = layer_input.reshape(rows, width)
    grad_own = cotangent.reshape(rows, width)
    inputs, w_mixer, swish_columns, out_rows, feed_columns, small = start(
        ring,
        lines,
        input_own,
        (query_weight, key_weight, value_weight, swish_weight),
        output_weight,
        gate_weight,
        up_weight,
        params,
    )
    inputs = inputs.reshape(length, width)
    grad_out = gathered(after(grad_own, inputs), ring)
    w_mixer = w_mixer.reshape(width, 3 * part)
    small = small.reshape(devices, -1)
    segment = lax.dynamic_index_in_dim(
        small.reshape(ring, lines, -1), lax.axis_index("batch"), 1, keepdims=False
    )[:, count : count + rows].reshape(length).astype(F32)
    cuts = np.cumsum([own, own, own, slots_all // devices, RANK * slots_all // devices])
    gain_one, gain_head, gain_two, bias_full, expand_t, w_squeeze = jnp.split(
        small[:, :count], cuts, axis=1
    )
    gain_one = gain_one.reshape(width).astype(F32)
    gain_head = lax.dynamic_slice_in_dim(gain_head.reshape(width), head * head_size, head_size, 0)
    gain_head = gain_head.astype(F32)
    gain_two = gain_two.reshape(width).astype(F32)
    bias_head = lax.dynamic_slice_in_dim(bias_full.reshape(slots_all), head * SLOTS, SLOTS, 0)
    expand_head = lax.dynamic_slice_in_dim(
        expand_t.reshape(slots_all, RANK), head * SLOTS, SLOTS, 0
    )
    w_squeeze = w_squeeze.reshape(width, RANK).T

    def over_batch(blocks):
        kinds, columns = blocks.shape[0], blocks.shape[-1]
        full = lax.all_gather(blocks.reshape(-1, columns), "batch", axis=0, tiled=False)
        full = full.reshape(lines, kinds, ring, own, columns)
        return full.transpose(1, 2, 0, 3, 4).reshape(kinds, width, columns)

    w_swish = over_batch(swish_columns[None])[0]
    w_output = lax.all_gather(out_rows, "batch", axis=0, tiled=True)
    w_gate, w_up = over_batch(feed_columns)
    w_down = lax.all_gather(after(down_weight, feed_columns), "batch", axis=0, tiled=True)

    chunked = segment.reshape(-1, CHUNK)
    before = jnp.concatenate([jnp.full((1,), -1.0, F32), chunked[:-1, -1]])
    previous = jnp.concatenate([jnp.full((1,), -1.0, F32), segment[:-1]])
    mask_rows = jnp.stack(
        [
            segment,
            (chunked == before[:, None]).astype(F32).reshape(-1),
            (chunked == chunked[:, -1:]).astype(F32).reshape(-1),
            (segment == previous).astype(F32),
        ]
        + [jnp.zeros_like(segment)] * 4
    )
    segment_col = segment[:, None]

    inputs = inputs.astype(F32)
    scale_one = rms_scale(inputs)
    plain_one = inputs * scale_one
    normed = (plain_one * gain_one).astype(BF16)
    mixer_pre = dot_nn(normed, w_mixer)
    query = whole_head(mixer_pre[:, :part].astype(BF16))
    key = whole_head(mixer_pre[:, part : 2 * part].astype(BF16))
    value = whole_head(mixer_pre[:, 2 * part : 3 * part].astype(BF16))
    swish_pre = whole_head(dot_nn(normed, w_swish))
    reduced = dot_nt(normed, w_squeeze).astype(BF16)
    forget_logit = dot_nt(expand_head, reduced) + bias_head.astype(F32)[:, None]
    log_rate = jax.nn.log_sigmoid(forget_logit) / TAU_GATE
    inflow = -jnp.expm1(log_rate)
    order = mine.reshape(1).astype(jnp.int32)
    query, grad_out = lax.optimization_barrier((query, grad_out))
    mixed, attention, logits, key_start, value_start = mixer_forward(
        order, ring, query, key, value, log_rate, inflow, mask_rows, segment_col
    )
    head_factor = rms_scale(mixed)
    head_plain = mixed * head_factor
    head_normed = head_plain * gain_head
    swish_sig = jax.nn.sigmoid(swish_pre)
    swish_act = swish_pre * swish_sig
    gated = own_part((head_normed * swish_act).astype(BF16))
    terms = dot_nn(gated, w_output).astype(BF16)
    if ring == 4:
        feed_in, hidden = fold(
            finish_forward,
            terms.reshape(ring, rows, width),
            (input_own, gain_two[None]),
            (jax.ShapeDtypeStruct((rows, width), F32),),
            "fold_forward",
        )
        feed_in = feed_in.reshape(length, width)
    else:
        hidden = input_own.astype(F32) + scattered(terms, ring)
        feed_in = gathered((hidden * rms_scale(hidden) * gain_two).astype(BF16), ring)

    gate_pre, up_pre = dot_nn(feed_in, w_gate), dot_nn(feed_in, w_up)
    gate_sig = jax.nn.sigmoid(gate_pre)
    gate_act = gate_pre * gate_sig
    inner = (gate_act * up_pre).astype(BF16)

    term_down = dot_tn(inner, grad_out).astype(BF16)
    grad_inner = dot_nt(after(grad_out, term_down), w_down)
    grad_gatepre = grad_inner * up_pre * (gate_sig * (1.0 + gate_pre * (1.0 - gate_sig)))
    grad_gatepre = grad_gatepre.astype(BF16)
    grad_uppre = (grad_inner * gate_act).astype(BF16)
    back_feedin = (dot_nt(grad_gatepre, w_gate) + dot_nt(grad_uppre, w_up)).astype(BF16)
    feed_rows = after(feed_in, back_feedin)
    term_gate = dot_tn(feed_rows, grad_gatepre).astype(BF16)
    term_up = dot_tn(feed_rows, grad_uppre).astype(BF16)
    result_terms = dot_nn(inner, w_down).astype(BF16)
    result = hidden + scattered(result_terms, ring)
    layer_output = result.astype(BF16).reshape(1, rows, width)
    down_share = lax.psum_scatter(term_down, "batch", scatter_dimension=0, tiled=True)
    term_feedpre = jnp.stack([term_gate, term_up]).reshape(2, ring, lines, own, hidden_part)
    term_feedpre = term_feedpre.transpose(2, 0, 1, 3, 4).reshape(-1, hidden_part)
    feed_sum = lax.psum_scatter(
        after(term_feedpre, down_share), "batch", scatter_dimension=0, tiled=True
    )
    if ring == 4:
        grad_branch, grad_hidden, term_feed = fold(
            finish_backward,
            after(back_feedin, term_feedpre).reshape(ring, rows, width),
            (grad_own, hidden, gain_two[None]),
            (
                jax.ShapeDtypeStruct((rows, width), F32),
                jax.ShapeDtypeStruct((1, width), F32),
            ),
            "fold_backward",
        )
        grad_branch, term_feed = grad_branch.reshape(length, width), term_feed[0]
    else:
        grad_feedin = scattered(back_feedin, ring)
        scale_two = rms_scale(hidden)
        term_feed = jnp.sum(grad_feedin * hidden * scale_two, axis=0)
        scaled_two = grad_feedin * gain_two
        grad_hidden = (
            grad_own.astype(F32)
            + scale_two * scaled_two
            - hidden * scale_two**3 * jnp.mean(scaled_two * hidden, axis=-1, keepdims=True)
        )
        grad_branch = gathered(grad_hidden.astype(BF16), ring)

    grad_gated = whole_head(dot_nt(grad_branch, w_output))
    term_output = dot_tn(gated, grad_branch).astype(BF16)

    def line_major(term):
        return term.reshape(ring, lines, own, -1).transpose(1, 0, 2, 3).reshape(width, -1)

    slope = swish_sig * (1.0 + swish_pre * (1.0 - swish_sig))
    grad_swishpre = own_part((grad_gated * head_normed * slope).astype(BF16))
    grad_normed_head = grad_gated * swish_act
    term_head = jnp.sum(grad_normed_head * head_plain, axis=0) / copies
    scaled_head = grad_normed_head * gain_head
    grad_mixed = head_factor * scaled_head - mixed * head_factor**3 * jnp.mean(
        scaled_head * mixed, axis=-1, keepdims=True
    )
    grad_query, grad_key, grad_value, grad_rate = mixer_backward(
        order,
        ring,
        query,
        key,
        value,
        grad_mixed.astype(BF16),
        log_rate,
        inflow,
        mask_rows,
        segment_col,
        attention,
        logits,
        (key_start, value_start),
    )
    grad_logit = (grad_rate * jax.nn.sigmoid(-forget_logit) / TAU_GATE).astype(BF16)
    term_bias = jnp.sum(grad_logit.astype(F32), axis=1) / copies
    term_expand = dot_nn(grad_logit, reduced) / copies
    grad_reduced = (dot_tn(grad_logit, expand_head) / copies).astype(BF16)
    grad_pre = jnp.concatenate(
        [own_part(grad_query), own_part(grad_key), own_part(grad_value)], axis=1
    )
    grad_normed = (
        dot_nt(grad_pre, w_mixer) + dot_nt(grad_swishpre, w_swish) + dot_nn(grad_reduced, w_squeeze)
    )
    term_pre = dot_tn(normed, jnp.concatenate([grad_pre, grad_swishpre], axis=1)).astype(BF16)
    term_mixer = (jnp.sum(grad_normed * plain_one, axis=0))
    term_squeeze = (dot_tn(grad_reduced, normed))
    def placed(array, size):
        full = jnp.zeros((HEADS, size) + array.shape[1:], F32)
        return lax.dynamic_update_slice_in_dim(full, array[None], head, 0)

    terms = jnp.concatenate(
        [
            term_mixer.reshape(devices, -1),
            placed(term_head, head_size).reshape(devices, -1),
            term_feed.reshape(devices, -1),
            placed(term_bias, SLOTS).reshape(devices, -1),
            placed(term_expand, SLOTS).reshape(devices, -1),
            term_squeeze.T.reshape(devices, -1),
        ],
        axis=1,
    )
    inputs_own = input_own.astype(F32)
    if ring == 4:
        padded = jnp.pad(terms, ((0, 0), (0, -terms.shape[1] % 1024)))
        outs = finish(
            lines,
            term_pre.reshape(ring, lines, own, width),
            term_output.reshape(lines, own, width),
            after(grad_normed.astype(BF16), layer_output).reshape(ring, rows, width),
            feed_sum.reshape(2, ring, own, hidden_part),
            padded.reshape(ring, lines, -1, 128),
            input_own,
            gain_one[None],
            grad_hidden,
        )
        query_share, key_share, value_share, swish_share, output_share, gate_share, up_share = outs[:7]
        grad_input, share = outs[7], outs[8].reshape(-1)[: terms.shape[1]]
    else:
        share = halved(halved(terms, "seq"), "batch")[0]
        grad_normed = scattered(grad_normed.astype(BF16), ring)
        scale_own = rms_scale(inputs_own)
        scaled_one = grad_normed * gain_one
        grad_input = (
            grad_hidden
            + scale_own * scaled_one
            - inputs_own * scale_own**3 * jnp.mean(scaled_one * inputs_own, axis=-1, keepdims=True)
        ).astype(BF16)
        output_share = lax.psum_scatter(term_output, "batch", scatter_dimension=0, tiled=True)
        pre_sum = lax.psum_scatter(line_major(term_pre), "batch", scatter_dimension=0, tiled=True)
        pre_share = exchanged(pre_sum.reshape(ring, own, 4 * part), mine, ring)
        pre_share = pre_share.reshape(ring, own, 4, part).transpose(2, 1, 0, 3)
        pre_share = pre_share.reshape(4, own, width).astype(F32)
        query_share, key_share, value_share, swish_share = pre_share
        feed_share = feed_sum.reshape(2, ring, own, hidden_part).transpose(1, 0, 2, 3)
        feed_share = exchanged(feed_share, mine, ring)
        gate_share = feed_share[:, 0].transpose(1, 0, 2).reshape(own, -1).astype(F32)
        up_share = feed_share[:, 1].transpose(1, 0, 2).reshape(own, -1).astype(F32)
        output_share = output_share.astype(F32)
    mixer_share, head_share, feedgain_share, bias_share, expand_share, squeeze_share = jnp.split(
        share, cuts
    )
    return (
        layer_output,
        grad_input.reshape(1, rows, width),
        mixer_share,
        query_share,
        key_share,
        value_share,
        squeeze_share.reshape(own, RANK),
        expand_share.reshape(-1, RANK).T,
        bias_share,
        swish_share,
        head_share,
        output_share,
        feedgain_share,
        gate_share,
        up_share,
        down_share.astype(F32),
    )


def solution(mesh):
    rows = P(BOTH, None)
    spread = P(BOTH)
    in_specs = (
        P("batch", "seq", None),
        P("batch", "seq"),
        spread,
        rows,
        rows,
        rows,
        rows,
        P(None, BOTH),
        spread,
        rows,
        spread,
        rows,
        spread,
        rows,
        rows,
        rows,
        P("batch", "seq", None),
    )
    out_specs = (
        P("batch", "seq", None),
        P("batch", "seq", None),
        spread,
        rows,
        rows,
        rows,
        rows,
        P(None, BOTH),
        spread,
        rows,
        spread,
        rows,
        spread,
        rows,
        rows,
        rows,
    )
    return jax.shard_map(local, mesh=mesh, in_specs=in_specs, out_specs=out_specs, check_vma=False)
```

```python
import functools

import jax
import jax.numpy as jnp
import numpy as np
from jax import lax
from jax.experimental import pallas as pl
from jax.experimental.pallas import tpu as pltpu
from jax.sharding import PartitionSpec as P

HEADS = 4
SLOTS = 64
RANK = 16
EPS = 1e-06
TAU_GATE = 8.0
CHUNK = 128
SUB = 16
BOTH = ("seq", "batch")
F32 = jnp.float32
BF16 = jnp.bfloat16
HIGHEST = lax.Precision.HIGHEST


def dot_nn(left, right):
    return lax.dot_general(left, right, (((1,), (0,)), ((), ())), preferred_element_type=F32)


def dot_nt(left, right):
    return lax.dot_general(left, right, (((1,), (1,)), ((), ())), preferred_element_type=F32)


def dot_tn(left, right):
    return lax.dot_general(left, right, (((0,), (0,)), ((), ())), preferred_element_type=F32)


def exact_nn(left, right):
    return lax.dot_general(
        left, right, (((1,), (0,)), ((), ())), precision=HIGHEST, preferred_element_type=F32
    )


def exact_nt(left, right):
    return lax.dot_general(
        left, right, (((1,), (1,)), ((), ())), precision=HIGHEST, preferred_element_type=F32
    )


def halves(value):
    high = value.astype(BF16)
    return high, (value - high.astype(F32)).astype(BF16)


def split_nn(left, right):
    high, rest = halves(left)
    return dot_nn(high, right) + dot_nn(rest, right)


def split_nt(left, right):
    high, rest = halves(left)
    return dot_nt(high, right) + dot_nt(rest, right)


LEVELS = (CHUNK // SUB).bit_length() - 1


def fill_tables(sums, covers, apart):
    source = lax.broadcasted_iota(jnp.int32, (CHUNK, CHUNK), 0)
    target = lax.broadcasted_iota(jnp.int32, (CHUNK, CHUNK), 1)

    def group(at, size):
        return jnp.bitwise_and(at, CHUNK - size)

    for level in range(LEVELS):
        half = SUB << level
        right = jnp.bitwise_and(target, half) != 0
        edge = group(target, 2 * half) + (half - 1)
        low, high = jnp.where(right, edge, target), jnp.where(right, target, edge)
        sums[:, level * CHUNK : (level + 1) * CHUNK] = jnp.where(
            (source > low) & (source <= high), 1.0, 0.0
        )
        same = group(source, 2 * half) == group(target, 2 * half)
        covers[level] = jnp.where(same & (jnp.bitwise_and(source, half) == 0) & right, 1.0, 0.0)
    sums[:, LEVELS * CHUNK : (LEVELS + 1) * CHUNK] = jnp.where(source <= target, 1.0, 0.0)
    sums[:, (LEVELS + 1) * CHUNK :] = jnp.where(source > target, 1.0, 0.0)
    apart[...] = jnp.where(group(source, SUB) == group(target, SUB), target - source, -1)


TABLES = [
    pltpu.VMEM((CHUNK, (LEVELS + 2) * CHUNK), F32),
    pltpu.VMEM((LEVELS, CHUNK, CHUNK), F32),
    pltpu.VMEM((CHUNK, CHUNK), jnp.int32),
]


def same_document(rows):
    source = lax.broadcasted_iota(jnp.int32, (CHUNK, CHUNK), 0)
    target = lax.broadcasted_iota(jnp.int32, (CHUNK, CHUNK), 1)
    number = rows[0:1, :]
    column = jnp.sum(jnp.where(source == target, number, 0.0), axis=1, keepdims=True)
    return column == number


def rolled(value, by):
    return value if by % CHUNK == 0 else pltpu.roll(value, by % CHUNK, 1)


def exponents(rate, sums):
    return jnp.exp(exact_nn(rate, sums))


def piece(value, at):
    return value[:, at * CHUNK : (at + 1) * CHUNK]


def mixer_forward_kernel(
    factor, mine, query, key, value, rate, rows, output, choice_out, start_out, state, sums, covers, apart
):
    levels = LEVELS

    @pl.when(pl.program_id(0) == 0)
    def _():
        state[...] = jnp.zeros_like(state)
        fill_tables(sums, covers, apart)

    key_in, value_in = state[:SLOTS, :], state[SLOTS:, :]
    start_out[0] = state[...]
    q, k, v = query[...], key[...], value[...]
    a, g = rate[:SLOTS, :], rate[SLOTS:, :]
    decay = exponents(a, sums[...])
    before, after = piece(decay, levels), piece(decay, levels + 1)
    carried = before * rows[1:2, :]
    visible = same_document(rows)
    scores = jnp.where(visible, dot_nt(k, q) * factor, 0.0)
    logits = carried * (split_nt(key_in, q) * factor)
    for level in range(levels):
        part = piece(decay, level)
        logits = logits + part * exact_nn(part * g, scores * covers[level])
    gap = apart[...]
    total = jnp.zeros_like(a)
    weights = []
    for by in range(SUB):
        if by:
            total = total + rolled(a, by - 1)
        weight = jnp.exp(total) * rolled(g, by)
        weights.append(weight)
        logits = logits + weight * jnp.sum(
            jnp.where(gap == by, scores, 0.0), axis=0, keepdims=True
        )
    attention = jnp.exp(logits - jnp.max(logits, axis=0, keepdims=True))
    attention = attention / jnp.sum(attention, axis=0, keepdims=True)
    choice_out[:SLOTS, :] = attention
    choice_out[SLOTS:, :] = logits
    mixing = jnp.zeros((CHUNK, CHUNK), F32)
    for level in range(levels):
        part = piece(decay, level)
        mixing = mixing + covers[level] * dot_tn(
            (part * g).astype(BF16), (part * attention).astype(BF16)
        )
    for by in range(SUB):
        row = jnp.sum(weights[by] * attention, axis=0, keepdims=True)
        mixing = jnp.where(gap == by, row, mixing)
    mixing = jnp.where(visible, mixing, 0.0).astype(BF16)
    output[...] = dot_tn(mixing, v) + dot_tn(
        (carried * attention).astype(BF16), value_in.astype(BF16)
    )
    ends = after * g * rows[2:3, :]
    keep = carried[:, CHUNK - 1 : CHUNK]
    state[:SLOTS, :] = keep * key_in + split_nn(ends, k)
    state[SLOTS:, :] = keep * value_in + split_nn(ends, v)


def mixer_backward_kernel(
    factor, mine, query, key, value, grad_output, rate, rows, choice, start, grad_all, grad_rate,
    state_grad, flow, sums, covers, apart,
):
    levels = LEVELS

    @pl.when(pl.program_id(0) == 0)
    def _():
        state_grad[...] = jnp.zeros_like(state_grad)
        flow[...] = jnp.zeros_like(flow)
        fill_tables(sums, covers, apart)

    key_in, value_in = start[0, :SLOTS, :], start[0, SLOTS:, :]
    key_after, value_after = state_grad[:SLOTS, :], state_grad[SLOTS:, :]
    q, k, v, d = query[...], key[...], value[...], grad_output[...]
    size = q.shape[1]
    a, g = rate[:SLOTS, :], rate[SLOTS:, :]
    attention, logits = choice[:SLOTS, :], choice[SLOTS:, :]
    decay = exponents(a, sums[...])
    before, after = piece(decay, levels), piece(decay, levels + 1)
    carried = before * rows[1:2, :]
    visible = same_document(rows)
    scores = jnp.where(visible, dot_nt(k, q) * factor, 0.0)
    reads = jnp.where(visible, dot_nt(v, d), 0.0)
    gap = apart[...]
    grad_att = carried * split_nt(value_in, d)
    for level in range(levels):
        part = piece(decay, level)
        grad_att = grad_att + part * exact_nn(part * g, reads * covers[level])
    total = jnp.zeros_like(a)
    bare, weights, score_rows, read_rows = [], [], [], []
    for by in range(SUB):
        if by:
            total = total + rolled(a, by - 1)
        bare.append(jnp.exp(total))
        weights.append(bare[by] * rolled(g, by))
        score_rows.append(jnp.sum(jnp.where(gap == by, scores, 0.0), axis=0, keepdims=True))
        read_rows.append(jnp.sum(jnp.where(gap == by, reads, 0.0), axis=0, keepdims=True))
        grad_att = grad_att + weights[by] * read_rows[by]
    grad_logits = attention * (
        grad_att - jnp.sum(attention * grad_att, axis=0, keepdims=True)
    )
    mixing = jnp.zeros((CHUNK, CHUNK), F32)
    spread = jnp.zeros((CHUNK, CHUNK), F32)
    ends = after * rows[2:3, :]
    grad_inflow = ends * (split_nt(key_after, k) + split_nt(value_after, v))
    for level in range(levels):
        part = piece(decay, level)
        left = (part * g).astype(BF16)
        att_part, log_part = part * attention, part * grad_logits
        mixing = mixing + covers[level] * dot_tn(left, att_part.astype(BF16))
        spread = spread + covers[level] * dot_tn(left, log_part.astype(BF16))
        grad_inflow = grad_inflow + part * (
            exact_nt(log_part, scores * covers[level]) + exact_nt(att_part, reads * covers[level])
        )
    for by in range(SUB):
        row = jnp.sum(weights[by] * attention, axis=0, keepdims=True)
        mixing = jnp.where(gap == by, row, mixing)
        row = jnp.sum(weights[by] * grad_logits, axis=0, keepdims=True)
        spread = jnp.where(gap == by, row, spread)
        terms = bare[by] * (grad_logits * score_rows[by] + attention * read_rows[by])
        grad_inflow = grad_inflow + rolled(terms, -by)
    mixing = jnp.where(visible, mixing, 0.0).astype(BF16)
    spread = (jnp.where(visible, spread, 0.0) * factor).astype(BF16)
    log_carried = carried * grad_logits * factor
    att_carried = carried * attention
    ends = (ends * g).astype(BF16)
    grad_all[:, :size] = (
        dot_tn(spread, k) + dot_tn(log_carried.astype(BF16), key_in.astype(BF16))
    ).astype(BF16)
    grad_all[:, size : 2 * size] = (dot_nn(spread, q) + dot_tn(ends, key_after.astype(BF16))).astype(BF16)
    grad_all[:, 2 * size :] = (dot_nn(mixing, d) + dot_tn(ends, value_after.astype(BF16))).astype(BF16)
    change = grad_logits * logits + attention * grad_att - g * grad_inflow
    later = piece(sums, levels + 1) + jnp.where(gap == 0, 1.0, 0.0)
    same = jnp.where(visible, later, 0.0)
    flows = exact_nn(change, same) + rows[2:3, :] * flow[:, 0:1]
    grad_rate[...] = rows[3:4, :] * flows - jnp.exp(a) * grad_inflow
    keep = carried[:, CHUNK - 1 : CHUNK]
    key_before = keep * key_after + split_nn(log_carried, q)
    value_before = keep * value_after + split_nn(att_carried, d)
    state_grad[:SLOTS, :] = key_before
    state_grad[SLOTS:, :] = value_before
    flow[...] = jnp.broadcast_to(
        jnp.sum(key_before * key_in + value_before * value_in, axis=1, keepdims=True), flow.shape
    )


def mixer_specs(length, size, ring, backward):
    count = length // CHUNK
    per = count // ring

    def natural(step):
        return count - 1 - step if backward else step

    def moved(step, mine):
        at = natural(step)
        return lax.bitwise_xor(at // per, mine[0]) * per + at % per

    wide = [
        pl.BlockSpec((CHUNK, size), lambda step, mine, at=at: (moved(step, mine), at))
        for at in range(3)
    ]
    everything = pl.BlockSpec((CHUNK, 3 * size), lambda step, mine: (moved(step, mine), 0))
    pair = pl.BlockSpec((2 * SLOTS, CHUNK), lambda step, mine: (0, moved(step, mine)))
    slim = pl.BlockSpec((SLOTS, CHUNK), lambda step, mine: (0, moved(step, mine)))
    rows = pl.BlockSpec((8, CHUNK), lambda step, mine: (0, natural(step)))
    state = pl.BlockSpec((1, 2 * SLOTS, size), lambda step, mine: (natural(step), 0, 0))
    return count, wide, everything, pair, slim, rows, state


def mixer_forward(mine, ring, joined, rates, rows):
    length, size = joined.shape[0], joined.shape[1] // 3
    count, wide, _, pair, _, row_spec, state = mixer_specs(length, size, ring, False)
    return pl.pallas_call(
        functools.partial(mixer_forward_kernel, size ** (-0.25)),
        out_shape=(
            jax.ShapeDtypeStruct((length, size), F32),
            jax.ShapeDtypeStruct((2 * SLOTS, length), F32),
            jax.ShapeDtypeStruct((count, 2 * SLOTS, size), F32),
        ),
        grid_spec=pltpu.PrefetchScalarGridSpec(
            num_scalar_prefetch=1,
            grid=(count,),
            in_specs=wide + [pair, row_spec],
            out_specs=[wide[0], pair, state],
            scratch_shapes=[pltpu.VMEM((2 * SLOTS, size), F32)] + TABLES,
        ),
        compiler_params=pltpu.CompilerParams(vmem_limit_bytes=32 << 20),
        cost_estimate=pl.CostEstimate(
            flops=length * size * 2000, bytes_accessed=length * size * 12, transcendentals=length * 4096
        ),
        name="mixer_forward",
    )(mine, joined, joined, joined, rates, rows)


def mixer_backward(mine, ring, joined, grad, rates, rows, choice, starts):
    length, size = grad.shape
    count, wide, everything, pair, slim, row_spec, state = mixer_specs(length, size, ring, True)
    return pl.pallas_call(
        functools.partial(mixer_backward_kernel, size ** (-0.25)),
        out_shape=(
            jax.ShapeDtypeStruct((length, 3 * size), BF16),
            jax.ShapeDtypeStruct((SLOTS, length), F32),
        ),
        grid_spec=pltpu.PrefetchScalarGridSpec(
            num_scalar_prefetch=1,
            grid=(count,),
            in_specs=wide + [wide[0], pair, row_spec, pair, state],
            out_specs=[everything, slim],
            scratch_shapes=[pltpu.VMEM((2 * SLOTS, size), F32), pltpu.VMEM((SLOTS, 128), F32)]
            + TABLES,
        ),
        compiler_params=pltpu.CompilerParams(vmem_limit_bytes=32 << 20),
        cost_estimate=pl.CostEstimate(
            flops=length * size * 4000, bytes_accessed=length * size * 20, transcendentals=length * 4096
        ),
        name="mixer_backward",
    )(mine, joined, joined, joined, grad, rates, rows, choice, starts)


def peers(ring, mine):
    found = []
    for by in range(1, ring):
        at, bit = mine, 1
        while bit <= by:
            if by & bit:
                at = at + bit * (1 - 2 * ((at // bit) % 2))
            bit *= 2
        found.append(at)
    return found


class Copies:
    def __init__(self, local, send, recv):
        self.local, self.send, self.recv = local, send, recv
        self.here, self.away = 0, 0
        self.open = []

    def near(self, source, target):
        copy = pltpu.make_async_copy(source, target, self.local.at[self.here])
        self.here += 1
        copy.start()
        return copy

    def far(self, source, target, landed, device, when=None):
        at = self.away
        self.away += 1
        copy = pltpu.make_async_remote_copy(
            source, target, self.send.at[at], self.recv.at[at], device_id=device,
            device_id_type=pl.DeviceIdType.MESH,
        )
        if when is None:
            copy.start()
        else:
            pl.when(when)(copy.start)
        self.open.append((copy, when))
        return pltpu.make_async_remote_copy(
            landed, landed, self.send.at[at], self.recv.at[at], device_id=device,
            device_id_type=pl.DeviceIdType.MESH,
        ).wait_recv

    def close(self):
        for copy, when in self.open:
            if when is None:
                copy.wait_send()
            else:
                pl.when(when)(copy.wait_send)


def slab_chain(copies, chips, place):
    mine, batch = lax.axis_index("seq"), lax.axis_index("batch")
    chip, core = batch // 2, batch % 2
    other = (mine, chip * 2 + (1 - core))

    def at(where):
        return jnp.clip(where, 0, chips - 1) * 2 + core

    def send(step, way):
        block, come = chip - way * (step - 1), chip - way * step
        when = (block >= 0) & (block < chips) & (chip + way >= 0) & (chip + way < chips)
        came = (come >= 0) & (come < chips)
        wait = copies.far(
            place(at(block)), place(at(block)), place(at(come)), (mine, at(chip + way)), when
        )
        return wait, came, at(come)

    crossing = [(copies.far(place(batch), place(batch), place(other[1]), other), None)]
    flying = [send(1, 1), send(1, -1)] if chips > 1 else []
    yield
    for step in range(1, chips):
        coming = []
        for way, (wait, came, landed) in zip((1, -1), flying):
            pl.when(came)(wait)
            if step + 1 < chips:
                coming.append(send(step + 1, way))
            there = landed + 1 - 2 * core
            crossing.append(
                (copies.far(place(landed), place(landed), place(there), other, came), came)
            )
        flying = coming
        yield
    for wait, came in crossing:
        if came is None:
            wait()
        else:
            pl.when(came)(wait)
    yield


def start_kernel(
    ring, lines, inputs, w_query, w_key, w_value, w_swish, w_out, gate, up, small,
    inputs_all, w_mixer, swish_columns, w_output, gate_columns, up_columns, small_all,
    own_input, mixer_blocks, swish_blocks, own_out, gate_blocks, up_blocks,
    local_sem, send_sem, recv_sem,
):
    mine, batch = lax.axis_index("seq"), lax.axis_index("batch")
    chips = lines // 2
    copies = Copies(local_sem, send_sem, recv_sem)
    part = swish_columns.shape[2]
    half = inputs.shape[0] // 2
    others = peers(ring, mine)

    def columns(ref, blocks, first, size):
        return [
            copies.near(
                ref.at[at] if len(ref.shape) == 3 else ref.at[:, pl.ds(at * size, size)],
                blocks.at[at, :, pl.ds(first, size)],
            )
            for at in range(ring)
        ]

    loads = []
    for at, ref in enumerate((w_query, w_key, w_value)):
        loads += columns(ref, mixer_blocks, at * part, part)
    direct = 2 if ring == 4 else ring - 1
    input_waits = [
        copies.far(inputs, inputs_all.at[by + 1], inputs_all.at[by + 1], (others[by], batch))
        for by in range(direct)
    ]
    own_load = copies.near(inputs, own_input)
    hidden = gate_columns.shape[2]
    out_load = copies.near(w_out, own_out)
    other_loads = columns(w_swish, swish_blocks, 0, part)
    other_loads += columns(gate, gate_blocks, 0, hidden) + columns(up, up_blocks, 0, hidden)
    for copy in loads:
        copy.wait()
    column_waits = [
        copies.far(
            mixer_blocks.at[to], w_mixer.at[mine, batch], w_mixer.at[to, batch], (to, batch)
        )
        for to in others
    ]
    near = [
        copies.near(mixer_blocks.at[mine], w_mixer.at[mine, batch]),
        copies.near(small, small_all.at[mine, batch]),
    ]
    small_waits = [
        copies.far(small, small_all.at[mine, batch], small_all.at[to, batch], (to, batch))
        for to in others
    ]
    for copy in near:
        copy.wait()

    def started(place):
        chain = slab_chain(copies, chips, place)
        next(chain)
        chains.append(chain)

    chains = []
    started(lambda at: w_mixer.at[mine, at])
    for wait, source in zip(column_waits, others):
        wait()
        started(lambda at, source=source: w_mixer.at[source, at])
    for wait, source in zip(small_waits, others):
        wait()
        started(lambda at, source=source: small_all.at[source, at])
    started(lambda at: small_all.at[mine, at])
    out_load.wait()
    near = copies.near(own_out, w_output.at[batch])
    near.wait()
    started(lambda at: w_output.at[at])
    own_load.wait()
    stores = [copies.near(own_input, inputs_all.at[0])]
    for copy in other_loads:
        copy.wait()
    moved = (
        (swish_blocks, swish_columns), (gate_blocks, gate_columns), (up_blocks, up_columns)
    )
    stores += [copies.near(blocks.at[mine], array.at[mine]) for blocks, array in moved]
    for wait in input_waits:
        wait()
    if ring == 4:
        low, high = pl.ds(0, half), pl.ds(half, half)
        input_waits = [
            copies.far(
                inputs_all.at[have, rows], inputs_all.at[3, rows], inputs_all.at[3, rows], (to, batch)
            )
            for have, rows, to in ((2, low, others[0]), (1, high, others[1]))
        ]
    else:
        input_waits = []
    other_waits = [
        copies.far(blocks.at[to], array.at[mine], array.at[to], (to, batch))
        for blocks, array in moved
        for to in others
    ]
    for step in range(1, chips + 1):
        for chain in chains:
            next(chain)
    for wait in input_waits + other_waits:
        wait()
    for copy in stores:
        copy.wait()
    copies.close()


def start(ring, lines, inputs, columns, w_out, gate, up, small):
    own, width = columns[0].shape
    part, hidden = width // ring, gate.shape[1] // ring
    if hidden % 128:
        gate, up = (a.reshape(own, ring, hidden).transpose(1, 0, 2) for a in (gate, up))
    anywhere, outside = (pl.BlockSpec(memory_space=space) for space in (pl.ANY, pltpu.HBM))
    away = (ring - 1) * 6 + 2 + (2 * ring + 1) * (4 * (lines // 2 - 1) + 1)
    thin = (ring, own, hidden)
    return pl.pallas_call(
        functools.partial(start_kernel, ring, lines),
        out_shape=(
            jax.ShapeDtypeStruct((ring,) + inputs.shape, BF16),
            jax.ShapeDtypeStruct((ring, lines, own, 3 * part), BF16),
            jax.ShapeDtypeStruct((ring, own, part), BF16),
            jax.ShapeDtypeStruct((lines,) + w_out.shape, BF16),
            jax.ShapeDtypeStruct(thin, BF16),
            jax.ShapeDtypeStruct(thin, BF16),
            jax.ShapeDtypeStruct((ring, lines) + small.shape, BF16),
        ),
        in_specs=[anywhere] * 9,
        out_specs=[outside] * 7,
        scratch_shapes=[
            pltpu.VMEM(inputs.shape, BF16),
            pltpu.VMEM((ring, own, 3 * part), BF16),
            pltpu.VMEM((ring, own, part), BF16),
            pltpu.VMEM(w_out.shape, BF16),
            pltpu.VMEM(thin, BF16),
            pltpu.VMEM(thin, BF16),
            pltpu.SemaphoreType.DMA((6 * ring + 9,)),
            pltpu.SemaphoreType.DMA((away,)),
            pltpu.SemaphoreType.DMA((away,)),
        ],
        compiler_params=pltpu.CompilerParams(has_side_effects=True, vmem_limit_bytes=32 << 20),
        name="start",
    )(inputs, *columns, w_out, gate, up, small)


PARTS = 4


def fold_kernel(finish, extras, *refs):
    terms, given = refs[0], refs[1 : 1 + extras]
    blocks = refs[1 + extras]
    made = refs[2 + extras : -9]
    first, second, third, two_low, one_high, own, local_sem, send_sem, recv_sem = refs[-9:]
    mine, batch = lax.axis_index("seq"), lax.axis_index("batch")
    others = peers(4, mine)
    row, col = (others[0], batch), (others[1], batch)
    copies = Copies(local_sem, send_sem, recv_sem)
    size = terms.shape[1] // PARTS

    def span(at):
        low = pl.ds(at * size, size // 2)
        return pl.ds(at * size, size), low, pl.ds(at * size + size // 2, size // 2)

    opening, direct = [], []

    def open_part(at):
        _, low, high = span(at)
        opening.append(
            (
                copies.far(terms.at[3, low], first.at[low], first.at[low], row),
                copies.far(terms.at[3, high], first.at[high], first.at[high], col),
            )
        )

    def pass_part(at):
        _, low, high = span(at)
        waits = [
            copies.far(terms.at[2, high], second.at[high], second.at[high], col),
            copies.far(terms.at[1, low], third.at[low], third.at[low], row),
        ]
        opening[at][0]()
        two_low[low, :] = added(terms[2, low, :], first[low, :])
        waits.append(copies.far(two_low.at[low], second.at[low], second.at[low], col))
        opening[at][1]()
        one_high[high, :] = added(terms[1, high, :], first[high, :])
        waits.append(copies.far(one_high.at[high], third.at[high], third.at[high], row))
        direct.append(waits)

    spread, local, passed = [], [], []

    def close_part(at):
        full, _, _ = span(at)
        for wait in direct[at]:
            wait()
        total = terms[0, full, :].astype(F32) + second[full, :].astype(F32) + third[full, :].astype(F32)
        own[full, :] = finish(total, full, at, given, made)
        spread.append(
            (
                copies.far(own.at[full], blocks.at[1, full], blocks.at[1, full], row),
                copies.far(own.at[full], blocks.at[2, full], blocks.at[2, full], col),
            )
        )
        local.append(copies.near(own.at[full], blocks.at[0, full]))

    def forward_part(at):
        _, low, high = span(at)
        for wait in spread[at]:
            wait()
        passed.append(copies.far(blocks.at[2, low], blocks.at[3, low], blocks.at[3, low], row))
        passed.append(copies.far(blocks.at[1, high], blocks.at[3, high], blocks.at[3, high], col))

    open_part(0)
    for at in range(PARTS + 2):
        if at + 1 < PARTS:
            open_part(at + 1)
        if at < PARTS:
            pass_part(at)
        if 1 <= at <= PARTS:
            close_part(at - 1)
        if at >= 2:
            forward_part(at - 2)
    for wait in passed:
        wait()
    for copy in local:
        copy.wait()
    copies.close()


def half_blocks(value, order):
    lane = lax.broadcasted_iota(jnp.int32, (value.shape[0], 128), 1)
    made = []
    for pair in zip(order[::2], order[1::2]):
        low, high = (
            value[:, block * 128 : (block + 1) * 128]
            if half == want
            else pltpu.roll(value[:, block * 128 : (block + 1) * 128], 64, 1)
            for want, (block, half) in enumerate(pair)
        )
        made.append(jnp.where(lane < 64, low, high))
    return jnp.concatenate(made, axis=1)


def by_line(value):
    lines = value.shape[1] // 256
    return half_blocks(
        value, [divmod(ring * lines + line, 2) for line in range(lines) for ring in range(4)]
    )


def by_ring(value):
    lines = value.shape[1] // 256
    return half_blocks(
        value, [divmod(line * 4 + ring, 2) for ring in range(4) for line in range(lines)]
    )


def finish_forward(total, full, at, given, made):
    inputs, gain = given
    hidden = inputs[full, :].astype(F32) + total
    made[0][full, :] = hidden
    return by_line(hidden * rms_scale(hidden) * gain[...]).astype(BF16)


def finish_backward(total, full, at, given, made):
    cotangent, hidden_ref, gain = given
    total = by_ring(total)
    hidden = hidden_ref[full, :]
    scale = rms_scale(hidden)
    plain = hidden * scale
    term = jnp.sum(total * plain, axis=0, keepdims=True)
    made[1][...] = term if at == 0 else made[1][...] + term
    scaled = total * gain[...]
    grad = (
        cotangent[full, :].astype(F32)
        + scale * scaled
        - plain * (scale * jnp.mean(scaled * plain, axis=-1, keepdims=True))
    )
    made[0][full, :] = grad
    return grad.astype(BF16)


def finish_kernel(
    lines, mixer_terms, out_terms, input_terms, gate_sum, up_sum, small_terms, inputs, gain, grad_hidden,
    grad_query, grad_key, grad_value, grad_swish, grad_out, grad_gate, grad_up, grad_input, small_sum,
    crossed, staged, arrived, summed, outgoing, mixer_blocks, feed_blocks, small_ring, small_mine, small_line,
    first, second, third, two_low, one_high, local_sem, send_sem, recv_sem,
):
    mine, batch = lax.axis_index("seq"), lax.axis_index("batch")
    chips = lines // 2
    chip, core = batch // 2, batch % 2
    sibling = chip * 2 + (1 - core)
    others = peers(4, mine)
    row, col = (others[0], batch), (others[1], batch)
    copies = Copies(local_sem, send_sem, recv_sem)
    slabs = others + [mine, None]

    def term(slab, owner):
        return out_terms.at[owner] if slabs[slab] is None else mixer_terms.at[slabs[slab], owner]

    cross_waits = {}
    for slab in range(len(slabs)):
        for owner in range(chips):
            cross_waits[slab, owner] = copies.far(
                term(slab, owner * 2 + (1 - core)),
                crossed.at[slab, owner],
                crossed.at[slab, owner],
                (mine, sibling),
            )
    small_waits = [
        copies.far(small_terms.at[to], small_ring.at[at], small_ring.at[at], (to, batch))
        for at, to in enumerate(others)
    ]
    feed_waits = [
        copies.far(
            array.at[to], feed_blocks.at[mine, at], feed_blocks.at[to, at], (to, batch)
        )
        for to in others
        for at, array in enumerate((gate_sum, up_sum))
    ]

    size = input_terms.shape[1] // PARTS
    opening, direct = [], []

    def span(at):
        low = pl.ds(at * size, size // 2)
        return pl.ds(at * size, size), low, pl.ds(at * size + size // 2, size // 2)

    def open_part(at):
        _, low, high = span(at)
        opening.append(
            (
                copies.far(input_terms.at[3, low], first.at[low], first.at[low], row),
                copies.far(input_terms.at[3, high], first.at[high], first.at[high], col),
            )
        )

    def pass_part(at):
        _, low, high = span(at)
        waits = [
            copies.far(input_terms.at[2, high], second.at[high], second.at[high], col),
            copies.far(input_terms.at[1, low], third.at[low], third.at[low], row),
        ]
        opening[at][0]()
        two_low[low, :] = added(input_terms[2, low, :], first[low, :])
        waits.append(copies.far(two_low.at[low], second.at[low], second.at[low], col))
        opening[at][1]()
        one_high[high, :] = added(input_terms[1, high, :], first[high, :])
        waits.append(copies.far(one_high.at[high], third.at[high], third.at[high], row))
        direct.append(waits)

    def close_part(at):
        full, _, _ = span(at)
        for wait in direct[at]:
            wait()
        total = (
            input_terms[0, full, :].astype(F32)
            + second[full, :].astype(F32)
            + third[full, :].astype(F32)
        )
        features = inputs[full, :].astype(F32)
        scale = rms_scale(features)
        plain = features * scale
        scaled = total * gain[...]
        grad = (
            grad_hidden[full, :]
            + scale * scaled
            - plain * (scale * jnp.mean(scaled * plain, axis=-1, keepdims=True))
        )
        grad_input[full, :] = grad.astype(BF16)

    def small_part():
        for wait in small_waits:
            wait()
        small_mine[...] = small_terms[mine] + small_ring[0] + small_ring[1] + small_ring[2]
        for by in range(1, lines):
            to, source = (batch + by) % lines, (batch + lines - by) % lines
            small_waits.append(
                copies.far(small_mine.at[to], small_line.at[by], small_line.at[by], (mine, to))
            )

    def feed_part():
        for wait in feed_waits:
            wait()
        feed_blocks[mine, 0] = gate_sum[mine]
        feed_blocks[mine, 1] = up_sum[mine]
        wide = gate_sum.shape[2]
        for source in range(4):
            at = pl.ds(source * wide, wide)
            grad_gate[:, at] = feed_blocks[source, 0].astype(F32)
            grad_up[:, at] = feed_blocks[source, 1].astype(F32)

    beside = [functools.partial(open_part, 1)]
    for at in range(PARTS):
        if at + 2 <= PARTS - 1:
            beside.append(functools.partial(open_part, at + 2))
        beside.append(functools.partial(pass_part, at))
        if at == 0:
            beside.append(small_part)
        if at:
            beside.append(functools.partial(close_part, at - 1))
    beside.append(functools.partial(close_part, PARTS - 1))
    beside.append(feed_part)
    open_part(0)

    def both_cores(slab, owner):
        return term(slab, owner * 2 + core)[...].astype(F32) + crossed[slab, owner].astype(F32)

    crossed_in = set()

    def wait_cross(slab):
        if slab not in crossed_in:
            crossed_in.add(slab)
            for owner in range(chips):
                cross_waits[slab, owner]()

    flying = {}
    for far in range(chips - 1, 0, -1):
        for slab in range(len(slabs)):
            wait_cross(slab)
            for side, way in enumerate((1, -1)):
                owner = chip + way * far
                sends = (owner >= 0) & (owner < chips)
                held = jnp.clip(owner, 0, chips - 1)
                before = chip - way
                gets = sends & (before >= 0) & (before < chips)
                here = staged.at[side, far - 1, slab]
                if far < chips - 1:
                    wait = flying[side, far + 1, slab]

                    @pl.when(gets)
                    def _(wait=wait, slab=slab, held=held, here=here, side=side, far=far):
                        wait()
                        here[...] = (
                            both_cores(slab, held) + arrived[side, far, slab].astype(F32)
                        ).astype(BF16)

                    @pl.when(sends & jnp.logical_not((before >= 0) & (before < chips)))
                    def _(slab=slab, held=held, here=here):
                        here[...] = both_cores(slab, held).astype(BF16)
                else:

                    @pl.when(sends)
                    def _(slab=slab, held=held, here=here):
                        here[...] = both_cores(slab, held).astype(BF16)

                target = jnp.clip(chip + way, 0, chips - 1) * 2 + core
                flying[side, far, slab] = copies.far(
                    here,
                    arrived.at[side, far - 1, slab],
                    arrived.at[side, far - 1, slab],
                    (mine, target),
                    sends,
                )
            if beside:
                beside.pop(0)()
    ring_waits = []
    for slab in range(len(slabs)):
        total = summed.at[slab]
        total[...] = both_cores(slab, chip)
        for side, way in enumerate((1, -1)):
            before = chip - way
            wait = flying[side, 1, slab]

            @pl.when((before >= 0) & (before < chips))
            def _(wait=wait, total=total, slab=slab, side=side):
                wait()
                total[...] += arrived[side, 0, slab].astype(F32)

        if slabs[slab] is None:
            grad_out[...] = total[...]
        elif slab == len(others):
            mixer_blocks[mine] = total[...].astype(BF16)
        else:
            outgoing[slab] = total[...].astype(BF16)
            to = slabs[slab]
            ring_waits.append(
                copies.far(
                    outgoing.at[slab], mixer_blocks.at[mine], mixer_blocks.at[to], (to, batch)
                )
            )
        if beside:
            beside.pop(0)()
    for piece in beside:
        piece()
    for wait in small_waits[3:]:
        wait()
    total = small_mine[batch]
    for by in range(1, lines):
        total = total + small_line[by]
    small_sum[...] = total
    for wait in ring_waits:
        wait()
    part = grad_query.shape[1] // 4
    for source in range(4):
        at = pl.ds(source * part, part)
        for piece, out in enumerate((grad_query, grad_key, grad_value, grad_swish)):
            out[:, at] = mixer_blocks[source, :, piece * part : (piece + 1) * part].astype(F32)
    copies.close()


def finish(lines, mixer_terms, out_terms, input_terms, gate_sum, up_sum, small_terms, inputs, gain, grad_hidden):
    ring, _, own, width = mixer_terms.shape
    rows, hidden = inputs.shape[0], gate_sum.shape[2]
    chips = lines // 2
    inside = pl.BlockSpec(memory_space=pltpu.VMEM)
    block = pltpu.VMEM((rows, width), BF16)
    small = small_terms.shape[2:]
    away = (ring + 1) * (chips + 2 * (chips - 1)) + 4 * (ring - 1) + PARTS * 6 + lines - 1
    square = jax.ShapeDtypeStruct((own, width), F32)
    wide = jax.ShapeDtypeStruct((own, ring * hidden), F32)
    return pl.pallas_call(
        functools.partial(finish_kernel, lines),
        out_shape=(square,) * 5
        + (wide,) * 2
        + (jax.ShapeDtypeStruct((rows, width), BF16), jax.ShapeDtypeStruct(small, F32)),
        in_specs=[inside] * 9,
        out_specs=[inside] * 9,
        scratch_shapes=[
            pltpu.VMEM((ring + 1, chips, own, width), BF16),
            pltpu.VMEM((2, chips - 1, ring + 1, own, width), BF16),
            pltpu.VMEM((2, chips - 1, ring + 1, own, width), BF16),
            pltpu.VMEM((ring + 1, own, width), F32),
            pltpu.VMEM((ring - 1, own, width), BF16),
            pltpu.VMEM((ring, own, width), BF16),
            pltpu.VMEM((ring, 2, own, hidden), BF16),
            pltpu.VMEM((ring - 1, lines) + small, F32),
            pltpu.VMEM((lines,) + small, F32),
            pltpu.VMEM((lines,) + small, F32),
        ]
        + [block] * 5
        + [
            pltpu.SemaphoreType.DMA((1,)),
            pltpu.SemaphoreType.DMA((away,)),
            pltpu.SemaphoreType.DMA((away,)),
        ],
        compiler_params=pltpu.CompilerParams(has_side_effects=True, vmem_limit_bytes=58 << 20),
        name="finish",
    )(mixer_terms, out_terms, input_terms, gate_sum, up_sum, small_terms, inputs, gain, grad_hidden)


def fold(finish, terms, given, made, name):
    ring, rows, width = terms.shape
    inside = pl.BlockSpec(memory_space=pltpu.VMEM)
    block = pltpu.VMEM((rows, width), BF16)
    return pl.pallas_call(
        functools.partial(fold_kernel, finish, len(given)),
        out_shape=(jax.ShapeDtypeStruct((ring, rows, width), BF16),) + made,
        in_specs=[inside] * (1 + len(given)),
        out_specs=[pl.BlockSpec(memory_space=pltpu.HBM)] + [inside] * len(made),
        scratch_shapes=[block] * 6
        + [
            pltpu.SemaphoreType.DMA((PARTS,)),
            pltpu.SemaphoreType.DMA((PARTS * 10,)),
            pltpu.SemaphoreType.DMA((PARTS * 10,)),
        ],
        compiler_params=pltpu.CompilerParams(has_side_effects=True, vmem_limit_bytes=40 << 20),
        name=name,
    )(terms, *given)


def rms_scale(features):
    return lax.rsqrt(jnp.mean(features * features, axis=-1, keepdims=True) + EPS)


def swapped(block, by, ring):
    return lax.ppermute(block, "seq", [(i, i ^ by) for i in range(ring)])


def gathered(block, ring):
    if ring != 4:
        return jnp.concatenate([block] + [swapped(block, by, ring) for by in range(1, ring)], axis=0)
    half = block.shape[0] // 2
    one, two = swapped(block, 1, ring), swapped(block, 2, ring)
    low, high = swapped(two[:half], 1, ring), swapped(one[half:], 2, ring)
    return jnp.concatenate([block, one, two, low, high], axis=0)


def scattered(terms, ring):
    rows = terms.shape[0] // ring
    parts = [terms[by * rows : (by + 1) * rows] for by in range(ring)]
    total = parts[0].astype(F32)
    if ring != 4:
        for by in range(1, ring):
            total = total + swapped(parts[by], by, ring).astype(F32)
        return total
    half = rows // 2
    low, high = swapped(parts[3][:half], 1, ring), swapped(parts[3][half:], 2, ring)
    two = jnp.concatenate([added(parts[2][:half], low), parts[2][half:]], axis=0)
    one = jnp.concatenate([parts[1][:half], added(parts[1][half:], high)], axis=0)
    return total + swapped(one, 1, ring).astype(F32) + swapped(two, 2, ring).astype(F32)


def added(left, right):
    return (left.astype(F32) + right.astype(F32)).astype(BF16)


def flipped(block, axis, by):
    return lax.ppermute(block, axis, [(i, i ^ by) for i in range(lax.axis_size(axis))])


def doubled(block, axis):
    by, mine = 1, lax.axis_index(axis)
    while by < lax.axis_size(axis):
        other = flipped(block, axis, by)
        first = (mine & by) == 0
        block = jnp.concatenate(
            [jnp.where(first, block, other), jnp.where(first, other, block)], axis=0
        )
        by *= 2
    return block


def halved(block, axis):
    by, mine = lax.axis_size(axis) // 2, lax.axis_index(axis)
    while by:
        low, high = jnp.split(block, 2, axis=0)
        first = (mine & by) == 0
        block = jnp.where(first, low, high) + flipped(jnp.where(first, high, low), axis, by)
        by //= 2
    return block


def after(value, *others):
    return lax.optimization_barrier((value,) + others)[0]


def exchanged(blocks, mine, ring):
    parts = [
        swapped(lax.dynamic_index_in_dim(blocks, mine ^ by, 0, keepdims=False), by, ring)
        if by
        else lax.dynamic_index_in_dim(blocks, mine, 0, keepdims=False)
        for by in range(ring)
    ]
    made = jnp.stack(parts)
    return jnp.concatenate(
        [lax.dynamic_index_in_dim(made, mine ^ j, 0, keepdims=True) for j in range(ring)], axis=0
    )


def local(
    layer_input,
    segments,
    mixer_gain,
    query_weight,
    key_weight,
    value_weight,
    squeeze,
    expand,
    forget_bias,
    swish_weight,
    head_gain,
    output_weight,
    feed_gain,
    gate_weight,
    up_weight,
    down_weight,
    cotangent,
):
    ring, lines = lax.axis_size("seq"), lax.axis_size("batch")
    devices = ring * lines
    mine = lax.axis_index("seq")
    rows, width = layer_input.shape[1], layer_input.shape[2]
    length = rows * ring
    own = width // devices
    head_size = width // HEADS
    copies = ring // HEADS
    part = width // ring
    head = mine // copies
    hidden_part = gate_weight.shape[1] // ring
    slots_all = HEADS * SLOTS

    def to_order(array):
        if copies == 1:
            return array
        blocks = array.reshape((ring, rows) + array.shape[1:])
        moved = [lax.dynamic_index_in_dim(blocks, mine ^ by, 0, keepdims=False) for by in range(ring)]
        return jnp.concatenate(moved, axis=0)

    def whole_head(array):
        if copies == 1:
            return array
        full = lax.all_gather(to_order(array), "seq", axis=1, tiled=True)
        return to_order(lax.dynamic_slice_in_dim(full, head * head_size, head_size, 1))

    def own_part(array):
        if copies == 1:
            return array
        return lax.dynamic_slice_in_dim(array, (mine % copies) * part, part, 1)

    params = jnp.concatenate(
        [
            mixer_gain,
            head_gain,
            feed_gain,
            forget_bias,
            expand.T.reshape(-1),
            squeeze.reshape(-1),
        ]
    )
    count = params.shape[0]
    params = jnp.concatenate([params, segments.reshape(rows).astype(BF16)])
    params = jnp.pad(params, (0, -params.shape[0] % 2048)).reshape(-1, 128)
    input_own = layer_input.reshape(rows, width)
    grad_own = cotangent.reshape(rows, width)
    inputs, w_mixer, swish_columns, w_output, gate_columns, up_columns, small = start(
        ring,
        lines,
        input_own,
        (query_weight, key_weight, value_weight, swish_weight),
        output_weight,
        gate_weight,
        up_weight,
        params,
    )
    inputs = inputs.reshape(length, width)
    grad_out = gathered(after(grad_own, inputs), ring)
    w_mixer = w_mixer.reshape(width, 3 * part)
    small = small.reshape(devices, -1)
    segment = lax.dynamic_index_in_dim(
        small.reshape(ring, lines, -1), lax.axis_index("batch"), 1, keepdims=False
    )[:, count : count + rows].reshape(length).astype(F32)
    cuts = np.cumsum([own, own, own, slots_all // devices, RANK * slots_all // devices])
    gain_one, gain_head, gain_two, bias_full, expand_t, w_squeeze = jnp.split(
        small[:, :count], cuts, axis=1
    )
    gain_one = gain_one.reshape(width).astype(F32)
    gain_head = lax.dynamic_slice_in_dim(gain_head.reshape(width), head * head_size, head_size, 0)
    gain_head = gain_head.astype(F32)
    gain_two = gain_two.reshape(width).astype(F32)
    bias_head = lax.dynamic_slice_in_dim(bias_full.reshape(slots_all), head * SLOTS, SLOTS, 0)
    expand_head = lax.dynamic_slice_in_dim(
        expand_t.reshape(slots_all, RANK), head * SLOTS, SLOTS, 0
    )
    w_squeeze = w_squeeze.reshape(width, RANK).T

    w_output = w_output.reshape(part, width)

    def over_batch(blocks):
        return lax.all_gather(blocks.reshape(ring * own, -1), "batch", axis=0, tiled=True)

    def own_order(array):
        return array.reshape(lines, ring, own, -1).transpose(1, 0, 2, 3).reshape(width, -1)

    def line_major(term):
        return term.reshape(ring, lines, own, -1).transpose(1, 0, 2, 3).reshape(width, -1)

    w_swish = own_order(over_batch(swish_columns))
    w_gate, w_up = over_batch(gate_columns), over_batch(up_columns)
    if ring != 4:
        w_gate, w_up = own_order(w_gate), own_order(w_up)
    w_down = lax.all_gather(after(down_weight, gate_columns), "batch", axis=0, tiled=True)

    chunked = segment.reshape(-1, CHUNK)
    before = jnp.concatenate([jnp.full((1,), -1.0, F32), chunked[:-1, -1]])
    previous = jnp.concatenate([jnp.full((1,), -1.0, F32), segment[:-1]])
    mask_rows = jnp.stack(
        [
            segment,
            (chunked == before[:, None]).astype(F32).reshape(-1),
            (chunked == chunked[:, -1:]).astype(F32).reshape(-1),
            (segment == previous).astype(F32),
        ]
        + [jnp.zeros_like(segment)] * 4
    )

    inputs = inputs.astype(F32)
    scale_one = rms_scale(inputs)
    plain_one = inputs * scale_one
    normed = (plain_one * gain_one).astype(BF16)
    mixer_pre = dot_nn(normed, w_mixer)
    joined = mixer_pre.astype(BF16)
    if copies > 1:
        joined = jnp.concatenate(
            [whole_head(joined[:, at * part : (at + 1) * part]) for at in range(3)], axis=1
        )
    swish_pre = whole_head(dot_nn(normed, w_swish))
    reduced = dot_nt(normed, w_squeeze).astype(BF16)
    forget_logit = dot_nt(expand_head, reduced) + bias_head.astype(F32)[:, None]
    log_rate = jax.nn.log_sigmoid(forget_logit) / TAU_GATE
    rates = jnp.concatenate([log_rate, -jnp.expm1(log_rate)], axis=0)
    order = mine.reshape(1).astype(jnp.int32)
    mixed, choice, starts = mixer_forward(order, ring, joined, rates, mask_rows)
    mixed, grad_out = lax.optimization_barrier((mixed, grad_out))
    head_factor = rms_scale(mixed)
    head_plain = mixed * head_factor
    head_normed = head_plain * gain_head
    swish_sig = jax.nn.sigmoid(swish_pre)
    swish_act = swish_pre * swish_sig
    gated = own_part((head_normed * swish_act).astype(BF16))
    terms = dot_nn(gated, w_output).astype(BF16)
    if ring == 4:
        feed_in, hidden = fold(
            finish_forward,
            terms.reshape(ring, rows, width),
            (input_own, gain_two[None]),
            (jax.ShapeDtypeStruct((rows, width), F32),),
            "fold_forward",
        )
        feed_in = feed_in.reshape(length, width)
    else:
        hidden = input_own.astype(F32) + scattered(terms, ring)
        feed_in = gathered((hidden * rms_scale(hidden) * gain_two).astype(BF16), ring)

    gate_pre, up_pre = dot_nn(feed_in, w_gate), dot_nn(feed_in, w_up)
    gate_sig = jax.nn.sigmoid(gate_pre)
    gate_act = gate_pre * gate_sig
    inner = (gate_act * up_pre).astype(BF16)

    term_down = dot_tn(inner, grad_out).astype(BF16)
    grad_inner = dot_nt(after(grad_out, term_down), w_down)
    grad_gatepre = grad_inner * up_pre * (gate_sig * (1.0 + gate_pre * (1.0 - gate_sig)))
    grad_gatepre = grad_gatepre.astype(BF16)
    grad_uppre = (grad_inner * gate_act).astype(BF16)
    back_feedin = (dot_nt(grad_gatepre, w_gate) + dot_nt(grad_uppre, w_up)).astype(BF16)
    feed_rows = after(feed_in, back_feedin)
    term_gate = dot_tn(feed_rows, grad_gatepre).astype(BF16)
    term_up = dot_tn(feed_rows, grad_uppre).astype(BF16)
    result_terms = dot_nn(inner, w_down).astype(BF16)
    result = hidden + scattered(result_terms, ring)
    layer_output = result.astype(BF16).reshape(1, rows, width)
    down_share = lax.psum_scatter(term_down, "batch", scatter_dimension=0, tiled=True)
    if ring != 4:
        term_gate, term_up = line_major(term_gate), line_major(term_up)
    gate_sum = lax.psum_scatter(
        after(term_gate, down_share), "batch", scatter_dimension=0, tiled=True
    )
    up_sum = lax.psum_scatter(
        after(term_up, down_share), "batch", scatter_dimension=0, tiled=True
    )
    if ring == 4:
        grad_branch, grad_hidden, term_feed = fold(
            finish_backward,
            after(back_feedin, term_gate, term_up).reshape(ring, rows, width),
            (grad_own, hidden, gain_two[None]),
            (
                jax.ShapeDtypeStruct((rows, width), F32),
                jax.ShapeDtypeStruct((1, width), F32),
            ),
            "fold_backward",
        )
        grad_branch, term_feed = grad_branch.reshape(length, width), term_feed[0]
    else:
        grad_feedin = scattered(back_feedin, ring)
        scale_two = rms_scale(hidden)
        term_feed = jnp.sum(grad_feedin * hidden * scale_two, axis=0)
        scaled_two = grad_feedin * gain_two
        grad_hidden = (
            grad_own.astype(F32)
            + scale_two * scaled_two
            - hidden * scale_two**3 * jnp.mean(scaled_two * hidden, axis=-1, keepdims=True)
        )
        grad_branch = gathered(grad_hidden.astype(BF16), ring)

    grad_gated = whole_head(dot_nt(grad_branch, w_output))
    term_output = dot_tn(gated, grad_branch).astype(BF16)

    slope = swish_sig * (1.0 + swish_pre * (1.0 - swish_sig))
    grad_swishpre = own_part((grad_gated * head_normed * slope).astype(BF16))
    grad_normed_head = grad_gated * swish_act
    term_head = jnp.sum(grad_normed_head * head_plain, axis=0) / copies
    scaled_head = grad_normed_head * gain_head
    grad_mixed = head_factor * scaled_head - mixed * head_factor**3 * jnp.mean(
        scaled_head * mixed, axis=-1, keepdims=True
    )
    grad_pre, grad_rate = mixer_backward(
        order, ring, joined, grad_mixed.astype(BF16), rates, mask_rows, choice, starts
    )
    grad_logit = (grad_rate * jax.nn.sigmoid(-forget_logit) / TAU_GATE).astype(BF16)
    term_bias = jnp.sum(grad_logit.astype(F32), axis=1) / copies
    term_expand = dot_nn(grad_logit, reduced) / copies
    grad_reduced = (dot_tn(grad_logit, expand_head) / copies).astype(BF16)
    if copies > 1:
        grad_pre = jnp.concatenate(
            [own_part(grad_pre[:, at * head_size : (at + 1) * head_size]) for at in range(3)], axis=1
        )
    grad_normed = (
        dot_nt(grad_pre, w_mixer) + dot_nt(grad_swishpre, w_swish) + dot_nn(grad_reduced, w_squeeze)
    )
    term_pre = dot_tn(normed, jnp.concatenate([grad_pre, grad_swishpre], axis=1)).astype(BF16)
    term_mixer = (jnp.sum(grad_normed * plain_one, axis=0))
    term_squeeze = (dot_tn(grad_reduced, normed))
    def placed(array, size):
        full = jnp.zeros((HEADS, size) + array.shape[1:], F32)
        return lax.dynamic_update_slice_in_dim(full, array[None], head, 0)

    terms = jnp.concatenate(
        [
            term_mixer.reshape(devices, -1),
            placed(term_head, head_size).reshape(devices, -1),
            term_feed.reshape(devices, -1),
            placed(term_bias, SLOTS).reshape(devices, -1),
            placed(term_expand, SLOTS).reshape(devices, -1),
            term_squeeze.T.reshape(devices, -1),
        ],
        axis=1,
    )
    inputs_own = input_own.astype(F32)
    if ring == 4:
        padded = jnp.pad(terms, ((0, 0), (0, -terms.shape[1] % 1024)))
        outs = finish(
            lines,
            term_pre.reshape(ring, lines, own, width),
            term_output.reshape(lines, own, width),
            after(grad_normed.astype(BF16), layer_output).reshape(ring, rows, width),
            gate_sum.reshape(ring, own, hidden_part),
            up_sum.reshape(ring, own, hidden_part),
            padded.reshape(ring, lines, -1, 128),
            input_own,
            gain_one[None],
            grad_hidden,
        )
        query_share, key_share, value_share, swish_share, output_share, gate_share, up_share = outs[:7]
        grad_input, share = outs[7], outs[8].reshape(-1)[: terms.shape[1]]
    else:
        share = halved(halved(terms, "seq"), "batch")[0]
        grad_normed = scattered(grad_normed.astype(BF16), ring)
        scale_own = rms_scale(inputs_own)
        scaled_one = grad_normed * gain_one
        grad_input = (
            grad_hidden
            + scale_own * scaled_one
            - inputs_own * scale_own**3 * jnp.mean(scaled_one * inputs_own, axis=-1, keepdims=True)
        ).astype(BF16)
        output_share = lax.psum_scatter(term_output, "batch", scatter_dimension=0, tiled=True)
        pre_sum = lax.psum_scatter(line_major(term_pre), "batch", scatter_dimension=0, tiled=True)
        pre_share = exchanged(pre_sum.reshape(ring, own, 4 * part), mine, ring)
        pre_share = pre_share.reshape(ring, own, 4, part).transpose(2, 1, 0, 3)
        pre_share = pre_share.reshape(4, own, width).astype(F32)
        query_share, key_share, value_share, swish_share = pre_share
        gate_share, up_share = (
            exchanged(total.reshape(ring, own, hidden_part), mine, ring)
            .transpose(1, 0, 2)
            .reshape(own, -1)
            .astype(F32)
            for total in (gate_sum, up_sum)
        )
        output_share = output_share.astype(F32)
    mixer_share, head_share, feedgain_share, bias_share, expand_share, squeeze_share = jnp.split(
        share, cuts
    )
    return (
        layer_output,
        grad_input.reshape(1, rows, width),
        mixer_share,
        query_share,
        key_share,
        value_share,
        squeeze_share.reshape(own, RANK),
        expand_share.reshape(-1, RANK).T,
        bias_share,
        swish_share,
        head_share,
        output_share,
        feedgain_share,
        gate_share,
        up_share,
        down_share.astype(F32),
    )


def solution(mesh):
    rows = P(BOTH, None)
    spread = P(BOTH)
    in_specs = (
        P("batch", "seq", None),
        P("batch", "seq"),
        spread,
        rows,
        rows,
        rows,
        rows,
        P(None, BOTH),
        spread,
        rows,
        spread,
        rows,
        spread,
        rows,
        rows,
        rows,
        P("batch", "seq", None),
    )
    out_specs = (
        P("batch", "seq", None),
        P("batch", "seq", None),
        spread,
        rows,
        rows,
        rows,
        rows,
        P(None, BOTH),
        spread,
        rows,
        spread,
        rows,
        spread,
        rows,
        rows,
        rows,
    )
    return jax.shard_map(local, mesh=mesh, in_specs=in_specs, out_specs=out_specs, check_vma=False)
```

```python
import functools

import jax
import jax.numpy as jnp
import numpy as np
from jax import lax
from jax.experimental import pallas as pl
from jax.experimental.pallas import tpu as pltpu
from jax.sharding import PartitionSpec as P

HEADS = 4
SLOTS = 64
RANK = 16
EPS = 1e-06
TAU_GATE = 8.0
CHUNK = 128
SUB = 16
BOTH = ("seq", "batch")
F32 = jnp.float32
BF16 = jnp.bfloat16
HIGHEST = lax.Precision.HIGHEST


def dot_nn(left, right):
    return lax.dot_general(left, right, (((1,), (0,)), ((), ())), preferred_element_type=F32)


def dot_nt(left, right):
    return lax.dot_general(left, right, (((1,), (1,)), ((), ())), preferred_element_type=F32)


def dot_tn(left, right):
    return lax.dot_general(left, right, (((0,), (0,)), ((), ())), preferred_element_type=F32)


def exact_nn(left, right):
    return lax.dot_general(
        left, right, (((1,), (0,)), ((), ())), precision=HIGHEST, preferred_element_type=F32
    )


def exact_nt(left, right):
    return lax.dot_general(
        left, right, (((1,), (1,)), ((), ())), precision=HIGHEST, preferred_element_type=F32
    )


def halves(value):
    high = value.astype(BF16)
    return high, (value - high.astype(F32)).astype(BF16)


def split_nn(left, right):
    high, rest = halves(left)
    return dot_nn(high, right) + dot_nn(rest, right)


def split_nt(left, right):
    high, rest = halves(left)
    return dot_nt(high, right) + dot_nt(rest, right)


LEVELS = (CHUNK // SUB).bit_length() - 1


def fill_tables(sums, covers, apart):
    source = lax.broadcasted_iota(jnp.int32, (CHUNK, CHUNK), 0)
    target = lax.broadcasted_iota(jnp.int32, (CHUNK, CHUNK), 1)

    def group(at, size):
        return jnp.bitwise_and(at, CHUNK - size)

    for level in range(LEVELS):
        half = SUB << level
        right = jnp.bitwise_and(target, half) != 0
        edge = group(target, 2 * half) + (half - 1)
        low, high = jnp.where(right, edge, target), jnp.where(right, target, edge)
        sums[:, level * CHUNK : (level + 1) * CHUNK] = jnp.where(
            (source > low) & (source <= high), 1.0, 0.0
        )
        same = group(source, 2 * half) == group(target, 2 * half)
        covers[level] = jnp.where(same & (jnp.bitwise_and(source, half) == 0) & right, 1.0, 0.0)
    sums[:, LEVELS * CHUNK : (LEVELS + 1) * CHUNK] = jnp.where(source <= target, 1.0, 0.0)
    sums[:, (LEVELS + 1) * CHUNK :] = jnp.where(source > target, 1.0, 0.0)
    apart[...] = jnp.where(group(source, SUB) == group(target, SUB), target - source, -1)


TABLES = [
    pltpu.VMEM((CHUNK, (LEVELS + 2) * CHUNK), F32),
    pltpu.VMEM((LEVELS, CHUNK, CHUNK), F32),
    pltpu.VMEM((CHUNK, CHUNK), jnp.int32),
]


def same_document(rows):
    source = lax.broadcasted_iota(jnp.int32, (CHUNK, CHUNK), 0)
    target = lax.broadcasted_iota(jnp.int32, (CHUNK, CHUNK), 1)
    number = rows[0:1, :]
    column = jnp.sum(jnp.where(source == target, number, 0.0), axis=1, keepdims=True)
    return column == number


def rolled(value, by):
    return value if by % CHUNK == 0 else pltpu.roll(value, by % CHUNK, 1)


def exponents(rate, sums):
    return jnp.exp(exact_nn(rate, sums))


def piece(value, at):
    return value[:, at * CHUNK : (at + 1) * CHUNK]


def mixer_forward_kernel(
    factor, mine, query, key, value, rate, rows, output, choice_out, start_out, state, sums, covers, apart
):
    levels = LEVELS

    @pl.when(pl.program_id(0) == 0)
    def _():
        state[...] = jnp.zeros_like(state)
        fill_tables(sums, covers, apart)

    key_in, value_in = state[:SLOTS, :], state[SLOTS:, :]
    start_out[0] = state[...]
    q, k, v = query[...], key[...], value[...]
    a, g = rate[:SLOTS, :], rate[SLOTS:, :]
    decay = exponents(a, sums[...])
    before, after = piece(decay, levels), piece(decay, levels + 1)
    carried = before * rows[1:2, :]
    visible = same_document(rows)
    scores = jnp.where(visible, dot_nt(k, q) * factor, 0.0)
    logits = carried * (split_nt(key_in, q) * factor)
    for level in range(levels):
        part = piece(decay, level)
        logits = logits + part * exact_nn(part * g, scores * covers[level])
    gap = apart[...]
    total = jnp.zeros_like(a)
    weights = []
    for by in range(SUB):
        if by:
            total = total + rolled(a, by - 1)
        weight = jnp.exp(total) * rolled(g, by)
        weights.append(weight)
        logits = logits + weight * jnp.sum(
            jnp.where(gap == by, scores, 0.0), axis=0, keepdims=True
        )
    attention = jnp.exp(logits - jnp.max(logits, axis=0, keepdims=True))
    attention = attention / jnp.sum(attention, axis=0, keepdims=True)
    choice_out[:SLOTS, :] = attention
    choice_out[SLOTS:, :] = logits
    mixing = jnp.zeros((CHUNK, CHUNK), F32)
    for level in range(levels):
        part = piece(decay, level)
        mixing = mixing + covers[level] * dot_tn(
            (part * g).astype(BF16), (part * attention).astype(BF16)
        )
    for by in range(SUB):
        row = jnp.sum(weights[by] * attention, axis=0, keepdims=True)
        mixing = jnp.where(gap == by, row, mixing)
    mixing = jnp.where(visible, mixing, 0.0).astype(BF16)
    output[...] = dot_tn(mixing, v) + dot_tn(
        (carried * attention).astype(BF16), value_in.astype(BF16)
    )
    ends = after * g * rows[2:3, :]
    keep = carried[:, CHUNK - 1 : CHUNK]
    state[:SLOTS, :] = keep * key_in + split_nn(ends, k)
    state[SLOTS:, :] = keep * value_in + split_nn(ends, v)


def mixer_backward_kernel(
    factor, mine, query, key, value, grad_output, rate, rows, choice, start, grad_all, grad_rate,
    state_grad, flow, sums, covers, apart,
):
    levels = LEVELS

    @pl.when(pl.program_id(0) == 0)
    def _():
        state_grad[...] = jnp.zeros_like(state_grad)
        flow[...] = jnp.zeros_like(flow)
        fill_tables(sums, covers, apart)

    key_in, value_in = start[0, :SLOTS, :], start[0, SLOTS:, :]
    key_after, value_after = state_grad[:SLOTS, :], state_grad[SLOTS:, :]
    q, k, v, d = query[...], key[...], value[...], grad_output[...]
    size = q.shape[1]
    a, g = rate[:SLOTS, :], rate[SLOTS:, :]
    attention, logits = choice[:SLOTS, :], choice[SLOTS:, :]
    decay = exponents(a, sums[...])
    before, after = piece(decay, levels), piece(decay, levels + 1)
    carried = before * rows[1:2, :]
    visible = same_document(rows)
    scores = jnp.where(visible, dot_nt(k, q) * factor, 0.0)
    reads = jnp.where(visible, dot_nt(v, d), 0.0)
    gap = apart[...]
    grad_att = carried * split_nt(value_in, d)
    for level in range(levels):
        part = piece(decay, level)
        grad_att = grad_att + part * exact_nn(part * g, reads * covers[level])
    total = jnp.zeros_like(a)
    bare, weights, score_rows, read_rows = [], [], [], []
    for by in range(SUB):
        if by:
            total = total + rolled(a, by - 1)
        bare.append(jnp.exp(total))
        weights.append(bare[by] * rolled(g, by))
        score_rows.append(jnp.sum(jnp.where(gap == by, scores, 0.0), axis=0, keepdims=True))
        read_rows.append(jnp.sum(jnp.where(gap == by, reads, 0.0), axis=0, keepdims=True))
        grad_att = grad_att + weights[by] * read_rows[by]
    grad_logits = attention * (
        grad_att - jnp.sum(attention * grad_att, axis=0, keepdims=True)
    )
    mixing = jnp.zeros((CHUNK, CHUNK), F32)
    spread = jnp.zeros((CHUNK, CHUNK), F32)
    ends = after * rows[2:3, :]
    grad_inflow = ends * (split_nt(key_after, k) + split_nt(value_after, v))
    for level in range(levels):
        part = piece(decay, level)
        left = (part * g).astype(BF16)
        att_part, log_part = part * attention, part * grad_logits
        mixing = mixing + covers[level] * dot_tn(left, att_part.astype(BF16))
        spread = spread + covers[level] * dot_tn(left, log_part.astype(BF16))
        grad_inflow = grad_inflow + part * (
            exact_nt(log_part, scores * covers[level]) + exact_nt(att_part, reads * covers[level])
        )
    for by in range(SUB):
        row = jnp.sum(weights[by] * attention, axis=0, keepdims=True)
        mixing = jnp.where(gap == by, row, mixing)
        row = jnp.sum(weights[by] * grad_logits, axis=0, keepdims=True)
        spread = jnp.where(gap == by, row, spread)
        terms = bare[by] * (grad_logits * score_rows[by] + attention * read_rows[by])
        grad_inflow = grad_inflow + rolled(terms, -by)
    mixing = jnp.where(visible, mixing, 0.0).astype(BF16)
    spread = (jnp.where(visible, spread, 0.0) * factor).astype(BF16)
    log_carried = carried * grad_logits * factor
    att_carried = carried * attention
    ends = (ends * g).astype(BF16)
    grad_all[:, :size] = (
        dot_tn(spread, k) + dot_tn(log_carried.astype(BF16), key_in.astype(BF16))
    ).astype(BF16)
    grad_all[:, size : 2 * size] = (dot_nn(spread, q) + dot_tn(ends, key_after.astype(BF16))).astype(BF16)
    grad_all[:, 2 * size :] = (dot_nn(mixing, d) + dot_tn(ends, value_after.astype(BF16))).astype(BF16)
    change = grad_logits * logits + attention * grad_att - g * grad_inflow
    later = piece(sums, levels + 1) + jnp.where(gap == 0, 1.0, 0.0)
    same = jnp.where(visible, later, 0.0)
    flows = exact_nn(change, same) + rows[2:3, :] * flow[:, 0:1]
    grad_rate[...] = rows[3:4, :] * flows - jnp.exp(a) * grad_inflow
    keep = carried[:, CHUNK - 1 : CHUNK]
    key_before = keep * key_after + split_nn(log_carried, q)
    value_before = keep * value_after + split_nn(att_carried, d)
    state_grad[:SLOTS, :] = key_before
    state_grad[SLOTS:, :] = value_before
    flow[...] = jnp.broadcast_to(
        jnp.sum(key_before * key_in + value_before * value_in, axis=1, keepdims=True), flow.shape
    )


def mixer_specs(length, size, ring, backward):
    count = length // CHUNK
    per = count // ring

    def natural(step):
        return count - 1 - step if backward else step

    def moved(step, mine):
        at = natural(step)
        return lax.bitwise_xor(at // per, mine[0]) * per + at % per

    wide = [
        pl.BlockSpec((CHUNK, size), lambda step, mine, at=at: (moved(step, mine), at))
        for at in range(3)
    ]
    everything = pl.BlockSpec((CHUNK, 3 * size), lambda step, mine: (moved(step, mine), 0))
    pair = pl.BlockSpec((2 * SLOTS, CHUNK), lambda step, mine: (0, moved(step, mine)))
    slim = pl.BlockSpec((SLOTS, CHUNK), lambda step, mine: (0, moved(step, mine)))
    rows = pl.BlockSpec((8, CHUNK), lambda step, mine: (0, natural(step)))
    state = pl.BlockSpec((1, 2 * SLOTS, size), lambda step, mine: (natural(step), 0, 0))
    return count, wide, everything, pair, slim, rows, state


def mixer_forward(mine, ring, size, joined, rates, rows):
    length = joined.shape[0]
    count, wide, _, pair, _, row_spec, state = mixer_specs(length, size, ring, False)
    return pl.pallas_call(
        functools.partial(mixer_forward_kernel, size ** (-0.25)),
        out_shape=(
            jax.ShapeDtypeStruct((length, size), F32),
            jax.ShapeDtypeStruct((2 * SLOTS, length), F32),
            jax.ShapeDtypeStruct((count, 2 * SLOTS, size), F32),
        ),
        grid_spec=pltpu.PrefetchScalarGridSpec(
            num_scalar_prefetch=1,
            grid=(count,),
            in_specs=wide + [pair, row_spec],
            out_specs=[wide[0], pair, state],
            scratch_shapes=[pltpu.VMEM((2 * SLOTS, size), F32)] + TABLES,
        ),
        compiler_params=pltpu.CompilerParams(vmem_limit_bytes=32 << 20),
        cost_estimate=pl.CostEstimate(
            flops=length * size * 2000, bytes_accessed=length * size * 12, transcendentals=length * 4096
        ),
        name="mixer_forward",
    )(mine, joined, joined, joined, rates, rows)


def mixer_backward(mine, ring, joined, grad, rates, rows, choice, starts):
    length, size = grad.shape
    count, wide, everything, pair, slim, row_spec, state = mixer_specs(length, size, ring, True)
    return pl.pallas_call(
        functools.partial(mixer_backward_kernel, size ** (-0.25)),
        out_shape=(
            jax.ShapeDtypeStruct((length, 3 * size), BF16),
            jax.ShapeDtypeStruct((SLOTS, length), F32),
        ),
        grid_spec=pltpu.PrefetchScalarGridSpec(
            num_scalar_prefetch=1,
            grid=(count,),
            in_specs=wide + [wide[0], pair, row_spec, pair, state],
            out_specs=[everything, slim],
            scratch_shapes=[pltpu.VMEM((2 * SLOTS, size), F32), pltpu.VMEM((SLOTS, 128), F32)]
            + TABLES,
        ),
        compiler_params=pltpu.CompilerParams(vmem_limit_bytes=32 << 20),
        cost_estimate=pl.CostEstimate(
            flops=length * size * 4000, bytes_accessed=length * size * 20, transcendentals=length * 4096
        ),
        name="mixer_backward",
    )(mine, joined, joined, joined, grad, rates, rows, choice, starts)


def peers(ring, mine):
    found = []
    for by in range(1, ring):
        at, bit = mine, 1
        while bit <= by:
            if by & bit:
                at = at + bit * (1 - 2 * ((at // bit) % 2))
            bit *= 2
        found.append(at)
    return found


class Copies:
    def __init__(self, local, send, recv):
        self.local, self.send, self.recv = local, send, recv
        self.here, self.away = 0, 0
        self.open = []

    def near(self, source, target):
        copy = pltpu.make_async_copy(source, target, self.local.at[self.here])
        self.here += 1
        copy.start()
        return copy

    def far(self, source, target, landed, device, when=None):
        at = self.away
        self.away += 1
        copy = pltpu.make_async_remote_copy(
            source, target, self.send.at[at], self.recv.at[at], device_id=device,
            device_id_type=pl.DeviceIdType.MESH,
        )
        if when is None:
            copy.start()
        else:
            pl.when(when)(copy.start)
        self.open.append((copy, when))
        return pltpu.make_async_remote_copy(
            landed, landed, self.send.at[at], self.recv.at[at], device_id=device,
            device_id_type=pl.DeviceIdType.MESH,
        ).wait_recv

    def close(self):
        for copy, when in self.open:
            if when is None:
                copy.wait_send()
            else:
                pl.when(when)(copy.wait_send)


PARTS = 4


def fold_kernel(finish, extras, *refs):
    terms, given = refs[0], refs[1 : 1 + extras]
    blocks = refs[1 + extras]
    made = refs[2 + extras : -9]
    first, second, third, two_low, one_high, own, local_sem, send_sem, recv_sem = refs[-9:]
    mine, batch = lax.axis_index("seq"), lax.axis_index("batch")
    others = peers(4, mine)
    row, col = (others[0], batch), (others[1], batch)
    copies = Copies(local_sem, send_sem, recv_sem)
    size = terms.shape[1] // PARTS

    def span(at):
        low = pl.ds(at * size, size // 2)
        return pl.ds(at * size, size), low, pl.ds(at * size + size // 2, size // 2)

    opening, direct = [], []

    def open_part(at):
        _, low, high = span(at)
        opening.append(
            (
                copies.far(terms.at[3, low], first.at[low], first.at[low], row),
                copies.far(terms.at[3, high], first.at[high], first.at[high], col),
            )
        )

    def pass_part(at):
        _, low, high = span(at)
        waits = [
            copies.far(terms.at[2, high], second.at[high], second.at[high], col),
            copies.far(terms.at[1, low], third.at[low], third.at[low], row),
        ]
        opening[at][0]()
        two_low[low, :] = added(terms[2, low, :], first[low, :])
        waits.append(copies.far(two_low.at[low], second.at[low], second.at[low], col))
        opening[at][1]()
        one_high[high, :] = added(terms[1, high, :], first[high, :])
        waits.append(copies.far(one_high.at[high], third.at[high], third.at[high], row))
        direct.append(waits)

    spread, local, passed = [], [], []

    def close_part(at):
        full, _, _ = span(at)
        for wait in direct[at]:
            wait()
        total = terms[0, full, :].astype(F32) + second[full, :].astype(F32) + third[full, :].astype(F32)
        own[full, :] = finish(total, full, at, given, made)
        spread.append(
            (
                copies.far(own.at[full], blocks.at[1, full], blocks.at[1, full], row),
                copies.far(own.at[full], blocks.at[2, full], blocks.at[2, full], col),
            )
        )
        local.append(copies.near(own.at[full], blocks.at[0, full]))

    def forward_part(at):
        _, low, high = span(at)
        for wait in spread[at]:
            wait()
        passed.append(copies.far(blocks.at[2, low], blocks.at[3, low], blocks.at[3, low], row))
        passed.append(copies.far(blocks.at[1, high], blocks.at[3, high], blocks.at[3, high], col))

    open_part(0)
    for at in range(PARTS + 2):
        if at + 1 < PARTS:
            open_part(at + 1)
        if at < PARTS:
            pass_part(at)
        if 1 <= at <= PARTS:
            close_part(at - 1)
        if at >= 2:
            forward_part(at - 2)
    for wait in passed:
        wait()
    for copy in local:
        copy.wait()
    copies.close()


def half_blocks(value, order):
    lane = lax.broadcasted_iota(jnp.int32, (value.shape[0], 128), 1)
    made = []
    for pair in zip(order[::2], order[1::2]):
        low, high = (
            value[:, block * 128 : (block + 1) * 128]
            if half == want
            else pltpu.roll(value[:, block * 128 : (block + 1) * 128], 64, 1)
            for want, (block, half) in enumerate(pair)
        )
        made.append(jnp.where(lane < 64, low, high))
    return jnp.concatenate(made, axis=1)


def by_line(value):
    lines = value.shape[1] // 256
    return half_blocks(
        value, [divmod(ring * lines + line, 2) for line in range(lines) for ring in range(4)]
    )


def by_ring(value):
    lines = value.shape[1] // 256
    return half_blocks(
        value, [divmod(line * 4 + ring, 2) for ring in range(4) for line in range(lines)]
    )


def finish_forward(total, full, at, given, made):
    inputs, gain = given
    hidden = inputs[full, :].astype(F32) + total
    made[0][full, :] = hidden
    return by_line(hidden * rms_scale(hidden) * gain[...]).astype(BF16)


def finish_backward(total, full, at, given, made):
    cotangent, hidden_ref, gain = given
    total = by_ring(total)
    hidden = hidden_ref[full, :]
    scale = rms_scale(hidden)
    plain = hidden * scale
    term = jnp.sum(total * plain, axis=0, keepdims=True)
    made[1][...] = term if at == 0 else made[1][...] + term
    scaled = total * gain[...]
    grad = (
        cotangent[full, :].astype(F32)
        + scale * scaled
        - plain * (scale * jnp.mean(scaled * plain, axis=-1, keepdims=True))
    )
    made[0][full, :] = grad
    return grad.astype(BF16)


def fold(finish, terms, given, made, name):
    ring, rows, width = terms.shape
    inside = pl.BlockSpec(memory_space=pltpu.VMEM)
    block = pltpu.VMEM((rows, width), BF16)
    return pl.pallas_call(
        functools.partial(fold_kernel, finish, len(given)),
        out_shape=(jax.ShapeDtypeStruct((ring, rows, width), BF16),) + made,
        in_specs=[inside] * (1 + len(given)),
        out_specs=[pl.BlockSpec(memory_space=pltpu.HBM)] + [inside] * len(made),
        scratch_shapes=[block] * 6
        + [
            pltpu.SemaphoreType.DMA((PARTS,)),
            pltpu.SemaphoreType.DMA((PARTS * 10,)),
            pltpu.SemaphoreType.DMA((PARTS * 10,)),
        ],
        compiler_params=pltpu.CompilerParams(has_side_effects=True, vmem_limit_bytes=40 << 20),
        name=name,
    )(terms, *given)


def rms_scale(features):
    return lax.rsqrt(jnp.mean(features * features, axis=-1, keepdims=True) + EPS)


def swapped(block, by, ring):
    return lax.ppermute(block, "seq", [(i, i ^ by) for i in range(ring)])


def gathered(block, ring):
    if ring != 4:
        return jnp.concatenate([block] + [swapped(block, by, ring) for by in range(1, ring)], axis=0)
    half = block.shape[0] // 2
    one, two = swapped(block, 1, ring), swapped(block, 2, ring)
    low, high = swapped(two[:half], 1, ring), swapped(one[half:], 2, ring)
    return jnp.concatenate([block, one, two, low, high], axis=0)


def scattered(terms, ring):
    rows = terms.shape[0] // ring
    parts = [terms[by * rows : (by + 1) * rows] for by in range(ring)]
    total = parts[0].astype(F32)
    if ring != 4:
        for by in range(1, ring):
            total = total + swapped(parts[by], by, ring).astype(F32)
        return total
    half = rows // 2
    low, high = swapped(parts[3][:half], 1, ring), swapped(parts[3][half:], 2, ring)
    two = jnp.concatenate([added(parts[2][:half], low), parts[2][half:]], axis=0)
    one = jnp.concatenate([parts[1][:half], added(parts[1][half:], high)], axis=0)
    return total + swapped(one, 1, ring).astype(F32) + swapped(two, 2, ring).astype(F32)


def added(left, right):
    return (left.astype(F32) + right.astype(F32)).astype(BF16)


def flipped(block, axis, by):
    return lax.ppermute(block, axis, [(i, i ^ by) for i in range(lax.axis_size(axis))])


def doubled(block, axis):
    by, mine = 1, lax.axis_index(axis)
    while by < lax.axis_size(axis):
        other = flipped(block, axis, by)
        first = (mine & by) == 0
        block = jnp.concatenate(
            [jnp.where(first, block, other), jnp.where(first, other, block)], axis=0
        )
        by *= 2
    return block


def halved(block, axis):
    by, mine = lax.axis_size(axis) // 2, lax.axis_index(axis)
    while by:
        low, high = jnp.split(block, 2, axis=0)
        first = (mine & by) == 0
        block = jnp.where(first, low, high) + flipped(jnp.where(first, high, low), axis, by)
        by //= 2
    return block


def after(value, *others):
    return lax.optimization_barrier((value,) + others)[0]


def exchanged(blocks, mine, ring):
    parts = [
        swapped(lax.dynamic_index_in_dim(blocks, mine ^ by, 0, keepdims=False), by, ring)
        if by
        else lax.dynamic_index_in_dim(blocks, mine, 0, keepdims=False)
        for by in range(ring)
    ]
    made = jnp.stack(parts)
    return jnp.concatenate(
        [lax.dynamic_index_in_dim(made, mine ^ j, 0, keepdims=True) for j in range(ring)], axis=0
    )


def local(
    layer_input,
    segments,
    mixer_gain,
    query_weight,
    key_weight,
    value_weight,
    squeeze,
    expand,
    forget_bias,
    swish_weight,
    head_gain,
    output_weight,
    feed_gain,
    gate_weight,
    up_weight,
    down_weight,
    cotangent,
):
    ring, lines = lax.axis_size("seq"), lax.axis_size("batch")
    devices = ring * lines
    mine = lax.axis_index("seq")
    rows, width = layer_input.shape[1], layer_input.shape[2]
    length = rows * ring
    own = width // devices
    head_size = width // HEADS
    copies = ring // HEADS
    part = width // ring
    head = mine // copies
    hidden_part = gate_weight.shape[1] // ring
    slots_all = HEADS * SLOTS

    def to_order(array):
        if copies == 1:
            return array
        blocks = array.reshape((ring, rows) + array.shape[1:])
        moved = [lax.dynamic_index_in_dim(blocks, mine ^ by, 0, keepdims=False) for by in range(ring)]
        return jnp.concatenate(moved, axis=0)

    def whole_head(array):
        if copies == 1:
            return array
        full = lax.all_gather(to_order(array), "seq", axis=1, tiled=True)
        return to_order(lax.dynamic_slice_in_dim(full, head * head_size, head_size, 1))

    def own_part(array):
        if copies == 1:
            return array
        return lax.dynamic_slice_in_dim(array, (mine % copies) * part, part, 1)

    params = jnp.concatenate(
        [
            mixer_gain,
            head_gain,
            feed_gain,
            forget_bias,
            expand.T.reshape(-1),
            squeeze.reshape(-1),
        ]
    )
    count = params.shape[0]
    params = jnp.concatenate([params, segments.reshape(rows).astype(BF16)])
    input_own = layer_input.reshape(rows, width)
    grad_own = cotangent.reshape(rows, width)

    def permuted(array):
        shape = array.shape[:-1]
        array = array.reshape(shape + (ring, lines, own))
        return jnp.swapaxes(array, -3, -2).reshape(shape + (width,))

    def restored(array):
        shape = array.shape[:-1]
        array = array.reshape(shape + (lines, ring, own))
        return jnp.swapaxes(array, -3, -2).reshape(shape + (width,))

    def columns(*arrays):
        blocks = [a.reshape(own, ring, a.shape[1] // ring) for a in arrays]
        return jnp.concatenate(blocks, axis=2).transpose(1, 0, 2)

    w_output = lax.all_gather(output_weight, "batch", axis=0, tiled=True)
    mixer_columns = exchanged(
        columns(query_weight, key_weight, value_weight, swish_weight), mine, ring
    )
    w_mixer = lax.all_gather(mixer_columns.reshape(ring * own, -1), "batch", axis=0, tiled=True)
    feed_columns = exchanged(columns(gate_weight, up_weight), mine, ring)
    w_feed = lax.all_gather(feed_columns.reshape(ring * own, -1), "batch", axis=0, tiled=True)
    w_down = lax.all_gather(after(down_weight, feed_columns), "batch", axis=0, tiled=True)
    if ring != 4:
        w_feed = w_feed.reshape(lines, ring, own, -1).transpose(1, 0, 2, 3).reshape(width, -1)

    def line_major(term):
        return term.reshape(ring, lines, own, -1).transpose(1, 0, 2, 3).reshape(width, -1)

    inputs = after(gathered(permuted(input_own), ring), w_output)
    small = doubled(doubled(params[None], "batch"), "seq")
    grad_out = gathered(after(grad_own, inputs), ring)
    small = small.reshape(devices, -1)
    segment = lax.dynamic_index_in_dim(
        small.reshape(ring, lines, -1), lax.axis_index("batch"), 1, keepdims=False
    )[:, count : count + rows].reshape(length).astype(F32)
    cuts = np.cumsum([own, own, own, slots_all // devices, RANK * slots_all // devices])
    gain_one, gain_head, gain_two, bias_full, expand_t, w_squeeze = jnp.split(
        small[:, :count], cuts, axis=1
    )
    gain_one = permuted(gain_one.reshape(width)).astype(F32)
    gain_head = lax.dynamic_slice_in_dim(gain_head.reshape(width), head * head_size, head_size, 0)
    gain_head = gain_head.astype(F32)
    gain_two = gain_two.reshape(width).astype(F32)
    bias_head = lax.dynamic_slice_in_dim(bias_full.reshape(slots_all), head * SLOTS, SLOTS, 0)
    expand_head = lax.dynamic_slice_in_dim(
        expand_t.reshape(slots_all, RANK), head * SLOTS, SLOTS, 0
    )
    w_squeeze = permuted(w_squeeze.reshape(width, RANK).T)

    chunked = segment.reshape(-1, CHUNK)
    before = jnp.concatenate([jnp.full((1,), -1.0, F32), chunked[:-1, -1]])
    previous = jnp.concatenate([jnp.full((1,), -1.0, F32), segment[:-1]])
    mask_rows = jnp.stack(
        [
            segment,
            (chunked == before[:, None]).astype(F32).reshape(-1),
            (chunked == chunked[:, -1:]).astype(F32).reshape(-1),
            (segment == previous).astype(F32),
        ]
        + [jnp.zeros_like(segment)] * 4
    )

    inputs = inputs.astype(F32)
    scale_one = rms_scale(inputs)
    plain_one = inputs * scale_one
    normed = (plain_one * gain_one).astype(BF16)
    mixer_pre = dot_nn(normed, w_mixer)
    joined = mixer_pre.astype(BF16)
    if copies > 1:
        joined = jnp.concatenate(
            [whole_head(joined[:, at * part : (at + 1) * part]) for at in range(3)], axis=1
        )
    swish_pre = whole_head(mixer_pre[:, 3 * part :])
    reduced = dot_nt(normed, w_squeeze).astype(BF16)
    forget_logit = dot_nt(expand_head, reduced) + bias_head.astype(F32)[:, None]
    log_rate = jax.nn.log_sigmoid(forget_logit) / TAU_GATE
    rates = jnp.concatenate([log_rate, -jnp.expm1(log_rate)], axis=0)
    order = mine.reshape(1).astype(jnp.int32)
    mixed, choice, starts = mixer_forward(order, ring, head_size, joined, rates, mask_rows)
    mixed, grad_out = lax.optimization_barrier((mixed, grad_out))
    head_factor = rms_scale(mixed)
    head_plain = mixed * head_factor
    head_normed = head_plain * gain_head
    swish_sig = jax.nn.sigmoid(swish_pre)
    swish_act = swish_pre * swish_sig
    gated = own_part((head_normed * swish_act).astype(BF16))
    terms = dot_nn(gated, w_output).astype(BF16)
    if ring == 4:
        feed_in, hidden = fold(
            finish_forward,
            terms.reshape(ring, rows, width),
            (input_own, gain_two[None]),
            (jax.ShapeDtypeStruct((rows, width), F32),),
            "fold_forward",
        )
        feed_in = feed_in.reshape(length, width)
    else:
        hidden = input_own.astype(F32) + scattered(terms, ring)
        feed_in = gathered((hidden * rms_scale(hidden) * gain_two).astype(BF16), ring)

    feed_pre = dot_nn(feed_in, w_feed)
    gate_pre, up_pre = feed_pre[:, :hidden_part], feed_pre[:, hidden_part:]
    gate_sig = jax.nn.sigmoid(gate_pre)
    gate_act = gate_pre * gate_sig
    inner = (gate_act * up_pre).astype(BF16)

    term_down = dot_tn(inner, grad_out).astype(BF16)
    grad_inner = dot_nt(after(grad_out, term_down), w_down)
    grad_gatepre = grad_inner * up_pre * (gate_sig * (1.0 + gate_pre * (1.0 - gate_sig)))
    grad_feedpre = jnp.concatenate(
        [grad_gatepre.astype(BF16), (grad_inner * gate_act).astype(BF16)], axis=1
    )
    back_feedin = dot_nt(grad_feedpre, w_feed).astype(BF16)
    term_feedpre = dot_tn(after(feed_in, back_feedin), grad_feedpre).astype(BF16)
    result_terms = dot_nn(inner, w_down).astype(BF16)
    result = hidden + scattered(result_terms, ring)
    layer_output = result.astype(BF16).reshape(1, rows, width)
    down_share = lax.psum_scatter(term_down, "batch", scatter_dimension=0, tiled=True)
    feed_terms = term_feedpre if ring == 4 else line_major(term_feedpre)
    feed_sum = lax.psum_scatter(
        after(feed_terms, down_share), "batch", scatter_dimension=0, tiled=True
    )
    if ring == 4:
        grad_branch, grad_hidden, term_feed = fold(
            finish_backward,
            after(back_feedin, term_feedpre).reshape(ring, rows, width),
            (grad_own, hidden, gain_two[None]),
            (
                jax.ShapeDtypeStruct((rows, width), F32),
                jax.ShapeDtypeStruct((1, width), F32),
            ),
            "fold_backward",
        )
        grad_branch, term_feed = grad_branch.reshape(length, width), term_feed[0]
    else:
        grad_feedin = scattered(back_feedin, ring)
        scale_two = rms_scale(hidden)
        term_feed = jnp.sum(grad_feedin * hidden * scale_two, axis=0)
        scaled_two = grad_feedin * gain_two
        grad_hidden = (
            grad_own.astype(F32)
            + scale_two * scaled_two
            - hidden * scale_two**3 * jnp.mean(scaled_two * hidden, axis=-1, keepdims=True)
        )
        grad_branch = gathered(grad_hidden.astype(BF16), ring)

    grad_gated = whole_head(dot_nt(grad_branch, w_output))
    term_output = dot_tn(gated, grad_branch).astype(BF16)

    slope = swish_sig * (1.0 + swish_pre * (1.0 - swish_sig))
    grad_swishpre = own_part((grad_gated * head_normed * slope).astype(BF16))
    grad_normed_head = grad_gated * swish_act
    term_head = jnp.sum(grad_normed_head * head_plain, axis=0) / copies
    scaled_head = grad_normed_head * gain_head
    grad_mixed = head_factor * scaled_head - mixed * head_factor**3 * jnp.mean(
        scaled_head * mixed, axis=-1, keepdims=True
    )
    grad_pre, grad_rate = mixer_backward(
        order, ring, joined, grad_mixed.astype(BF16), rates, mask_rows, choice, starts
    )
    grad_logit = (grad_rate * jax.nn.sigmoid(-forget_logit) / TAU_GATE).astype(BF16)
    term_bias = jnp.sum(grad_logit.astype(F32), axis=1) / copies
    term_expand = dot_nn(grad_logit, reduced) / copies
    grad_reduced = (dot_tn(grad_logit, expand_head) / copies).astype(BF16)
    if copies > 1:
        grad_pre = jnp.concatenate(
            [own_part(grad_pre[:, at * head_size : (at + 1) * head_size]) for at in range(3)], axis=1
        )
    grad_pre = jnp.concatenate([grad_pre, grad_swishpre], axis=1)
    term_pre = dot_tn(normed, grad_pre).astype(BF16)
    pre_sum = lax.psum_scatter(after(term_pre, feed_sum), "batch", scatter_dimension=0, tiled=True)
    output_share = lax.psum_scatter(
        after(term_output, pre_sum), "batch", scatter_dimension=0, tiled=True
    )
    grad_normed = dot_nt(grad_pre, w_mixer) + dot_nn(grad_reduced, w_squeeze)
    term_mixer = restored(jnp.sum(grad_normed * plain_one, axis=0))
    term_squeeze = restored(dot_tn(grad_reduced, normed))
    grad_normed = restored(scattered(grad_normed.astype(BF16), ring))
    inputs_own = input_own.astype(F32)
    scale_own = rms_scale(inputs_own)
    scaled_one = grad_normed * restored(gain_one)
    grad_input = (
        grad_hidden
        + scale_own * scaled_one
        - inputs_own * scale_own**3 * jnp.mean(scaled_one * inputs_own, axis=-1, keepdims=True)
    ).astype(BF16)
    pre_share = exchanged(pre_sum.reshape(ring, own, 4 * part), mine, ring)
    pre_share = pre_share.reshape(ring, own, 4, part).transpose(2, 1, 0, 3)
    query_share, key_share, value_share, swish_share = pre_share.reshape(4, own, width).astype(F32)
    feed_share = exchanged(feed_sum.reshape(ring, own, 2 * hidden_part), mine, ring)
    gate_share = feed_share[:, :, :hidden_part].transpose(1, 0, 2).reshape(own, -1).astype(F32)
    up_share = feed_share[:, :, hidden_part:].transpose(1, 0, 2).reshape(own, -1).astype(F32)

    def placed(array, size):
        full = jnp.zeros((HEADS, size) + array.shape[1:], F32)
        return lax.dynamic_update_slice_in_dim(full, array[None], head, 0)

    terms = jnp.concatenate(
        [
            term_mixer.reshape(devices, -1),
            placed(term_head, head_size).reshape(devices, -1),
            term_feed.reshape(devices, -1),
            placed(term_bias, SLOTS).reshape(devices, -1),
            placed(term_expand, SLOTS).reshape(devices, -1),
            term_squeeze.T.reshape(devices, -1),
        ],
        axis=1,
    )
    share = halved(halved(terms, "seq"), "batch")[0]
    mixer_share, head_share, feedgain_share, bias_share, expand_share, squeeze_share = jnp.split(
        share, cuts
    )
    return (
        layer_output,
        grad_input.reshape(1, rows, width),
        mixer_share,
        query_share,
        key_share,
        value_share,
        squeeze_share.reshape(own, RANK),
        expand_share.reshape(-1, RANK).T,
        bias_share,
        swish_share,
        head_share,
        output_share.astype(F32),
        feedgain_share,
        gate_share,
        up_share,
        down_share.astype(F32),
    )


def solution(mesh):
    rows = P(BOTH, None)
    spread = P(BOTH)
    in_specs = (
        P("batch", "seq", None),
        P("batch", "seq"),
        spread,
        rows,
        rows,
        rows,
        rows,
        P(None, BOTH),
        spread,
        rows,
        spread,
        rows,
        spread,
        rows,
        rows,
        rows,
        P("batch", "seq", None),
    )
    out_specs = (
        P("batch", "seq", None),
        P("batch", "seq", None),
        spread,
        rows,
        rows,
        rows,
        rows,
        P(None, BOTH),
        spread,
        rows,
        spread,
        rows,
        spread,
        rows,
        rows,
        rows,
    )
    return jax.shard_map(local, mesh=mesh, in_specs=in_specs, out_specs=out_specs, check_vma=False)
```

```python
import functools

import jax
import jax.numpy as jnp
import numpy as np
from jax import lax
from jax.experimental import pallas as pl
from jax.experimental.pallas import tpu as pltpu
from jax.sharding import PartitionSpec as P

HEADS = 4
SLOTS = 64
RANK = 16
EPS = 1e-06
TAU_GATE = 8.0
CHUNK = 128
SUB = 16
BOTH = ("seq", "batch")
F32 = jnp.float32
BF16 = jnp.bfloat16
HIGHEST = lax.Precision.HIGHEST


def dot_nn(left, right):
    return lax.dot_general(left, right, (((1,), (0,)), ((), ())), preferred_element_type=F32)


def dot_nt(left, right):
    return lax.dot_general(left, right, (((1,), (1,)), ((), ())), preferred_element_type=F32)


def dot_tn(left, right):
    return lax.dot_general(left, right, (((0,), (0,)), ((), ())), preferred_element_type=F32)


def exact_nn(left, right):
    return lax.dot_general(
        left, right, (((1,), (0,)), ((), ())), precision=HIGHEST, preferred_element_type=F32
    )


def exact_nt(left, right):
    return lax.dot_general(
        left, right, (((1,), (1,)), ((), ())), precision=HIGHEST, preferred_element_type=F32
    )


def halves(value):
    high = value.astype(BF16)
    return high, (value - high.astype(F32)).astype(BF16)


def split_nn(left, right):
    high, rest = halves(left)
    return dot_nn(high, right) + dot_nn(rest, right)


def split_nt(left, right):
    high, rest = halves(left)
    return dot_nt(high, right) + dot_nt(rest, right)


LEVELS = (CHUNK // SUB).bit_length() - 1


def fill_tables(sums, covers, apart):
    source = lax.broadcasted_iota(jnp.int32, (CHUNK, CHUNK), 0)
    target = lax.broadcasted_iota(jnp.int32, (CHUNK, CHUNK), 1)

    def group(at, size):
        return jnp.bitwise_and(at, CHUNK - size)

    for level in range(LEVELS):
        half = SUB << level
        right = jnp.bitwise_and(target, half) != 0
        edge = group(target, 2 * half) + (half - 1)
        low, high = jnp.where(right, edge, target), jnp.where(right, target, edge)
        sums[:, level * CHUNK : (level + 1) * CHUNK] = jnp.where(
            (source > low) & (source <= high), 1.0, 0.0
        )
        same = group(source, 2 * half) == group(target, 2 * half)
        covers[level] = jnp.where(same & (jnp.bitwise_and(source, half) == 0) & right, 1.0, 0.0)
    sums[:, LEVELS * CHUNK : (LEVELS + 1) * CHUNK] = jnp.where(source <= target, 1.0, 0.0)
    sums[:, (LEVELS + 1) * CHUNK :] = jnp.where(source > target, 1.0, 0.0)
    apart[...] = jnp.where(group(source, SUB) == group(target, SUB), target - source, -1)


TABLES = [
    pltpu.VMEM((CHUNK, (LEVELS + 2) * CHUNK), F32),
    pltpu.VMEM((LEVELS, CHUNK, CHUNK), F32),
    pltpu.VMEM((CHUNK, CHUNK), jnp.int32),
]


def same_document(rows):
    source = lax.broadcasted_iota(jnp.int32, (CHUNK, CHUNK), 0)
    target = lax.broadcasted_iota(jnp.int32, (CHUNK, CHUNK), 1)
    number = rows[0:1, :]
    column = jnp.sum(jnp.where(source == target, number, 0.0), axis=1, keepdims=True)
    return column == number


def rolled(value, by):
    return value if by % CHUNK == 0 else pltpu.roll(value, by % CHUNK, 1)


def exponents(rate, sums):
    return jnp.exp(exact_nn(rate, sums))


def piece(value, at):
    return value[:, at * CHUNK : (at + 1) * CHUNK]


def mixer_forward_kernel(
    factor, mine, query, key, value, rate, rows, output, choice_out, start_out, state, sums, covers, apart
):
    levels = LEVELS

    @pl.when(pl.program_id(0) == 0)
    def _():
        state[...] = jnp.zeros_like(state)
        fill_tables(sums, covers, apart)

    key_in, value_in = state[:SLOTS, :], state[SLOTS:, :]
    start_out[0] = state[...]
    q, k, v = query[...], key[...], value[...]
    a, g = rate[:SLOTS, :], rate[SLOTS:, :]
    decay = exponents(a, sums[...])
    before, after = piece(decay, levels), piece(decay, levels + 1)
    carried = before * rows[1:2, :]
    visible = same_document(rows)
    scores = jnp.where(visible, dot_nt(k, q) * factor, 0.0)
    logits = carried * (split_nt(key_in, q) * factor)
    for level in range(levels):
        part = piece(decay, level)
        logits = logits + part * exact_nn(part * g, scores * covers[level])
    gap = apart[...]
    total = jnp.zeros_like(a)
    weights = []
    for by in range(SUB):
        if by:
            total = total + rolled(a, by - 1)
        weight = jnp.exp(total) * rolled(g, by)
        weights.append(weight)
        logits = logits + weight * jnp.sum(
            jnp.where(gap == by, scores, 0.0), axis=0, keepdims=True
        )
    attention = jnp.exp(logits - jnp.max(logits, axis=0, keepdims=True))
    attention = attention / jnp.sum(attention, axis=0, keepdims=True)
    choice_out[:SLOTS, :] = attention
    choice_out[SLOTS:, :] = logits
    mixing = jnp.zeros((CHUNK, CHUNK), F32)
    for level in range(levels):
        part = piece(decay, level)
        mixing = mixing + covers[level] * dot_tn(
            (part * g).astype(BF16), (part * attention).astype(BF16)
        )
    for by in range(SUB):
        row = jnp.sum(weights[by] * attention, axis=0, keepdims=True)
        mixing = jnp.where(gap == by, row, mixing)
    mixing = jnp.where(visible, mixing, 0.0).astype(BF16)
    output[...] = dot_tn(mixing, v) + dot_tn(
        (carried * attention).astype(BF16), value_in.astype(BF16)
    )
    ends = after * g * rows[2:3, :]
    keep = carried[:, CHUNK - 1 : CHUNK]
    state[:SLOTS, :] = keep * key_in + split_nn(ends, k)
    state[SLOTS:, :] = keep * value_in + split_nn(ends, v)


def mixer_backward_kernel(
    factor, mine, query, key, value, grad_output, rate, rows, choice, start, grad_all, grad_rate,
    state_grad, flow, sums, covers, apart,
):
    levels = LEVELS

    @pl.when(pl.program_id(0) == 0)
    def _():
        state_grad[...] = jnp.zeros_like(state_grad)
        flow[...] = jnp.zeros_like(flow)
        fill_tables(sums, covers, apart)

    key_in, value_in = start[0, :SLOTS, :], start[0, SLOTS:, :]
    key_after, value_after = state_grad[:SLOTS, :], state_grad[SLOTS:, :]
    q, k, v, d = query[...], key[...], value[...], grad_output[...]
    size = q.shape[1]
    a, g = rate[:SLOTS, :], rate[SLOTS:, :]
    attention, logits = choice[:SLOTS, :], choice[SLOTS:, :]
    decay = exponents(a, sums[...])
    before, after = piece(decay, levels), piece(decay, levels + 1)
    carried = before * rows[1:2, :]
    visible = same_document(rows)
    scores = jnp.where(visible, dot_nt(k, q) * factor, 0.0)
    reads = jnp.where(visible, dot_nt(v, d), 0.0)
    gap = apart[...]
    grad_att = carried * split_nt(value_in, d)
    for level in range(levels):
        part = piece(decay, level)
        grad_att = grad_att + part * exact_nn(part * g, reads * covers[level])
    total = jnp.zeros_like(a)
    bare, weights, score_rows, read_rows = [], [], [], []
    for by in range(SUB):
        if by:
            total = total + rolled(a, by - 1)
        bare.append(jnp.exp(total))
        weights.append(bare[by] * rolled(g, by))
        score_rows.append(jnp.sum(jnp.where(gap == by, scores, 0.0), axis=0, keepdims=True))
        read_rows.append(jnp.sum(jnp.where(gap == by, reads, 0.0), axis=0, keepdims=True))
        grad_att = grad_att + weights[by] * read_rows[by]
    grad_logits = attention * (
        grad_att - jnp.sum(attention * grad_att, axis=0, keepdims=True)
    )
    mixing = jnp.zeros((CHUNK, CHUNK), F32)
    spread = jnp.zeros((CHUNK, CHUNK), F32)
    ends = after * rows[2:3, :]
    grad_inflow = ends * (split_nt(key_after, k) + split_nt(value_after, v))
    for level in range(levels):
        part = piece(decay, level)
        left = (part * g).astype(BF16)
        att_part, log_part = part * attention, part * grad_logits
        mixing = mixing + covers[level] * dot_tn(left, att_part.astype(BF16))
        spread = spread + covers[level] * dot_tn(left, log_part.astype(BF16))
        grad_inflow = grad_inflow + part * (
            exact_nt(log_part, scores * covers[level]) + exact_nt(att_part, reads * covers[level])
        )
    for by in range(SUB):
        row = jnp.sum(weights[by] * attention, axis=0, keepdims=True)
        mixing = jnp.where(gap == by, row, mixing)
        row = jnp.sum(weights[by] * grad_logits, axis=0, keepdims=True)
        spread = jnp.where(gap == by, row, spread)
        terms = bare[by] * (grad_logits * score_rows[by] + attention * read_rows[by])
        grad_inflow = grad_inflow + rolled(terms, -by)
    mixing = jnp.where(visible, mixing, 0.0).astype(BF16)
    spread = (jnp.where(visible, spread, 0.0) * factor).astype(BF16)
    log_carried = carried * grad_logits * factor
    att_carried = carried * attention
    ends = (ends * g).astype(BF16)
    grad_all[:, :size] = (
        dot_tn(spread, k) + dot_tn(log_carried.astype(BF16), key_in.astype(BF16))
    ).astype(BF16)
    grad_all[:, size : 2 * size] = (dot_nn(spread, q) + dot_tn(ends, key_after.astype(BF16))).astype(BF16)
    grad_all[:, 2 * size :] = (dot_nn(mixing, d) + dot_tn(ends, value_after.astype(BF16))).astype(BF16)
    change = grad_logits * logits + attention * grad_att - g * grad_inflow
    later = piece(sums, levels + 1) + jnp.where(gap == 0, 1.0, 0.0)
    same = jnp.where(visible, later, 0.0)
    flows = exact_nn(change, same) + rows[2:3, :] * flow[:, 0:1]
    grad_rate[...] = rows[3:4, :] * flows - jnp.exp(a) * grad_inflow
    keep = carried[:, CHUNK - 1 : CHUNK]
    key_before = keep * key_after + split_nn(log_carried, q)
    value_before = keep * value_after + split_nn(att_carried, d)
    state_grad[:SLOTS, :] = key_before
    state_grad[SLOTS:, :] = value_before
    flow[...] = jnp.broadcast_to(
        jnp.sum(key_before * key_in + value_before * value_in, axis=1, keepdims=True), flow.shape
    )


def mixer_specs(length, size, ring, backward):
    count = length // CHUNK
    per = count // ring

    def natural(step):
        return count - 1 - step if backward else step

    def moved(step, mine):
        at = natural(step)
        return lax.bitwise_xor(at // per, mine[0]) * per + at % per

    wide = [
        pl.BlockSpec((CHUNK, size), lambda step, mine, at=at: (moved(step, mine), at))
        for at in range(3)
    ]
    everything = pl.BlockSpec((CHUNK, 3 * size), lambda step, mine: (moved(step, mine), 0))
    pair = pl.BlockSpec((2 * SLOTS, CHUNK), lambda step, mine: (0, moved(step, mine)))
    slim = pl.BlockSpec((SLOTS, CHUNK), lambda step, mine: (0, moved(step, mine)))
    rows = pl.BlockSpec((8, CHUNK), lambda step, mine: (0, natural(step)))
    state = pl.BlockSpec((1, 2 * SLOTS, size), lambda step, mine: (natural(step), 0, 0))
    return count, wide, everything, pair, slim, rows, state


def mixer_forward(mine, ring, size, joined, rates, rows):
    length = joined.shape[0]
    count, wide, _, pair, _, row_spec, state = mixer_specs(length, size, ring, False)
    return pl.pallas_call(
        functools.partial(mixer_forward_kernel, size ** (-0.25)),
        out_shape=(
            jax.ShapeDtypeStruct((length, size), F32),
            jax.ShapeDtypeStruct((2 * SLOTS, length), F32),
            jax.ShapeDtypeStruct((count, 2 * SLOTS, size), F32),
        ),
        grid_spec=pltpu.PrefetchScalarGridSpec(
            num_scalar_prefetch=1,
            grid=(count,),
            in_specs=wide + [pair, row_spec],
            out_specs=[wide[0], pair, state],
            scratch_shapes=[pltpu.VMEM((2 * SLOTS, size), F32)] + TABLES,
        ),
        compiler_params=pltpu.CompilerParams(vmem_limit_bytes=32 << 20),
        cost_estimate=pl.CostEstimate(
            flops=length * size * 2000, bytes_accessed=length * size * 12, transcendentals=length * 4096
        ),
        name="mixer_forward",
    )(mine, joined, joined, joined, rates, rows)


def mixer_backward(mine, ring, joined, grad, rates, rows, choice, starts):
    length, size = grad.shape
    count, wide, everything, pair, slim, row_spec, state = mixer_specs(length, size, ring, True)
    return pl.pallas_call(
        functools.partial(mixer_backward_kernel, size ** (-0.25)),
        out_shape=(
            jax.ShapeDtypeStruct((length, 3 * size), BF16),
            jax.ShapeDtypeStruct((SLOTS, length), F32),
        ),
        grid_spec=pltpu.PrefetchScalarGridSpec(
            num_scalar_prefetch=1,
            grid=(count,),
            in_specs=wide + [wide[0], pair, row_spec, pair, state],
            out_specs=[everything, slim],
            scratch_shapes=[pltpu.VMEM((2 * SLOTS, size), F32), pltpu.VMEM((SLOTS, 128), F32)]
            + TABLES,
        ),
        compiler_params=pltpu.CompilerParams(vmem_limit_bytes=32 << 20),
        cost_estimate=pl.CostEstimate(
            flops=length * size * 4000, bytes_accessed=length * size * 20, transcendentals=length * 4096
        ),
        name="mixer_backward",
    )(mine, joined, joined, joined, grad, rates, rows, choice, starts)


def peers(ring, mine):
    found = []
    for by in range(1, ring):
        at, bit = mine, 1
        while bit <= by:
            if by & bit:
                at = at + bit * (1 - 2 * ((at // bit) % 2))
            bit *= 2
        found.append(at)
    return found


class Copies:
    def __init__(self, local, send, recv):
        self.local, self.send, self.recv = local, send, recv
        self.here, self.away = 0, 0
        self.open = []

    def near(self, source, target):
        copy = pltpu.make_async_copy(source, target, self.local.at[self.here])
        self.here += 1
        copy.start()
        return copy

    def far(self, source, target, landed, device, when=None):
        at = self.away
        self.away += 1
        copy = pltpu.make_async_remote_copy(
            source, target, self.send.at[at], self.recv.at[at], device_id=device,
            device_id_type=pl.DeviceIdType.MESH,
        )
        if when is None:
            copy.start()
        else:
            pl.when(when)(copy.start)
        self.open.append((copy, when))
        return pltpu.make_async_remote_copy(
            landed, landed, self.send.at[at], self.recv.at[at], device_id=device,
            device_id_type=pl.DeviceIdType.MESH,
        ).wait_recv

    def close(self):
        for copy, when in self.open:
            if when is None:
                copy.wait_send()
            else:
                pl.when(when)(copy.wait_send)


PARTS = 4


def fold_kernel(finish, extras, *refs):
    terms, given = refs[0], refs[1 : 1 + extras]
    blocks = refs[1 + extras]
    made = refs[2 + extras : -9]
    first, second, third, two_low, one_high, own, local_sem, send_sem, recv_sem = refs[-9:]
    mine, batch = lax.axis_index("seq"), lax.axis_index("batch")
    others = peers(4, mine)
    row, col = (others[0], batch), (others[1], batch)
    copies = Copies(local_sem, send_sem, recv_sem)
    size = terms.shape[1] // PARTS

    def span(at):
        low = pl.ds(at * size, size // 2)
        return pl.ds(at * size, size), low, pl.ds(at * size + size // 2, size // 2)

    opening, direct = [], []

    def open_part(at):
        _, low, high = span(at)
        opening.append(
            (
                copies.far(terms.at[3, low], first.at[low], first.at[low], row),
                copies.far(terms.at[3, high], first.at[high], first.at[high], col),
            )
        )

    def pass_part(at):
        _, low, high = span(at)
        waits = [
            copies.far(terms.at[2, high], second.at[high], second.at[high], col),
            copies.far(terms.at[1, low], third.at[low], third.at[low], row),
        ]
        opening[at][0]()
        two_low[low, :] = added(terms[2, low, :], first[low, :])
        waits.append(copies.far(two_low.at[low], second.at[low], second.at[low], col))
        opening[at][1]()
        one_high[high, :] = added(terms[1, high, :], first[high, :])
        waits.append(copies.far(one_high.at[high], third.at[high], third.at[high], row))
        direct.append(waits)

    spread, local, passed = [], [], []

    def close_part(at):
        full, _, _ = span(at)
        for wait in direct[at]:
            wait()
        total = terms[0, full, :].astype(F32) + second[full, :].astype(F32) + third[full, :].astype(F32)
        own[full, :] = finish(total, full, at, given, made)
        spread.append(
            (
                copies.far(own.at[full], blocks.at[1, full], blocks.at[1, full], row),
                copies.far(own.at[full], blocks.at[2, full], blocks.at[2, full], col),
            )
        )
        local.append(copies.near(own.at[full], blocks.at[0, full]))

    def forward_part(at):
        _, low, high = span(at)
        for wait in spread[at]:
            wait()
        passed.append(copies.far(blocks.at[2, low], blocks.at[3, low], blocks.at[3, low], row))
        passed.append(copies.far(blocks.at[1, high], blocks.at[3, high], blocks.at[3, high], col))

    open_part(0)
    for at in range(PARTS + 2):
        if at + 1 < PARTS:
            open_part(at + 1)
        if at < PARTS:
            pass_part(at)
        if 1 <= at <= PARTS:
            close_part(at - 1)
        if at >= 2:
            forward_part(at - 2)
    for wait in passed:
        wait()
    for copy in local:
        copy.wait()
    copies.close()


def half_blocks(value, order):
    lane = lax.broadcasted_iota(jnp.int32, (value.shape[0], 128), 1)
    made = []
    for pair in zip(order[::2], order[1::2]):
        low, high = (
            value[:, block * 128 : (block + 1) * 128]
            if half == want
            else pltpu.roll(value[:, block * 128 : (block + 1) * 128], 64, 1)
            for want, (block, half) in enumerate(pair)
        )
        made.append(jnp.where(lane < 64, low, high))
    return jnp.concatenate(made, axis=1)


def by_line(value):
    lines = value.shape[1] // 256
    return half_blocks(
        value, [divmod(ring * lines + line, 2) for line in range(lines) for ring in range(4)]
    )


def by_ring(value):
    lines = value.shape[1] // 256
    return half_blocks(
        value, [divmod(line * 4 + ring, 2) for ring in range(4) for line in range(lines)]
    )


def finish_forward(total, full, at, given, made):
    inputs, gain = given
    hidden = inputs[full, :].astype(F32) + total
    made[0][full, :] = hidden
    return by_line(hidden * rms_scale(hidden) * gain[...]).astype(BF16)


def finish_backward(total, full, at, given, made):
    cotangent, hidden_ref, gain = given
    total = by_ring(total)
    hidden = hidden_ref[full, :]
    scale = rms_scale(hidden)
    plain = hidden * scale
    term = jnp.sum(total * plain, axis=0, keepdims=True)
    made[1][...] = term if at == 0 else made[1][...] + term
    scaled = total * gain[...]
    grad = (
        cotangent[full, :].astype(F32)
        + scale * scaled
        - plain * (scale * jnp.mean(scaled * plain, axis=-1, keepdims=True))
    )
    made[0][full, :] = grad
    return grad.astype(BF16)


def fold(finish, terms, given, made, name):
    ring, rows, width = terms.shape
    inside = pl.BlockSpec(memory_space=pltpu.VMEM)
    block = pltpu.VMEM((rows, width), BF16)
    return pl.pallas_call(
        functools.partial(fold_kernel, finish, len(given)),
        out_shape=(jax.ShapeDtypeStruct((ring, rows, width), BF16),) + made,
        in_specs=[inside] * (1 + len(given)),
        out_specs=[pl.BlockSpec(memory_space=pltpu.HBM)] + [inside] * len(made),
        scratch_shapes=[block] * 6
        + [
            pltpu.SemaphoreType.DMA((PARTS,)),
            pltpu.SemaphoreType.DMA((PARTS * 10,)),
            pltpu.SemaphoreType.DMA((PARTS * 10,)),
        ],
        compiler_params=pltpu.CompilerParams(has_side_effects=True, vmem_limit_bytes=40 << 20),
        name=name,
    )(terms, *given)


def rms_scale(features):
    return lax.rsqrt(jnp.mean(features * features, axis=-1, keepdims=True) + EPS)


def swapped(block, by, ring):
    return lax.ppermute(block, "seq", [(i, i ^ by) for i in range(ring)])


def gathered(block, ring):
    if ring != 4:
        return jnp.concatenate([block] + [swapped(block, by, ring) for by in range(1, ring)], axis=0)
    half = block.shape[0] // 2
    one, two = swapped(block, 1, ring), swapped(block, 2, ring)
    low, high = swapped(two[:half], 1, ring), swapped(one[half:], 2, ring)
    return jnp.concatenate([block, one, two, low, high], axis=0)


def scattered(terms, ring):
    rows = terms.shape[0] // ring
    parts = [terms[by * rows : (by + 1) * rows] for by in range(ring)]
    total = parts[0].astype(F32)
    if ring != 4:
        for by in range(1, ring):
            total = total + swapped(parts[by], by, ring).astype(F32)
        return total
    half = rows // 2
    low, high = swapped(parts[3][:half], 1, ring), swapped(parts[3][half:], 2, ring)
    two = jnp.concatenate([added(parts[2][:half], low), parts[2][half:]], axis=0)
    one = jnp.concatenate([parts[1][:half], added(parts[1][half:], high)], axis=0)
    return total + swapped(one, 1, ring).astype(F32) + swapped(two, 2, ring).astype(F32)


def added(left, right):
    return (left.astype(F32) + right.astype(F32)).astype(BF16)


def flipped(block, axis, by):
    return lax.ppermute(block, axis, [(i, i ^ by) for i in range(lax.axis_size(axis))])


def doubled(block, axis):
    by, mine = 1, lax.axis_index(axis)
    while by < lax.axis_size(axis):
        other = flipped(block, axis, by)
        first = (mine & by) == 0
        block = jnp.concatenate(
            [jnp.where(first, block, other), jnp.where(first, other, block)], axis=0
        )
        by *= 2
    return block


def halved(block, axis):
    by, mine = lax.axis_size(axis) // 2, lax.axis_index(axis)
    while by:
        low, high = jnp.split(block, 2, axis=0)
        first = (mine & by) == 0
        block = jnp.where(first, low, high) + flipped(jnp.where(first, high, low), axis, by)
        by //= 2
    return block


def core_halves(array, lines, axis):
    size = array.shape[axis] // lines
    even, odd = (
        jnp.concatenate(
            [
                lax.slice_in_dim(array, line * size, (line + 1) * size, axis=axis)
                for line in range(which, lines, 2)
            ],
            axis=axis,
        )
        for which in range(2)
    )
    first = lax.axis_index("batch") % 2 == 0
    return jnp.where(first, even, odd), jnp.where(first, odd, even)


def core_sum(features, grads, lines, fill=()):
    if (features.shape[1] // lines) % 128:
        mine, others = core_halves(dot_tn(features, grads).astype(BF16), lines, 0)
        return added(mine, flipped(others, "batch", 1))
    mine, others = core_halves(features, lines, 1)
    sent = flipped(dot_tn(others, grads).astype(BF16), "batch", 1)
    mine = after(mine, *fill) if fill else mine
    return (dot_tn(mine, grads) + sent.astype(F32)).astype(BF16)


def line_sum(terms, lines):
    groups = [list(range(core, lines, 2)) for core in range(2)]
    return lax.psum_scatter(
        terms, "batch", scatter_dimension=0, axis_index_groups=groups, tiled=True
    )


def after(value, *others):
    return lax.optimization_barrier((value,) + others)[0]


def exchanged(blocks, mine, ring):
    parts = [
        swapped(lax.dynamic_index_in_dim(blocks, mine ^ by, 0, keepdims=False), by, ring)
        if by
        else lax.dynamic_index_in_dim(blocks, mine, 0, keepdims=False)
        for by in range(ring)
    ]
    made = jnp.stack(parts)
    return jnp.concatenate(
        [lax.dynamic_index_in_dim(made, mine ^ j, 0, keepdims=True) for j in range(ring)], axis=0
    )


def local(
    layer_input,
    segments,
    mixer_gain,
    query_weight,
    key_weight,
    value_weight,
    squeeze,
    expand,
    forget_bias,
    swish_weight,
    head_gain,
    output_weight,
    feed_gain,
    gate_weight,
    up_weight,
    down_weight,
    cotangent,
):
    ring, lines = lax.axis_size("seq"), lax.axis_size("batch")
    devices = ring * lines
    mine = lax.axis_index("seq")
    rows, width = layer_input.shape[1], layer_input.shape[2]
    length = rows * ring
    own = width // devices
    head_size = width // HEADS
    copies = ring // HEADS
    part = width // ring
    head = mine // copies
    hidden_part = gate_weight.shape[1] // ring
    slots_all = HEADS * SLOTS

    def to_order(array):
        if copies == 1:
            return array
        blocks = array.reshape((ring, rows) + array.shape[1:])
        moved = [lax.dynamic_index_in_dim(blocks, mine ^ by, 0, keepdims=False) for by in range(ring)]
        return jnp.concatenate(moved, axis=0)

    def whole_head(array):
        if copies == 1:
            return array
        full = lax.all_gather(to_order(array), "seq", axis=1, tiled=True)
        return to_order(lax.dynamic_slice_in_dim(full, head * head_size, head_size, 1))

    def own_part(array):
        if copies == 1:
            return array
        return lax.dynamic_slice_in_dim(array, (mine % copies) * part, part, 1)

    params = jnp.concatenate(
        [
            mixer_gain,
            head_gain,
            feed_gain,
            forget_bias,
            expand.T.reshape(-1),
            squeeze.reshape(-1),
        ]
    )
    count = params.shape[0]
    params = jnp.concatenate([params, segments.reshape(rows).astype(BF16)])
    input_own = layer_input.reshape(rows, width)
    grad_own = cotangent.reshape(rows, width)

    def permuted(array):
        shape = array.shape[:-1]
        array = array.reshape(shape + (ring, lines, own))
        return jnp.swapaxes(array, -3, -2).reshape(shape + (width,))

    def restored(array):
        shape = array.shape[:-1]
        array = array.reshape(shape + (lines, ring, own))
        return jnp.swapaxes(array, -3, -2).reshape(shape + (width,))

    def columns(*arrays):
        blocks = [a.reshape(own, ring, a.shape[1] // ring) for a in arrays]
        return jnp.concatenate(blocks, axis=2).transpose(1, 0, 2)

    w_output = lax.all_gather(output_weight, "batch", axis=0, tiled=True)
    mixer_columns = exchanged(
        columns(query_weight, key_weight, value_weight, swish_weight), mine, ring
    )
    w_mixer = lax.all_gather(mixer_columns.reshape(ring * own, -1), "batch", axis=0, tiled=True)
    feed_columns = exchanged(columns(gate_weight, up_weight), mine, ring)
    w_feed = lax.all_gather(feed_columns.reshape(ring * own, -1), "batch", axis=0, tiled=True)
    w_down = lax.all_gather(after(down_weight, feed_columns), "batch", axis=0, tiled=True)
    if ring != 4:
        w_feed = w_feed.reshape(lines, ring, own, -1).transpose(1, 0, 2, 3).reshape(width, -1)

    inputs = after(gathered(permuted(input_own), ring), w_output)
    small = doubled(doubled(params[None], "batch"), "seq")
    grad_out = gathered(after(grad_own, inputs, w_mixer), ring)
    small = small.reshape(devices, -1)
    segment = lax.dynamic_index_in_dim(
        small.reshape(ring, lines, -1), lax.axis_index("batch"), 1, keepdims=False
    )[:, count : count + rows].reshape(length).astype(F32)
    cuts = np.cumsum([own, own, own, slots_all // devices, RANK * slots_all // devices])
    gain_one, gain_head, gain_two, bias_full, expand_t, w_squeeze = jnp.split(
        small[:, :count], cuts, axis=1
    )
    gain_one = permuted(gain_one.reshape(width)).astype(F32)
    gain_head = lax.dynamic_slice_in_dim(gain_head.reshape(width), head * head_size, head_size, 0)
    gain_head = gain_head.astype(F32)
    gain_two = gain_two.reshape(width).astype(F32)
    bias_head = lax.dynamic_slice_in_dim(bias_full.reshape(slots_all), head * SLOTS, SLOTS, 0)
    expand_head = lax.dynamic_slice_in_dim(
        expand_t.reshape(slots_all, RANK), head * SLOTS, SLOTS, 0
    )
    w_squeeze = permuted(w_squeeze.reshape(width, RANK).T)

    chunked = segment.reshape(-1, CHUNK)
    before = jnp.concatenate([jnp.full((1,), -1.0, F32), chunked[:-1, -1]])
    previous = jnp.concatenate([jnp.full((1,), -1.0, F32), segment[:-1]])
    mask_rows = jnp.stack(
        [
            segment,
            (chunked == before[:, None]).astype(F32).reshape(-1),
            (chunked == chunked[:, -1:]).astype(F32).reshape(-1),
            (segment == previous).astype(F32),
        ]
        + [jnp.zeros_like(segment)] * 4
    )

    inputs = inputs.astype(F32)
    scale_one = rms_scale(inputs)
    plain_one = inputs * scale_one
    normed = (plain_one * gain_one).astype(BF16)
    mixer_pre = dot_nn(normed, w_mixer)
    joined = mixer_pre.astype(BF16)
    if copies > 1:
        joined = jnp.concatenate(
            [whole_head(joined[:, at * part : (at + 1) * part]) for at in range(3)], axis=1
        )
    swish_pre = whole_head(mixer_pre[:, 3 * part :])
    reduced = dot_nt(normed, w_squeeze).astype(BF16)
    forget_logit = dot_nt(expand_head, reduced) + bias_head.astype(F32)[:, None]
    log_rate = jax.nn.log_sigmoid(forget_logit) / TAU_GATE
    rates = jnp.concatenate([log_rate, -jnp.expm1(log_rate)], axis=0)
    order = mine.reshape(1).astype(jnp.int32)
    mixed, choice, starts = mixer_forward(order, ring, head_size, joined, rates, mask_rows)
    head_factor = rms_scale(mixed)
    head_plain = mixed * head_factor
    head_normed = head_plain * gain_head
    swish_sig = jax.nn.sigmoid(swish_pre)
    swish_act = swish_pre * swish_sig
    gated = own_part((head_normed * swish_act).astype(BF16))
    terms = dot_nn(gated, w_output).astype(BF16)
    terms, grad_out = lax.optimization_barrier((terms, grad_out))
    if ring == 4:
        feed_in, hidden = fold(
            finish_forward,
            terms.reshape(ring, rows, width),
            (input_own, gain_two[None]),
            (jax.ShapeDtypeStruct((rows, width), F32),),
            "fold_forward",
        )
        feed_in = feed_in.reshape(length, width)
    else:
        hidden = input_own.astype(F32) + scattered(terms, ring)
        feed_in = gathered((hidden * rms_scale(hidden) * gain_two).astype(BF16), ring)

    feed_pre = dot_nn(feed_in, w_feed)
    gate_pre, up_pre = feed_pre[:, :hidden_part], feed_pre[:, hidden_part:]
    gate_sig = jax.nn.sigmoid(gate_pre)
    gate_act = gate_pre * gate_sig
    inner = (gate_act * up_pre).astype(BF16)

    term_down = dot_tn(inner, grad_out).astype(BF16)
    grad_inner = dot_nt(after(grad_out, term_down), w_down)
    grad_gatepre = grad_inner * up_pre * (gate_sig * (1.0 + gate_pre * (1.0 - gate_sig)))
    grad_feedpre = jnp.concatenate(
        [grad_gatepre.astype(BF16), (grad_inner * gate_act).astype(BF16)], axis=1
    )
    back_feedin = dot_nt(grad_feedpre, w_feed).astype(BF16)
    result_terms = dot_nn(after(inner, back_feedin), w_down).astype(BF16)
    feed_lines = feed_in if ring == 4 else permuted(feed_in)
    term_feedpre = core_sum(after(feed_lines, back_feedin), grad_feedpre, lines, (result_terms,))
    down_share = lax.psum_scatter(term_down, "batch", scatter_dimension=0, tiled=True)
    feed_sum = line_sum(after(term_feedpre, down_share), lines)
    if ring == 4:
        grad_branch, grad_hidden, term_feed = fold(
            finish_backward,
            after(back_feedin, term_feedpre).reshape(ring, rows, width),
            (grad_own, hidden, gain_two[None]),
            (
                jax.ShapeDtypeStruct((rows, width), F32),
                jax.ShapeDtypeStruct((1, width), F32),
            ),
            "fold_backward",
        )
        grad_branch, term_feed = grad_branch.reshape(length, width), term_feed[0]
    else:
        grad_feedin = scattered(back_feedin, ring)
        scale_two = rms_scale(hidden)
        term_feed = jnp.sum(grad_feedin * hidden * scale_two, axis=0)
        scaled_two = grad_feedin * gain_two
        grad_hidden = (
            grad_own.astype(F32)
            + scale_two * scaled_two
            - hidden * scale_two**3 * jnp.mean(scaled_two * hidden, axis=-1, keepdims=True)
        )
        grad_branch = gathered(grad_hidden.astype(BF16), ring)

    result = hidden + scattered(after(result_terms, grad_branch), ring)
    layer_output = result.astype(BF16).reshape(1, rows, width)

    grad_gated = whole_head(dot_nt(grad_branch, w_output))
    term_output = core_sum(gated, grad_branch, lines)

    slope = swish_sig * (1.0 + swish_pre * (1.0 - swish_sig))
    grad_swishpre = own_part((grad_gated * head_normed * slope).astype(BF16))
    grad_normed_head = grad_gated * swish_act
    term_head = jnp.sum(grad_normed_head * head_plain, axis=0) / copies
    scaled_head = grad_normed_head * gain_head
    grad_mixed = head_factor * scaled_head - mixed * head_factor**3 * jnp.mean(
        scaled_head * mixed, axis=-1, keepdims=True
    )
    grad_pre, grad_rate = mixer_backward(
        order, ring, joined, grad_mixed.astype(BF16), rates, mask_rows, choice, starts
    )
    grad_logit = (grad_rate * jax.nn.sigmoid(-forget_logit) / TAU_GATE).astype(BF16)
    term_bias = jnp.sum(grad_logit.astype(F32), axis=1) / copies
    term_expand = dot_nn(grad_logit, reduced) / copies
    grad_reduced = (dot_tn(grad_logit, expand_head) / copies).astype(BF16)
    if copies > 1:
        grad_pre = jnp.concatenate(
            [own_part(grad_pre[:, at * head_size : (at + 1) * head_size]) for at in range(3)], axis=1
        )
    grad_pre = jnp.concatenate([grad_pre, grad_swishpre], axis=1)
    normed_own, normed_other = core_halves(normed, lines, 1)
    term_other = dot_tn(normed_other, grad_pre).astype(BF16)
    term_sent = flipped(term_other, "batch", 1)
    grad_sent, normed_own = lax.optimization_barrier(
        (grad_pre, normed_own, term_other, feed_sum)
    )[:2]
    grad_normed = dot_nt(grad_sent, w_mixer) + dot_nn(grad_reduced, w_squeeze)
    term_pre = dot_tn(after(normed_own, grad_normed), grad_pre) + term_sent.astype(F32)
    term_pre = term_pre.astype(BF16)
    if 4 * part == width:
        chips = lines // 2
        joint = jnp.concatenate(
            [term_pre.reshape(chips, ring * own, width), term_output.reshape(chips, own, width)], axis=1
        )
        joint = line_sum(after(joint.reshape(-1, width), feed_sum), lines)
        pre_sum, output_share = joint[: ring * own], joint[ring * own :]
    else:
        pre_sum, output_share = line_sum(term_pre, lines), line_sum(term_output, lines)
    term_mixer = restored(jnp.sum(grad_normed * plain_one, axis=0))
    term_squeeze = restored(dot_tn(grad_reduced, normed))
    grad_normed = restored(scattered(grad_normed.astype(BF16), ring))
    inputs_own = input_own.astype(F32)
    scale_own = rms_scale(inputs_own)
    scaled_one = grad_normed * restored(gain_one)
    grad_input = (
        grad_hidden
        + scale_own * scaled_one
        - inputs_own * scale_own**3 * jnp.mean(scaled_one * inputs_own, axis=-1, keepdims=True)
    ).astype(BF16)
    pre_share = exchanged(pre_sum.reshape(ring, own, 4 * part), mine, ring)
    pre_share = pre_share.reshape(ring, own, 4, part).transpose(2, 1, 0, 3)
    query_share, key_share, value_share, swish_share = pre_share.reshape(4, own, width).astype(F32)
    feed_share = exchanged(feed_sum.reshape(ring, own, 2 * hidden_part), mine, ring)
    gate_share = feed_share[:, :, :hidden_part].transpose(1, 0, 2).reshape(own, -1).astype(F32)
    up_share = feed_share[:, :, hidden_part:].transpose(1, 0, 2).reshape(own, -1).astype(F32)

    def placed(array, size):
        full = jnp.zeros((HEADS, size) + array.shape[1:], F32)
        return lax.dynamic_update_slice_in_dim(full, array[None], head, 0)

    terms = jnp.concatenate(
        [
            term_mixer.reshape(devices, -1),
            placed(term_head, head_size).reshape(devices, -1),
            term_feed.reshape(devices, -1),
            placed(term_bias, SLOTS).reshape(devices, -1),
            placed(term_expand, SLOTS).reshape(devices, -1),
            term_squeeze.T.reshape(devices, -1),
        ],
        axis=1,
    )
    share = halved(halved(terms, "seq"), "batch")[0]
    mixer_share, head_share, feedgain_share, bias_share, expand_share, squeeze_share = jnp.split(
        share, cuts
    )
    return (
        layer_output,
        grad_input.reshape(1, rows, width),
        mixer_share,
        query_share,
        key_share,
        value_share,
        squeeze_share.reshape(own, RANK),
        expand_share.reshape(-1, RANK).T,
        bias_share,
        swish_share,
        head_share,
        output_share.astype(F32),
        feedgain_share,
        gate_share,
        up_share,
        down_share.astype(F32),
    )


def solution(mesh):
    rows = P(BOTH, None)
    spread = P(BOTH)
    in_specs = (
        P("batch", "seq", None),
        P("batch", "seq"),
        spread,
        rows,
        rows,
        rows,
        rows,
        P(None, BOTH),
        spread,
        rows,
        spread,
        rows,
        spread,
        rows,
        rows,
        rows,
        P("batch", "seq", None),
    )
    out_specs = (
        P("batch", "seq", None),
        P("batch", "seq", None),
        spread,
        rows,
        rows,
        rows,
        rows,
        P(None, BOTH),
        spread,
        rows,
        spread,
        rows,
        spread,
        rows,
        rows,
        rows,
    )
    return jax.shard_map(local, mesh=mesh, in_specs=in_specs, out_specs=out_specs, check_vma=False)
```

```python
import functools

import jax
import jax.numpy as jnp
import numpy as np
from jax import lax
from jax.experimental import pallas as pl
from jax.experimental.pallas import tpu as pltpu
from jax.sharding import PartitionSpec as P

HEADS = 4
SLOTS = 64
RANK = 16
EPS = 1e-06
TAU_GATE = 8.0
CHUNK = 128
SUB = 16
BOTH = ("seq", "batch")
F32 = jnp.float32
BF16 = jnp.bfloat16
HIGHEST = lax.Precision.HIGHEST


def dot_nn(left, right):
    return lax.dot_general(left, right, (((1,), (0,)), ((), ())), preferred_element_type=F32)


def dot_nt(left, right):
    return lax.dot_general(left, right, (((1,), (1,)), ((), ())), preferred_element_type=F32)


def dot_tn(left, right):
    return lax.dot_general(left, right, (((0,), (0,)), ((), ())), preferred_element_type=F32)


def exact_nn(left, right):
    return lax.dot_general(
        left, right, (((1,), (0,)), ((), ())), precision=HIGHEST, preferred_element_type=F32
    )


def exact_nt(left, right):
    return lax.dot_general(
        left, right, (((1,), (1,)), ((), ())), precision=HIGHEST, preferred_element_type=F32
    )


def halves(value):
    high = value.astype(BF16)
    return high, (value - high.astype(F32)).astype(BF16)


def split_nn(left, right):
    high, rest = halves(left)
    return dot_nn(high, right) + dot_nn(rest, right)


def split_nt(left, right):
    high, rest = halves(left)
    return dot_nt(high, right) + dot_nt(rest, right)


LEVELS = (CHUNK // SUB).bit_length() - 1


def fill_tables(sums, covers, apart):
    source = lax.broadcasted_iota(jnp.int32, (CHUNK, CHUNK), 0)
    target = lax.broadcasted_iota(jnp.int32, (CHUNK, CHUNK), 1)

    def group(at, size):
        return jnp.bitwise_and(at, CHUNK - size)

    for level in range(LEVELS):
        half = SUB << level
        right = jnp.bitwise_and(target, half) != 0
        edge = group(target, 2 * half) + (half - 1)
        low, high = jnp.where(right, edge, target), jnp.where(right, target, edge)
        sums[:, level * CHUNK : (level + 1) * CHUNK] = jnp.where(
            (source > low) & (source <= high), 1.0, 0.0
        )
        same = group(source, 2 * half) == group(target, 2 * half)
        covers[level] = jnp.where(same & (jnp.bitwise_and(source, half) == 0) & right, 1.0, 0.0)
    sums[:, LEVELS * CHUNK : (LEVELS + 1) * CHUNK] = jnp.where(source <= target, 1.0, 0.0)
    sums[:, (LEVELS + 1) * CHUNK :] = jnp.where(source > target, 1.0, 0.0)
    apart[...] = jnp.where(group(source, SUB) == group(target, SUB), target - source, -1)


TABLES = [
    pltpu.VMEM((CHUNK, (LEVELS + 2) * CHUNK), F32),
    pltpu.VMEM((LEVELS, CHUNK, CHUNK), F32),
    pltpu.VMEM((CHUNK, CHUNK), jnp.int32),
]


def same_document(rows):
    source = lax.broadcasted_iota(jnp.int32, (CHUNK, CHUNK), 0)
    target = lax.broadcasted_iota(jnp.int32, (CHUNK, CHUNK), 1)
    number = rows[0:1, :]
    column = jnp.sum(jnp.where(source == target, number, 0.0), axis=1, keepdims=True)
    return column == number


def rolled(value, by):
    return value if by % CHUNK == 0 else pltpu.roll(value, by % CHUNK, 1)


def exponents(rate, sums):
    return jnp.exp(exact_nn(rate, sums))


def piece(value, at):
    return value[:, at * CHUNK : (at + 1) * CHUNK]


def mixer_forward_kernel(
    factor, mine, query, key, value, rate, rows, output, choice_out, start_out, state, sums, covers, apart
):
    levels = LEVELS

    @pl.when(pl.program_id(0) == 0)
    def _():
        state[...] = jnp.zeros_like(state)
        fill_tables(sums, covers, apart)

    key_in, value_in = state[:SLOTS, :], state[SLOTS:, :]
    start_out[0] = state[...]
    q, k, v = query[...], key[...], value[...]
    a, g = rate[:SLOTS, :], rate[SLOTS:, :]
    decay = exponents(a, sums[...])
    before, after = piece(decay, levels), piece(decay, levels + 1)
    carried = before * rows[1:2, :]
    visible = same_document(rows)
    scores = jnp.where(visible, dot_nt(k, q) * factor, 0.0)
    logits = carried * (split_nt(key_in, q) * factor)
    for level in range(levels):
        part = piece(decay, level)
        logits = logits + part * exact_nn(part * g, scores * covers[level])
    gap = apart[...]
    total = jnp.zeros_like(a)
    weights = []
    for by in range(SUB):
        if by:
            total = total + rolled(a, by - 1)
        weight = jnp.exp(total) * rolled(g, by)
        weights.append(weight)
        logits = logits + weight * jnp.sum(
            jnp.where(gap == by, scores, 0.0), axis=0, keepdims=True
        )
    attention = jnp.exp(logits - jnp.max(logits, axis=0, keepdims=True))
    attention = attention / jnp.sum(attention, axis=0, keepdims=True)
    choice_out[:SLOTS, :] = attention
    choice_out[SLOTS:, :] = logits
    mixing = jnp.zeros((CHUNK, CHUNK), F32)
    for level in range(levels):
        part = piece(decay, level)
        mixing = mixing + covers[level] * dot_tn(
            (part * g).astype(BF16), (part * attention).astype(BF16)
        )
    for by in range(SUB):
        row = jnp.sum(weights[by] * attention, axis=0, keepdims=True)
        mixing = jnp.where(gap == by, row, mixing)
    mixing = jnp.where(visible, mixing, 0.0).astype(BF16)
    output[...] = dot_tn(mixing, v) + dot_tn(
        (carried * attention).astype(BF16), value_in.astype(BF16)
    )
    ends = after * g * rows[2:3, :]
    keep = carried[:, CHUNK - 1 : CHUNK]
    state[:SLOTS, :] = keep * key_in + split_nn(ends, k)
    state[SLOTS:, :] = keep * value_in + split_nn(ends, v)


def mixer_backward_kernel(
    factor, mine, query, key, value, grad_output, rate, rows, choice, start, grad_all, grad_rate,
    state_grad, flow, sums, covers, apart,
):
    levels = LEVELS

    @pl.when(pl.program_id(0) == 0)
    def _():
        state_grad[...] = jnp.zeros_like(state_grad)
        flow[...] = jnp.zeros_like(flow)
        fill_tables(sums, covers, apart)

    key_in, value_in = start[0, :SLOTS, :], start[0, SLOTS:, :]
    key_after, value_after = state_grad[:SLOTS, :], state_grad[SLOTS:, :]
    q, k, v, d = query[...], key[...], value[...], grad_output[...]
    size = q.shape[1]
    a, g = rate[:SLOTS, :], rate[SLOTS:, :]
    attention, logits = choice[:SLOTS, :], choice[SLOTS:, :]
    decay = exponents(a, sums[...])
    before, after = piece(decay, levels), piece(decay, levels + 1)
    carried = before * rows[1:2, :]
    visible = same_document(rows)
    scores = jnp.where(visible, dot_nt(k, q) * factor, 0.0)
    reads = jnp.where(visible, dot_nt(v, d), 0.0)
    gap = apart[...]
    grad_att = carried * split_nt(value_in, d)
    for level in range(levels):
        part = piece(decay, level)
        grad_att = grad_att + part * exact_nn(part * g, reads * covers[level])
    total = jnp.zeros_like(a)
    bare, weights, score_rows, read_rows = [], [], [], []
    for by in range(SUB):
        if by:
            total = total + rolled(a, by - 1)
        bare.append(jnp.exp(total))
        weights.append(bare[by] * rolled(g, by))
        score_rows.append(jnp.sum(jnp.where(gap == by, scores, 0.0), axis=0, keepdims=True))
        read_rows.append(jnp.sum(jnp.where(gap == by, reads, 0.0), axis=0, keepdims=True))
        grad_att = grad_att + weights[by] * read_rows[by]
    grad_logits = attention * (
        grad_att - jnp.sum(attention * grad_att, axis=0, keepdims=True)
    )
    mixing = jnp.zeros((CHUNK, CHUNK), F32)
    spread = jnp.zeros((CHUNK, CHUNK), F32)
    ends = after * rows[2:3, :]
    grad_inflow = ends * (split_nt(key_after, k) + split_nt(value_after, v))
    for level in range(levels):
        part = piece(decay, level)
        left = (part * g).astype(BF16)
        att_part, log_part = part * attention, part * grad_logits
        mixing = mixing + covers[level] * dot_tn(left, att_part.astype(BF16))
        spread = spread + covers[level] * dot_tn(left, log_part.astype(BF16))
        grad_inflow = grad_inflow + part * (
            exact_nt(log_part, scores * covers[level]) + exact_nt(att_part, reads * covers[level])
        )
    for by in range(SUB):
        row = jnp.sum(weights[by] * attention, axis=0, keepdims=True)
        mixing = jnp.where(gap == by, row, mixing)
        row = jnp.sum(weights[by] * grad_logits, axis=0, keepdims=True)
        spread = jnp.where(gap == by, row, spread)
        terms = bare[by] * (grad_logits * score_rows[by] + attention * read_rows[by])
        grad_inflow = grad_inflow + rolled(terms, -by)
    mixing = jnp.where(visible, mixing, 0.0).astype(BF16)
    spread = (jnp.where(visible, spread, 0.0) * factor).astype(BF16)
    log_carried = carried * grad_logits * factor
    att_carried = carried * attention
    ends = (ends * g).astype(BF16)
    grad_all[:, :size] = (
        dot_tn(spread, k) + dot_tn(log_carried.astype(BF16), key_in.astype(BF16))
    ).astype(BF16)
    grad_all[:, size : 2 * size] = (dot_nn(spread, q) + dot_tn(ends, key_after.astype(BF16))).astype(BF16)
    grad_all[:, 2 * size :] = (dot_nn(mixing, d) + dot_tn(ends, value_after.astype(BF16))).astype(BF16)
    change = grad_logits * logits + attention * grad_att - g * grad_inflow
    later = piece(sums, levels + 1) + jnp.where(gap == 0, 1.0, 0.0)
    same = jnp.where(visible, later, 0.0)
    flows = exact_nn(change, same) + rows[2:3, :] * flow[:, 0:1]
    grad_rate[...] = rows[3:4, :] * flows - jnp.exp(a) * grad_inflow
    keep = carried[:, CHUNK - 1 : CHUNK]
    key_before = keep * key_after + split_nn(log_carried, q)
    value_before = keep * value_after + split_nn(att_carried, d)
    state_grad[:SLOTS, :] = key_before
    state_grad[SLOTS:, :] = value_before
    flow[...] = jnp.broadcast_to(
        jnp.sum(key_before * key_in + value_before * value_in, axis=1, keepdims=True), flow.shape
    )


def mixer_specs(length, size, ring, backward):
    count = length // CHUNK
    per = count // ring

    def natural(step):
        return count - 1 - step if backward else step

    def moved(step, mine):
        at = natural(step)
        return lax.bitwise_xor(at // per, mine[0]) * per + at % per

    wide = [
        pl.BlockSpec((CHUNK, size), lambda step, mine, at=at: (moved(step, mine), at))
        for at in range(3)
    ]
    everything = pl.BlockSpec((CHUNK, 3 * size), lambda step, mine: (moved(step, mine), 0))
    pair = pl.BlockSpec((2 * SLOTS, CHUNK), lambda step, mine: (0, moved(step, mine)))
    slim = pl.BlockSpec((SLOTS, CHUNK), lambda step, mine: (0, moved(step, mine)))
    rows = pl.BlockSpec((8, CHUNK), lambda step, mine: (0, natural(step)))
    state = pl.BlockSpec((1, 2 * SLOTS, size), lambda step, mine: (natural(step), 0, 0))
    return count, wide, everything, pair, slim, rows, state


def mixer_forward(mine, ring, size, joined, rates, rows):
    length = joined.shape[0]
    count, wide, _, pair, _, row_spec, state = mixer_specs(length, size, ring, False)
    return pl.pallas_call(
        functools.partial(mixer_forward_kernel, size ** (-0.25)),
        out_shape=(
            jax.ShapeDtypeStruct((length, size), F32),
            jax.ShapeDtypeStruct((2 * SLOTS, length), F32),
            jax.ShapeDtypeStruct((count, 2 * SLOTS, size), F32),
        ),
        grid_spec=pltpu.PrefetchScalarGridSpec(
            num_scalar_prefetch=1,
            grid=(count,),
            in_specs=wide + [pair, row_spec],
            out_specs=[wide[0], pair, state],
            scratch_shapes=[pltpu.VMEM((2 * SLOTS, size), F32)] + TABLES,
        ),
        compiler_params=pltpu.CompilerParams(vmem_limit_bytes=32 << 20),
        cost_estimate=pl.CostEstimate(
            flops=length * size * 2000, bytes_accessed=length * size * 12, transcendentals=length * 4096
        ),
        name="mixer_forward",
    )(mine, joined, joined, joined, rates, rows)


def mixer_backward(mine, ring, joined, grad, rates, rows, choice, starts):
    length, size = grad.shape
    count, wide, everything, pair, slim, row_spec, state = mixer_specs(length, size, ring, True)
    return pl.pallas_call(
        functools.partial(mixer_backward_kernel, size ** (-0.25)),
        out_shape=(
            jax.ShapeDtypeStruct((length, 3 * size), BF16),
            jax.ShapeDtypeStruct((SLOTS, length), F32),
        ),
        grid_spec=pltpu.PrefetchScalarGridSpec(
            num_scalar_prefetch=1,
            grid=(count,),
            in_specs=wide + [wide[0], pair, row_spec, pair, state],
            out_specs=[everything, slim],
            scratch_shapes=[pltpu.VMEM((2 * SLOTS, size), F32), pltpu.VMEM((SLOTS, 128), F32)]
            + TABLES,
        ),
        compiler_params=pltpu.CompilerParams(vmem_limit_bytes=32 << 20),
        cost_estimate=pl.CostEstimate(
            flops=length * size * 4000, bytes_accessed=length * size * 20, transcendentals=length * 4096
        ),
        name="mixer_backward",
    )(mine, joined, joined, joined, grad, rates, rows, choice, starts)


def peers(ring, mine):
    found = []
    for by in range(1, ring):
        at, bit = mine, 1
        while bit <= by:
            if by & bit:
                at = at + bit * (1 - 2 * ((at // bit) % 2))
            bit *= 2
        found.append(at)
    return found


class Copies:
    def __init__(self, local, send, recv):
        self.local, self.send, self.recv = local, send, recv
        self.here, self.away = 0, 0
        self.open = []

    def near(self, source, target):
        copy = pltpu.make_async_copy(source, target, self.local.at[self.here])
        self.here += 1
        copy.start()
        return copy

    def far(self, source, target, landed, device, when=None):
        at = self.away
        self.away += 1
        copy = pltpu.make_async_remote_copy(
            source, target, self.send.at[at], self.recv.at[at], device_id=device,
            device_id_type=pl.DeviceIdType.MESH,
        )
        if when is None:
            copy.start()
        else:
            pl.when(when)(copy.start)
        self.open.append((copy, when))
        return pltpu.make_async_remote_copy(
            landed, landed, self.send.at[at], self.recv.at[at], device_id=device,
            device_id_type=pl.DeviceIdType.MESH,
        ).wait_recv

    def close(self):
        for copy, when in self.open:
            if when is None:
                copy.wait_send()
            else:
                pl.when(when)(copy.wait_send)


PARTS = 4


def fold_kernel(finish, extras, *refs):
    terms, given = refs[0], refs[1 : 1 + extras]
    blocks = refs[1 + extras]
    made = refs[2 + extras : -9]
    first, second, third, two_low, one_high, own, local_sem, send_sem, recv_sem = refs[-9:]
    mine, batch = lax.axis_index("seq"), lax.axis_index("batch")
    others = peers(4, mine)
    row, col = (others[0], batch), (others[1], batch)
    copies = Copies(local_sem, send_sem, recv_sem)
    size = terms.shape[1] // PARTS

    def span(at):
        low = pl.ds(at * size, size // 2)
        return pl.ds(at * size, size), low, pl.ds(at * size + size // 2, size // 2)

    opening, direct = [], []

    def open_part(at):
        _, low, high = span(at)
        opening.append(
            (
                copies.far(terms.at[3, low], first.at[low], first.at[low], row),
                copies.far(terms.at[3, high], first.at[high], first.at[high], col),
            )
        )

    def pass_part(at):
        _, low, high = span(at)
        waits = [
            copies.far(terms.at[2, high], second.at[high], second.at[high], col),
            copies.far(terms.at[1, low], third.at[low], third.at[low], row),
        ]
        opening[at][0]()
        two_low[low, :] = added(terms[2, low, :], first[low, :])
        waits.append(copies.far(two_low.at[low], second.at[low], second.at[low], col))
        opening[at][1]()
        one_high[high, :] = added(terms[1, high, :], first[high, :])
        waits.append(copies.far(one_high.at[high], third.at[high], third.at[high], row))
        direct.append(waits)

    spread, local, passed = [], [], []

    def close_part(at):
        full, _, _ = span(at)
        for wait in direct[at]:
            wait()
        total = terms[0, full, :].astype(F32) + second[full, :].astype(F32) + third[full, :].astype(F32)
        own[full, :] = finish(total, full, at, given, made)
        spread.append(
            (
                copies.far(own.at[full], blocks.at[1, full], blocks.at[1, full], row),
                copies.far(own.at[full], blocks.at[2, full], blocks.at[2, full], col),
            )
        )
        local.append(copies.near(own.at[full], blocks.at[0, full]))

    def forward_part(at):
        _, low, high = span(at)
        for wait in spread[at]:
            wait()
        passed.append(copies.far(blocks.at[2, low], blocks.at[3, low], blocks.at[3, low], row))
        passed.append(copies.far(blocks.at[1, high], blocks.at[3, high], blocks.at[3, high], col))

    open_part(0)
    for at in range(PARTS + 2):
        if at + 1 < PARTS:
            open_part(at + 1)
        if at < PARTS:
            pass_part(at)
        if 1 <= at <= PARTS:
            close_part(at - 1)
        if at >= 2:
            forward_part(at - 2)
    for wait in passed:
        wait()
    for copy in local:
        copy.wait()
    copies.close()


def half_blocks(value, order):
    lane = lax.broadcasted_iota(jnp.int32, (value.shape[0], 128), 1)
    made = []
    for pair in zip(order[::2], order[1::2]):
        low, high = (
            value[:, block * 128 : (block + 1) * 128]
            if half == want
            else pltpu.roll(value[:, block * 128 : (block + 1) * 128], 64, 1)
            for want, (block, half) in enumerate(pair)
        )
        made.append(jnp.where(lane < 64, low, high))
    return jnp.concatenate(made, axis=1)


def by_line(value):
    lines = value.shape[1] // 256
    return half_blocks(
        value, [divmod(ring * lines + line, 2) for line in range(lines) for ring in range(4)]
    )


def by_ring(value):
    lines = value.shape[1] // 256
    return half_blocks(
        value, [divmod(line * 4 + ring, 2) for ring in range(4) for line in range(lines)]
    )


def finish_forward(total, full, at, given, made):
    inputs, gain = given
    hidden = inputs[full, :].astype(F32) + total
    made[0][full, :] = hidden
    return by_line(hidden * rms_scale(hidden) * gain[...]).astype(BF16)


def finish_backward(total, full, at, given, made):
    cotangent, hidden_ref, gain = given
    total = by_ring(total)
    hidden = hidden_ref[full, :]
    scale = rms_scale(hidden)
    plain = hidden * scale
    term = jnp.sum(total * plain, axis=0, keepdims=True)
    made[1][...] = term if at == 0 else made[1][...] + term
    scaled = total * gain[...]
    grad = (
        cotangent[full, :].astype(F32)
        + scale * scaled
        - plain * (scale * jnp.mean(scaled * plain, axis=-1, keepdims=True))
    )
    made[0][full, :] = grad
    return grad.astype(BF16)


def fold(finish, terms, given, made, name):
    ring, rows, width = terms.shape
    inside = pl.BlockSpec(memory_space=pltpu.VMEM)
    block = pltpu.VMEM((rows, width), BF16)
    return pl.pallas_call(
        functools.partial(fold_kernel, finish, len(given)),
        out_shape=(jax.ShapeDtypeStruct((ring, rows, width), BF16),) + made,
        in_specs=[inside] * (1 + len(given)),
        out_specs=[pl.BlockSpec(memory_space=pltpu.HBM)] + [inside] * len(made),
        scratch_shapes=[block] * 6
        + [
            pltpu.SemaphoreType.DMA((PARTS,)),
            pltpu.SemaphoreType.DMA((PARTS * 10,)),
            pltpu.SemaphoreType.DMA((PARTS * 10,)),
        ],
        compiler_params=pltpu.CompilerParams(has_side_effects=True, vmem_limit_bytes=40 << 20),
        name=name,
    )(terms, *given)


def rms_scale(features):
    return lax.rsqrt(jnp.mean(features * features, axis=-1, keepdims=True) + EPS)


def swapped(block, by, ring):
    return lax.ppermute(block, "seq", [(i, i ^ by) for i in range(ring)])


def gathered(block, ring):
    if ring != 4:
        return jnp.concatenate([block] + [swapped(block, by, ring) for by in range(1, ring)], axis=0)
    half = block.shape[0] // 2
    one, two = swapped(block, 1, ring), swapped(block, 2, ring)
    low, high = swapped(two[:half], 1, ring), swapped(one[half:], 2, ring)
    return jnp.concatenate([block, one, two, low, high], axis=0)


def scattered(terms, ring, middle=(), end=()):
    rows = terms.shape[0] // ring
    parts = [terms[by * rows : (by + 1) * rows] for by in range(ring)]
    total = parts[0].astype(F32)
    if ring != 4:
        for by in range(1, ring):
            total = total + swapped(parts[by], by, ring).astype(F32)
        return total
    half = rows // 2
    low, high = swapped(parts[3][:half], 1, ring), swapped(parts[3][half:], 2, ring)
    low, high = lax.optimization_barrier((low, high) + middle)[:2]
    two = jnp.concatenate([added(parts[2][:half], low), parts[2][half:]], axis=0)
    one = jnp.concatenate([parts[1][:half], added(parts[1][half:], high)], axis=0)
    one, two = swapped(one, 1, ring), swapped(two, 2, ring)
    one, two = lax.optimization_barrier((one, two) + end)[:2]
    return total + one.astype(F32) + two.astype(F32)


def added(left, right):
    return (left.astype(F32) + right.astype(F32)).astype(BF16)


def flipped(block, axis, by):
    return lax.ppermute(block, axis, [(i, i ^ by) for i in range(lax.axis_size(axis))])


def doubled(block, axis):
    by, mine = 1, lax.axis_index(axis)
    while by < lax.axis_size(axis):
        other = flipped(block, axis, by)
        first = (mine & by) == 0
        block = jnp.concatenate(
            [jnp.where(first, block, other), jnp.where(first, other, block)], axis=0
        )
        by *= 2
    return block


def halved(block, axis):
    by, mine = lax.axis_size(axis) // 2, lax.axis_index(axis)
    while by:
        low, high = jnp.split(block, 2, axis=0)
        first = (mine & by) == 0
        block = jnp.where(first, low, high) + flipped(jnp.where(first, high, low), axis, by)
        by //= 2
    return block


def core_halves(array, lines, axis):
    size = array.shape[axis] // lines
    even, odd = (
        jnp.concatenate(
            [
                lax.slice_in_dim(array, line * size, (line + 1) * size, axis=axis)
                for line in range(which, lines, 2)
            ],
            axis=axis,
        )
        for which in range(2)
    )
    first = lax.axis_index("batch") % 2 == 0
    return jnp.where(first, even, odd), jnp.where(first, odd, even)


def core_sum(features, grads, lines, fill=()):
    if (features.shape[1] // lines) % 128:
        mine, others = core_halves(dot_tn(features, grads).astype(BF16), lines, 0)
        return added(mine, flipped(others, "batch", 1))
    mine, others = core_halves(features, lines, 1)
    sent = flipped(dot_tn(others, grads).astype(BF16), "batch", 1)
    mine = after(mine, *fill) if fill else mine
    return (dot_tn(mine, grads) + sent.astype(F32)).astype(BF16)


def line_sum(terms, lines):
    groups = [list(range(core, lines, 2)) for core in range(2)]
    return lax.psum_scatter(
        terms, "batch", scatter_dimension=0, axis_index_groups=groups, tiled=True
    )


def after(value, *others):
    return lax.optimization_barrier((value,) + others)[0]


def exchanged(blocks, mine, ring):
    parts = [
        swapped(lax.dynamic_index_in_dim(blocks, mine ^ by, 0, keepdims=False), by, ring)
        if by
        else lax.dynamic_index_in_dim(blocks, mine, 0, keepdims=False)
        for by in range(ring)
    ]
    made = jnp.stack(parts)
    return jnp.concatenate(
        [lax.dynamic_index_in_dim(made, mine ^ j, 0, keepdims=True) for j in range(ring)], axis=0
    )


def local(
    layer_input,
    segments,
    mixer_gain,
    query_weight,
    key_weight,
    value_weight,
    squeeze,
    expand,
    forget_bias,
    swish_weight,
    head_gain,
    output_weight,
    feed_gain,
    gate_weight,
    up_weight,
    down_weight,
    cotangent,
):
    ring, lines = lax.axis_size("seq"), lax.axis_size("batch")
    devices = ring * lines
    mine = lax.axis_index("seq")
    rows, width = layer_input.shape[1], layer_input.shape[2]
    length = rows * ring
    own = width // devices
    head_size = width // HEADS
    copies = ring // HEADS
    part = width // ring
    head = mine // copies
    hidden_part = gate_weight.shape[1] // ring
    slots_all = HEADS * SLOTS

    def to_order(array):
        if copies == 1:
            return array
        blocks = array.reshape((ring, rows) + array.shape[1:])
        moved = [lax.dynamic_index_in_dim(blocks, mine ^ by, 0, keepdims=False) for by in range(ring)]
        return jnp.concatenate(moved, axis=0)

    def whole_head(array):
        if copies == 1:
            return array
        full = lax.all_gather(to_order(array), "seq", axis=1, tiled=True)
        return to_order(lax.dynamic_slice_in_dim(full, head * head_size, head_size, 1))

    def own_part(array):
        if copies == 1:
            return array
        return lax.dynamic_slice_in_dim(array, (mine % copies) * part, part, 1)

    params = jnp.concatenate(
        [
            mixer_gain,
            head_gain,
            feed_gain,
            forget_bias,
            expand.T.reshape(-1),
            squeeze.reshape(-1),
        ]
    )
    count = params.shape[0]
    params = jnp.concatenate([params, segments.reshape(rows).astype(BF16)])
    input_own = layer_input.reshape(rows, width)
    grad_own = cotangent.reshape(rows, width)

    def permuted(array):
        shape = array.shape[:-1]
        array = array.reshape(shape + (ring, lines, own))
        return jnp.swapaxes(array, -3, -2).reshape(shape + (width,))

    def restored(array):
        shape = array.shape[:-1]
        array = array.reshape(shape + (lines, ring, own))
        return jnp.swapaxes(array, -3, -2).reshape(shape + (width,))

    def columns(*arrays):
        blocks = [a.reshape(own, ring, a.shape[1] // ring) for a in arrays]
        return jnp.concatenate(blocks, axis=2).transpose(1, 0, 2)

    w_output = lax.all_gather(output_weight, "batch", axis=0, tiled=True)
    mixer_columns = exchanged(
        columns(query_weight, key_weight, value_weight, swish_weight), mine, ring
    )
    w_mixer = lax.all_gather(mixer_columns.reshape(ring * own, -1), "batch", axis=0, tiled=True)
    feed_columns = exchanged(columns(gate_weight, up_weight), mine, ring)
    w_feed = lax.all_gather(feed_columns.reshape(ring * own, -1), "batch", axis=0, tiled=True)
    w_down = lax.all_gather(after(down_weight, feed_columns), "batch", axis=0, tiled=True)
    if ring != 4:
        w_feed = w_feed.reshape(lines, ring, own, -1).transpose(1, 0, 2, 3).reshape(width, -1)

    inputs = after(gathered(permuted(input_own), ring), w_output)
    small = doubled(doubled(params[None], "batch"), "seq")
    grad_out = gathered(after(grad_own, inputs, w_mixer), ring)
    small = small.reshape(devices, -1)
    segment = lax.dynamic_index_in_dim(
        small.reshape(ring, lines, -1), lax.axis_index("batch"), 1, keepdims=False
    )[:, count : count + rows].reshape(length).astype(F32)
    cuts = np.cumsum([own, own, own, slots_all // devices, RANK * slots_all // devices])
    gain_one, gain_head, gain_two, bias_full, expand_t, w_squeeze = jnp.split(
        small[:, :count], cuts, axis=1
    )
    gain_one = permuted(gain_one.reshape(width)).astype(F32)
    gain_head = lax.dynamic_slice_in_dim(gain_head.reshape(width), head * head_size, head_size, 0)
    gain_head = gain_head.astype(F32)
    gain_two = gain_two.reshape(width).astype(F32)
    bias_head = lax.dynamic_slice_in_dim(bias_full.reshape(slots_all), head * SLOTS, SLOTS, 0)
    expand_head = lax.dynamic_slice_in_dim(
        expand_t.reshape(slots_all, RANK), head * SLOTS, SLOTS, 0
    )
    w_squeeze = permuted(w_squeeze.reshape(width, RANK).T)

    chunked = segment.reshape(-1, CHUNK)
    before = jnp.concatenate([jnp.full((1,), -1.0, F32), chunked[:-1, -1]])
    previous = jnp.concatenate([jnp.full((1,), -1.0, F32), segment[:-1]])
    mask_rows = jnp.stack(
        [
            segment,
            (chunked == before[:, None]).astype(F32).reshape(-1),
            (chunked == chunked[:, -1:]).astype(F32).reshape(-1),
            (segment == previous).astype(F32),
        ]
        + [jnp.zeros_like(segment)] * 4
    )

    inputs = inputs.astype(F32)
    scale_one = rms_scale(inputs)
    plain_one = inputs * scale_one
    normed = (plain_one * gain_one).astype(BF16)
    mixer_pre = dot_nn(normed, w_mixer)
    joined = mixer_pre.astype(BF16)
    if copies > 1:
        joined = jnp.concatenate(
            [whole_head(joined[:, at * part : (at + 1) * part]) for at in range(3)], axis=1
        )
    swish_pre = whole_head(mixer_pre[:, 3 * part :])
    reduced = dot_nt(normed, w_squeeze).astype(BF16)
    forget_logit = dot_nt(expand_head, reduced) + bias_head.astype(F32)[:, None]
    log_rate = jax.nn.log_sigmoid(forget_logit) / TAU_GATE
    rates = jnp.concatenate([log_rate, -jnp.expm1(log_rate)], axis=0)
    order = mine.reshape(1).astype(jnp.int32)
    mixed, choice, starts = mixer_forward(order, ring, head_size, joined, rates, mask_rows)
    head_factor = rms_scale(mixed)
    head_plain = mixed * head_factor
    head_normed = head_plain * gain_head
    swish_sig = jax.nn.sigmoid(swish_pre)
    swish_act = swish_pre * swish_sig
    gated = own_part((head_normed * swish_act).astype(BF16))
    terms = dot_nn(gated, w_output).astype(BF16)
    terms, grad_out = lax.optimization_barrier((terms, grad_out))
    if ring == 4:
        feed_in, hidden = fold(
            finish_forward,
            terms.reshape(ring, rows, width),
            (input_own, gain_two[None]),
            (jax.ShapeDtypeStruct((rows, width), F32),),
            "fold_forward",
        )
        feed_in = feed_in.reshape(length, width)
    else:
        hidden = input_own.astype(F32) + scattered(terms, ring)
        feed_in = gathered((hidden * rms_scale(hidden) * gain_two).astype(BF16), ring)

    feed_pre = dot_nn(feed_in, w_feed)
    gate_pre, up_pre = feed_pre[:, :hidden_part], feed_pre[:, hidden_part:]
    gate_sig = jax.nn.sigmoid(gate_pre)
    gate_act = gate_pre * gate_sig
    inner = (gate_act * up_pre).astype(BF16)

    term_down = dot_tn(inner, grad_out).astype(BF16)
    grad_inner = dot_nt(after(grad_out, term_down), w_down)
    grad_gatepre = grad_inner * up_pre * (gate_sig * (1.0 + gate_pre * (1.0 - gate_sig)))
    grad_feedpre = jnp.concatenate(
        [grad_gatepre.astype(BF16), (grad_inner * gate_act).astype(BF16)], axis=1
    )
    back_feedin = dot_nt(grad_feedpre, w_feed).astype(BF16)
    result_terms = dot_nn(after(inner, back_feedin), w_down).astype(BF16)
    feed_lines = feed_in if ring == 4 else permuted(feed_in)
    term_feedpre = core_sum(after(feed_lines, back_feedin), grad_feedpre, lines, (result_terms,))
    down_share = lax.psum_scatter(term_down, "batch", scatter_dimension=0, tiled=True)
    feed_sum = line_sum(after(term_feedpre, down_share), lines)
    if ring == 4:
        grad_branch, grad_hidden, term_feed = fold(
            finish_backward,
            after(back_feedin, term_feedpre).reshape(ring, rows, width),
            (grad_own, hidden, gain_two[None]),
            (
                jax.ShapeDtypeStruct((rows, width), F32),
                jax.ShapeDtypeStruct((1, width), F32),
            ),
            "fold_backward",
        )
        grad_branch, term_feed = grad_branch.reshape(length, width), term_feed[0]
    else:
        grad_feedin = scattered(back_feedin, ring)
        scale_two = rms_scale(hidden)
        term_feed = jnp.sum(grad_feedin * hidden * scale_two, axis=0)
        scaled_two = grad_feedin * gain_two
        grad_hidden = (
            grad_own.astype(F32)
            + scale_two * scaled_two
            - hidden * scale_two**3 * jnp.mean(scaled_two * hidden, axis=-1, keepdims=True)
        )
        grad_branch = gathered(grad_hidden.astype(BF16), ring)

    grad_gated = whole_head(dot_nt(grad_branch, w_output))
    term_output = core_sum(gated, grad_branch, lines)
    output_share = line_sum(after(term_output, feed_sum), lines)

    slope = swish_sig * (1.0 + swish_pre * (1.0 - swish_sig))
    grad_swishpre = own_part((grad_gated * head_normed * slope).astype(BF16))
    grad_normed_head = grad_gated * swish_act
    term_head = jnp.sum(grad_normed_head * head_plain, axis=0) / copies
    scaled_head = grad_normed_head * gain_head
    scaled_head = after(scaled_head, term_output)
    grad_mixed = head_factor * scaled_head - mixed * head_factor**3 * jnp.mean(
        scaled_head * mixed, axis=-1, keepdims=True
    )
    grad_pre, grad_rate = mixer_backward(
        order, ring, joined, grad_mixed.astype(BF16), rates, mask_rows, choice, starts
    )
    grad_logit = (grad_rate * jax.nn.sigmoid(-forget_logit) / TAU_GATE).astype(BF16)
    term_bias = jnp.sum(grad_logit.astype(F32), axis=1) / copies
    term_expand = dot_nn(grad_logit, reduced) / copies
    grad_reduced = (dot_tn(grad_logit, expand_head) / copies).astype(BF16)
    if copies > 1:
        grad_pre = jnp.concatenate(
            [own_part(grad_pre[:, at * head_size : (at + 1) * head_size]) for at in range(3)], axis=1
        )
    grad_pre = jnp.concatenate([grad_pre, grad_swishpre], axis=1)
    term_pre = dot_tn(after(normed, output_share), grad_pre).astype(BF16)
    pre_sum = lax.psum_scatter(term_pre, "batch", scatter_dimension=0, tiled=True)
    grad_normed = dot_nt(after(grad_pre, term_pre), w_mixer) + dot_nn(grad_reduced, w_squeeze)
    result = hidden + scattered(after(result_terms, grad_branch), ring, (term_pre,))
    layer_output = result.astype(BF16).reshape(1, rows, width)
    grad_normed = dot_nt(after(grad_pre, term_pre), w_mixer) + dot_nn(grad_reduced, w_squeeze)
    term_mixer = restored(jnp.sum(grad_normed * plain_one, axis=0))
    term_squeeze = restored(dot_tn(grad_reduced, normed))
    grad_normed = restored(scattered(grad_normed.astype(BF16), ring))
    inputs_own = input_own.astype(F32)
    scale_own = rms_scale(inputs_own)
    scaled_one = grad_normed * restored(gain_one)
    grad_input = (
        grad_hidden
        + scale_own * scaled_one
        - inputs_own * scale_own**3 * jnp.mean(scaled_one * inputs_own, axis=-1, keepdims=True)
    ).astype(BF16)
    pre_share = exchanged(pre_sum.reshape(ring, own, 4 * part), mine, ring)
    pre_share = pre_share.reshape(ring, own, 4, part).transpose(2, 1, 0, 3)
    query_share, key_share, value_share, swish_share = pre_share.reshape(4, own, width).astype(F32)
    feed_share = exchanged(after(feed_sum, term_pre).reshape(ring, own, 2 * hidden_part), mine, ring)
    gate_share = feed_share[:, :, :hidden_part].transpose(1, 0, 2).reshape(own, -1).astype(F32)
    up_share = feed_share[:, :, hidden_part:].transpose(1, 0, 2).reshape(own, -1).astype(F32)

    def placed(array, size):
        full = jnp.zeros((HEADS, size) + array.shape[1:], F32)
        return lax.dynamic_update_slice_in_dim(full, array[None], head, 0)

    terms = jnp.concatenate(
        [
            term_mixer.reshape(devices, -1),
            placed(term_head, head_size).reshape(devices, -1),
            term_feed.reshape(devices, -1),
            placed(term_bias, SLOTS).reshape(devices, -1),
            placed(term_expand, SLOTS).reshape(devices, -1),
            term_squeeze.T.reshape(devices, -1),
        ],
        axis=1,
    )
    share = halved(halved(terms, "seq"), "batch")[0]
    mixer_share, head_share, feedgain_share, bias_share, expand_share, squeeze_share = jnp.split(
        share, cuts
    )
    return (
        layer_output,
        grad_input.reshape(1, rows, width),
        mixer_share,
        query_share,
        key_share,
        value_share,
        squeeze_share.reshape(own, RANK),
        expand_share.reshape(-1, RANK).T,
        bias_share,
        swish_share,
        head_share,
        output_share.astype(F32),
        feedgain_share,
        gate_share,
        up_share,
        down_share.astype(F32),
    )


def solution(mesh):
    rows = P(BOTH, None)
    spread = P(BOTH)
    in_specs = (
        P("batch", "seq", None),
        P("batch", "seq"),
        spread,
        rows,
        rows,
        rows,
        rows,
        P(None, BOTH),
        spread,
        rows,
        spread,
        rows,
        spread,
        rows,
        rows,
        rows,
        P("batch", "seq", None),
    )
    out_specs = (
        P("batch", "seq", None),
        P("batch", "seq", None),
        spread,
        rows,
        rows,
        rows,
        rows,
        P(None, BOTH),
        spread,
        rows,
        spread,
        rows,
        spread,
        rows,
        rows,
        rows,
    )
    return jax.shard_map(local, mesh=mesh, in_specs=in_specs, out_specs=out_specs, check_vma=False)
```

```python
import functools

import jax
import jax.numpy as jnp
import numpy as np
from jax import lax
from jax.experimental import pallas as pl
from jax.experimental.pallas import tpu as pltpu
from jax.sharding import PartitionSpec as P

HEADS = 4
SLOTS = 64
RANK = 16
EPS = 1e-06
TAU_GATE = 8.0
CHUNK = 128
SUB = 16
BOTH = ("seq", "batch")
F32 = jnp.float32
BF16 = jnp.bfloat16
HIGHEST = lax.Precision.HIGHEST


def dot_nn(left, right):
    return lax.dot_general(left, right, (((1,), (0,)), ((), ())), preferred_element_type=F32)


def dot_nt(left, right):
    return lax.dot_general(left, right, (((1,), (1,)), ((), ())), preferred_element_type=F32)


def dot_tn(left, right):
    return lax.dot_general(left, right, (((0,), (0,)), ((), ())), preferred_element_type=F32)


def exact_nn(left, right):
    return lax.dot_general(
        left, right, (((1,), (0,)), ((), ())), precision=HIGHEST, preferred_element_type=F32
    )


def exact_nt(left, right):
    return lax.dot_general(
        left, right, (((1,), (1,)), ((), ())), precision=HIGHEST, preferred_element_type=F32
    )


def halves(value):
    high = value.astype(BF16)
    return high, (value - high.astype(F32)).astype(BF16)


def split_nn(left, right):
    high, rest = halves(left)
    return dot_nn(high, right) + dot_nn(rest, right)


def split_nt(left, right):
    high, rest = halves(left)
    return dot_nt(high, right) + dot_nt(rest, right)


LEVELS = (CHUNK // SUB).bit_length() - 1


def fill_tables(sums, covers, apart):
    source = lax.broadcasted_iota(jnp.int32, (CHUNK, CHUNK), 0)
    target = lax.broadcasted_iota(jnp.int32, (CHUNK, CHUNK), 1)

    def group(at, size):
        return jnp.bitwise_and(at, CHUNK - size)

    for level in range(LEVELS):
        half = SUB << level
        right = jnp.bitwise_and(target, half) != 0
        edge = group(target, 2 * half) + (half - 1)
        low, high = jnp.where(right, edge, target), jnp.where(right, target, edge)
        sums[:, level * CHUNK : (level + 1) * CHUNK] = jnp.where(
            (source > low) & (source <= high), 1.0, 0.0
        )
        same = group(source, 2 * half) == group(target, 2 * half)
        covers[level] = jnp.where(same & (jnp.bitwise_and(source, half) == 0) & right, 1.0, 0.0)
    sums[:, LEVELS * CHUNK : (LEVELS + 1) * CHUNK] = jnp.where(source <= target, 1.0, 0.0)
    sums[:, (LEVELS + 1) * CHUNK :] = jnp.where(source > target, 1.0, 0.0)
    apart[...] = jnp.where(group(source, SUB) == group(target, SUB), target - source, -1)


TABLES = [
    pltpu.VMEM((CHUNK, (LEVELS + 2) * CHUNK), F32),
    pltpu.VMEM((LEVELS, CHUNK, CHUNK), F32),
    pltpu.VMEM((CHUNK, CHUNK), jnp.int32),
]


def same_document(rows):
    source = lax.broadcasted_iota(jnp.int32, (CHUNK, CHUNK), 0)
    target = lax.broadcasted_iota(jnp.int32, (CHUNK, CHUNK), 1)
    number = rows[0:1, :]
    column = jnp.sum(jnp.where(source == target, number, 0.0), axis=1, keepdims=True)
    return column == number


def rolled(value, by):
    return value if by % CHUNK == 0 else pltpu.roll(value, by % CHUNK, 1)


def exponents(rate, sums):
    return jnp.exp(exact_nn(rate, sums))


def piece(value, at):
    return value[:, at * CHUNK : (at + 1) * CHUNK]


def mixer_forward_kernel(
    factor, mine, query, key, value, rate, rows, output, choice_out, start_out, state, sums, covers, apart
):
    levels = LEVELS

    @pl.when(pl.program_id(0) == 0)
    def _():
        state[...] = jnp.zeros_like(state)
        fill_tables(sums, covers, apart)

    key_in, value_in = state[:SLOTS, :], state[SLOTS:, :]
    start_out[0] = state[...]
    q, k, v = query[...], key[...], value[...]
    a, g = rate[:SLOTS, :], rate[SLOTS:, :]
    decay = exponents(a, sums[...])
    before, after = piece(decay, levels), piece(decay, levels + 1)
    carried = before * rows[1:2, :]
    visible = same_document(rows)
    scores = jnp.where(visible, dot_nt(k, q) * factor, 0.0)
    logits = carried * (split_nt(key_in, q) * factor)
    for level in range(levels):
        part = piece(decay, level)
        logits = logits + part * exact_nn(part * g, scores * covers[level])
    gap = apart[...]
    total = jnp.zeros_like(a)
    weights = []
    for by in range(SUB):
        if by:
            total = total + rolled(a, by - 1)
        weight = jnp.exp(total) * rolled(g, by)
        weights.append(weight)
        logits = logits + weight * jnp.sum(
            jnp.where(gap == by, scores, 0.0), axis=0, keepdims=True
        )
    attention = jnp.exp(logits - jnp.max(logits, axis=0, keepdims=True))
    attention = attention / jnp.sum(attention, axis=0, keepdims=True)
    choice_out[:SLOTS, :] = attention
    choice_out[SLOTS:, :] = logits
    mixing = jnp.zeros((CHUNK, CHUNK), F32)
    for level in range(levels):
        part = piece(decay, level)
        mixing = mixing + covers[level] * dot_tn(
            (part * g).astype(BF16), (part * attention).astype(BF16)
        )
    for by in range(SUB):
        row = jnp.sum(weights[by] * attention, axis=0, keepdims=True)
        mixing = jnp.where(gap == by, row, mixing)
    mixing = jnp.where(visible, mixing, 0.0).astype(BF16)
    output[...] = dot_tn(mixing, v) + dot_tn(
        (carried * attention).astype(BF16), value_in.astype(BF16)
    )
    ends = after * g * rows[2:3, :]
    keep = carried[:, CHUNK - 1 : CHUNK]
    state[:SLOTS, :] = keep * key_in + split_nn(ends, k)
    state[SLOTS:, :] = keep * value_in + split_nn(ends, v)


def mixer_backward_kernel(
    factor, mine, query, key, value, grad_output, rate, rows, choice, start, grad_all, grad_rate,
    state_grad, flow, sums, covers, apart,
):
    levels = LEVELS

    @pl.when(pl.program_id(0) == 0)
    def _():
        state_grad[...] = jnp.zeros_like(state_grad)
        flow[...] = jnp.zeros_like(flow)
        fill_tables(sums, covers, apart)

    key_in, value_in = start[0, :SLOTS, :], start[0, SLOTS:, :]
    key_after, value_after = state_grad[:SLOTS, :], state_grad[SLOTS:, :]
    q, k, v, d = query[...], key[...], value[...], grad_output[...]
    size = q.shape[1]
    a, g = rate[:SLOTS, :], rate[SLOTS:, :]
    attention, logits = choice[:SLOTS, :], choice[SLOTS:, :]
    decay = exponents(a, sums[...])
    before, after = piece(decay, levels), piece(decay, levels + 1)
    carried = before * rows[1:2, :]
    visible = same_document(rows)
    scores = jnp.where(visible, dot_nt(k, q) * factor, 0.0)
    reads = jnp.where(visible, dot_nt(v, d), 0.0)
    gap = apart[...]
    grad_att = carried * split_nt(value_in, d)
    for level in range(levels):
        part = piece(decay, level)
        grad_att = grad_att + part * exact_nn(part * g, reads * covers[level])
    total = jnp.zeros_like(a)
    bare, weights, score_rows, read_rows = [], [], [], []
    for by in range(SUB):
        if by:
            total = total + rolled(a, by - 1)
        bare.append(jnp.exp(total))
        weights.append(bare[by] * rolled(g, by))
        score_rows.append(jnp.sum(jnp.where(gap == by, scores, 0.0), axis=0, keepdims=True))
        read_rows.append(jnp.sum(jnp.where(gap == by, reads, 0.0), axis=0, keepdims=True))
        grad_att = grad_att + weights[by] * read_rows[by]
    grad_logits = attention * (
        grad_att - jnp.sum(attention * grad_att, axis=0, keepdims=True)
    )
    mixing = jnp.zeros((CHUNK, CHUNK), F32)
    spread = jnp.zeros((CHUNK, CHUNK), F32)
    ends = after * rows[2:3, :]
    grad_inflow = ends * (split_nt(key_after, k) + split_nt(value_after, v))
    for level in range(levels):
        part = piece(decay, level)
        left = (part * g).astype(BF16)
        att_part, log_part = part * attention, part * grad_logits
        mixing = mixing + covers[level] * dot_tn(left, att_part.astype(BF16))
        spread = spread + covers[level] * dot_tn(left, log_part.astype(BF16))
        grad_inflow = grad_inflow + part * (
            exact_nt(log_part, scores * covers[level]) + exact_nt(att_part, reads * covers[level])
        )
    for by in range(SUB):
        row = jnp.sum(weights[by] * attention, axis=0, keepdims=True)
        mixing = jnp.where(gap == by, row, mixing)
        row = jnp.sum(weights[by] * grad_logits, axis=0, keepdims=True)
        spread = jnp.where(gap == by, row, spread)
        terms = bare[by] * (grad_logits * score_rows[by] + attention * read_rows[by])
        grad_inflow = grad_inflow + rolled(terms, -by)
    mixing = jnp.where(visible, mixing, 0.0).astype(BF16)
    spread = (jnp.where(visible, spread, 0.0) * factor).astype(BF16)
    log_carried = carried * grad_logits * factor
    att_carried = carried * attention
    ends = (ends * g).astype(BF16)
    grad_all[:, :size] = (
        dot_tn(spread, k) + dot_tn(log_carried.astype(BF16), key_in.astype(BF16))
    ).astype(BF16)
    grad_all[:, size : 2 * size] = (dot_nn(spread, q) + dot_tn(ends, key_after.astype(BF16))).astype(BF16)
    grad_all[:, 2 * size :] = (dot_nn(mixing, d) + dot_tn(ends, value_after.astype(BF16))).astype(BF16)
    change = grad_logits * logits + attention * grad_att - g * grad_inflow
    later = piece(sums, levels + 1) + jnp.where(gap == 0, 1.0, 0.0)
    same = jnp.where(visible, later, 0.0)
    flows = exact_nn(change, same) + rows[2:3, :] * flow[:, 0:1]
    grad_rate[...] = rows[3:4, :] * flows - jnp.exp(a) * grad_inflow
    keep = carried[:, CHUNK - 1 : CHUNK]
    key_before = keep * key_after + split_nn(log_carried, q)
    value_before = keep * value_after + split_nn(att_carried, d)
    state_grad[:SLOTS, :] = key_before
    state_grad[SLOTS:, :] = value_before
    flow[...] = jnp.broadcast_to(
        jnp.sum(key_before * key_in + value_before * value_in, axis=1, keepdims=True), flow.shape
    )


def mixer_specs(length, size, ring, backward):
    count = length // CHUNK
    per = count // ring

    def natural(step):
        return count - 1 - step if backward else step

    def moved(step, mine):
        at = natural(step)
        return lax.bitwise_xor(at // per, mine[0]) * per + at % per

    wide = [
        pl.BlockSpec((CHUNK, size), lambda step, mine, at=at: (moved(step, mine), at))
        for at in range(3)
    ]
    everything = pl.BlockSpec((CHUNK, 3 * size), lambda step, mine: (moved(step, mine), 0))
    pair = pl.BlockSpec((2 * SLOTS, CHUNK), lambda step, mine: (0, moved(step, mine)))
    slim = pl.BlockSpec((SLOTS, CHUNK), lambda step, mine: (0, moved(step, mine)))
    rows = pl.BlockSpec((8, CHUNK), lambda step, mine: (0, natural(step)))
    state = pl.BlockSpec((1, 2 * SLOTS, size), lambda step, mine: (natural(step), 0, 0))
    return count, wide, everything, pair, slim, rows, state


def mixer_forward(mine, ring, size, joined, rates, rows):
    length = joined.shape[0]
    count, wide, _, pair, _, row_spec, state = mixer_specs(length, size, ring, False)
    return pl.pallas_call(
        functools.partial(mixer_forward_kernel, size ** (-0.25)),
        out_shape=(
            jax.ShapeDtypeStruct((length, size), F32),
            jax.ShapeDtypeStruct((2 * SLOTS, length), F32),
            jax.ShapeDtypeStruct((count, 2 * SLOTS, size), F32),
        ),
        grid_spec=pltpu.PrefetchScalarGridSpec(
            num_scalar_prefetch=1,
            grid=(count,),
            in_specs=wide + [pair, row_spec],
            out_specs=[wide[0], pair, state],
            scratch_shapes=[pltpu.VMEM((2 * SLOTS, size), F32)] + TABLES,
        ),
        compiler_params=pltpu.CompilerParams(vmem_limit_bytes=32 << 20),
        cost_estimate=pl.CostEstimate(
            flops=length * size * 2000, bytes_accessed=length * size * 12, transcendentals=length * 4096
        ),
        name="mixer_forward",
    )(mine, joined, joined, joined, rates, rows)


def mixer_backward(mine, ring, joined, grad, rates, rows, choice, starts):
    length, size = grad.shape
    count, wide, everything, pair, slim, row_spec, state = mixer_specs(length, size, ring, True)
    return pl.pallas_call(
        functools.partial(mixer_backward_kernel, size ** (-0.25)),
        out_shape=(
            jax.ShapeDtypeStruct((length, 3 * size), BF16),
            jax.ShapeDtypeStruct((SLOTS, length), F32),
        ),
        grid_spec=pltpu.PrefetchScalarGridSpec(
            num_scalar_prefetch=1,
            grid=(count,),
            in_specs=wide + [wide[0], pair, row_spec, pair, state],
            out_specs=[everything, slim],
            scratch_shapes=[pltpu.VMEM((2 * SLOTS, size), F32), pltpu.VMEM((SLOTS, 128), F32)]
            + TABLES,
        ),
        compiler_params=pltpu.CompilerParams(vmem_limit_bytes=32 << 20),
        cost_estimate=pl.CostEstimate(
            flops=length * size * 4000, bytes_accessed=length * size * 20, transcendentals=length * 4096
        ),
        name="mixer_backward",
    )(mine, joined, joined, joined, grad, rates, rows, choice, starts)


def peers(ring, mine):
    found = []
    for by in range(1, ring):
        at, bit = mine, 1
        while bit <= by:
            if by & bit:
                at = at + bit * (1 - 2 * ((at // bit) % 2))
            bit *= 2
        found.append(at)
    return found


class Copies:
    def __init__(self, local, send, recv):
        self.local, self.send, self.recv = local, send, recv
        self.here, self.away = 0, 0
        self.open = []

    def near(self, source, target):
        copy = pltpu.make_async_copy(source, target, self.local.at[self.here])
        self.here += 1
        copy.start()
        return copy

    def far(self, source, target, landed, device, when=None):
        at = self.away
        self.away += 1
        copy = pltpu.make_async_remote_copy(
            source, target, self.send.at[at], self.recv.at[at], device_id=device,
            device_id_type=pl.DeviceIdType.MESH,
        )
        if when is None:
            copy.start()
        else:
            pl.when(when)(copy.start)
        self.open.append((copy, when))
        return pltpu.make_async_remote_copy(
            landed, landed, self.send.at[at], self.recv.at[at], device_id=device,
            device_id_type=pl.DeviceIdType.MESH,
        ).wait_recv

    def close(self):
        for copy, when in self.open:
            if when is None:
                copy.wait_send()
            else:
                pl.when(when)(copy.wait_send)


PARTS = 4


def fold_kernel(finish, extras, *refs):
    terms, given = refs[0], refs[1 : 1 + extras]
    blocks = refs[1 + extras]
    made = refs[2 + extras : -9]
    first, second, third, two_low, one_high, own, local_sem, send_sem, recv_sem = refs[-9:]
    mine, batch = lax.axis_index("seq"), lax.axis_index("batch")
    others = peers(4, mine)
    row, col = (others[0], batch), (others[1], batch)
    copies = Copies(local_sem, send_sem, recv_sem)
    size = terms.shape[1] // PARTS

    def span(at):
        low = pl.ds(at * size, size // 2)
        return pl.ds(at * size, size), low, pl.ds(at * size + size // 2, size // 2)

    opening, direct = [], []

    def open_part(at):
        _, low, high = span(at)
        opening.append(
            (
                copies.far(terms.at[3, low], first.at[low], first.at[low], row),
                copies.far(terms.at[3, high], first.at[high], first.at[high], col),
            )
        )

    def pass_part(at):
        _, low, high = span(at)
        waits = [
            copies.far(terms.at[2, high], second.at[high], second.at[high], col),
            copies.far(terms.at[1, low], third.at[low], third.at[low], row),
        ]
        opening[at][0]()
        two_low[low, :] = added(terms[2, low, :], first[low, :])
        waits.append(copies.far(two_low.at[low], second.at[low], second.at[low], col))
        opening[at][1]()
        one_high[high, :] = added(terms[1, high, :], first[high, :])
        waits.append(copies.far(one_high.at[high], third.at[high], third.at[high], row))
        direct.append(waits)

    spread, local, passed = [], [], []

    def close_part(at):
        full, _, _ = span(at)
        for wait in direct[at]:
            wait()
        total = terms[0, full, :].astype(F32) + second[full, :].astype(F32) + third[full, :].astype(F32)
        own[full, :] = finish(total, full, at, given, made)
        spread.append(
            (
                copies.far(own.at[full], blocks.at[1, full], blocks.at[1, full], row),
                copies.far(own.at[full], blocks.at[2, full], blocks.at[2, full], col),
            )
        )
        local.append(copies.near(own.at[full], blocks.at[0, full]))

    def forward_part(at):
        _, low, high = span(at)
        for wait in spread[at]:
            wait()
        passed.append(copies.far(blocks.at[2, low], blocks.at[3, low], blocks.at[3, low], row))
        passed.append(copies.far(blocks.at[1, high], blocks.at[3, high], blocks.at[3, high], col))

    open_part(0)
    for at in range(PARTS + 2):
        if at + 1 < PARTS:
            open_part(at + 1)
        if at < PARTS:
            pass_part(at)
        if 1 <= at <= PARTS:
            close_part(at - 1)
        if at >= 2:
            forward_part(at - 2)
    for wait in passed:
        wait()
    for copy in local:
        copy.wait()
    copies.close()


def half_blocks(value, order):
    lane = lax.broadcasted_iota(jnp.int32, (value.shape[0], 128), 1)
    made = []
    for pair in zip(order[::2], order[1::2]):
        low, high = (
            value[:, block * 128 : (block + 1) * 128]
            if half == want
            else pltpu.roll(value[:, block * 128 : (block + 1) * 128], 64, 1)
            for want, (block, half) in enumerate(pair)
        )
        made.append(jnp.where(lane < 64, low, high))
    return jnp.concatenate(made, axis=1)


def by_line(value):
    lines = value.shape[1] // 256
    return half_blocks(
        value, [divmod(ring * lines + line, 2) for line in range(lines) for ring in range(4)]
    )


def by_ring(value):
    lines = value.shape[1] // 256
    return half_blocks(
        value, [divmod(line * 4 + ring, 2) for ring in range(4) for line in range(lines)]
    )


def finish_forward(total, full, at, given, made):
    inputs, gain = given
    hidden = inputs[full, :].astype(F32) + total
    made[0][full, :] = hidden
    return by_line(hidden * rms_scale(hidden) * gain[...]).astype(BF16)


def finish_backward(total, full, at, given, made):
    cotangent, hidden_ref, gain = given
    total = by_ring(total)
    hidden = hidden_ref[full, :]
    scale = rms_scale(hidden)
    plain = hidden * scale
    term = jnp.sum(total * plain, axis=0, keepdims=True)
    made[1][...] = term if at == 0 else made[1][...] + term
    scaled = total * gain[...]
    grad = (
        cotangent[full, :].astype(F32)
        + scale * scaled
        - plain * (scale * jnp.mean(scaled * plain, axis=-1, keepdims=True))
    )
    made[0][full, :] = grad
    return grad.astype(BF16)


def fold(finish, terms, given, made, name):
    ring, rows, width = terms.shape
    inside = pl.BlockSpec(memory_space=pltpu.VMEM)
    block = pltpu.VMEM((rows, width), BF16)
    return pl.pallas_call(
        functools.partial(fold_kernel, finish, len(given)),
        out_shape=(jax.ShapeDtypeStruct((ring, rows, width), BF16),) + made,
        in_specs=[inside] * (1 + len(given)),
        out_specs=[pl.BlockSpec(memory_space=pltpu.HBM)] + [inside] * len(made),
        scratch_shapes=[block] * 6
        + [
            pltpu.SemaphoreType.DMA((PARTS,)),
            pltpu.SemaphoreType.DMA((PARTS * 10,)),
            pltpu.SemaphoreType.DMA((PARTS * 10,)),
        ],
        compiler_params=pltpu.CompilerParams(has_side_effects=True, vmem_limit_bytes=40 << 20),
        name=name,
    )(terms, *given)


def rms_scale(features):
    return lax.rsqrt(jnp.mean(features * features, axis=-1, keepdims=True) + EPS)


def swapped(block, by, ring):
    return lax.ppermute(block, "seq", [(i, i ^ by) for i in range(ring)])


def gathered(block, ring):
    if ring != 4:
        return jnp.concatenate([block] + [swapped(block, by, ring) for by in range(1, ring)], axis=0)
    half = block.shape[0] // 2
    one, two = swapped(block, 1, ring), swapped(block, 2, ring)
    low, high = swapped(two[:half], 1, ring), swapped(one[half:], 2, ring)
    return jnp.concatenate([block, one, two, low, high], axis=0)


def scattered(terms, ring, wait_first=None, wait_second=None):
    rows = terms.shape[0] // ring
    parts = [terms[by * rows : (by + 1) * rows] for by in range(ring)]
    total = parts[0].astype(F32)
    if ring != 4:
        for by in range(1, ring):
            total = total + swapped(parts[by], by, ring).astype(F32)
        return total if wait_first is None else (total, wait_first, wait_second)
    half = rows // 2
    low, high = swapped(parts[3][:half], 1, ring), swapped(parts[3][half:], 2, ring)
    if wait_first is not None:
        low, high, wait_first = lax.optimization_barrier((low, high, wait_first))
    two = jnp.concatenate([added(parts[2][:half], low), parts[2][half:]], axis=0)
    one = jnp.concatenate([parts[1][:half], added(parts[1][half:], high)], axis=0)
    one, two = swapped(one, 1, ring), swapped(two, 2, ring)
    if wait_first is not None:
        one, two, wait_second = lax.optimization_barrier((one, two, wait_second))
    total = total + one.astype(F32) + two.astype(F32)
    return total if wait_first is None else (total, wait_first, wait_second)


def added(left, right):
    return (left.astype(F32) + right.astype(F32)).astype(BF16)


def flipped(block, axis, by):
    return lax.ppermute(block, axis, [(i, i ^ by) for i in range(lax.axis_size(axis))])


def doubled(block, axis):
    by, mine = 1, lax.axis_index(axis)
    while by < lax.axis_size(axis):
        other = flipped(block, axis, by)
        first = (mine & by) == 0
        block = jnp.concatenate(
            [jnp.where(first, block, other), jnp.where(first, other, block)], axis=0
        )
        by *= 2
    return block


def halved(block, axis):
    by, mine = lax.axis_size(axis) // 2, lax.axis_index(axis)
    while by:
        low, high = jnp.split(block, 2, axis=0)
        first = (mine & by) == 0
        block = jnp.where(first, low, high) + flipped(jnp.where(first, high, low), axis, by)
        by //= 2
    return block


def core_halves(array, lines, axis):
    size = array.shape[axis] // lines
    even, odd = (
        jnp.concatenate(
            [
                lax.slice_in_dim(array, line * size, (line + 1) * size, axis=axis)
                for line in range(which, lines, 2)
            ],
            axis=axis,
        )
        for which in range(2)
    )
    first = lax.axis_index("batch") % 2 == 0
    return jnp.where(first, even, odd), jnp.where(first, odd, even)


def core_sum(features, grads, lines, fill=()):
    if (features.shape[1] // lines) % 128:
        mine, others = core_halves(dot_tn(features, grads).astype(BF16), lines, 0)
        return added(mine, flipped(others, "batch", 1))
    mine, others = core_halves(features, lines, 1)
    sent = flipped(dot_tn(others, grads).astype(BF16), "batch", 1)
    mine = after(mine, *fill) if fill else mine
    return (dot_tn(mine, grads) + sent.astype(F32)).astype(BF16)


def line_sum(terms, lines):
    groups = [list(range(core, lines, 2)) for core in range(2)]
    return lax.psum_scatter(
        terms, "batch", scatter_dimension=0, axis_index_groups=groups, tiled=True
    )


def after(value, *others):
    return lax.optimization_barrier((value,) + others)[0]


def exchanged(blocks, mine, ring):
    parts = [
        swapped(lax.dynamic_index_in_dim(blocks, mine ^ by, 0, keepdims=False), by, ring)
        if by
        else lax.dynamic_index_in_dim(blocks, mine, 0, keepdims=False)
        for by in range(ring)
    ]
    made = jnp.stack(parts)
    return jnp.concatenate(
        [lax.dynamic_index_in_dim(made, mine ^ j, 0, keepdims=True) for j in range(ring)], axis=0
    )


def local(
    layer_input,
    segments,
    mixer_gain,
    query_weight,
    key_weight,
    value_weight,
    squeeze,
    expand,
    forget_bias,
    swish_weight,
    head_gain,
    output_weight,
    feed_gain,
    gate_weight,
    up_weight,
    down_weight,
    cotangent,
):
    ring, lines = lax.axis_size("seq"), lax.axis_size("batch")
    devices = ring * lines
    mine = lax.axis_index("seq")
    rows, width = layer_input.shape[1], layer_input.shape[2]
    length = rows * ring
    own = width // devices
    head_size = width // HEADS
    copies = ring // HEADS
    part = width // ring
    head = mine // copies
    hidden_part = gate_weight.shape[1] // ring
    slots_all = HEADS * SLOTS

    def to_order(array):
        if copies == 1:
            return array
        blocks = array.reshape((ring, rows) + array.shape[1:])
        moved = [lax.dynamic_index_in_dim(blocks, mine ^ by, 0, keepdims=False) for by in range(ring)]
        return jnp.concatenate(moved, axis=0)

    def whole_head(array):
        if copies == 1:
            return array
        full = lax.all_gather(to_order(array), "seq", axis=1, tiled=True)
        return to_order(lax.dynamic_slice_in_dim(full, head * head_size, head_size, 1))

    def own_part(array):
        if copies == 1:
            return array
        return lax.dynamic_slice_in_dim(array, (mine % copies) * part, part, 1)

    params = jnp.concatenate(
        [
            mixer_gain,
            head_gain,
            feed_gain,
            forget_bias,
            expand.T.reshape(-1),
            squeeze.reshape(-1),
        ]
    )
    count = params.shape[0]
    params = jnp.concatenate([params, segments.reshape(rows).astype(BF16)])
    input_own = layer_input.reshape(rows, width)
    grad_own = cotangent.reshape(rows, width)

    def permuted(array):
        shape = array.shape[:-1]
        array = array.reshape(shape + (ring, lines, own))
        return jnp.swapaxes(array, -3, -2).reshape(shape + (width,))

    def restored(array):
        shape = array.shape[:-1]
        array = array.reshape(shape + (lines, ring, own))
        return jnp.swapaxes(array, -3, -2).reshape(shape + (width,))

    def columns(*arrays):
        blocks = [a.reshape(own, ring, a.shape[1] // ring) for a in arrays]
        return jnp.concatenate(blocks, axis=2).transpose(1, 0, 2)

    w_output = lax.all_gather(output_weight, "batch", axis=0, tiled=True)
    mixer_columns = exchanged(
        columns(query_weight, key_weight, value_weight, swish_weight), mine, ring
    )
    w_mixer = lax.all_gather(mixer_columns.reshape(ring * own, -1), "batch", axis=0, tiled=True)
    feed_columns = exchanged(columns(gate_weight, up_weight), mine, ring)
    w_feed = lax.all_gather(feed_columns.reshape(ring * own, -1), "batch", axis=0, tiled=True)
    w_down = lax.all_gather(after(down_weight, feed_columns), "batch", axis=0, tiled=True)
    if ring != 4:
        w_feed = w_feed.reshape(lines, ring, own, -1).transpose(1, 0, 2, 3).reshape(width, -1)

    inputs = after(gathered(permuted(input_own), ring), w_output)
    small = doubled(doubled(params[None], "batch"), "seq")
    grad_out = gathered(after(grad_own, inputs, w_mixer), ring)
    small = small.reshape(devices, -1)
    segment = lax.dynamic_index_in_dim(
        small.reshape(ring, lines, -1), lax.axis_index("batch"), 1, keepdims=False
    )[:, count : count + rows].reshape(length).astype(F32)
    cuts = np.cumsum([own, own, own, slots_all // devices, RANK * slots_all // devices])
    gain_one, gain_head, gain_two, bias_full, expand_t, w_squeeze = jnp.split(
        small[:, :count], cuts, axis=1
    )
    gain_one = permuted(gain_one.reshape(width)).astype(F32)
    gain_head = lax.dynamic_slice_in_dim(gain_head.reshape(width), head * head_size, head_size, 0)
    gain_head = gain_head.astype(F32)
    gain_two = gain_two.reshape(width).astype(F32)
    bias_head = lax.dynamic_slice_in_dim(bias_full.reshape(slots_all), head * SLOTS, SLOTS, 0)
    expand_head = lax.dynamic_slice_in_dim(
        expand_t.reshape(slots_all, RANK), head * SLOTS, SLOTS, 0
    )
    w_squeeze = permuted(w_squeeze.reshape(width, RANK).T)

    chunked = segment.reshape(-1, CHUNK)
    before = jnp.concatenate([jnp.full((1,), -1.0, F32), chunked[:-1, -1]])
    previous = jnp.concatenate([jnp.full((1,), -1.0, F32), segment[:-1]])
    mask_rows = jnp.stack(
        [
            segment,
            (chunked == before[:, None]).astype(F32).reshape(-1),
            (chunked == chunked[:, -1:]).astype(F32).reshape(-1),
            (segment == previous).astype(F32),
        ]
        + [jnp.zeros_like(segment)] * 4
    )

    inputs = inputs.astype(F32)
    scale_one = rms_scale(inputs)
    plain_one = inputs * scale_one
    normed = (plain_one * gain_one).astype(BF16)
    mixer_pre = dot_nn(normed, w_mixer)
    joined = mixer_pre.astype(BF16)
    if copies > 1:
        joined = jnp.concatenate(
            [whole_head(joined[:, at * part : (at + 1) * part]) for at in range(3)], axis=1
        )
    swish_pre = whole_head(mixer_pre[:, 3 * part :])
    reduced = dot_nt(normed, w_squeeze).astype(BF16)
    forget_logit = dot_nt(expand_head, reduced) + bias_head.astype(F32)[:, None]
    log_rate = jax.nn.log_sigmoid(forget_logit) / TAU_GATE
    rates = jnp.concatenate([log_rate, -jnp.expm1(log_rate)], axis=0)
    order = mine.reshape(1).astype(jnp.int32)
    mixed, choice, starts = mixer_forward(order, ring, head_size, joined, rates, mask_rows)
    head_factor = rms_scale(mixed)
    head_plain = mixed * head_factor
    head_normed = head_plain * gain_head
    swish_sig = jax.nn.sigmoid(swish_pre)
    swish_act = swish_pre * swish_sig
    gated = own_part((head_normed * swish_act).astype(BF16))
    terms = dot_nn(gated, w_output).astype(BF16)
    terms, grad_out = lax.optimization_barrier((terms, grad_out))
    if ring == 4:
        feed_in, hidden = fold(
            finish_forward,
            terms.reshape(ring, rows, width),
            (input_own, gain_two[None]),
            (jax.ShapeDtypeStruct((rows, width), F32),),
            "fold_forward",
        )
        feed_in = feed_in.reshape(length, width)
    else:
        hidden = input_own.astype(F32) + scattered(terms, ring)
        feed_in = gathered((hidden * rms_scale(hidden) * gain_two).astype(BF16), ring)

    feed_pre = dot_nn(feed_in, w_feed)
    gate_pre, up_pre = feed_pre[:, :hidden_part], feed_pre[:, hidden_part:]
    gate_sig = jax.nn.sigmoid(gate_pre)
    gate_act = gate_pre * gate_sig
    inner = (gate_act * up_pre).astype(BF16)

    term_down = dot_tn(inner, grad_out).astype(BF16)
    grad_inner = dot_nt(after(grad_out, term_down), w_down)
    grad_gatepre = grad_inner * up_pre * (gate_sig * (1.0 + gate_pre * (1.0 - gate_sig)))
    grad_feedpre = jnp.concatenate(
        [grad_gatepre.astype(BF16), (grad_inner * gate_act).astype(BF16)], axis=1
    )
    back_feedin = dot_nt(grad_feedpre, w_feed).astype(BF16)
    result_terms = dot_nn(after(inner, back_feedin), w_down).astype(BF16)
    feed_lines = feed_in if ring == 4 else permuted(feed_in)
    term_feedpre = core_sum(after(feed_lines, back_feedin), grad_feedpre, lines, (result_terms,))
    down_share = lax.psum_scatter(term_down, "batch", scatter_dimension=0, tiled=True)
    feed_sum = line_sum(after(term_feedpre, down_share), lines)
    if ring == 4:
        grad_branch, grad_hidden, term_feed = fold(
            finish_backward,
            after(back_feedin, term_feedpre).reshape(ring, rows, width),
            (grad_own, hidden, gain_two[None]),
            (
                jax.ShapeDtypeStruct((rows, width), F32),
                jax.ShapeDtypeStruct((1, width), F32),
            ),
            "fold_backward",
        )
        grad_branch, term_feed = grad_branch.reshape(length, width), term_feed[0]
    else:
        grad_feedin = scattered(back_feedin, ring)
        scale_two = rms_scale(hidden)
        term_feed = jnp.sum(grad_feedin * hidden * scale_two, axis=0)
        scaled_two = grad_feedin * gain_two
        grad_hidden = (
            grad_own.astype(F32)
            + scale_two * scaled_two
            - hidden * scale_two**3 * jnp.mean(scaled_two * hidden, axis=-1, keepdims=True)
        )
        grad_branch = gathered(grad_hidden.astype(BF16), ring)

    grad_gated = whole_head(dot_nt(grad_branch, w_output))
    term_output = core_sum(gated, grad_branch, lines)

    slope = swish_sig * (1.0 + swish_pre * (1.0 - swish_sig))
    grad_swishpre = own_part((grad_gated * head_normed * slope).astype(BF16))
    grad_normed_head = grad_gated * swish_act
    term_head = jnp.sum(grad_normed_head * head_plain, axis=0) / copies
    scaled_head = grad_normed_head * gain_head
    grad_mixed = head_factor * scaled_head - mixed * head_factor**3 * jnp.mean(
        scaled_head * mixed, axis=-1, keepdims=True
    )
    result, grad_mixed, normed_late = scattered(
        after(result_terms, grad_branch), ring, grad_mixed.astype(BF16), normed
    )
    layer_output = (hidden + result).astype(BF16).reshape(1, rows, width)
    grad_pre, grad_rate = mixer_backward(
        order, ring, joined, grad_mixed, rates, mask_rows, choice, starts
    )
    grad_logit = (grad_rate * jax.nn.sigmoid(-forget_logit) / TAU_GATE).astype(BF16)
    term_bias = jnp.sum(grad_logit.astype(F32), axis=1) / copies
    term_expand = dot_nn(grad_logit, reduced) / copies
    grad_reduced = (dot_tn(grad_logit, expand_head) / copies).astype(BF16)
    if copies > 1:
        grad_pre = jnp.concatenate(
            [own_part(grad_pre[:, at * head_size : (at + 1) * head_size]) for at in range(3)], axis=1
        )
    grad_pre = jnp.concatenate([grad_pre, grad_swishpre], axis=1)
    term_pre = dot_tn(normed_late, grad_pre).astype(BF16)
    pre_sum = lax.psum_scatter(
        after(term_pre, feed_sum), "batch", scatter_dimension=0, tiled=True
    )
    output_share = line_sum(after(term_output, pre_sum), lines)
    grad_normed = dot_nt(after(grad_pre, term_pre), w_mixer) + dot_nn(grad_reduced, w_squeeze)
    grad_normed = dot_nt(after(grad_pre, term_pre), w_mixer) + dot_nn(grad_reduced, w_squeeze)
    term_mixer = restored(jnp.sum(grad_normed * plain_one, axis=0))
    term_squeeze = restored(dot_tn(grad_reduced, normed))
    grad_normed = restored(scattered(grad_normed.astype(BF16), ring))
    inputs_own = input_own.astype(F32)
    scale_own = rms_scale(inputs_own)
    scaled_one = grad_normed * restored(gain_one)
    grad_input = (
        grad_hidden
        + scale_own * scaled_one
        - inputs_own * scale_own**3 * jnp.mean(scaled_one * inputs_own, axis=-1, keepdims=True)
    ).astype(BF16)
    pre_share = exchanged(pre_sum.reshape(ring, own, 4 * part), mine, ring)
    pre_share = pre_share.reshape(ring, own, 4, part).transpose(2, 1, 0, 3)
    query_share, key_share, value_share, swish_share = pre_share.reshape(4, own, width).astype(F32)
    feed_share = exchanged(after(feed_sum, term_pre).reshape(ring, own, 2 * hidden_part), mine, ring)
    gate_share = feed_share[:, :, :hidden_part].transpose(1, 0, 2).reshape(own, -1).astype(F32)
    up_share = feed_share[:, :, hidden_part:].transpose(1, 0, 2).reshape(own, -1).astype(F32)

    def placed(array, size):
        full = jnp.zeros((HEADS, size) + array.shape[1:], F32)
        return lax.dynamic_update_slice_in_dim(full, array[None], head, 0)

    terms = jnp.concatenate(
        [
            term_mixer.reshape(devices, -1),
            placed(term_head, head_size).reshape(devices, -1),
            term_feed.reshape(devices, -1),
            placed(term_bias, SLOTS).reshape(devices, -1),
            placed(term_expand, SLOTS).reshape(devices, -1),
            term_squeeze.T.reshape(devices, -1),
        ],
        axis=1,
    )
    share = halved(halved(terms, "seq"), "batch")[0]
    mixer_share, head_share, feedgain_share, bias_share, expand_share, squeeze_share = jnp.split(
        share, cuts
    )
    return (
        layer_output,
        grad_input.reshape(1, rows, width),
        mixer_share,
        query_share,
        key_share,
        value_share,
        squeeze_share.reshape(own, RANK),
        expand_share.reshape(-1, RANK).T,
        bias_share,
        swish_share,
        head_share,
        output_share.astype(F32),
        feedgain_share,
        gate_share,
        up_share,
        down_share.astype(F32),
    )


def solution(mesh):
    rows = P(BOTH, None)
    spread = P(BOTH)
    in_specs = (
        P("batch", "seq", None),
        P("batch", "seq"),
        spread,
        rows,
        rows,
        rows,
        rows,
        P(None, BOTH),
        spread,
        rows,
        spread,
        rows,
        spread,
        rows,
        rows,
        rows,
        P("batch", "seq", None),
    )
    out_specs = (
        P("batch", "seq", None),
        P("batch", "seq", None),
        spread,
        rows,
        rows,
        rows,
        rows,
        P(None, BOTH),
        spread,
        rows,
        spread,
        rows,
        spread,
        rows,
        rows,
        rows,
    )
    return jax.shard_map(local, mesh=mesh, in_specs=in_specs, out_specs=out_specs, check_vma=False)
```

```python
import functools

import jax
import jax.numpy as jnp
import numpy as np
from jax import lax
from jax.experimental import pallas as pl
from jax.experimental.pallas import tpu as pltpu
from jax.sharding import PartitionSpec as P

HEADS = 4
SLOTS = 64
RANK = 16
EPS = 1e-06
TAU_GATE = 8.0
CHUNK = 128
SUB = 16
BOTH = ("seq", "batch")
F32 = jnp.float32
BF16 = jnp.bfloat16
HIGHEST = lax.Precision.HIGHEST


def dot_nn(left, right):
    return lax.dot_general(left, right, (((1,), (0,)), ((), ())), preferred_element_type=F32)


def dot_nt(left, right):
    return lax.dot_general(left, right, (((1,), (1,)), ((), ())), preferred_element_type=F32)


def dot_tn(left, right):
    return lax.dot_general(left, right, (((0,), (0,)), ((), ())), preferred_element_type=F32)


def exact_nn(left, right):
    return lax.dot_general(
        left, right, (((1,), (0,)), ((), ())), precision=HIGHEST, preferred_element_type=F32
    )


def exact_nt(left, right):
    return lax.dot_general(
        left, right, (((1,), (1,)), ((), ())), precision=HIGHEST, preferred_element_type=F32
    )


def halves(value):
    high = value.astype(BF16)
    return high, (value - high.astype(F32)).astype(BF16)


def split_nn(left, right):
    high, rest = halves(left)
    return dot_nn(high, right) + dot_nn(rest, right)


def split_nt(left, right):
    high, rest = halves(left)
    return dot_nt(high, right) + dot_nt(rest, right)


LEVELS = (CHUNK // SUB).bit_length() - 1


def fill_tables(sums, covers, apart):
    source = lax.broadcasted_iota(jnp.int32, (CHUNK, CHUNK), 0)
    target = lax.broadcasted_iota(jnp.int32, (CHUNK, CHUNK), 1)

    def group(at, size):
        return jnp.bitwise_and(at, CHUNK - size)

    for level in range(LEVELS):
        half = SUB << level
        right = jnp.bitwise_and(target, half) != 0
        edge = group(target, 2 * half) + (half - 1)
        low, high = jnp.where(right, edge, target), jnp.where(right, target, edge)
        sums[:, level * CHUNK : (level + 1) * CHUNK] = jnp.where(
            (source > low) & (source <= high), 1.0, 0.0
        )
        same = group(source, 2 * half) == group(target, 2 * half)
        covers[level] = jnp.where(same & (jnp.bitwise_and(source, half) == 0) & right, 1.0, 0.0)
    sums[:, LEVELS * CHUNK : (LEVELS + 1) * CHUNK] = jnp.where(source <= target, 1.0, 0.0)
    sums[:, (LEVELS + 1) * CHUNK :] = jnp.where(source > target, 1.0, 0.0)
    apart[...] = jnp.where(group(source, SUB) == group(target, SUB), target - source, -1)


TABLES = [
    pltpu.VMEM((CHUNK, (LEVELS + 2) * CHUNK), F32),
    pltpu.VMEM((LEVELS, CHUNK, CHUNK), F32),
    pltpu.VMEM((CHUNK, CHUNK), jnp.int32),
]


def same_document(rows):
    source = lax.broadcasted_iota(jnp.int32, (CHUNK, CHUNK), 0)
    target = lax.broadcasted_iota(jnp.int32, (CHUNK, CHUNK), 1)
    number = rows[0:1, :]
    column = jnp.sum(jnp.where(source == target, number, 0.0), axis=1, keepdims=True)
    return column == number


def rolled(value, by):
    return value if by % CHUNK == 0 else pltpu.roll(value, by % CHUNK, 1)


def exponents(rate, sums):
    return jnp.exp(exact_nn(rate, sums))


def piece(value, at):
    return value[:, at * CHUNK : (at + 1) * CHUNK]


def mixer_forward_kernel(
    factor, mine, query, key, value, rate, rows, output, choice_out, start_out, state, sums, covers, apart
):
    levels = LEVELS

    @pl.when(pl.program_id(0) == 0)
    def _():
        state[...] = jnp.zeros_like(state)
        fill_tables(sums, covers, apart)

    key_in, value_in = state[:SLOTS, :], state[SLOTS:, :]
    start_out[0] = state[...]
    q, k, v = query[...], key[...], value[...]
    a, g = rate[:SLOTS, :], rate[SLOTS:, :]
    decay = exponents(a, sums[...])
    before, after = piece(decay, levels), piece(decay, levels + 1)
    carried = before * rows[1:2, :]
    visible = same_document(rows)
    scores = jnp.where(visible, dot_nt(k, q) * factor, 0.0)
    logits = carried * (split_nt(key_in, q) * factor)
    for level in range(levels):
        part = piece(decay, level)
        logits = logits + part * exact_nn(part * g, scores * covers[level])
    gap = apart[...]
    total = jnp.zeros_like(a)
    weights = []
    for by in range(SUB):
        if by:
            total = total + rolled(a, by - 1)
        weight = jnp.exp(total) * rolled(g, by)
        weights.append(weight)
        logits = logits + weight * jnp.sum(
            jnp.where(gap == by, scores, 0.0), axis=0, keepdims=True
        )
    attention = jnp.exp(logits - jnp.max(logits, axis=0, keepdims=True))
    attention = attention / jnp.sum(attention, axis=0, keepdims=True)
    choice_out[:SLOTS, :] = attention
    choice_out[SLOTS:, :] = logits
    mixing = jnp.zeros((CHUNK, CHUNK), F32)
    for level in range(levels):
        part = piece(decay, level)
        mixing = mixing + covers[level] * dot_tn(
            (part * g).astype(BF16), (part * attention).astype(BF16)
        )
    for by in range(SUB):
        row = jnp.sum(weights[by] * attention, axis=0, keepdims=True)
        mixing = jnp.where(gap == by, row, mixing)
    mixing = jnp.where(visible, mixing, 0.0).astype(BF16)
    output[...] = dot_tn(mixing, v) + dot_tn(
        (carried * attention).astype(BF16), value_in.astype(BF16)
    )
    ends = after * g * rows[2:3, :]
    keep = carried[:, CHUNK - 1 : CHUNK]
    state[:SLOTS, :] = keep * key_in + split_nn(ends, k)
    state[SLOTS:, :] = keep * value_in + split_nn(ends, v)


def mixer_backward_kernel(
    factor, mine, query, key, value, grad_output, rate, rows, choice, start, grad_all, grad_rate,
    state_grad, flow, sums, covers, apart,
):
    levels = LEVELS

    @pl.when(pl.program_id(0) == 0)
    def _():
        state_grad[...] = jnp.zeros_like(state_grad)
        flow[...] = jnp.zeros_like(flow)
        fill_tables(sums, covers, apart)

    key_in, value_in = start[0, :SLOTS, :], start[0, SLOTS:, :]
    key_after, value_after = state_grad[:SLOTS, :], state_grad[SLOTS:, :]
    q, k, v, d = query[...], key[...], value[...], grad_output[...]
    size = q.shape[1]
    a, g = rate[:SLOTS, :], rate[SLOTS:, :]
    attention, logits = choice[:SLOTS, :], choice[SLOTS:, :]
    decay = exponents(a, sums[...])
    before, after = piece(decay, levels), piece(decay, levels + 1)
    carried = before * rows[1:2, :]
    visible = same_document(rows)
    scores = jnp.where(visible, dot_nt(k, q) * factor, 0.0)
    reads = jnp.where(visible, dot_nt(v, d), 0.0)
    gap = apart[...]
    grad_att = carried * split_nt(value_in, d)
    for level in range(levels):
        part = piece(decay, level)
        grad_att = grad_att + part * exact_nn(part * g, reads * covers[level])
    total = jnp.zeros_like(a)
    bare, weights, score_rows, read_rows = [], [], [], []
    for by in range(SUB):
        if by:
            total = total + rolled(a, by - 1)
        bare.append(jnp.exp(total))
        weights.append(bare[by] * rolled(g, by))
        score_rows.append(jnp.sum(jnp.where(gap == by, scores, 0.0), axis=0, keepdims=True))
        read_rows.append(jnp.sum(jnp.where(gap == by, reads, 0.0), axis=0, keepdims=True))
        grad_att = grad_att + weights[by] * read_rows[by]
    grad_logits = attention * (
        grad_att - jnp.sum(attention * grad_att, axis=0, keepdims=True)
    )
    mixing = jnp.zeros((CHUNK, CHUNK), F32)
    spread = jnp.zeros((CHUNK, CHUNK), F32)
    ends = after * rows[2:3, :]
    grad_inflow = ends * (split_nt(key_after, k) + split_nt(value_after, v))
    for level in range(levels):
        part = piece(decay, level)
        left = (part * g).astype(BF16)
        att_part, log_part = part * attention, part * grad_logits
        mixing = mixing + covers[level] * dot_tn(left, att_part.astype(BF16))
        spread = spread + covers[level] * dot_tn(left, log_part.astype(BF16))
        grad_inflow = grad_inflow + part * (
            exact_nt(log_part, scores * covers[level]) + exact_nt(att_part, reads * covers[level])
        )
    for by in range(SUB):
        row = jnp.sum(weights[by] * attention, axis=0, keepdims=True)
        mixing = jnp.where(gap == by, row, mixing)
        row = jnp.sum(weights[by] * grad_logits, axis=0, keepdims=True)
        spread = jnp.where(gap == by, row, spread)
        terms = bare[by] * (grad_logits * score_rows[by] + attention * read_rows[by])
        grad_inflow = grad_inflow + rolled(terms, -by)
    mixing = jnp.where(visible, mixing, 0.0).astype(BF16)
    spread = (jnp.where(visible, spread, 0.0) * factor).astype(BF16)
    log_carried = carried * grad_logits * factor
    att_carried = carried * attention
    ends = (ends * g).astype(BF16)
    grad_all[:, :size] = (
        dot_tn(spread, k) + dot_tn(log_carried.astype(BF16), key_in.astype(BF16))
    ).astype(BF16)
    grad_all[:, size : 2 * size] = (dot_nn(spread, q) + dot_tn(ends, key_after.astype(BF16))).astype(BF16)
    grad_all[:, 2 * size :] = (dot_nn(mixing, d) + dot_tn(ends, value_after.astype(BF16))).astype(BF16)
    change = grad_logits * logits + attention * grad_att - g * grad_inflow
    later = piece(sums, levels + 1) + jnp.where(gap == 0, 1.0, 0.0)
    same = jnp.where(visible, later, 0.0)
    flows = exact_nn(change, same) + rows[2:3, :] * flow[:, 0:1]
    grad_rate[...] = rows[3:4, :] * flows - jnp.exp(a) * grad_inflow
    keep = carried[:, CHUNK - 1 : CHUNK]
    key_before = keep * key_after + split_nn(log_carried, q)
    value_before = keep * value_after + split_nn(att_carried, d)
    state_grad[:SLOTS, :] = key_before
    state_grad[SLOTS:, :] = value_before
    flow[...] = jnp.broadcast_to(
        jnp.sum(key_before * key_in + value_before * value_in, axis=1, keepdims=True), flow.shape
    )


def mixer_specs(length, size, ring, backward):
    count = length // CHUNK
    per = count // ring

    def natural(step):
        return count - 1 - step if backward else step

    def moved(step, mine):
        at = natural(step)
        return lax.bitwise_xor(at // per, mine[0]) * per + at % per

    wide = [
        pl.BlockSpec((CHUNK, size), lambda step, mine, at=at: (moved(step, mine), at))
        for at in range(3)
    ]
    everything = pl.BlockSpec((CHUNK, 3 * size), lambda step, mine: (moved(step, mine), 0))
    pair = pl.BlockSpec((2 * SLOTS, CHUNK), lambda step, mine: (0, moved(step, mine)))
    slim = pl.BlockSpec((SLOTS, CHUNK), lambda step, mine: (0, moved(step, mine)))
    rows = pl.BlockSpec((8, CHUNK), lambda step, mine: (0, natural(step)))
    state = pl.BlockSpec((1, 2 * SLOTS, size), lambda step, mine: (natural(step), 0, 0))
    return count, wide, everything, pair, slim, rows, state


def mixer_forward(mine, ring, size, joined, rates, rows):
    length = joined.shape[0]
    count, wide, _, pair, _, row_spec, state = mixer_specs(length, size, ring, False)
    return pl.pallas_call(
        functools.partial(mixer_forward_kernel, size ** (-0.25)),
        out_shape=(
            jax.ShapeDtypeStruct((length, size), F32),
            jax.ShapeDtypeStruct((2 * SLOTS, length), F32),
            jax.ShapeDtypeStruct((count, 2 * SLOTS, size), F32),
        ),
        grid_spec=pltpu.PrefetchScalarGridSpec(
            num_scalar_prefetch=1,
            grid=(count,),
            in_specs=wide + [pair, row_spec],
            out_specs=[wide[0], pair, state],
            scratch_shapes=[pltpu.VMEM((2 * SLOTS, size), F32)] + TABLES,
        ),
        compiler_params=pltpu.CompilerParams(vmem_limit_bytes=32 << 20),
        cost_estimate=pl.CostEstimate(
            flops=length * size * 2000, bytes_accessed=length * size * 12, transcendentals=length * 4096
        ),
        name="mixer_forward",
    )(mine, joined, joined, joined, rates, rows)


def mixer_backward(mine, ring, joined, grad, rates, rows, choice, starts):
    length, size = grad.shape
    count, wide, everything, pair, slim, row_spec, state = mixer_specs(length, size, ring, True)
    return pl.pallas_call(
        functools.partial(mixer_backward_kernel, size ** (-0.25)),
        out_shape=(
            jax.ShapeDtypeStruct((length, 3 * size), BF16),
            jax.ShapeDtypeStruct((SLOTS, length), F32),
        ),
        grid_spec=pltpu.PrefetchScalarGridSpec(
            num_scalar_prefetch=1,
            grid=(count,),
            in_specs=wide + [wide[0], pair, row_spec, pair, state],
            out_specs=[everything, slim],
            scratch_shapes=[pltpu.VMEM((2 * SLOTS, size), F32), pltpu.VMEM((SLOTS, 128), F32)]
            + TABLES,
        ),
        compiler_params=pltpu.CompilerParams(vmem_limit_bytes=32 << 20),
        cost_estimate=pl.CostEstimate(
            flops=length * size * 4000, bytes_accessed=length * size * 20, transcendentals=length * 4096
        ),
        name="mixer_backward",
    )(mine, joined, joined, joined, grad, rates, rows, choice, starts)


def peers(ring, mine):
    found = []
    for by in range(1, ring):
        at, bit = mine, 1
        while bit <= by:
            if by & bit:
                at = at + bit * (1 - 2 * ((at // bit) % 2))
            bit *= 2
        found.append(at)
    return found


class Copies:
    def __init__(self, local, send, recv):
        self.local, self.send, self.recv = local, send, recv
        self.here, self.away = 0, 0
        self.open = []

    def near(self, source, target):
        copy = pltpu.make_async_copy(source, target, self.local.at[self.here])
        self.here += 1
        copy.start()
        return copy

    def far(self, source, target, landed, device, when=None):
        at = self.away
        self.away += 1
        copy = pltpu.make_async_remote_copy(
            source, target, self.send.at[at], self.recv.at[at], device_id=device,
            device_id_type=pl.DeviceIdType.MESH,
        )
        if when is None:
            copy.start()
        else:
            pl.when(when)(copy.start)
        self.open.append((copy, when))
        return pltpu.make_async_remote_copy(
            landed, landed, self.send.at[at], self.recv.at[at], device_id=device,
            device_id_type=pl.DeviceIdType.MESH,
        ).wait_recv

    def close(self):
        for copy, when in self.open:
            if when is None:
                copy.wait_send()
            else:
                pl.when(when)(copy.wait_send)


PARTS = 4


def fold_kernel(finish, extras, *refs):
    terms, given = refs[0], refs[1 : 1 + extras]
    blocks = refs[1 + extras]
    made = refs[2 + extras : -9]
    first, second, third, two_low, one_high, own, local_sem, send_sem, recv_sem = refs[-9:]
    mine, batch = lax.axis_index("seq"), lax.axis_index("batch")
    others = peers(4, mine)
    row, col = (others[0], batch), (others[1], batch)
    copies = Copies(local_sem, send_sem, recv_sem)
    size = terms.shape[1] // PARTS

    def span(at):
        low = pl.ds(at * size, size // 2)
        return pl.ds(at * size, size), low, pl.ds(at * size + size // 2, size // 2)

    opening, direct = [], []

    def open_part(at):
        _, low, high = span(at)
        opening.append(
            (
                copies.far(terms.at[3, low], first.at[low], first.at[low], row),
                copies.far(terms.at[3, high], first.at[high], first.at[high], col),
            )
        )

    def pass_part(at):
        _, low, high = span(at)
        waits = [
            copies.far(terms.at[2, high], second.at[high], second.at[high], col),
            copies.far(terms.at[1, low], third.at[low], third.at[low], row),
        ]
        opening[at][0]()
        two_low[low, :] = added(terms[2, low, :], first[low, :])
        waits.append(copies.far(two_low.at[low], second.at[low], second.at[low], col))
        opening[at][1]()
        one_high[high, :] = added(terms[1, high, :], first[high, :])
        waits.append(copies.far(one_high.at[high], third.at[high], third.at[high], row))
        direct.append(waits)

    spread, local, passed = [], [], []

    def close_part(at):
        full, _, _ = span(at)
        for wait in direct[at]:
            wait()
        total = terms[0, full, :].astype(F32) + second[full, :].astype(F32) + third[full, :].astype(F32)
        own[full, :] = finish(total, full, at, given, made)
        spread.append(
            (
                copies.far(own.at[full], blocks.at[1, full], blocks.at[1, full], row),
                copies.far(own.at[full], blocks.at[2, full], blocks.at[2, full], col),
            )
        )
        local.append(copies.near(own.at[full], blocks.at[0, full]))

    def forward_part(at):
        _, low, high = span(at)
        for wait in spread[at]:
            wait()
        passed.append(copies.far(blocks.at[2, low], blocks.at[3, low], blocks.at[3, low], row))
        passed.append(copies.far(blocks.at[1, high], blocks.at[3, high], blocks.at[3, high], col))

    open_part(0)
    for at in range(PARTS + 2):
        if at + 1 < PARTS:
            open_part(at + 1)
        if at < PARTS:
            pass_part(at)
        if 1 <= at <= PARTS:
            close_part(at - 1)
        if at >= 2:
            forward_part(at - 2)
    for wait in passed:
        wait()
    for copy in local:
        copy.wait()
    copies.close()


def half_blocks(value, order):
    lane = lax.broadcasted_iota(jnp.int32, (value.shape[0], 128), 1)
    made = []
    for pair in zip(order[::2], order[1::2]):
        low, high = (
            value[:, block * 128 : (block + 1) * 128]
            if half == want
            else pltpu.roll(value[:, block * 128 : (block + 1) * 128], 64, 1)
            for want, (block, half) in enumerate(pair)
        )
        made.append(jnp.where(lane < 64, low, high))
    return jnp.concatenate(made, axis=1)


def by_line(value):
    lines = value.shape[1] // 256
    return half_blocks(
        value, [divmod(ring * lines + line, 2) for line in range(lines) for ring in range(4)]
    )


def by_ring(value):
    lines = value.shape[1] // 256
    return half_blocks(
        value, [divmod(line * 4 + ring, 2) for ring in range(4) for line in range(lines)]
    )


def finish_forward(total, full, at, given, made):
    inputs, gain = given
    hidden = inputs[full, :].astype(F32) + total
    made[0][full, :] = hidden
    return by_line(hidden * rms_scale(hidden) * gain[...]).astype(BF16)


def finish_backward(total, full, at, given, made):
    cotangent, hidden_ref, gain = given
    total = by_ring(total)
    hidden = hidden_ref[full, :]
    scale = rms_scale(hidden)
    plain = hidden * scale
    term = jnp.sum(total * plain, axis=0, keepdims=True)
    made[1][...] = term if at == 0 else made[1][...] + term
    scaled = total * gain[...]
    grad = (
        cotangent[full, :].astype(F32)
        + scale * scaled
        - plain * (scale * jnp.mean(scaled * plain, axis=-1, keepdims=True))
    )
    made[0][full, :] = grad
    return grad.astype(BF16)


def fold(finish, terms, given, made, name):
    ring, rows, width = terms.shape
    inside = pl.BlockSpec(memory_space=pltpu.VMEM)
    block = pltpu.VMEM((rows, width), BF16)
    return pl.pallas_call(
        functools.partial(fold_kernel, finish, len(given)),
        out_shape=(jax.ShapeDtypeStruct((ring, rows, width), BF16),) + made,
        in_specs=[inside] * (1 + len(given)),
        out_specs=[pl.BlockSpec(memory_space=pltpu.HBM)] + [inside] * len(made),
        scratch_shapes=[block] * 6
        + [
            pltpu.SemaphoreType.DMA((PARTS,)),
            pltpu.SemaphoreType.DMA((PARTS * 10,)),
            pltpu.SemaphoreType.DMA((PARTS * 10,)),
        ],
        compiler_params=pltpu.CompilerParams(has_side_effects=True, vmem_limit_bytes=40 << 20),
        name=name,
    )(terms, *given)


def rms_scale(features):
    return lax.rsqrt(jnp.mean(features * features, axis=-1, keepdims=True) + EPS)


def swapped(block, by, ring):
    return lax.ppermute(block, "seq", [(i, i ^ by) for i in range(ring)])


def gathered(block, ring):
    if ring != 4:
        return jnp.concatenate([block] + [swapped(block, by, ring) for by in range(1, ring)], axis=0)
    half = block.shape[0] // 2
    one, two = swapped(block, 1, ring), swapped(block, 2, ring)
    low, high = swapped(two[:half], 1, ring), swapped(one[half:], 2, ring)
    return jnp.concatenate([block, one, two, low, high], axis=0)


def scattered(terms, ring, wait_first=None, wait_second=None):
    rows = terms.shape[0] // ring
    parts = [terms[by * rows : (by + 1) * rows] for by in range(ring)]
    total = parts[0].astype(F32)
    if ring != 4:
        for by in range(1, ring):
            total = total + swapped(parts[by], by, ring).astype(F32)
        return total if wait_first is None else (total, wait_first, wait_second)
    half = rows // 2
    low, high = swapped(parts[3][:half], 1, ring), swapped(parts[3][half:], 2, ring)
    if wait_first is not None:
        low, high, wait_first = lax.optimization_barrier((low, high, wait_first))
    two = jnp.concatenate([added(parts[2][:half], low), parts[2][half:]], axis=0)
    one = jnp.concatenate([parts[1][:half], added(parts[1][half:], high)], axis=0)
    one, two = swapped(one, 1, ring), swapped(two, 2, ring)
    if wait_first is not None:
        one, two, wait_second = lax.optimization_barrier((one, two, wait_second))
    total = total + one.astype(F32) + two.astype(F32)
    return total if wait_first is None else (total, wait_first, wait_second)


def added(left, right):
    return (left.astype(F32) + right.astype(F32)).astype(BF16)


def flipped(block, axis, by):
    return lax.ppermute(block, axis, [(i, i ^ by) for i in range(lax.axis_size(axis))])


def doubled(block, axis):
    by, mine = 1, lax.axis_index(axis)
    while by < lax.axis_size(axis):
        other = flipped(block, axis, by)
        first = (mine & by) == 0
        block = jnp.concatenate(
            [jnp.where(first, block, other), jnp.where(first, other, block)], axis=0
        )
        by *= 2
    return block


def halved(block, axis):
    by, mine = lax.axis_size(axis) // 2, lax.axis_index(axis)
    while by:
        low, high = jnp.split(block, 2, axis=0)
        first = (mine & by) == 0
        block = jnp.where(first, low, high) + flipped(jnp.where(first, high, low), axis, by)
        by //= 2
    return block


def core_halves(array, lines, axis):
    size = array.shape[axis] // lines
    even, odd = (
        jnp.concatenate(
            [
                lax.slice_in_dim(array, line * size, (line + 1) * size, axis=axis)
                for line in range(which, lines, 2)
            ],
            axis=axis,
        )
        for which in range(2)
    )
    first = lax.axis_index("batch") % 2 == 0
    return jnp.where(first, even, odd), jnp.where(first, odd, even)


def core_sum(features, grads, lines, fill=()):
    if (features.shape[1] // lines) % 128:
        mine, others = core_halves(dot_tn(features, grads).astype(BF16), lines, 0)
        return added(mine, flipped(others, "batch", 1))
    mine, others = core_halves(features, lines, 1)
    sent = flipped(dot_tn(others, grads).astype(BF16), "batch", 1)
    mine = after(mine, *fill) if fill else mine
    return (dot_tn(mine, grads) + sent.astype(F32)).astype(BF16)


def line_sum(terms, lines):
    groups = [list(range(core, lines, 2)) for core in range(2)]
    return lax.psum_scatter(
        terms, "batch", scatter_dimension=0, axis_index_groups=groups, tiled=True
    )


def after(value, *others):
    return lax.optimization_barrier((value,) + others)[0]


def exchanged(blocks, mine, ring):
    parts = [
        swapped(lax.dynamic_index_in_dim(blocks, mine ^ by, 0, keepdims=False), by, ring)
        if by
        else lax.dynamic_index_in_dim(blocks, mine, 0, keepdims=False)
        for by in range(ring)
    ]
    made = jnp.stack(parts)
    return jnp.concatenate(
        [lax.dynamic_index_in_dim(made, mine ^ j, 0, keepdims=True) for j in range(ring)], axis=0
    )


def local(
    layer_input,
    segments,
    mixer_gain,
    query_weight,
    key_weight,
    value_weight,
    squeeze,
    expand,
    forget_bias,
    swish_weight,
    head_gain,
    output_weight,
    feed_gain,
    gate_weight,
    up_weight,
    down_weight,
    cotangent,
):
    ring, lines = lax.axis_size("seq"), lax.axis_size("batch")
    devices = ring * lines
    mine = lax.axis_index("seq")
    rows, width = layer_input.shape[1], layer_input.shape[2]
    length = rows * ring
    own = width // devices
    head_size = width // HEADS
    copies = ring // HEADS
    part = width // ring
    head = mine // copies
    hidden_part = gate_weight.shape[1] // ring
    slots_all = HEADS * SLOTS

    def to_order(array):
        if copies == 1:
            return array
        blocks = array.reshape((ring, rows) + array.shape[1:])
        moved = [lax.dynamic_index_in_dim(blocks, mine ^ by, 0, keepdims=False) for by in range(ring)]
        return jnp.concatenate(moved, axis=0)

    def whole_head(array):
        if copies == 1:
            return array
        full = lax.all_gather(to_order(array), "seq", axis=1, tiled=True)
        return to_order(lax.dynamic_slice_in_dim(full, head * head_size, head_size, 1))

    def own_part(array):
        if copies == 1:
            return array
        return lax.dynamic_slice_in_dim(array, (mine % copies) * part, part, 1)

    params = jnp.concatenate(
        [
            mixer_gain,
            head_gain,
            feed_gain,
            forget_bias,
            expand.T.reshape(-1),
            squeeze.reshape(-1),
        ]
    )
    count = params.shape[0]
    params = jnp.concatenate([params, segments.reshape(rows).astype(BF16)])
    input_own = layer_input.reshape(rows, width)
    grad_own = cotangent.reshape(rows, width)

    def permuted(array):
        shape = array.shape[:-1]
        array = array.reshape(shape + (ring, lines, own))
        return jnp.swapaxes(array, -3, -2).reshape(shape + (width,))

    def restored(array):
        shape = array.shape[:-1]
        array = array.reshape(shape + (lines, ring, own))
        return jnp.swapaxes(array, -3, -2).reshape(shape + (width,))

    def columns(*arrays):
        blocks = [a.reshape(own, ring, a.shape[1] // ring) for a in arrays]
        return jnp.concatenate(blocks, axis=2).transpose(1, 0, 2)

    w_output = lax.all_gather(output_weight, "batch", axis=0, tiled=True)
    mixer_columns = exchanged(
        columns(query_weight, key_weight, value_weight, swish_weight), mine, ring
    )
    w_mixer = lax.all_gather(mixer_columns.reshape(ring * own, -1), "batch", axis=0, tiled=True)
    feed_columns = exchanged(columns(gate_weight, up_weight), mine, ring)
    w_feed = lax.all_gather(feed_columns.reshape(ring * own, -1), "batch", axis=0, tiled=True)
    w_down = lax.all_gather(after(down_weight, feed_columns), "batch", axis=0, tiled=True)
    if ring != 4:
        w_feed = w_feed.reshape(lines, ring, own, -1).transpose(1, 0, 2, 3).reshape(width, -1)

    inputs = after(gathered(permuted(input_own), ring), w_output)
    small = doubled(doubled(params[None], "batch"), "seq")
    grad_out = gathered(after(grad_own, inputs, w_mixer), ring)
    small = small.reshape(devices, -1)
    segment = lax.dynamic_index_in_dim(
        small.reshape(ring, lines, -1), lax.axis_index("batch"), 1, keepdims=False
    )[:, count : count + rows].reshape(length).astype(F32)
    cuts = np.cumsum([own, own, own, slots_all // devices, RANK * slots_all // devices])
    gain_one, gain_head, gain_two, bias_full, expand_t, w_squeeze = jnp.split(
        small[:, :count], cuts, axis=1
    )
    gain_one = permuted(gain_one.reshape(width)).astype(F32)
    gain_head = lax.dynamic_slice_in_dim(gain_head.reshape(width), head * head_size, head_size, 0)
    gain_head = gain_head.astype(F32)
    gain_two = gain_two.reshape(width).astype(F32)
    bias_head = lax.dynamic_slice_in_dim(bias_full.reshape(slots_all), head * SLOTS, SLOTS, 0)
    expand_head = lax.dynamic_slice_in_dim(
        expand_t.reshape(slots_all, RANK), head * SLOTS, SLOTS, 0
    )
    w_squeeze = permuted(w_squeeze.reshape(width, RANK).T)

    chunked = segment.reshape(-1, CHUNK)
    before = jnp.concatenate([jnp.full((1,), -1.0, F32), chunked[:-1, -1]])
    previous = jnp.concatenate([jnp.full((1,), -1.0, F32), segment[:-1]])
    mask_rows = jnp.stack(
        [
            segment,
            (chunked == before[:, None]).astype(F32).reshape(-1),
            (chunked == chunked[:, -1:]).astype(F32).reshape(-1),
            (segment == previous).astype(F32),
        ]
        + [jnp.zeros_like(segment)] * 4
    )

    inputs = inputs.astype(F32)
    scale_one = rms_scale(inputs)
    plain_one = inputs * scale_one
    normed = (plain_one * gain_one).astype(BF16)
    mixer_pre = dot_nn(normed, w_mixer)
    joined = mixer_pre.astype(BF16)
    if copies > 1:
        joined = jnp.concatenate(
            [whole_head(joined[:, at * part : (at + 1) * part]) for at in range(3)], axis=1
        )
    swish_pre = whole_head(mixer_pre[:, 3 * part :])
    reduced = dot_nt(normed, w_squeeze).astype(BF16)
    forget_logit = dot_nt(expand_head, reduced) + bias_head.astype(F32)[:, None]
    log_rate = jax.nn.log_sigmoid(forget_logit) / TAU_GATE
    rates = jnp.concatenate([log_rate, -jnp.expm1(log_rate)], axis=0)
    order = mine.reshape(1).astype(jnp.int32)
    mixed, choice, starts = mixer_forward(order, ring, head_size, joined, rates, mask_rows)
    head_factor = rms_scale(mixed)
    head_plain = mixed * head_factor
    head_normed = head_plain * gain_head
    swish_sig = jax.nn.sigmoid(swish_pre)
    swish_act = swish_pre * swish_sig
    gated = own_part((head_normed * swish_act).astype(BF16))
    terms = dot_nn(gated, w_output).astype(BF16)
    terms, grad_out = lax.optimization_barrier((terms, grad_out))
    if ring == 4:
        feed_in, hidden = fold(
            finish_forward,
            terms.reshape(ring, rows, width),
            (input_own, gain_two[None]),
            (jax.ShapeDtypeStruct((rows, width), F32),),
            "fold_forward",
        )
        feed_in = feed_in.reshape(length, width)
    else:
        hidden = input_own.astype(F32) + scattered(terms, ring)
        feed_in = gathered((hidden * rms_scale(hidden) * gain_two).astype(BF16), ring)

    feed_pre = dot_nn(feed_in, w_feed)
    gate_pre, up_pre = feed_pre[:, :hidden_part], feed_pre[:, hidden_part:]
    gate_sig = jax.nn.sigmoid(gate_pre)
    gate_act = gate_pre * gate_sig
    inner = (gate_act * up_pre).astype(BF16)

    term_down = dot_tn(inner, grad_out).astype(BF16)
    grad_inner = dot_nt(after(grad_out, term_down), w_down)
    grad_gatepre = grad_inner * up_pre * (gate_sig * (1.0 + gate_pre * (1.0 - gate_sig)))
    grad_feedpre = jnp.concatenate(
        [grad_gatepre.astype(BF16), (grad_inner * gate_act).astype(BF16)], axis=1
    )
    back_feedin = dot_nt(grad_feedpre, w_feed).astype(BF16)
    result_terms = dot_nn(after(inner, back_feedin), w_down).astype(BF16)
    feed_lines = feed_in if ring == 4 else permuted(feed_in)
    term_feedpre = core_sum(after(feed_lines, back_feedin), grad_feedpre, lines, (result_terms,))
    down_share = lax.psum_scatter(term_down, "batch", scatter_dimension=0, tiled=True)
    feed_sum = line_sum(after(term_feedpre, down_share), lines)
    if ring == 4:
        grad_branch, grad_hidden, term_feed = fold(
            finish_backward,
            after(back_feedin, term_feedpre).reshape(ring, rows, width),
            (grad_own, hidden, gain_two[None]),
            (
                jax.ShapeDtypeStruct((rows, width), F32),
                jax.ShapeDtypeStruct((1, width), F32),
            ),
            "fold_backward",
        )
        grad_branch, term_feed = grad_branch.reshape(length, width), term_feed[0]
    else:
        grad_feedin = scattered(back_feedin, ring)
        scale_two = rms_scale(hidden)
        term_feed = jnp.sum(grad_feedin * hidden * scale_two, axis=0)
        scaled_two = grad_feedin * gain_two
        grad_hidden = (
            grad_own.astype(F32)
            + scale_two * scaled_two
            - hidden * scale_two**3 * jnp.mean(scaled_two * hidden, axis=-1, keepdims=True)
        )
        grad_branch = gathered(grad_hidden.astype(BF16), ring)

    grad_gated = whole_head(dot_nt(grad_branch, w_output))

    slope = swish_sig * (1.0 + swish_pre * (1.0 - swish_sig))
    grad_swishpre = own_part((grad_gated * head_normed * slope).astype(BF16))
    grad_normed_head = grad_gated * swish_act
    term_head = jnp.sum(grad_normed_head * head_plain, axis=0) / copies
    scaled_head = grad_normed_head * gain_head
    grad_mixed = head_factor * scaled_head - mixed * head_factor**3 * jnp.mean(
        scaled_head * mixed, axis=-1, keepdims=True
    )
    result, grad_mixed, normed_late = scattered(
        after(result_terms, grad_branch), ring, grad_mixed.astype(BF16), normed
    )
    layer_output = (hidden + result).astype(BF16).reshape(1, rows, width)
    term_output = core_sum(after(gated, grad_mixed), grad_branch, lines)
    output_share = line_sum(after(term_output, feed_sum), lines)
    grad_mixed = after(grad_mixed, term_output)
    grad_pre, grad_rate = mixer_backward(
        order, ring, joined, grad_mixed, rates, mask_rows, choice, starts
    )
    grad_logit = (grad_rate * jax.nn.sigmoid(-forget_logit) / TAU_GATE).astype(BF16)
    term_bias = jnp.sum(grad_logit.astype(F32), axis=1) / copies
    term_expand = dot_nn(grad_logit, reduced) / copies
    grad_reduced = (dot_tn(grad_logit, expand_head) / copies).astype(BF16)
    if copies > 1:
        grad_pre = jnp.concatenate(
            [own_part(grad_pre[:, at * head_size : (at + 1) * head_size]) for at in range(3)], axis=1
        )
    grad_pre = jnp.concatenate([grad_pre, grad_swishpre], axis=1)
    term_pre = dot_tn(normed_late, grad_pre).astype(BF16)
    pre_sum = lax.psum_scatter(
        after(term_pre, output_share), "batch", scatter_dimension=0, tiled=True
    )
    grad_normed = dot_nt(after(grad_pre, term_pre), w_mixer) + dot_nn(grad_reduced, w_squeeze)
    grad_normed = dot_nt(after(grad_pre, term_pre), w_mixer) + dot_nn(grad_reduced, w_squeeze)
    term_mixer = restored(jnp.sum(grad_normed * plain_one, axis=0))
    term_squeeze = restored(dot_tn(grad_reduced, normed))
    grad_normed = restored(scattered(grad_normed.astype(BF16), ring))
    inputs_own = input_own.astype(F32)
    scale_own = rms_scale(inputs_own)
    scaled_one = grad_normed * restored(gain_one)
    grad_input = (
        grad_hidden
        + scale_own * scaled_one
        - inputs_own * scale_own**3 * jnp.mean(scaled_one * inputs_own, axis=-1, keepdims=True)
    ).astype(BF16)
    pre_share = exchanged(pre_sum.reshape(ring, own, 4 * part), mine, ring)
    pre_share = pre_share.reshape(ring, own, 4, part).transpose(2, 1, 0, 3)
    query_share, key_share, value_share, swish_share = pre_share.reshape(4, own, width).astype(F32)
    feed_share = exchanged(after(feed_sum, term_pre).reshape(ring, own, 2 * hidden_part), mine, ring)
    gate_share = feed_share[:, :, :hidden_part].transpose(1, 0, 2).reshape(own, -1).astype(F32)
    up_share = feed_share[:, :, hidden_part:].transpose(1, 0, 2).reshape(own, -1).astype(F32)

    def placed(array, size):
        full = jnp.zeros((HEADS, size) + array.shape[1:], F32)
        return lax.dynamic_update_slice_in_dim(full, array[None], head, 0)

    terms = jnp.concatenate(
        [
            term_mixer.reshape(devices, -1),
            placed(term_head, head_size).reshape(devices, -1),
            term_feed.reshape(devices, -1),
            placed(term_bias, SLOTS).reshape(devices, -1),
            placed(term_expand, SLOTS).reshape(devices, -1),
            term_squeeze.T.reshape(devices, -1),
        ],
        axis=1,
    )
    share = halved(halved(terms, "seq"), "batch")[0]
    mixer_share, head_share, feedgain_share, bias_share, expand_share, squeeze_share = jnp.split(
        share, cuts
    )
    return (
        layer_output,
        grad_input.reshape(1, rows, width),
        mixer_share,
        query_share,
        key_share,
        value_share,
        squeeze_share.reshape(own, RANK),
        expand_share.reshape(-1, RANK).T,
        bias_share,
        swish_share,
        head_share,
        output_share.astype(F32),
        feedgain_share,
        gate_share,
        up_share,
        down_share.astype(F32),
    )


def solution(mesh):
    rows = P(BOTH, None)
    spread = P(BOTH)
    in_specs = (
        P("batch", "seq", None),
        P("batch", "seq"),
        spread,
        rows,
        rows,
        rows,
        rows,
        P(None, BOTH),
        spread,
        rows,
        spread,
        rows,
        spread,
        rows,
        rows,
        rows,
        P("batch", "seq", None),
    )
    out_specs = (
        P("batch", "seq", None),
        P("batch", "seq", None),
        spread,
        rows,
        rows,
        rows,
        rows,
        P(None, BOTH),
        spread,
        rows,
        spread,
        rows,
        spread,
        rows,
        rows,
        rows,
    )
    return jax.shard_map(local, mesh=mesh, in_specs=in_specs, out_specs=out_specs, check_vma=False)
```

```python
import functools

import jax
import jax.numpy as jnp
import numpy as np
from jax import lax
from jax.experimental import pallas as pl
from jax.experimental.pallas import tpu as pltpu
from jax.sharding import PartitionSpec as P

HEADS = 4
SLOTS = 64
RANK = 16
EPS = 1e-06
TAU_GATE = 8.0
CHUNK = 128
SUB = 16
BOTH = ("seq", "batch")
F32 = jnp.float32
BF16 = jnp.bfloat16
HIGHEST = lax.Precision.HIGHEST


def dot_nn(left, right):
    return lax.dot_general(left, right, (((1,), (0,)), ((), ())), preferred_element_type=F32)


def dot_nt(left, right):
    return lax.dot_general(left, right, (((1,), (1,)), ((), ())), preferred_element_type=F32)


def dot_tn(left, right):
    return lax.dot_general(left, right, (((0,), (0,)), ((), ())), preferred_element_type=F32)


def exact_nn(left, right):
    return lax.dot_general(
        left, right, (((1,), (0,)), ((), ())), precision=HIGHEST, preferred_element_type=F32
    )


def exact_nt(left, right):
    return lax.dot_general(
        left, right, (((1,), (1,)), ((), ())), precision=HIGHEST, preferred_element_type=F32
    )


def halves(value):
    high = value.astype(BF16)
    return high, (value - high.astype(F32)).astype(BF16)


def split_nn(left, right):
    high, rest = halves(left)
    return dot_nn(high, right) + dot_nn(rest, right)


def split_nt(left, right):
    high, rest = halves(left)
    return dot_nt(high, right) + dot_nt(rest, right)


LEVELS = (CHUNK // SUB).bit_length() - 1


def fill_tables(sums, covers, apart):
    source = lax.broadcasted_iota(jnp.int32, (CHUNK, CHUNK), 0)
    target = lax.broadcasted_iota(jnp.int32, (CHUNK, CHUNK), 1)

    def group(at, size):
        return jnp.bitwise_and(at, CHUNK - size)

    for level in range(LEVELS):
        half = SUB << level
        right = jnp.bitwise_and(target, half) != 0
        edge = group(target, 2 * half) + (half - 1)
        low, high = jnp.where(right, edge, target), jnp.where(right, target, edge)
        sums[:, level * CHUNK : (level + 1) * CHUNK] = jnp.where(
            (source > low) & (source <= high), 1.0, 0.0
        )
        same = group(source, 2 * half) == group(target, 2 * half)
        covers[level] = jnp.where(same & (jnp.bitwise_and(source, half) == 0) & right, 1.0, 0.0)
    sums[:, LEVELS * CHUNK : (LEVELS + 1) * CHUNK] = jnp.where(source <= target, 1.0, 0.0)
    sums[:, (LEVELS + 1) * CHUNK :] = jnp.where(source > target, 1.0, 0.0)
    apart[...] = jnp.where(group(source, SUB) == group(target, SUB), target - source, -1)


TABLES = [
    pltpu.VMEM((CHUNK, (LEVELS + 2) * CHUNK), F32),
    pltpu.VMEM((LEVELS, CHUNK, CHUNK), F32),
    pltpu.VMEM((CHUNK, CHUNK), jnp.int32),
]


def same_document(rows):
    source = lax.broadcasted_iota(jnp.int32, (CHUNK, CHUNK), 0)
    target = lax.broadcasted_iota(jnp.int32, (CHUNK, CHUNK), 1)
    number = rows[0:1, :]
    column = jnp.sum(jnp.where(source == target, number, 0.0), axis=1, keepdims=True)
    return column == number


def rolled(value, by):
    return value if by % CHUNK == 0 else pltpu.roll(value, by % CHUNK, 1)


def exponents(rate, sums):
    return jnp.exp(exact_nn(rate, sums))


def piece(value, at):
    return value[:, at * CHUNK : (at + 1) * CHUNK]


def mixer_forward_kernel(
    factor, mine, query, key, value, rate, rows, output, choice_out, start_out, state, sums, covers, apart
):
    levels = LEVELS

    @pl.when(pl.program_id(0) == 0)
    def _():
        state[...] = jnp.zeros_like(state)
        fill_tables(sums, covers, apart)

    key_in, value_in = state[:SLOTS, :], state[SLOTS:, :]
    start_out[0] = state[...]
    q, k, v = query[...], key[...], value[...]
    a, g = rate[:SLOTS, :], rate[SLOTS:, :]
    decay = exponents(a, sums[...])
    before, after = piece(decay, levels), piece(decay, levels + 1)
    carried = before * rows[1:2, :]
    visible = same_document(rows)
    scores = jnp.where(visible, dot_nt(k, q) * factor, 0.0)
    logits = carried * (split_nt(key_in, q) * factor)
    for level in range(levels):
        part = piece(decay, level)
        logits = logits + part * exact_nn(part * g, scores * covers[level])
    gap = apart[...]
    total = jnp.zeros_like(a)
    weights = []
    for by in range(SUB):
        if by:
            total = total + rolled(a, by - 1)
        weight = jnp.exp(total) * rolled(g, by)
        weights.append(weight)
        logits = logits + weight * jnp.sum(
            jnp.where(gap == by, scores, 0.0), axis=0, keepdims=True
        )
    attention = jnp.exp(logits - jnp.max(logits, axis=0, keepdims=True))
    attention = attention / jnp.sum(attention, axis=0, keepdims=True)
    choice_out[:SLOTS, :] = attention
    choice_out[SLOTS:, :] = logits
    mixing = jnp.zeros((CHUNK, CHUNK), F32)
    for level in range(levels):
        part = piece(decay, level)
        mixing = mixing + covers[level] * dot_tn(
            (part * g).astype(BF16), (part * attention).astype(BF16)
        )
    for by in range(SUB):
        row = jnp.sum(weights[by] * attention, axis=0, keepdims=True)
        mixing = jnp.where(gap == by, row, mixing)
    mixing = jnp.where(visible, mixing, 0.0).astype(BF16)
    output[...] = dot_tn(mixing, v) + dot_tn(
        (carried * attention).astype(BF16), value_in.astype(BF16)
    )
    ends = after * g * rows[2:3, :]
    keep = carried[:, CHUNK - 1 : CHUNK]
    state[:SLOTS, :] = keep * key_in + split_nn(ends, k)
    state[SLOTS:, :] = keep * value_in + split_nn(ends, v)


def mixer_backward_kernel(
    factor, mine, query, key, value, grad_output, rate, rows, choice, start, grad_all, grad_rate,
    state_grad, flow, sums, covers, apart,
):
    levels = LEVELS

    @pl.when(pl.program_id(0) == 0)
    def _():
        state_grad[...] = jnp.zeros_like(state_grad)
        flow[...] = jnp.zeros_like(flow)
        fill_tables(sums, covers, apart)

    key_in, value_in = start[0, :SLOTS, :], start[0, SLOTS:, :]
    key_after, value_after = state_grad[:SLOTS, :], state_grad[SLOTS:, :]
    q, k, v, d = query[...], key[...], value[...], grad_output[...]
    size = q.shape[1]
    a, g = rate[:SLOTS, :], rate[SLOTS:, :]
    attention, logits = choice[:SLOTS, :], choice[SLOTS:, :]
    decay = exponents(a, sums[...])
    before, after = piece(decay, levels), piece(decay, levels + 1)
    carried = before * rows[1:2, :]
    visible = same_document(rows)
    scores = jnp.where(visible, dot_nt(k, q) * factor, 0.0)
    reads = jnp.where(visible, dot_nt(v, d), 0.0)
    gap = apart[...]
    grad_att = carried * split_nt(value_in, d)
    for level in range(levels):
        part = piece(decay, level)
        grad_att = grad_att + part * exact_nn(part * g, reads * covers[level])
    total = jnp.zeros_like(a)
    bare, weights, score_rows, read_rows = [], [], [], []
    for by in range(SUB):
        if by:
            total = total + rolled(a, by - 1)
        bare.append(jnp.exp(total))
        weights.append(bare[by] * rolled(g, by))
        score_rows.append(jnp.sum(jnp.where(gap == by, scores, 0.0), axis=0, keepdims=True))
        read_rows.append(jnp.sum(jnp.where(gap == by, reads, 0.0), axis=0, keepdims=True))
        grad_att = grad_att + weights[by] * read_rows[by]
    grad_logits = attention * (
        grad_att - jnp.sum(attention * grad_att, axis=0, keepdims=True)
    )
    mixing = jnp.zeros((CHUNK, CHUNK), F32)
    spread = jnp.zeros((CHUNK, CHUNK), F32)
    ends = after * rows[2:3, :]
    grad_inflow = ends * (split_nt(key_after, k) + split_nt(value_after, v))
    for level in range(levels):
        part = piece(decay, level)
        left = (part * g).astype(BF16)
        att_part, log_part = part * attention, part * grad_logits
        mixing = mixing + covers[level] * dot_tn(left, att_part.astype(BF16))
        spread = spread + covers[level] * dot_tn(left, log_part.astype(BF16))
        grad_inflow = grad_inflow + part * (
            exact_nt(log_part, scores * covers[level]) + exact_nt(att_part, reads * covers[level])
        )
    for by in range(SUB):
        row = jnp.sum(weights[by] * attention, axis=0, keepdims=True)
        mixing = jnp.where(gap == by, row, mixing)
        row = jnp.sum(weights[by] * grad_logits, axis=0, keepdims=True)
        spread = jnp.where(gap == by, row, spread)
        terms = bare[by] * (grad_logits * score_rows[by] + attention * read_rows[by])
        grad_inflow = grad_inflow + rolled(terms, -by)
    mixing = jnp.where(visible, mixing, 0.0).astype(BF16)
    spread = (jnp.where(visible, spread, 0.0) * factor).astype(BF16)
    log_carried = carried * grad_logits * factor
    att_carried = carried * attention
    ends = (ends * g).astype(BF16)
    grad_all[:, :size] = (
        dot_tn(spread, k) + dot_tn(log_carried.astype(BF16), key_in.astype(BF16))
    ).astype(BF16)
    grad_all[:, size : 2 * size] = (dot_nn(spread, q) + dot_tn(ends, key_after.astype(BF16))).astype(BF16)
    grad_all[:, 2 * size :] = (dot_nn(mixing, d) + dot_tn(ends, value_after.astype(BF16))).astype(BF16)
    change = grad_logits * logits + attention * grad_att - g * grad_inflow
    later = piece(sums, levels + 1) + jnp.where(gap == 0, 1.0, 0.0)
    same = jnp.where(visible, later, 0.0)
    flows = exact_nn(change, same) + rows[2:3, :] * flow[:, 0:1]
    grad_rate[...] = rows[3:4, :] * flows - jnp.exp(a) * grad_inflow
    keep = carried[:, CHUNK - 1 : CHUNK]
    key_before = keep * key_after + split_nn(log_carried, q)
    value_before = keep * value_after + split_nn(att_carried, d)
    state_grad[:SLOTS, :] = key_before
    state_grad[SLOTS:, :] = value_before
    flow[...] = jnp.broadcast_to(
        jnp.sum(key_before * key_in + value_before * value_in, axis=1, keepdims=True), flow.shape
    )


def mixer_specs(length, size, ring, backward):
    count = length // CHUNK
    per = count // ring

    def natural(step):
        return count - 1 - step if backward else step

    def moved(step, mine):
        at = natural(step)
        return lax.bitwise_xor(at // per, mine[0]) * per + at % per

    wide = [
        pl.BlockSpec((CHUNK, size), lambda step, mine, at=at: (moved(step, mine), at))
        for at in range(3)
    ]
    everything = pl.BlockSpec((CHUNK, 3 * size), lambda step, mine: (moved(step, mine), 0))
    pair = pl.BlockSpec((2 * SLOTS, CHUNK), lambda step, mine: (0, moved(step, mine)))
    slim = pl.BlockSpec((SLOTS, CHUNK), lambda step, mine: (0, moved(step, mine)))
    rows = pl.BlockSpec((8, CHUNK), lambda step, mine: (0, natural(step)))
    state = pl.BlockSpec((1, 2 * SLOTS, size), lambda step, mine: (natural(step), 0, 0))
    return count, wide, everything, pair, slim, rows, state


def mixer_forward(mine, ring, size, joined, rates, rows):
    length = joined.shape[0]
    count, wide, _, pair, _, row_spec, state = mixer_specs(length, size, ring, False)
    return pl.pallas_call(
        functools.partial(mixer_forward_kernel, size ** (-0.25)),
        out_shape=(
            jax.ShapeDtypeStruct((length, size), F32),
            jax.ShapeDtypeStruct((2 * SLOTS, length), F32),
            jax.ShapeDtypeStruct((count, 2 * SLOTS, size), F32),
        ),
        grid_spec=pltpu.PrefetchScalarGridSpec(
            num_scalar_prefetch=1,
            grid=(count,),
            in_specs=wide + [pair, row_spec],
            out_specs=[wide[0], pair, state],
            scratch_shapes=[pltpu.VMEM((2 * SLOTS, size), F32)] + TABLES,
        ),
        compiler_params=pltpu.CompilerParams(vmem_limit_bytes=32 << 20),
        cost_estimate=pl.CostEstimate(
            flops=length * size * 2000, bytes_accessed=length * size * 12, transcendentals=length * 4096
        ),
        name="mixer_forward",
    )(mine, joined, joined, joined, rates, rows)


def mixer_backward(mine, ring, joined, grad, rates, rows, choice, starts):
    length, size = grad.shape
    count, wide, everything, pair, slim, row_spec, state = mixer_specs(length, size, ring, True)
    return pl.pallas_call(
        functools.partial(mixer_backward_kernel, size ** (-0.25)),
        out_shape=(
            jax.ShapeDtypeStruct((length, 3 * size), BF16),
            jax.ShapeDtypeStruct((SLOTS, length), F32),
        ),
        grid_spec=pltpu.PrefetchScalarGridSpec(
            num_scalar_prefetch=1,
            grid=(count,),
            in_specs=wide + [wide[0], pair, row_spec, pair, state],
            out_specs=[everything, slim],
            scratch_shapes=[pltpu.VMEM((2 * SLOTS, size), F32), pltpu.VMEM((SLOTS, 128), F32)]
            + TABLES,
        ),
        compiler_params=pltpu.CompilerParams(vmem_limit_bytes=32 << 20),
        cost_estimate=pl.CostEstimate(
            flops=length * size * 4000, bytes_accessed=length * size * 20, transcendentals=length * 4096
        ),
        name="mixer_backward",
    )(mine, joined, joined, joined, grad, rates, rows, choice, starts)


def peers(ring, mine):
    found = []
    for by in range(1, ring):
        at, bit = mine, 1
        while bit <= by:
            if by & bit:
                at = at + bit * (1 - 2 * ((at // bit) % 2))
            bit *= 2
        found.append(at)
    return found


class Copies:
    def __init__(self, local, send, recv):
        self.local, self.send, self.recv = local, send, recv
        self.here, self.away = 0, 0
        self.open = []

    def near(self, source, target):
        copy = pltpu.make_async_copy(source, target, self.local.at[self.here])
        self.here += 1
        copy.start()
        return copy

    def far(self, source, target, landed, device, when=None):
        at = self.away
        self.away += 1
        copy = pltpu.make_async_remote_copy(
            source, target, self.send.at[at], self.recv.at[at], device_id=device,
            device_id_type=pl.DeviceIdType.MESH,
        )
        if when is None:
            copy.start()
        else:
            pl.when(when)(copy.start)
        self.open.append((copy, when))
        return pltpu.make_async_remote_copy(
            landed, landed, self.send.at[at], self.recv.at[at], device_id=device,
            device_id_type=pl.DeviceIdType.MESH,
        ).wait_recv

    def close(self):
        for copy, when in self.open:
            if when is None:
                copy.wait_send()
            else:
                pl.when(when)(copy.wait_send)


PARTS = 4


def fold_kernel(finish, extras, *refs):
    terms, given = refs[0], refs[1 : 1 + extras]
    blocks = refs[1 + extras]
    made = refs[2 + extras : -9]
    first, second, third, two_low, one_high, own, local_sem, send_sem, recv_sem = refs[-9:]
    mine, batch = lax.axis_index("seq"), lax.axis_index("batch")
    others = peers(4, mine)
    row, col = (others[0], batch), (others[1], batch)
    copies = Copies(local_sem, send_sem, recv_sem)
    size = terms.shape[1] // PARTS

    def span(at):
        low = pl.ds(at * size, size // 2)
        return pl.ds(at * size, size), low, pl.ds(at * size + size // 2, size // 2)

    opening, direct = [], []

    def open_part(at):
        _, low, high = span(at)
        opening.append(
            (
                copies.far(terms.at[3, low], first.at[low], first.at[low], row),
                copies.far(terms.at[3, high], first.at[high], first.at[high], col),
            )
        )

    def pass_part(at):
        _, low, high = span(at)
        waits = [
            copies.far(terms.at[2, high], second.at[high], second.at[high], col),
            copies.far(terms.at[1, low], third.at[low], third.at[low], row),
        ]
        opening[at][0]()
        two_low[low, :] = added(terms[2, low, :], first[low, :])
        waits.append(copies.far(two_low.at[low], second.at[low], second.at[low], col))
        opening[at][1]()
        one_high[high, :] = added(terms[1, high, :], first[high, :])
        waits.append(copies.far(one_high.at[high], third.at[high], third.at[high], row))
        direct.append(waits)

    spread, local, passed = [], [], []

    def close_part(at):
        full, _, _ = span(at)
        for wait in direct[at]:
            wait()
        total = terms[0, full, :].astype(F32) + second[full, :].astype(F32) + third[full, :].astype(F32)
        own[full, :] = finish(total, full, at, given, made)
        spread.append(
            (
                copies.far(own.at[full], blocks.at[1, full], blocks.at[1, full], row),
                copies.far(own.at[full], blocks.at[2, full], blocks.at[2, full], col),
            )
        )
        local.append(copies.near(own.at[full], blocks.at[0, full]))

    def forward_part(at):
        _, low, high = span(at)
        for wait in spread[at]:
            wait()
        passed.append(copies.far(blocks.at[2, low], blocks.at[3, low], blocks.at[3, low], row))
        passed.append(copies.far(blocks.at[1, high], blocks.at[3, high], blocks.at[3, high], col))

    open_part(0)
    for at in range(PARTS + 2):
        if at + 1 < PARTS:
            open_part(at + 1)
        if at < PARTS:
            pass_part(at)
        if 1 <= at <= PARTS:
            close_part(at - 1)
        if at >= 2:
            forward_part(at - 2)
    for wait in passed:
        wait()
    for copy in local:
        copy.wait()
    copies.close()


def half_blocks(value, order):
    lane = lax.broadcasted_iota(jnp.int32, (value.shape[0], 128), 1)
    made = []
    for pair in zip(order[::2], order[1::2]):
        low, high = (
            value[:, block * 128 : (block + 1) * 128]
            if half == want
            else pltpu.roll(value[:, block * 128 : (block + 1) * 128], 64, 1)
            for want, (block, half) in enumerate(pair)
        )
        made.append(jnp.where(lane < 64, low, high))
    return jnp.concatenate(made, axis=1)


def by_line(value):
    lines = value.shape[1] // 256
    return half_blocks(
        value, [divmod(ring * lines + line, 2) for line in range(lines) for ring in range(4)]
    )


def by_ring(value):
    lines = value.shape[1] // 256
    return half_blocks(
        value, [divmod(line * 4 + ring, 2) for ring in range(4) for line in range(lines)]
    )


def finish_forward(total, full, at, given, made):
    inputs, gain = given
    hidden = inputs[full, :].astype(F32) + total
    made[0][full, :] = hidden
    return by_line(hidden * rms_scale(hidden) * gain[...]).astype(BF16)


def finish_backward(total, full, at, given, made):
    cotangent, hidden_ref, gain = given
    total = by_ring(total)
    hidden = hidden_ref[full, :]
    scale = rms_scale(hidden)
    plain = hidden * scale
    term = jnp.sum(total * plain, axis=0, keepdims=True)
    made[1][...] = term if at == 0 else made[1][...] + term
    scaled = total * gain[...]
    grad = (
        cotangent[full, :].astype(F32)
        + scale * scaled
        - plain * (scale * jnp.mean(scaled * plain, axis=-1, keepdims=True))
    )
    made[0][full, :] = grad
    return grad.astype(BF16)


def fold(finish, terms, given, made, name):
    ring, rows, width = terms.shape
    inside = pl.BlockSpec(memory_space=pltpu.VMEM)
    block = pltpu.VMEM((rows, width), BF16)
    return pl.pallas_call(
        functools.partial(fold_kernel, finish, len(given)),
        out_shape=(jax.ShapeDtypeStruct((ring, rows, width), BF16),) + made,
        in_specs=[inside] * (1 + len(given)),
        out_specs=[pl.BlockSpec(memory_space=pltpu.HBM)] + [inside] * len(made),
        scratch_shapes=[block] * 6
        + [
            pltpu.SemaphoreType.DMA((PARTS,)),
            pltpu.SemaphoreType.DMA((PARTS * 10,)),
            pltpu.SemaphoreType.DMA((PARTS * 10,)),
        ],
        compiler_params=pltpu.CompilerParams(has_side_effects=True, vmem_limit_bytes=40 << 20),
        name=name,
    )(terms, *given)


def rms_scale(features):
    return lax.rsqrt(jnp.mean(features * features, axis=-1, keepdims=True) + EPS)


def swapped(block, by, ring):
    return lax.ppermute(block, "seq", [(i, i ^ by) for i in range(ring)])


def gathered(block, ring):
    if ring != 4:
        return jnp.concatenate([block] + [swapped(block, by, ring) for by in range(1, ring)], axis=0)
    half = block.shape[0] // 2
    one, two = swapped(block, 1, ring), swapped(block, 2, ring)
    low, high = swapped(two[:half], 1, ring), swapped(one[half:], 2, ring)
    return jnp.concatenate([block, one, two, low, high], axis=0)


def scattered(terms, ring, wait_first=None, wait_second=None):
    rows = terms.shape[0] // ring
    parts = [terms[by * rows : (by + 1) * rows] for by in range(ring)]
    total = parts[0].astype(F32)
    if ring != 4:
        for by in range(1, ring):
            total = total + swapped(parts[by], by, ring).astype(F32)
        return total if wait_first is None else (total, wait_first, wait_second)
    half = rows // 2
    low, high = swapped(parts[3][:half], 1, ring), swapped(parts[3][half:], 2, ring)
    if wait_first is not None:
        low, high, wait_first = lax.optimization_barrier((low, high, wait_first))
    two = jnp.concatenate([added(parts[2][:half], low), parts[2][half:]], axis=0)
    one = jnp.concatenate([parts[1][:half], added(parts[1][half:], high)], axis=0)
    one, two = swapped(one, 1, ring), swapped(two, 2, ring)
    if wait_first is not None:
        one, two, wait_second = lax.optimization_barrier((one, two, wait_second))
    total = total + one.astype(F32) + two.astype(F32)
    return total if wait_first is None else (total, wait_first, wait_second)


def added(left, right):
    return (left.astype(F32) + right.astype(F32)).astype(BF16)


def flipped(block, axis, by):
    return lax.ppermute(block, axis, [(i, i ^ by) for i in range(lax.axis_size(axis))])


def doubled(block, axis):
    by, mine = 1, lax.axis_index(axis)
    while by < lax.axis_size(axis):
        other = flipped(block, axis, by)
        first = (mine & by) == 0
        block = jnp.concatenate(
            [jnp.where(first, block, other), jnp.where(first, other, block)], axis=0
        )
        by *= 2
    return block


def halved(block, axis):
    by, mine = lax.axis_size(axis) // 2, lax.axis_index(axis)
    while by:
        low, high = jnp.split(block, 2, axis=0)
        first = (mine & by) == 0
        block = jnp.where(first, low, high) + flipped(jnp.where(first, high, low), axis, by)
        by //= 2
    return block


def core_halves(array, lines, axis):
    size = array.shape[axis] // lines
    even, odd = (
        jnp.concatenate(
            [
                lax.slice_in_dim(array, line * size, (line + 1) * size, axis=axis)
                for line in range(which, lines, 2)
            ],
            axis=axis,
        )
        for which in range(2)
    )
    first = lax.axis_index("batch") % 2 == 0
    return jnp.where(first, even, odd), jnp.where(first, odd, even)


def core_sum(features, grads, lines, fill=()):
    if (features.shape[1] // lines) % 128:
        mine, others = core_halves(dot_tn(features, grads).astype(BF16), lines, 0)
        return added(mine, flipped(others, "batch", 1))
    mine, others = core_halves(features, lines, 1)
    sent = flipped(dot_tn(others, grads).astype(BF16), "batch", 1)
    mine = after(mine, *fill) if fill else mine
    return (dot_tn(mine, grads) + sent.astype(F32)).astype(BF16)


def line_sum(terms, lines):
    groups = [list(range(core, lines, 2)) for core in range(2)]
    return lax.psum_scatter(
        terms, "batch", scatter_dimension=0, axis_index_groups=groups, tiled=True
    )


def after(value, *others):
    return lax.optimization_barrier((value,) + others)[0]


def exchanged(blocks, mine, ring):
    parts = [
        swapped(lax.dynamic_index_in_dim(blocks, mine ^ by, 0, keepdims=False), by, ring)
        if by
        else lax.dynamic_index_in_dim(blocks, mine, 0, keepdims=False)
        for by in range(ring)
    ]
    made = jnp.stack(parts)
    return jnp.concatenate(
        [lax.dynamic_index_in_dim(made, mine ^ j, 0, keepdims=True) for j in range(ring)], axis=0
    )


def local(
    layer_input,
    segments,
    mixer_gain,
    query_weight,
    key_weight,
    value_weight,
    squeeze,
    expand,
    forget_bias,
    swish_weight,
    head_gain,
    output_weight,
    feed_gain,
    gate_weight,
    up_weight,
    down_weight,
    cotangent,
):
    ring, lines = lax.axis_size("seq"), lax.axis_size("batch")
    devices = ring * lines
    mine = lax.axis_index("seq")
    rows, width = layer_input.shape[1], layer_input.shape[2]
    length = rows * ring
    own = width // devices
    head_size = width // HEADS
    copies = ring // HEADS
    part = width // ring
    head = mine // copies
    hidden_part = gate_weight.shape[1] // ring
    slots_all = HEADS * SLOTS

    def to_order(array):
        if copies == 1:
            return array
        blocks = array.reshape((ring, rows) + array.shape[1:])
        moved = [lax.dynamic_index_in_dim(blocks, mine ^ by, 0, keepdims=False) for by in range(ring)]
        return jnp.concatenate(moved, axis=0)

    def whole_head(array):
        if copies == 1:
            return array
        full = lax.all_gather(to_order(array), "seq", axis=1, tiled=True)
        return to_order(lax.dynamic_slice_in_dim(full, head * head_size, head_size, 1))

    def own_part(array):
        if copies == 1:
            return array
        return lax.dynamic_slice_in_dim(array, (mine % copies) * part, part, 1)

    params = jnp.concatenate(
        [
            mixer_gain,
            head_gain,
            feed_gain,
            forget_bias,
            expand.T.reshape(-1),
            squeeze.reshape(-1),
        ]
    )
    count = params.shape[0]
    params = jnp.concatenate([params, segments.reshape(rows).astype(BF16)])
    input_own = layer_input.reshape(rows, width)
    grad_own = cotangent.reshape(rows, width)

    def permuted(array):
        shape = array.shape[:-1]
        array = array.reshape(shape + (ring, lines, own))
        return jnp.swapaxes(array, -3, -2).reshape(shape + (width,))

    def restored(array):
        shape = array.shape[:-1]
        array = array.reshape(shape + (lines, ring, own))
        return jnp.swapaxes(array, -3, -2).reshape(shape + (width,))

    def columns(*arrays):
        blocks = [a.reshape(own, ring, a.shape[1] // ring) for a in arrays]
        return jnp.concatenate(blocks, axis=2).transpose(1, 0, 2)

    w_output = lax.all_gather(output_weight, "batch", axis=0, tiled=True)
    mixer_columns = exchanged(
        columns(query_weight, key_weight, value_weight, swish_weight), mine, ring
    )
    w_mixer = lax.all_gather(mixer_columns.reshape(ring * own, -1), "batch", axis=0, tiled=True)
    feed_columns = exchanged(columns(gate_weight, up_weight), mine, ring)
    w_feed = lax.all_gather(feed_columns.reshape(ring * own, -1), "batch", axis=0, tiled=True)
    w_down = lax.all_gather(after(down_weight, feed_columns), "batch", axis=0, tiled=True)
    if ring != 4:
        w_feed = w_feed.reshape(lines, ring, own, -1).transpose(1, 0, 2, 3).reshape(width, -1)

    inputs = after(gathered(permuted(input_own), ring), w_output)
    small = doubled(doubled(params[None], "batch"), "seq")
    grad_out = gathered(after(grad_own, inputs, w_mixer), ring)
    small = small.reshape(devices, -1)
    segment = lax.dynamic_index_in_dim(
        small.reshape(ring, lines, -1), lax.axis_index("batch"), 1, keepdims=False
    )[:, count : count + rows].reshape(length).astype(F32)
    cuts = np.cumsum([own, own, own, slots_all // devices, RANK * slots_all // devices])
    gain_one, gain_head, gain_two, bias_full, expand_t, w_squeeze = jnp.split(
        small[:, :count], cuts, axis=1
    )
    gain_one = permuted(gain_one.reshape(width)).astype(F32)
    gain_head = lax.dynamic_slice_in_dim(gain_head.reshape(width), head * head_size, head_size, 0)
    gain_head = gain_head.astype(F32)
    gain_two = gain_two.reshape(width).astype(F32)
    bias_head = lax.dynamic_slice_in_dim(bias_full.reshape(slots_all), head * SLOTS, SLOTS, 0)
    expand_head = lax.dynamic_slice_in_dim(
        expand_t.reshape(slots_all, RANK), head * SLOTS, SLOTS, 0
    )
    w_squeeze = permuted(w_squeeze.reshape(width, RANK).T)

    chunked = segment.reshape(-1, CHUNK)
    before = jnp.concatenate([jnp.full((1,), -1.0, F32), chunked[:-1, -1]])
    previous = jnp.concatenate([jnp.full((1,), -1.0, F32), segment[:-1]])
    mask_rows = jnp.stack(
        [
            segment,
            (chunked == before[:, None]).astype(F32).reshape(-1),
            (chunked == chunked[:, -1:]).astype(F32).reshape(-1),
            (segment == previous).astype(F32),
        ]
        + [jnp.zeros_like(segment)] * 4
    )

    inputs = inputs.astype(F32)
    scale_one = rms_scale(inputs)
    plain_one = inputs * scale_one
    normed = (plain_one * gain_one).astype(BF16)
    mixer_pre = dot_nn(normed, w_mixer)
    joined = mixer_pre.astype(BF16)
    if copies > 1:
        joined = jnp.concatenate(
            [whole_head(joined[:, at * part : (at + 1) * part]) for at in range(3)], axis=1
        )
    swish_pre = whole_head(mixer_pre[:, 3 * part :])
    reduced = dot_nt(normed, w_squeeze).astype(BF16)
    forget_logit = dot_nt(expand_head, reduced) + bias_head.astype(F32)[:, None]
    log_rate = jax.nn.log_sigmoid(forget_logit) / TAU_GATE
    rates = jnp.concatenate([log_rate, -jnp.expm1(log_rate)], axis=0)
    order = mine.reshape(1).astype(jnp.int32)
    mixed, choice, starts = mixer_forward(order, ring, head_size, joined, rates, mask_rows)
    head_factor = rms_scale(mixed)
    head_plain = mixed * head_factor
    head_normed = head_plain * gain_head
    swish_sig = jax.nn.sigmoid(swish_pre)
    swish_act = swish_pre * swish_sig
    gated = own_part((head_normed * swish_act).astype(BF16))
    terms = dot_nn(gated, w_output).astype(BF16)
    terms, grad_out = lax.optimization_barrier((terms, grad_out))
    if ring == 4:
        feed_in, hidden = fold(
            finish_forward,
            terms.reshape(ring, rows, width),
            (input_own, gain_two[None]),
            (jax.ShapeDtypeStruct((rows, width), F32),),
            "fold_forward",
        )
        feed_in = feed_in.reshape(length, width)
    else:
        hidden = input_own.astype(F32) + scattered(terms, ring)
        feed_in = gathered((hidden * rms_scale(hidden) * gain_two).astype(BF16), ring)

    feed_pre = dot_nn(feed_in, w_feed)
    gate_pre, up_pre = feed_pre[:, :hidden_part], feed_pre[:, hidden_part:]
    gate_sig = jax.nn.sigmoid(gate_pre)
    gate_act = gate_pre * gate_sig
    inner = (gate_act * up_pre).astype(BF16)

    term_down = dot_tn(inner, grad_out).astype(BF16)
    grad_inner = dot_nt(after(grad_out, term_down), w_down)
    grad_gatepre = grad_inner * up_pre * (gate_sig * (1.0 + gate_pre * (1.0 - gate_sig)))
    grad_feedpre = jnp.concatenate(
        [grad_gatepre.astype(BF16), (grad_inner * gate_act).astype(BF16)], axis=1
    )
    back_feedin = dot_nt(grad_feedpre, w_feed).astype(BF16)
    result_terms = dot_nn(after(inner, back_feedin), w_down).astype(BF16)
    feed_lines = feed_in if ring == 4 else permuted(feed_in)
    term_feedpre = core_sum(after(feed_lines, back_feedin), grad_feedpre, lines, (result_terms,))
    down_share = lax.psum_scatter(term_down, "batch", scatter_dimension=0, tiled=True)
    feed_sum = line_sum(after(term_feedpre, down_share), lines)
    if ring == 4:
        grad_branch, grad_hidden, term_feed = fold(
            finish_backward,
            after(back_feedin, term_feedpre).reshape(ring, rows, width),
            (grad_own, hidden, gain_two[None]),
            (
                jax.ShapeDtypeStruct((rows, width), F32),
                jax.ShapeDtypeStruct((1, width), F32),
            ),
            "fold_backward",
        )
        grad_branch, term_feed = grad_branch.reshape(length, width), term_feed[0]
    else:
        grad_feedin = scattered(back_feedin, ring)
        scale_two = rms_scale(hidden)
        term_feed = jnp.sum(grad_feedin * hidden * scale_two, axis=0)
        scaled_two = grad_feedin * gain_two
        grad_hidden = (
            grad_own.astype(F32)
            + scale_two * scaled_two
            - hidden * scale_two**3 * jnp.mean(scaled_two * hidden, axis=-1, keepdims=True)
        )
        grad_branch = gathered(grad_hidden.astype(BF16), ring)

    grad_gated = whole_head(dot_nt(grad_branch, w_output))

    slope = swish_sig * (1.0 + swish_pre * (1.0 - swish_sig))
    grad_swishpre = own_part((grad_gated * head_normed * slope).astype(BF16))
    grad_normed_head = grad_gated * swish_act
    term_head = jnp.sum(grad_normed_head * head_plain, axis=0) / copies
    scaled_head = grad_normed_head * gain_head
    grad_mixed = head_factor * scaled_head - mixed * head_factor**3 * jnp.mean(
        scaled_head * mixed, axis=-1, keepdims=True
    )
    result, grad_mixed, normed_late = scattered(
        after(result_terms, grad_branch), ring, grad_mixed.astype(BF16), normed
    )
    layer_output = (hidden + result).astype(BF16).reshape(1, rows, width)
    term_output = core_sum(after(gated, grad_mixed), grad_branch, lines)
    output_share = line_sum(after(term_output, feed_sum), lines)
    grad_mixed = after(grad_mixed, term_output)
    grad_pre, grad_rate = mixer_backward(
        order, ring, joined, grad_mixed, rates, mask_rows, choice, starts
    )
    grad_logit = (grad_rate * jax.nn.sigmoid(-forget_logit) / TAU_GATE).astype(BF16)
    term_bias = jnp.sum(grad_logit.astype(F32), axis=1) / copies
    term_expand = dot_nn(grad_logit, reduced) / copies
    grad_reduced = (dot_tn(grad_logit, expand_head) / copies).astype(BF16)
    if copies > 1:
        grad_pre = jnp.concatenate(
            [own_part(grad_pre[:, at * head_size : (at + 1) * head_size]) for at in range(3)], axis=1
        )
    grad_pre = jnp.concatenate([grad_pre, grad_swishpre], axis=1)
    term_pre = dot_tn(normed_late, grad_pre).astype(BF16)
    pre_sum = lax.psum_scatter(
        after(term_pre, output_share), "batch", scatter_dimension=0, tiled=True
    )
    grad_normed = dot_nt(after(grad_pre, term_pre), w_mixer) + dot_nn(grad_reduced, w_squeeze)
    grad_normed = dot_nt(after(grad_pre, term_pre), w_mixer) + dot_nn(grad_reduced, w_squeeze)
    term_mixer = restored(jnp.sum(grad_normed * plain_one, axis=0))
    term_squeeze = restored(dot_tn(grad_reduced, normed))
    grad_normed, _, (term_mixer, term_squeeze) = scattered(
        grad_normed.astype(BF16), ring, term_bias, (term_mixer, term_squeeze)
    )
    grad_normed = restored(grad_normed)
    inputs_own = input_own.astype(F32)
    scale_own = rms_scale(inputs_own)
    scaled_one = grad_normed * restored(gain_one)
    grad_input = (
        grad_hidden
        + scale_own * scaled_one
        - inputs_own * scale_own**3 * jnp.mean(scaled_one * inputs_own, axis=-1, keepdims=True)
    ).astype(BF16)
    pre_share = exchanged(pre_sum.reshape(ring, own, 4 * part), mine, ring)

    def joined_columns(blocks, first, size):
        return jnp.concatenate(
            [blocks[at, :, first : first + size] for at in range(ring)], axis=1
        ).astype(F32)

    query_share, key_share, value_share, swish_share = (
        joined_columns(pre_share, at * part, part) for at in range(4)
    )
    feed_share = exchanged(after(feed_sum, term_pre).reshape(ring, own, 2 * hidden_part), mine, ring)
    gate_share = joined_columns(feed_share, 0, hidden_part)
    up_share = joined_columns(feed_share, hidden_part, hidden_part)

    def placed(array, size):
        full = jnp.zeros((HEADS, size) + array.shape[1:], F32)
        return lax.dynamic_update_slice_in_dim(full, array[None], head, 0)

    terms = jnp.concatenate(
        [
            term_mixer.reshape(devices, -1),
            placed(term_head, head_size).reshape(devices, -1),
            term_feed.reshape(devices, -1),
            placed(term_bias, SLOTS).reshape(devices, -1),
            placed(term_expand, SLOTS).reshape(devices, -1),
            term_squeeze.T.reshape(devices, -1),
        ],
        axis=1,
    )
    share = halved(halved(terms, "seq"), "batch")[0]
    mixer_share, head_share, feedgain_share, bias_share, expand_share, squeeze_share = jnp.split(
        share, cuts
    )
    return (
        layer_output,
        grad_input.reshape(1, rows, width),
        mixer_share,
        query_share,
        key_share,
        value_share,
        squeeze_share.reshape(own, RANK),
        expand_share.reshape(-1, RANK).T,
        bias_share,
        swish_share,
        head_share,
        output_share.astype(F32),
        feedgain_share,
        gate_share,
        up_share,
        down_share.astype(F32),
    )


def solution(mesh):
    rows = P(BOTH, None)
    spread = P(BOTH)
    in_specs = (
        P("batch", "seq", None),
        P("batch", "seq"),
        spread,
        rows,
        rows,
        rows,
        rows,
        P(None, BOTH),
        spread,
        rows,
        spread,
        rows,
        spread,
        rows,
        rows,
        rows,
        P("batch", "seq", None),
    )
    out_specs = (
        P("batch", "seq", None),
        P("batch", "seq", None),
        spread,
        rows,
        rows,
        rows,
        rows,
        P(None, BOTH),
        spread,
        rows,
        spread,
        rows,
        spread,
        rows,
        rows,
        rows,
    )
    return jax.shard_map(local, mesh=mesh, in_specs=in_specs, out_specs=out_specs, check_vma=False)
```

```python
import functools

import jax
import jax.numpy as jnp
import numpy as np
from jax import lax
from jax.experimental import pallas as pl
from jax.experimental.pallas import tpu as pltpu
from jax.sharding import PartitionSpec as P

HEADS = 4
SLOTS = 64
RANK = 16
EPS = 1e-06
TAU_GATE = 8.0
CHUNK = 128
SUB = 16
BOTH = ("seq", "batch")
F32 = jnp.float32
BF16 = jnp.bfloat16
HIGHEST = lax.Precision.HIGHEST


def dot_nn(left, right):
    return lax.dot_general(left, right, (((1,), (0,)), ((), ())), preferred_element_type=F32)


def dot_nt(left, right):
    return lax.dot_general(left, right, (((1,), (1,)), ((), ())), preferred_element_type=F32)


def dot_tn(left, right):
    return lax.dot_general(left, right, (((0,), (0,)), ((), ())), preferred_element_type=F32)


def exact_nn(left, right):
    return lax.dot_general(
        left, right, (((1,), (0,)), ((), ())), precision=HIGHEST, preferred_element_type=F32
    )


def exact_nt(left, right):
    return lax.dot_general(
        left, right, (((1,), (1,)), ((), ())), precision=HIGHEST, preferred_element_type=F32
    )


def halves(value):
    high = value.astype(BF16)
    return high, (value - high.astype(F32)).astype(BF16)


def split_nn(left, right):
    high, rest = halves(left)
    return dot_nn(high, right) + dot_nn(rest, right)


def split_nt(left, right):
    high, rest = halves(left)
    return dot_nt(high, right) + dot_nt(rest, right)


LEVELS = (CHUNK // SUB).bit_length() - 1


def fill_tables(sums, covers, apart):
    source = lax.broadcasted_iota(jnp.int32, (CHUNK, CHUNK), 0)
    target = lax.broadcasted_iota(jnp.int32, (CHUNK, CHUNK), 1)

    def group(at, size):
        return jnp.bitwise_and(at, CHUNK - size)

    for level in range(LEVELS):
        half = SUB << level
        right = jnp.bitwise_and(target, half) != 0
        edge = group(target, 2 * half) + (half - 1)
        low, high = jnp.where(right, edge, target), jnp.where(right, target, edge)
        sums[:, level * CHUNK : (level + 1) * CHUNK] = jnp.where(
            (source > low) & (source <= high), 1.0, 0.0
        )
        same = group(source, 2 * half) == group(target, 2 * half)
        covers[level] = jnp.where(same & (jnp.bitwise_and(source, half) == 0) & right, 1.0, 0.0)
    sums[:, LEVELS * CHUNK : (LEVELS + 1) * CHUNK] = jnp.where(source <= target, 1.0, 0.0)
    sums[:, (LEVELS + 1) * CHUNK :] = jnp.where(source > target, 1.0, 0.0)
    apart[...] = jnp.where(group(source, SUB) == group(target, SUB), target - source, -1)


TABLES = [
    pltpu.VMEM((CHUNK, (LEVELS + 2) * CHUNK), F32),
    pltpu.VMEM((LEVELS, CHUNK, CHUNK), F32),
    pltpu.VMEM((CHUNK, CHUNK), jnp.int32),
]


def same_document(rows):
    source = lax.broadcasted_iota(jnp.int32, (CHUNK, CHUNK), 0)
    target = lax.broadcasted_iota(jnp.int32, (CHUNK, CHUNK), 1)
    number = rows[0:1, :]
    column = jnp.sum(jnp.where(source == target, number, 0.0), axis=1, keepdims=True)
    return column == number


def rolled(value, by):
    return value if by % CHUNK == 0 else pltpu.roll(value, by % CHUNK, 1)


def exponents(rate, sums):
    return jnp.exp(exact_nn(rate, sums))


def piece(value, at):
    return value[:, at * CHUNK : (at + 1) * CHUNK]


def mixer_forward_kernel(
    factor, mine, query, key, value, rate, rows, output, choice_out, start_out, state, sums, covers, apart
):
    levels = LEVELS

    @pl.when(pl.program_id(0) == 0)
    def _():
        state[...] = jnp.zeros_like(state)
        fill_tables(sums, covers, apart)

    key_in, value_in = state[:SLOTS, :], state[SLOTS:, :]
    start_out[0] = state[...]
    q, k, v = query[...], key[...], value[...]
    a, g = rate[:SLOTS, :], rate[SLOTS:, :]
    decay = exponents(a, sums[...])
    before, after = piece(decay, levels), piece(decay, levels + 1)
    carried = before * rows[1:2, :]
    visible = same_document(rows)
    scores = jnp.where(visible, dot_nt(k, q) * factor, 0.0)
    logits = carried * (split_nt(key_in, q) * factor)
    for level in range(levels):
        part = piece(decay, level)
        logits = logits + part * exact_nn(part * g, scores * covers[level])
    gap = apart[...]
    total = jnp.zeros_like(a)
    weights = []
    for by in range(SUB):
        if by:
            total = total + rolled(a, by - 1)
        weight = jnp.exp(total) * rolled(g, by)
        weights.append(weight)
        logits = logits + weight * jnp.sum(
            jnp.where(gap == by, scores, 0.0), axis=0, keepdims=True
        )
    attention = jnp.exp(logits - jnp.max(logits, axis=0, keepdims=True))
    attention = attention / jnp.sum(attention, axis=0, keepdims=True)
    choice_out[:SLOTS, :] = attention
    choice_out[SLOTS:, :] = logits
    mixing = jnp.zeros((CHUNK, CHUNK), F32)
    for level in range(levels):
        part = piece(decay, level)
        mixing = mixing + covers[level] * dot_tn(
            (part * g).astype(BF16), (part * attention).astype(BF16)
        )
    for by in range(SUB):
        row = jnp.sum(weights[by] * attention, axis=0, keepdims=True)
        mixing = jnp.where(gap == by, row, mixing)
    mixing = jnp.where(visible, mixing, 0.0).astype(BF16)
    output[...] = dot_tn(mixing, v) + dot_tn(
        (carried * attention).astype(BF16), value_in.astype(BF16)
    )
    ends = after * g * rows[2:3, :]
    keep = carried[:, CHUNK - 1 : CHUNK]
    state[:SLOTS, :] = keep * key_in + split_nn(ends, k)
    state[SLOTS:, :] = keep * value_in + split_nn(ends, v)


def mixer_backward_kernel(
    factor, mine, query, key, value, grad_output, rate, rows, choice, start, grad_all, grad_rate,
    state_grad, flow, sums, covers, apart,
):
    levels = LEVELS

    @pl.when(pl.program_id(0) == 0)
    def _():
        state_grad[...] = jnp.zeros_like(state_grad)
        flow[...] = jnp.zeros_like(flow)
        fill_tables(sums, covers, apart)

    key_in, value_in = start[0, :SLOTS, :], start[0, SLOTS:, :]
    key_after, value_after = state_grad[:SLOTS, :], state_grad[SLOTS:, :]
    q, k, v, d = query[...], key[...], value[...], grad_output[...]
    size = q.shape[1]
    a, g = rate[:SLOTS, :], rate[SLOTS:, :]
    attention, logits = choice[:SLOTS, :], choice[SLOTS:, :]
    decay = exponents(a, sums[...])
    before, after = piece(decay, levels), piece(decay, levels + 1)
    carried = before * rows[1:2, :]
    visible = same_document(rows)
    scores = jnp.where(visible, dot_nt(k, q) * factor, 0.0)
    reads = jnp.where(visible, dot_nt(v, d), 0.0)
    gap = apart[...]
    grad_att = carried * split_nt(value_in, d)
    for level in range(levels):
        part = piece(decay, level)
        grad_att = grad_att + part * exact_nn(part * g, reads * covers[level])
    total = jnp.zeros_like(a)
    bare, weights, score_rows, read_rows = [], [], [], []
    for by in range(SUB):
        if by:
            total = total + rolled(a, by - 1)
        bare.append(jnp.exp(total))
        weights.append(bare[by] * rolled(g, by))
        score_rows.append(jnp.sum(jnp.where(gap == by, scores, 0.0), axis=0, keepdims=True))
        read_rows.append(jnp.sum(jnp.where(gap == by, reads, 0.0), axis=0, keepdims=True))
        grad_att = grad_att + weights[by] * read_rows[by]
    grad_logits = attention * (
        grad_att - jnp.sum(attention * grad_att, axis=0, keepdims=True)
    )
    mixing = jnp.zeros((CHUNK, CHUNK), F32)
    spread = jnp.zeros((CHUNK, CHUNK), F32)
    ends = after * rows[2:3, :]
    grad_inflow = ends * (split_nt(key_after, k) + split_nt(value_after, v))
    for level in range(levels):
        part = piece(decay, level)
        left = (part * g).astype(BF16)
        att_part, log_part = part * attention, part * grad_logits
        mixing = mixing + covers[level] * dot_tn(left, att_part.astype(BF16))
        spread = spread + covers[level] * dot_tn(left, log_part.astype(BF16))
        grad_inflow = grad_inflow + part * (
            exact_nt(log_part, scores * covers[level]) + exact_nt(att_part, reads * covers[level])
        )
    for by in range(SUB):
        row = jnp.sum(weights[by] * attention, axis=0, keepdims=True)
        mixing = jnp.where(gap == by, row, mixing)
        row = jnp.sum(weights[by] * grad_logits, axis=0, keepdims=True)
        spread = jnp.where(gap == by, row, spread)
        terms = bare[by] * (grad_logits * score_rows[by] + attention * read_rows[by])
        grad_inflow = grad_inflow + rolled(terms, -by)
    mixing = jnp.where(visible, mixing, 0.0).astype(BF16)
    spread = (jnp.where(visible, spread, 0.0) * factor).astype(BF16)
    log_carried = carried * grad_logits * factor
    att_carried = carried * attention
    ends = (ends * g).astype(BF16)
    grad_all[:, :size] = (
        dot_tn(spread, k) + dot_tn(log_carried.astype(BF16), key_in.astype(BF16))
    ).astype(BF16)
    grad_all[:, size : 2 * size] = (dot_nn(spread, q) + dot_tn(ends, key_after.astype(BF16))).astype(BF16)
    grad_all[:, 2 * size :] = (dot_nn(mixing, d) + dot_tn(ends, value_after.astype(BF16))).astype(BF16)
    change = grad_logits * logits + attention * grad_att - g * grad_inflow
    later = piece(sums, levels + 1) + jnp.where(gap == 0, 1.0, 0.0)
    same = jnp.where(visible, later, 0.0)
    flows = exact_nn(change, same) + rows[2:3, :] * flow[:, 0:1]
    grad_rate[...] = rows[3:4, :] * flows - jnp.exp(a) * grad_inflow
    keep = carried[:, CHUNK - 1 : CHUNK]
    key_before = keep * key_after + split_nn(log_carried, q)
    value_before = keep * value_after + split_nn(att_carried, d)
    state_grad[:SLOTS, :] = key_before
    state_grad[SLOTS:, :] = value_before
    flow[...] = jnp.broadcast_to(
        jnp.sum(key_before * key_in + value_before * value_in, axis=1, keepdims=True), flow.shape
    )


def mixer_specs(length, size, ring, backward):
    count = length // CHUNK
    per = count // ring

    def natural(step):
        return count - 1 - step if backward else step

    def moved(step, mine):
        at = natural(step)
        return lax.bitwise_xor(at // per, mine[0]) * per + at % per

    wide = [
        pl.BlockSpec((CHUNK, size), lambda step, mine, at=at: (moved(step, mine), at))
        for at in range(3)
    ]
    everything = pl.BlockSpec((CHUNK, 3 * size), lambda step, mine: (moved(step, mine), 0))
    pair = pl.BlockSpec((2 * SLOTS, CHUNK), lambda step, mine: (0, moved(step, mine)))
    slim = pl.BlockSpec((SLOTS, CHUNK), lambda step, mine: (0, moved(step, mine)))
    rows = pl.BlockSpec((8, CHUNK), lambda step, mine: (0, natural(step)))
    state = pl.BlockSpec((1, 2 * SLOTS, size), lambda step, mine: (natural(step), 0, 0))
    return count, wide, everything, pair, slim, rows, state


def mixer_forward(mine, ring, size, joined, rates, rows):
    length = joined.shape[0]
    count, wide, _, pair, _, row_spec, state = mixer_specs(length, size, ring, False)
    return pl.pallas_call(
        functools.partial(mixer_forward_kernel, size ** (-0.25)),
        out_shape=(
            jax.ShapeDtypeStruct((length, size), F32),
            jax.ShapeDtypeStruct((2 * SLOTS, length), F32),
            jax.ShapeDtypeStruct((count, 2 * SLOTS, size), F32),
        ),
        grid_spec=pltpu.PrefetchScalarGridSpec(
            num_scalar_prefetch=1,
            grid=(count,),
            in_specs=wide + [pair, row_spec],
            out_specs=[wide[0], pair, state],
            scratch_shapes=[pltpu.VMEM((2 * SLOTS, size), F32)] + TABLES,
        ),
        compiler_params=pltpu.CompilerParams(vmem_limit_bytes=32 << 20),
        cost_estimate=pl.CostEstimate(
            flops=length * size * 2000, bytes_accessed=length * size * 12, transcendentals=length * 4096
        ),
        name="mixer_forward",
    )(mine, joined, joined, joined, rates, rows)


def mixer_backward(mine, ring, joined, grad, rates, rows, choice, starts):
    length, size = grad.shape
    count, wide, everything, pair, slim, row_spec, state = mixer_specs(length, size, ring, True)
    return pl.pallas_call(
        functools.partial(mixer_backward_kernel, size ** (-0.25)),
        out_shape=(
            jax.ShapeDtypeStruct((length, 3 * size), BF16),
            jax.ShapeDtypeStruct((SLOTS, length), F32),
        ),
        grid_spec=pltpu.PrefetchScalarGridSpec(
            num_scalar_prefetch=1,
            grid=(count,),
            in_specs=wide + [wide[0], pair, row_spec, pair, state],
            out_specs=[everything, slim],
            scratch_shapes=[pltpu.VMEM((2 * SLOTS, size), F32), pltpu.VMEM((SLOTS, 128), F32)]
            + TABLES,
        ),
        compiler_params=pltpu.CompilerParams(vmem_limit_bytes=32 << 20),
        cost_estimate=pl.CostEstimate(
            flops=length * size * 4000, bytes_accessed=length * size * 20, transcendentals=length * 4096
        ),
        name="mixer_backward",
    )(mine, joined, joined, joined, grad, rates, rows, choice, starts)


def peers(ring, mine):
    found = []
    for by in range(1, ring):
        at, bit = mine, 1
        while bit <= by:
            if by & bit:
                at = at + bit * (1 - 2 * ((at // bit) % 2))
            bit *= 2
        found.append(at)
    return found


class Copies:
    def __init__(self, local, send, recv):
        self.local, self.send, self.recv = local, send, recv
        self.here, self.away = 0, 0
        self.open = []

    def near(self, source, target):
        copy = pltpu.make_async_copy(source, target, self.local.at[self.here])
        self.here += 1
        copy.start()
        return copy

    def far(self, source, target, landed, device, when=None):
        at = self.away
        self.away += 1
        copy = pltpu.make_async_remote_copy(
            source, target, self.send.at[at], self.recv.at[at], device_id=device,
            device_id_type=pl.DeviceIdType.MESH,
        )
        if when is None:
            copy.start()
        else:
            pl.when(when)(copy.start)
        self.open.append((copy, when))
        return pltpu.make_async_remote_copy(
            landed, landed, self.send.at[at], self.recv.at[at], device_id=device,
            device_id_type=pl.DeviceIdType.MESH,
        ).wait_recv

    def close(self):
        for copy, when in self.open:
            if when is None:
                copy.wait_send()
            else:
                pl.when(when)(copy.wait_send)


PARTS = 4


def fold_kernel(finish, extras, *refs):
    terms, given = refs[0], refs[1 : 1 + extras]
    blocks = refs[1 + extras]
    made = refs[2 + extras : -9]
    first, second, third, two_low, one_high, own, local_sem, send_sem, recv_sem = refs[-9:]
    mine, batch = lax.axis_index("seq"), lax.axis_index("batch")
    others = peers(4, mine)
    row, col = (others[0], batch), (others[1], batch)
    copies = Copies(local_sem, send_sem, recv_sem)
    size = terms.shape[1] // PARTS

    def span(at):
        low = pl.ds(at * size, size // 2)
        return pl.ds(at * size, size), low, pl.ds(at * size + size // 2, size // 2)

    opening, direct = [], []

    def open_part(at):
        _, low, high = span(at)
        opening.append(
            (
                copies.far(terms.at[3, low], first.at[low], first.at[low], row),
                copies.far(terms.at[3, high], first.at[high], first.at[high], col),
            )
        )

    def pass_part(at):
        _, low, high = span(at)
        waits = [
            copies.far(terms.at[2, high], second.at[high], second.at[high], col),
            copies.far(terms.at[1, low], third.at[low], third.at[low], row),
        ]
        opening[at][0]()
        two_low[low, :] = added(terms[2, low, :], first[low, :])
        waits.append(copies.far(two_low.at[low], second.at[low], second.at[low], col))
        opening[at][1]()
        one_high[high, :] = added(terms[1, high, :], first[high, :])
        waits.append(copies.far(one_high.at[high], third.at[high], third.at[high], row))
        direct.append(waits)

    spread, local, passed = [], [], []

    def close_part(at):
        full, _, _ = span(at)
        for wait in direct[at]:
            wait()
        total = terms[0, full, :].astype(F32) + second[full, :].astype(F32) + third[full, :].astype(F32)
        own[full, :] = finish(total, full, at, given, made)
        spread.append(
            (
                copies.far(own.at[full], blocks.at[1, full], blocks.at[1, full], row),
                copies.far(own.at[full], blocks.at[2, full], blocks.at[2, full], col),
            )
        )
        local.append(copies.near(own.at[full], blocks.at[0, full]))

    def forward_part(at):
        _, low, high = span(at)
        for wait in spread[at]:
            wait()
        passed.append(copies.far(blocks.at[2, low], blocks.at[3, low], blocks.at[3, low], row))
        passed.append(copies.far(blocks.at[1, high], blocks.at[3, high], blocks.at[3, high], col))

    open_part(0)
    for at in range(PARTS + 2):
        if at + 1 < PARTS:
            open_part(at + 1)
        if at < PARTS:
            pass_part(at)
        if 1 <= at <= PARTS:
            close_part(at - 1)
        if at >= 2:
            forward_part(at - 2)
    for wait in passed:
        wait()
    for copy in local:
        copy.wait()
    copies.close()


def half_blocks(value, order):
    lane = lax.broadcasted_iota(jnp.int32, (value.shape[0], 128), 1)
    made = []
    for pair in zip(order[::2], order[1::2]):
        low, high = (
            value[:, block * 128 : (block + 1) * 128]
            if half == want
            else pltpu.roll(value[:, block * 128 : (block + 1) * 128], 64, 1)
            for want, (block, half) in enumerate(pair)
        )
        made.append(jnp.where(lane < 64, low, high))
    return jnp.concatenate(made, axis=1)


def by_line(value):
    lines = value.shape[1] // 256
    return half_blocks(
        value, [divmod(ring * lines + line, 2) for line in range(lines) for ring in range(4)]
    )


def by_ring(value):
    lines = value.shape[1] // 256
    return half_blocks(
        value, [divmod(line * 4 + ring, 2) for ring in range(4) for line in range(lines)]
    )


def finish_forward(total, full, at, given, made):
    inputs, gain = given
    hidden = inputs[full, :].astype(F32) + total
    made[0][full, :] = hidden
    return by_line(hidden * rms_scale(hidden) * gain[...]).astype(BF16)


def finish_backward(total, full, at, given, made):
    cotangent, hidden_ref, gain = given
    total = by_ring(total)
    hidden = hidden_ref[full, :]
    scale = rms_scale(hidden)
    plain = hidden * scale
    term = jnp.sum(total * plain, axis=0, keepdims=True)
    made[1][...] = term if at == 0 else made[1][...] + term
    scaled = total * gain[...]
    grad = (
        cotangent[full, :].astype(F32)
        + scale * scaled
        - plain * (scale * jnp.mean(scaled * plain, axis=-1, keepdims=True))
    )
    made[0][full, :] = grad
    return grad.astype(BF16)


def fold(finish, terms, given, made, name):
    ring, rows, width = terms.shape
    inside = pl.BlockSpec(memory_space=pltpu.VMEM)
    block = pltpu.VMEM((rows, width), BF16)
    return pl.pallas_call(
        functools.partial(fold_kernel, finish, len(given)),
        out_shape=(jax.ShapeDtypeStruct((ring, rows, width), BF16),) + made,
        in_specs=[inside] * (1 + len(given)),
        out_specs=[pl.BlockSpec(memory_space=pltpu.HBM)] + [inside] * len(made),
        scratch_shapes=[block] * 6
        + [
            pltpu.SemaphoreType.DMA((PARTS,)),
            pltpu.SemaphoreType.DMA((PARTS * 10,)),
            pltpu.SemaphoreType.DMA((PARTS * 10,)),
        ],
        compiler_params=pltpu.CompilerParams(has_side_effects=True, vmem_limit_bytes=40 << 20),
        name=name,
    )(terms, *given)


def rms_scale(features):
    return lax.rsqrt(jnp.mean(features * features, axis=-1, keepdims=True) + EPS)


def swapped(block, by, ring):
    return lax.ppermute(block, "seq", [(i, i ^ by) for i in range(ring)])


def gathered(block, ring):
    if ring != 4:
        return jnp.concatenate([block] + [swapped(block, by, ring) for by in range(1, ring)], axis=0)
    half = block.shape[0] // 2
    one, two = swapped(block, 1, ring), swapped(block, 2, ring)
    low, high = swapped(two[:half], 1, ring), swapped(one[half:], 2, ring)
    return jnp.concatenate([block, one, two, low, high], axis=0)


def scattered(terms, ring, wait_first=None, wait_second=None):
    rows = terms.shape[0] // ring
    parts = [terms[by * rows : (by + 1) * rows] for by in range(ring)]
    total = parts[0].astype(F32)
    if ring != 4:
        for by in range(1, ring):
            total = total + swapped(parts[by], by, ring).astype(F32)
        return total if wait_first is None else (total, wait_first, wait_second)
    half = rows // 2
    low, high = swapped(parts[3][:half], 1, ring), swapped(parts[3][half:], 2, ring)
    if wait_first is not None:
        low, high, wait_first = lax.optimization_barrier((low, high, wait_first))
    two = jnp.concatenate([added(parts[2][:half], low), parts[2][half:]], axis=0)
    one = jnp.concatenate([parts[1][:half], added(parts[1][half:], high)], axis=0)
    one, two = swapped(one, 1, ring), swapped(two, 2, ring)
    if wait_first is not None:
        one, two, wait_second = lax.optimization_barrier((one, two, wait_second))
    total = total + one.astype(F32) + two.astype(F32)
    return total if wait_first is None else (total, wait_first, wait_second)


def added(left, right):
    return (left.astype(F32) + right.astype(F32)).astype(BF16)


def flipped(block, axis, by):
    return lax.ppermute(block, axis, [(i, i ^ by) for i in range(lax.axis_size(axis))])


def doubled(block, axis):
    by, mine = 1, lax.axis_index(axis)
    while by < lax.axis_size(axis):
        other = flipped(block, axis, by)
        first = (mine & by) == 0
        block = jnp.concatenate(
            [jnp.where(first, block, other), jnp.where(first, other, block)], axis=0
        )
        by *= 2
    return block


def halved(block, axis):
    by, mine = lax.axis_size(axis) // 2, lax.axis_index(axis)
    while by:
        low, high = jnp.split(block, 2, axis=0)
        first = (mine & by) == 0
        block = jnp.where(first, low, high) + flipped(jnp.where(first, high, low), axis, by)
        by //= 2
    return block


def core_halves(array, lines, axis):
    size = array.shape[axis] // lines
    even, odd = (
        jnp.concatenate(
            [
                lax.slice_in_dim(array, line * size, (line + 1) * size, axis=axis)
                for line in range(which, lines, 2)
            ],
            axis=axis,
        )
        for which in range(2)
    )
    first = lax.axis_index("batch") % 2 == 0
    return jnp.where(first, even, odd), jnp.where(first, odd, even)


def core_sum(features, grads, lines, fill=()):
    if (features.shape[1] // lines) % 128:
        mine, others = core_halves(dot_tn(features, grads).astype(BF16), lines, 0)
        return added(mine, flipped(others, "batch", 1))
    mine, others = core_halves(features, lines, 1)
    sent = flipped(dot_tn(others, grads).astype(BF16), "batch", 1)
    mine = after(mine, *fill) if fill else mine
    return (dot_tn(mine, grads) + sent.astype(F32)).astype(BF16)


def line_sum(terms, lines):
    groups = [list(range(core, lines, 2)) for core in range(2)]
    return lax.psum_scatter(
        terms, "batch", scatter_dimension=0, axis_index_groups=groups, tiled=True
    )


def after(value, *others):
    return lax.optimization_barrier((value,) + others)[0]


def exchanged(blocks, mine, ring):
    parts = [
        swapped(lax.dynamic_index_in_dim(blocks, mine ^ by, 0, keepdims=False), by, ring)
        if by
        else lax.dynamic_index_in_dim(blocks, mine, 0, keepdims=False)
        for by in range(ring)
    ]
    made = jnp.stack(parts)
    return jnp.concatenate(
        [lax.dynamic_index_in_dim(made, mine ^ j, 0, keepdims=True) for j in range(ring)], axis=0
    )


def local(
    layer_input,
    segments,
    mixer_gain,
    query_weight,
    key_weight,
    value_weight,
    squeeze,
    expand,
    forget_bias,
    swish_weight,
    head_gain,
    output_weight,
    feed_gain,
    gate_weight,
    up_weight,
    down_weight,
    cotangent,
):
    ring, lines = lax.axis_size("seq"), lax.axis_size("batch")
    devices = ring * lines
    mine = lax.axis_index("seq")
    rows, width = layer_input.shape[1], layer_input.shape[2]
    length = rows * ring
    own = width // devices
    head_size = width // HEADS
    copies = ring // HEADS
    part = width // ring
    head = mine // copies
    hidden_part = gate_weight.shape[1] // ring
    slots_all = HEADS * SLOTS

    def to_order(array):
        if copies == 1:
            return array
        blocks = array.reshape((ring, rows) + array.shape[1:])
        moved = [lax.dynamic_index_in_dim(blocks, mine ^ by, 0, keepdims=False) for by in range(ring)]
        return jnp.concatenate(moved, axis=0)

    def whole_head(array):
        if copies == 1:
            return array
        full = lax.all_gather(to_order(array), "seq", axis=1, tiled=True)
        return to_order(lax.dynamic_slice_in_dim(full, head * head_size, head_size, 1))

    def own_part(array):
        if copies == 1:
            return array
        return lax.dynamic_slice_in_dim(array, (mine % copies) * part, part, 1)

    params = jnp.concatenate(
        [
            mixer_gain,
            head_gain,
            feed_gain,
            forget_bias,
            expand.T.reshape(-1),
            squeeze.reshape(-1),
        ]
    )
    count = params.shape[0]
    params = jnp.concatenate([params, segments.reshape(rows).astype(BF16)])
    input_own = layer_input.reshape(rows, width)
    grad_own = cotangent.reshape(rows, width)

    def permuted(array):
        shape = array.shape[:-1]
        array = array.reshape(shape + (ring, lines, own))
        return jnp.swapaxes(array, -3, -2).reshape(shape + (width,))

    def restored(array):
        shape = array.shape[:-1]
        array = array.reshape(shape + (lines, ring, own))
        return jnp.swapaxes(array, -3, -2).reshape(shape + (width,))

    def columns(*arrays):
        blocks = [a.reshape(own, ring, a.shape[1] // ring) for a in arrays]
        return jnp.concatenate(blocks, axis=2).transpose(1, 0, 2)

    w_output = lax.all_gather(output_weight, "batch", axis=0, tiled=True)
    mixer_columns = exchanged(
        columns(query_weight, key_weight, value_weight, swish_weight), mine, ring
    )
    w_mixer = lax.all_gather(mixer_columns.reshape(ring * own, -1), "batch", axis=0, tiled=True)
    feed_columns = exchanged(columns(gate_weight, up_weight), mine, ring)
    w_feed = lax.all_gather(feed_columns.reshape(ring * own, -1), "batch", axis=0, tiled=True)
    w_down = lax.all_gather(after(down_weight, feed_columns), "batch", axis=0, tiled=True)
    if ring != 4:
        w_feed = w_feed.reshape(lines, ring, own, -1).transpose(1, 0, 2, 3).reshape(width, -1)

    inputs = after(gathered(permuted(input_own), ring), w_output)
    small = doubled(doubled(params[None], "batch"), "seq")
    grad_out = gathered(after(grad_own, inputs, w_mixer), ring)
    small = small.reshape(devices, -1)
    segment = lax.dynamic_index_in_dim(
        small.reshape(ring, lines, -1), lax.axis_index("batch"), 1, keepdims=False
    )[:, count : count + rows].reshape(length).astype(F32)
    cuts = np.cumsum([own, own, own, slots_all // devices, RANK * slots_all // devices])
    gain_one, gain_head, gain_two, bias_full, expand_t, w_squeeze = jnp.split(
        small[:, :count], cuts, axis=1
    )
    gain_one = permuted(gain_one.reshape(width)).astype(F32)
    gain_head = lax.dynamic_slice_in_dim(gain_head.reshape(width), head * head_size, head_size, 0)
    gain_head = gain_head.astype(F32)
    gain_two = gain_two.reshape(width).astype(F32)
    bias_head = lax.dynamic_slice_in_dim(bias_full.reshape(slots_all), head * SLOTS, SLOTS, 0)
    expand_head = lax.dynamic_slice_in_dim(
        expand_t.reshape(slots_all, RANK), head * SLOTS, SLOTS, 0
    )
    w_squeeze = permuted(w_squeeze.reshape(width, RANK).T)

    chunked = segment.reshape(-1, CHUNK)
    before = jnp.concatenate([jnp.full((1,), -1.0, F32), chunked[:-1, -1]])
    previous = jnp.concatenate([jnp.full((1,), -1.0, F32), segment[:-1]])
    mask_rows = jnp.stack(
        [
            segment,
            (chunked == before[:, None]).astype(F32).reshape(-1),
            (chunked == chunked[:, -1:]).astype(F32).reshape(-1),
            (segment == previous).astype(F32),
        ]
        + [jnp.zeros_like(segment)] * 4
    )

    inputs = inputs.astype(F32)
    scale_one = rms_scale(inputs)
    plain_one = inputs * scale_one
    normed = (plain_one * gain_one).astype(BF16)
    mixer_pre = dot_nn(normed, w_mixer)
    joined = mixer_pre.astype(BF16)
    if copies > 1:
        joined = jnp.concatenate(
            [whole_head(joined[:, at * part : (at + 1) * part]) for at in range(3)], axis=1
        )
    swish_pre = whole_head(mixer_pre[:, 3 * part :])
    reduced = dot_nt(normed, w_squeeze).astype(BF16)
    forget_logit = dot_nt(expand_head, reduced) + bias_head.astype(F32)[:, None]
    log_rate = jax.nn.log_sigmoid(forget_logit) / TAU_GATE
    rates = jnp.concatenate([log_rate, -jnp.expm1(log_rate)], axis=0)
    order = mine.reshape(1).astype(jnp.int32)
    mixed, choice, starts = mixer_forward(order, ring, head_size, joined, rates, mask_rows)
    head_factor = rms_scale(mixed)
    head_plain = mixed * head_factor
    head_normed = head_plain * gain_head
    swish_sig = jax.nn.sigmoid(swish_pre)
    swish_act = swish_pre * swish_sig
    gated = own_part((head_normed * swish_act).astype(BF16))
    terms = dot_nn(gated, w_output).astype(BF16)
    terms, grad_out = lax.optimization_barrier((terms, grad_out))
    if ring == 4:
        feed_in, hidden = fold(
            finish_forward,
            terms.reshape(ring, rows, width),
            (input_own, gain_two[None]),
            (jax.ShapeDtypeStruct((rows, width), F32),),
            "fold_forward",
        )
        feed_in = feed_in.reshape(length, width)
    else:
        hidden = input_own.astype(F32) + scattered(terms, ring)
        feed_in = gathered((hidden * rms_scale(hidden) * gain_two).astype(BF16), ring)

    feed_pre = dot_nn(feed_in, w_feed)
    gate_pre, up_pre = feed_pre[:, :hidden_part], feed_pre[:, hidden_part:]
    gate_sig = jax.nn.sigmoid(gate_pre)
    gate_act = gate_pre * gate_sig
    inner = (gate_act * up_pre).astype(BF16)

    term_down = dot_tn(inner, grad_out).astype(BF16)
    grad_inner = dot_nt(after(grad_out, term_down), w_down)
    grad_gatepre = grad_inner * up_pre * (gate_sig * (1.0 + gate_pre * (1.0 - gate_sig)))
    grad_feedpre = jnp.concatenate(
        [grad_gatepre.astype(BF16), (grad_inner * gate_act).astype(BF16)], axis=1
    )
    back_feedin = dot_nt(grad_feedpre, w_feed).astype(BF16)
    result_terms = dot_nn(after(inner, back_feedin), w_down).astype(BF16)
    feed_lines = feed_in if ring == 4 else permuted(feed_in)
    term_feedpre = core_sum(after(feed_lines, back_feedin), grad_feedpre, lines, (result_terms,))
    down_share = lax.psum_scatter(term_down, "batch", scatter_dimension=0, tiled=True)
    feed_sum = line_sum(after(term_feedpre, down_share), lines)
    if ring == 4:
        grad_branch, grad_hidden, term_feed = fold(
            finish_backward,
            after(back_feedin, term_feedpre).reshape(ring, rows, width),
            (grad_own, hidden, gain_two[None]),
            (
                jax.ShapeDtypeStruct((rows, width), F32),
                jax.ShapeDtypeStruct((1, width), F32),
            ),
            "fold_backward",
        )
        grad_branch, term_feed = grad_branch.reshape(length, width), term_feed[0]
    else:
        grad_feedin = scattered(back_feedin, ring)
        scale_two = rms_scale(hidden)
        term_feed = jnp.sum(grad_feedin * hidden * scale_two, axis=0)
        scaled_two = grad_feedin * gain_two
        grad_hidden = (
            grad_own.astype(F32)
            + scale_two * scaled_two
            - hidden * scale_two**3 * jnp.mean(scaled_two * hidden, axis=-1, keepdims=True)
        )
        grad_branch = gathered(grad_hidden.astype(BF16), ring)

    grad_gated = whole_head(dot_nt(grad_branch, w_output))

    slope = swish_sig * (1.0 + swish_pre * (1.0 - swish_sig))
    grad_swishpre = own_part((grad_gated * head_normed * slope).astype(BF16))
    grad_normed_head = grad_gated * swish_act
    term_head = jnp.sum(grad_normed_head * head_plain, axis=0) / copies
    scaled_head = grad_normed_head * gain_head
    grad_mixed = head_factor * scaled_head - mixed * head_factor**3 * jnp.mean(
        scaled_head * mixed, axis=-1, keepdims=True
    )
    result, grad_mixed, normed_late = scattered(
        after(result_terms, grad_branch), ring, grad_mixed.astype(BF16), normed
    )
    layer_output = (hidden + result).astype(BF16).reshape(1, rows, width)
    term_output = core_sum(after(gated, grad_mixed), grad_branch, lines)
    output_share = line_sum(after(term_output, feed_sum), lines)
    grad_mixed = after(grad_mixed, term_output)
    grad_pre, grad_rate = mixer_backward(
        order, ring, joined, grad_mixed, rates, mask_rows, choice, starts
    )
    grad_logit = (grad_rate * jax.nn.sigmoid(-forget_logit) / TAU_GATE).astype(BF16)
    term_bias = jnp.sum(grad_logit.astype(F32), axis=1) / copies
    term_expand = dot_nn(grad_logit, reduced) / copies
    grad_reduced = (dot_tn(grad_logit, expand_head) / copies).astype(BF16)
    if copies > 1:
        grad_pre = jnp.concatenate(
            [own_part(grad_pre[:, at * head_size : (at + 1) * head_size]) for at in range(3)], axis=1
        )
    grad_pre = jnp.concatenate([grad_pre, grad_swishpre], axis=1)
    term_pre = dot_tn(normed_late, grad_pre).astype(BF16)
    pre_sum = lax.psum_scatter(
        after(term_pre, output_share), "batch", scatter_dimension=0, tiled=True
    )
    grad_normed = dot_nt(after(grad_pre, term_pre), w_mixer) + dot_nn(grad_reduced, w_squeeze)
    grad_normed = dot_nt(after(grad_pre, term_pre), w_mixer) + dot_nn(grad_reduced, w_squeeze)
    term_mixer = restored(jnp.sum(grad_normed * plain_one, axis=0))
    term_squeeze = restored(dot_tn(grad_reduced, normed))
    feed_share = exchanged(after(feed_sum, term_pre).reshape(ring, own, 2 * hidden_part), mine, ring)
    grad_normed, feed_share, (term_mixer, term_squeeze) = scattered(
        grad_normed.astype(BF16), ring, feed_share, (term_mixer, term_squeeze)
    )
    grad_normed = restored(grad_normed)
    inputs_own = input_own.astype(F32)
    scale_own = rms_scale(inputs_own)
    scaled_one = grad_normed * restored(gain_one)
    grad_input = (
        grad_hidden
        + scale_own * scaled_one
        - inputs_own * scale_own**3 * jnp.mean(scaled_one * inputs_own, axis=-1, keepdims=True)
    ).astype(BF16)
    pre_share = exchanged(pre_sum.reshape(ring, own, 4 * part), mine, ring)

    def joined_columns(blocks, first, size):
        return jnp.concatenate(
            [blocks[at, :, first : first + size] for at in range(ring)], axis=1
        ).astype(F32)

    query_share, key_share, value_share, swish_share = (
        joined_columns(pre_share, at * part, part) for at in range(4)
    )
    gate_share = joined_columns(feed_share, 0, hidden_part)
    up_share = joined_columns(feed_share, hidden_part, hidden_part)

    def placed(array, size):
        full = jnp.zeros((HEADS, size) + array.shape[1:], F32)
        return lax.dynamic_update_slice_in_dim(full, array[None], head, 0)

    terms = jnp.concatenate(
        [
            term_mixer.reshape(devices, -1),
            placed(term_head, head_size).reshape(devices, -1),
            term_feed.reshape(devices, -1),
            placed(term_bias, SLOTS).reshape(devices, -1),
            placed(term_expand, SLOTS).reshape(devices, -1),
            term_squeeze.T.reshape(devices, -1),
        ],
        axis=1,
    )
    share = halved(halved(terms, "seq"), "batch")[0]
    mixer_share, head_share, feedgain_share, bias_share, expand_share, squeeze_share = jnp.split(
        share, cuts
    )
    return (
        layer_output,
        grad_input.reshape(1, rows, width),
        mixer_share,
        query_share,
        key_share,
        value_share,
        squeeze_share.reshape(own, RANK),
        expand_share.reshape(-1, RANK).T,
        bias_share,
        swish_share,
        head_share,
        output_share.astype(F32),
        feedgain_share,
        gate_share,
        up_share,
        down_share.astype(F32),
    )


def solution(mesh):
    rows = P(BOTH, None)
    spread = P(BOTH)
    in_specs = (
        P("batch", "seq", None),
        P("batch", "seq"),
        spread,
        rows,
        rows,
        rows,
        rows,
        P(None, BOTH),
        spread,
        rows,
        spread,
        rows,
        spread,
        rows,
        rows,
        rows,
        P("batch", "seq", None),
    )
    out_specs = (
        P("batch", "seq", None),
        P("batch", "seq", None),
        spread,
        rows,
        rows,
        rows,
        rows,
        P(None, BOTH),
        spread,
        rows,
        spread,
        rows,
        spread,
        rows,
        rows,
        rows,
    )
    return jax.shard_map(local, mesh=mesh, in_specs=in_specs, out_specs=out_specs, check_vma=False)
```

```python
import functools

import jax
import jax.numpy as jnp
import numpy as np
from jax import lax
from jax.experimental import pallas as pl
from jax.experimental.pallas import tpu as pltpu
from jax.sharding import PartitionSpec as P

HEADS = 4
SLOTS = 64
RANK = 16
EPS = 1e-06
TAU_GATE = 8.0
CHUNK = 128
SUB = 16
BOTH = ("seq", "batch")
F32 = jnp.float32
BF16 = jnp.bfloat16
HIGHEST = lax.Precision.HIGHEST


def dot_nn(left, right):
    return lax.dot_general(left, right, (((1,), (0,)), ((), ())), preferred_element_type=F32)


def dot_nt(left, right):
    return lax.dot_general(left, right, (((1,), (1,)), ((), ())), preferred_element_type=F32)


def dot_tn(left, right):
    return lax.dot_general(left, right, (((0,), (0,)), ((), ())), preferred_element_type=F32)


def exact_nn(left, right):
    return lax.dot_general(
        left, right, (((1,), (0,)), ((), ())), precision=HIGHEST, preferred_element_type=F32
    )


def exact_nt(left, right):
    return lax.dot_general(
        left, right, (((1,), (1,)), ((), ())), precision=HIGHEST, preferred_element_type=F32
    )


def halves(value):
    high = value.astype(BF16)
    return high, (value - high.astype(F32)).astype(BF16)


def split_nn(left, right):
    high, rest = halves(left)
    return dot_nn(high, right) + dot_nn(rest, right)


def split_nt(left, right):
    high, rest = halves(left)
    return dot_nt(high, right) + dot_nt(rest, right)


LEVELS = (CHUNK // SUB).bit_length() - 1


def fill_tables(sums, covers, apart):
    source = lax.broadcasted_iota(jnp.int32, (CHUNK, CHUNK), 0)
    target = lax.broadcasted_iota(jnp.int32, (CHUNK, CHUNK), 1)

    def group(at, size):
        return jnp.bitwise_and(at, CHUNK - size)

    for level in range(LEVELS):
        half = SUB << level
        right = jnp.bitwise_and(target, half) != 0
        edge = group(target, 2 * half) + (half - 1)
        low, high = jnp.where(right, edge, target), jnp.where(right, target, edge)
        sums[:, level * CHUNK : (level + 1) * CHUNK] = jnp.where(
            (source > low) & (source <= high), 1.0, 0.0
        )
        same = group(source, 2 * half) == group(target, 2 * half)
        covers[level] = jnp.where(same & (jnp.bitwise_and(source, half) == 0) & right, 1.0, 0.0)
    sums[:, LEVELS * CHUNK : (LEVELS + 1) * CHUNK] = jnp.where(source <= target, 1.0, 0.0)
    sums[:, (LEVELS + 1) * CHUNK :] = jnp.where(source > target, 1.0, 0.0)
    apart[...] = jnp.where(group(source, SUB) == group(target, SUB), target - source, -1)


TABLES = [
    pltpu.VMEM((CHUNK, (LEVELS + 2) * CHUNK), F32),
    pltpu.VMEM((LEVELS, CHUNK, CHUNK), F32),
    pltpu.VMEM((CHUNK, CHUNK), jnp.int32),
]


def same_document(rows):
    source = lax.broadcasted_iota(jnp.int32, (CHUNK, CHUNK), 0)
    target = lax.broadcasted_iota(jnp.int32, (CHUNK, CHUNK), 1)
    number = rows[0:1, :]
    column = jnp.sum(jnp.where(source == target, number, 0.0), axis=1, keepdims=True)
    return column == number


def rolled(value, by):
    return value if by % CHUNK == 0 else pltpu.roll(value, by % CHUNK, 1)


def exponents(rate, sums):
    return jnp.exp(exact_nn(rate, sums))


def piece(value, at):
    return value[:, at * CHUNK : (at + 1) * CHUNK]


def mixer_forward_kernel(
    factor, mine, query, key, value, rate, rows, output, choice_out, start_out, state, sums, covers, apart
):
    levels = LEVELS

    @pl.when(pl.program_id(0) == 0)
    def _():
        state[...] = jnp.zeros_like(state)
        fill_tables(sums, covers, apart)

    key_in, value_in = state[:SLOTS, :], state[SLOTS:, :]
    start_out[0] = state[...]
    q, k, v = query[...], key[...], value[...]
    a, g = rate[:SLOTS, :], rate[SLOTS:, :]
    decay = exponents(a, sums[...])
    before, after = piece(decay, levels), piece(decay, levels + 1)
    carried = before * rows[1:2, :]
    visible = same_document(rows)
    scores = jnp.where(visible, dot_nt(k, q) * factor, 0.0)
    logits = carried * (split_nt(key_in, q) * factor)
    for level in range(levels):
        part = piece(decay, level)
        logits = logits + part * exact_nn(part * g, scores * covers[level])
    gap = apart[...]
    total = jnp.zeros_like(a)
    weights = []
    for by in range(SUB):
        if by:
            total = total + rolled(a, by - 1)
        weight = jnp.exp(total) * rolled(g, by)
        weights.append(weight)
        logits = logits + weight * jnp.sum(
            jnp.where(gap == by, scores, 0.0), axis=0, keepdims=True
        )
    attention = jnp.exp(logits - jnp.max(logits, axis=0, keepdims=True))
    attention = attention / jnp.sum(attention, axis=0, keepdims=True)
    choice_out[:SLOTS, :] = attention
    choice_out[SLOTS:, :] = logits
    mixing = jnp.zeros((CHUNK, CHUNK), F32)
    for level in range(levels):
        part = piece(decay, level)
        mixing = mixing + covers[level] * dot_tn(
            (part * g).astype(BF16), (part * attention).astype(BF16)
        )
    for by in range(SUB):
        row = jnp.sum(weights[by] * attention, axis=0, keepdims=True)
        mixing = jnp.where(gap == by, row, mixing)
    mixing = jnp.where(visible, mixing, 0.0).astype(BF16)
    output[...] = dot_tn(mixing, v) + dot_tn(
        (carried * attention).astype(BF16), value_in.astype(BF16)
    )
    ends = after * g * rows[2:3, :]
    keep = carried[:, CHUNK - 1 : CHUNK]
    state[:SLOTS, :] = keep * key_in + split_nn(ends, k)
    state[SLOTS:, :] = keep * value_in + split_nn(ends, v)


def mixer_backward_kernel(
    factor, mine, query, key, value, grad_output, rate, rows, choice, start, grad_all, grad_rate,
    state_grad, flow, sums, covers, apart,
):
    levels = LEVELS

    @pl.when(pl.program_id(0) == 0)
    def _():
        state_grad[...] = jnp.zeros_like(state_grad)
        flow[...] = jnp.zeros_like(flow)
        fill_tables(sums, covers, apart)

    key_in, value_in = start[0, :SLOTS, :], start[0, SLOTS:, :]
    key_after, value_after = state_grad[:SLOTS, :], state_grad[SLOTS:, :]
    q, k, v, d = query[...], key[...], value[...], grad_output[...]
    size = q.shape[1]
    a, g = rate[:SLOTS, :], rate[SLOTS:, :]
    attention, logits = choice[:SLOTS, :], choice[SLOTS:, :]
    decay = exponents(a, sums[...])
    before, after = piece(decay, levels), piece(decay, levels + 1)
    carried = before * rows[1:2, :]
    visible = same_document(rows)
    scores = jnp.where(visible, dot_nt(k, q) * factor, 0.0)
    reads = jnp.where(visible, dot_nt(v, d), 0.0)
    gap = apart[...]
    grad_att = carried * split_nt(value_in, d)
    for level in range(levels):
        part = piece(decay, level)
        grad_att = grad_att + part * exact_nn(part * g, reads * covers[level])
    total = jnp.zeros_like(a)
    bare, weights, score_rows, read_rows = [], [], [], []
    for by in range(SUB):
        if by:
            total = total + rolled(a, by - 1)
        bare.append(jnp.exp(total))
        weights.append(bare[by] * rolled(g, by))
        score_rows.append(jnp.sum(jnp.where(gap == by, scores, 0.0), axis=0, keepdims=True))
        read_rows.append(jnp.sum(jnp.where(gap == by, reads, 0.0), axis=0, keepdims=True))
        grad_att = grad_att + weights[by] * read_rows[by]
    grad_logits = attention * (
        grad_att - jnp.sum(attention * grad_att, axis=0, keepdims=True)
    )
    mixing = jnp.zeros((CHUNK, CHUNK), F32)
    spread = jnp.zeros((CHUNK, CHUNK), F32)
    ends = after * rows[2:3, :]
    grad_inflow = ends * (split_nt(key_after, k) + split_nt(value_after, v))
    for level in range(levels):
        part = piece(decay, level)
        left = (part * g).astype(BF16)
        att_part, log_part = part * attention, part * grad_logits
        mixing = mixing + covers[level] * dot_tn(left, att_part.astype(BF16))
        spread = spread + covers[level] * dot_tn(left, log_part.astype(BF16))
        grad_inflow = grad_inflow + part * (
            exact_nt(log_part, scores * covers[level]) + exact_nt(att_part, reads * covers[level])
        )
    for by in range(SUB):
        row = jnp.sum(weights[by] * attention, axis=0, keepdims=True)
        mixing = jnp.where(gap == by, row, mixing)
        row = jnp.sum(weights[by] * grad_logits, axis=0, keepdims=True)
        spread = jnp.where(gap == by, row, spread)
        terms = bare[by] * (grad_logits * score_rows[by] + attention * read_rows[by])
        grad_inflow = grad_inflow + rolled(terms, -by)
    mixing = jnp.where(visible, mixing, 0.0).astype(BF16)
    spread = (jnp.where(visible, spread, 0.0) * factor).astype(BF16)
    log_carried = carried * grad_logits * factor
    att_carried = carried * attention
    ends = (ends * g).astype(BF16)
    grad_all[:, :size] = (
        dot_tn(spread, k) + dot_tn(log_carried.astype(BF16), key_in.astype(BF16))
    ).astype(BF16)
    grad_all[:, size : 2 * size] = (dot_nn(spread, q) + dot_tn(ends, key_after.astype(BF16))).astype(BF16)
    grad_all[:, 2 * size :] = (dot_nn(mixing, d) + dot_tn(ends, value_after.astype(BF16))).astype(BF16)
    change = grad_logits * logits + attention * grad_att - g * grad_inflow
    later = piece(sums, levels + 1) + jnp.where(gap == 0, 1.0, 0.0)
    same = jnp.where(visible, later, 0.0)
    flows = exact_nn(change, same) + rows[2:3, :] * flow[:, 0:1]
    grad_rate[...] = rows[3:4, :] * flows - jnp.exp(a) * grad_inflow
    keep = carried[:, CHUNK - 1 : CHUNK]
    key_before = keep * key_after + split_nn(log_carried, q)
    value_before = keep * value_after + split_nn(att_carried, d)
    state_grad[:SLOTS, :] = key_before
    state_grad[SLOTS:, :] = value_before
    flow[...] = jnp.broadcast_to(
        jnp.sum(key_before * key_in + value_before * value_in, axis=1, keepdims=True), flow.shape
    )


def mixer_specs(length, size, ring, backward):
    count = length // CHUNK
    per = count // ring

    def natural(step):
        return count - 1 - step if backward else step

    def moved(step, mine):
        at = natural(step)
        return lax.bitwise_xor(at // per, mine[0]) * per + at % per

    wide = [
        pl.BlockSpec((CHUNK, size), lambda step, mine, at=at: (moved(step, mine), at))
        for at in range(3)
    ]
    everything = pl.BlockSpec((CHUNK, 3 * size), lambda step, mine: (moved(step, mine), 0))
    pair = pl.BlockSpec((2 * SLOTS, CHUNK), lambda step, mine: (0, moved(step, mine)))
    slim = pl.BlockSpec((SLOTS, CHUNK), lambda step, mine: (0, moved(step, mine)))
    rows = pl.BlockSpec((8, CHUNK), lambda step, mine: (0, natural(step)))
    state = pl.BlockSpec((1, 2 * SLOTS, size), lambda step, mine: (natural(step), 0, 0))
    return count, wide, everything, pair, slim, rows, state


def mixer_forward(mine, ring, size, joined, rates, rows):
    length = joined.shape[0]
    count, wide, _, pair, _, row_spec, state = mixer_specs(length, size, ring, False)
    return pl.pallas_call(
        functools.partial(mixer_forward_kernel, size ** (-0.25)),
        out_shape=(
            jax.ShapeDtypeStruct((length, size), F32),
            jax.ShapeDtypeStruct((2 * SLOTS, length), F32),
            jax.ShapeDtypeStruct((count, 2 * SLOTS, size), F32),
        ),
        grid_spec=pltpu.PrefetchScalarGridSpec(
            num_scalar_prefetch=1,
            grid=(count,),
            in_specs=wide + [pair, row_spec],
            out_specs=[wide[0], pair, state],
            scratch_shapes=[pltpu.VMEM((2 * SLOTS, size), F32)] + TABLES,
        ),
        compiler_params=pltpu.CompilerParams(vmem_limit_bytes=32 << 20),
        cost_estimate=pl.CostEstimate(
            flops=length * size * 2000, bytes_accessed=length * size * 12, transcendentals=length * 4096
        ),
        name="mixer_forward",
    )(mine, joined, joined, joined, rates, rows)


def mixer_backward(mine, ring, joined, grad, rates, rows, choice, starts):
    length, size = grad.shape
    count, wide, everything, pair, slim, row_spec, state = mixer_specs(length, size, ring, True)
    return pl.pallas_call(
        functools.partial(mixer_backward_kernel, size ** (-0.25)),
        out_shape=(
            jax.ShapeDtypeStruct((length, 3 * size), BF16),
            jax.ShapeDtypeStruct((SLOTS, length), F32),
        ),
        grid_spec=pltpu.PrefetchScalarGridSpec(
            num_scalar_prefetch=1,
            grid=(count,),
            in_specs=wide + [wide[0], pair, row_spec, pair, state],
            out_specs=[everything, slim],
            scratch_shapes=[pltpu.VMEM((2 * SLOTS, size), F32), pltpu.VMEM((SLOTS, 128), F32)]
            + TABLES,
        ),
        compiler_params=pltpu.CompilerParams(vmem_limit_bytes=32 << 20),
        cost_estimate=pl.CostEstimate(
            flops=length * size * 4000, bytes_accessed=length * size * 20, transcendentals=length * 4096
        ),
        name="mixer_backward",
    )(mine, joined, joined, joined, grad, rates, rows, choice, starts)


def peers(ring, mine):
    found = []
    for by in range(1, ring):
        at, bit = mine, 1
        while bit <= by:
            if by & bit:
                at = at + bit * (1 - 2 * ((at // bit) % 2))
            bit *= 2
        found.append(at)
    return found


class Copies:
    def __init__(self, local, send, recv):
        self.local, self.send, self.recv = local, send, recv
        self.here, self.away = 0, 0
        self.open = []

    def near(self, source, target):
        copy = pltpu.make_async_copy(source, target, self.local.at[self.here])
        self.here += 1
        copy.start()
        return copy

    def far(self, source, target, landed, device, when=None):
        at = self.away
        self.away += 1
        copy = pltpu.make_async_remote_copy(
            source, target, self.send.at[at], self.recv.at[at], device_id=device,
            device_id_type=pl.DeviceIdType.MESH,
        )
        if when is None:
            copy.start()
        else:
            pl.when(when)(copy.start)
        self.open.append((copy, when))
        return pltpu.make_async_remote_copy(
            landed, landed, self.send.at[at], self.recv.at[at], device_id=device,
            device_id_type=pl.DeviceIdType.MESH,
        ).wait_recv

    def close(self):
        for copy, when in self.open:
            if when is None:
                copy.wait_send()
            else:
                pl.when(when)(copy.wait_send)


PARTS = 4


def fold_kernel(finish, extras, *refs):
    terms, given = refs[0], refs[1 : 1 + extras]
    blocks = refs[1 + extras]
    made = refs[2 + extras : -9]
    first, second, third, two_low, one_high, own, local_sem, send_sem, recv_sem = refs[-9:]
    mine, batch = lax.axis_index("seq"), lax.axis_index("batch")
    others = peers(4, mine)
    row, col = (others[0], batch), (others[1], batch)
    copies = Copies(local_sem, send_sem, recv_sem)
    size = terms.shape[1] // PARTS

    def span(at):
        low = pl.ds(at * size, size // 2)
        return pl.ds(at * size, size), low, pl.ds(at * size + size // 2, size // 2)

    opening, direct = [], []

    def open_part(at):
        _, low, high = span(at)
        opening.append(
            (
                copies.far(terms.at[3, low], first.at[low], first.at[low], row),
                copies.far(terms.at[3, high], first.at[high], first.at[high], col),
            )
        )

    def pass_part(at):
        _, low, high = span(at)
        waits = [
            copies.far(terms.at[2, high], second.at[high], second.at[high], col),
            copies.far(terms.at[1, low], third.at[low], third.at[low], row),
        ]
        opening[at][0]()
        two_low[low, :] = added(terms[2, low, :], first[low, :])
        waits.append(copies.far(two_low.at[low], second.at[low], second.at[low], col))
        opening[at][1]()
        one_high[high, :] = added(terms[1, high, :], first[high, :])
        waits.append(copies.far(one_high.at[high], third.at[high], third.at[high], row))
        direct.append(waits)

    spread, local, passed = [], [], []

    def close_part(at):
        full, _, _ = span(at)
        for wait in direct[at]:
            wait()
        total = terms[0, full, :].astype(F32) + second[full, :].astype(F32) + third[full, :].astype(F32)
        own[full, :] = finish(total, full, at, given, made)
        spread.append(
            (
                copies.far(own.at[full], blocks.at[1, full], blocks.at[1, full], row),
                copies.far(own.at[full], blocks.at[2, full], blocks.at[2, full], col),
            )
        )
        local.append(copies.near(own.at[full], blocks.at[0, full]))

    def forward_part(at):
        _, low, high = span(at)
        for wait in spread[at]:
            wait()
        passed.append(copies.far(blocks.at[2, low], blocks.at[3, low], blocks.at[3, low], row))
        passed.append(copies.far(blocks.at[1, high], blocks.at[3, high], blocks.at[3, high], col))

    open_part(0)
    for at in range(PARTS + 2):
        if at + 1 < PARTS:
            open_part(at + 1)
        if at < PARTS:
            pass_part(at)
        if 1 <= at <= PARTS:
            close_part(at - 1)
        if at >= 2:
            forward_part(at - 2)
    for wait in passed:
        wait()
    for copy in local:
        copy.wait()
    copies.close()


def half_blocks(value, order):
    lane = lax.broadcasted_iota(jnp.int32, (value.shape[0], 128), 1)
    made = []
    for pair in zip(order[::2], order[1::2]):
        low, high = (
            value[:, block * 128 : (block + 1) * 128]
            if half == want
            else pltpu.roll(value[:, block * 128 : (block + 1) * 128], 64, 1)
            for want, (block, half) in enumerate(pair)
        )
        made.append(jnp.where(lane < 64, low, high))
    return jnp.concatenate(made, axis=1)


def by_line(value):
    lines = value.shape[1] // 256
    return half_blocks(
        value, [divmod(ring * lines + line, 2) for line in range(lines) for ring in range(4)]
    )


def by_ring(value):
    lines = value.shape[1] // 256
    return half_blocks(
        value, [divmod(line * 4 + ring, 2) for ring in range(4) for line in range(lines)]
    )


def finish_forward(total, full, at, given, made):
    inputs, gain = given
    hidden = inputs[full, :].astype(F32) + total
    made[0][full, :] = hidden
    return by_line(hidden * rms_scale(hidden) * gain[...]).astype(BF16)


def finish_backward(total, full, at, given, made):
    cotangent, hidden_ref, gain = given
    total = by_ring(total)
    hidden = hidden_ref[full, :]
    scale = rms_scale(hidden)
    plain = hidden * scale
    term = jnp.sum(total * plain, axis=0, keepdims=True)
    made[1][...] = term if at == 0 else made[1][...] + term
    scaled = total * gain[...]
    grad = (
        cotangent[full, :].astype(F32)
        + scale * scaled
        - plain * (scale * jnp.mean(scaled * plain, axis=-1, keepdims=True))
    )
    made[0][full, :] = grad
    return grad.astype(BF16)


def fold(finish, terms, given, made, name):
    ring, rows, width = terms.shape
    inside = pl.BlockSpec(memory_space=pltpu.VMEM)
    block = pltpu.VMEM((rows, width), BF16)
    return pl.pallas_call(
        functools.partial(fold_kernel, finish, len(given)),
        out_shape=(jax.ShapeDtypeStruct((ring, rows, width), BF16),) + made,
        in_specs=[inside] * (1 + len(given)),
        out_specs=[pl.BlockSpec(memory_space=pltpu.HBM)] + [inside] * len(made),
        scratch_shapes=[block] * 6
        + [
            pltpu.SemaphoreType.DMA((PARTS,)),
            pltpu.SemaphoreType.DMA((PARTS * 10,)),
            pltpu.SemaphoreType.DMA((PARTS * 10,)),
        ],
        compiler_params=pltpu.CompilerParams(has_side_effects=True, vmem_limit_bytes=40 << 20),
        name=name,
    )(terms, *given)


def rms_scale(features):
    return lax.rsqrt(jnp.mean(features * features, axis=-1, keepdims=True) + EPS)


def swapped(block, by, ring):
    return lax.ppermute(block, "seq", [(i, i ^ by) for i in range(ring)])


def gathered(block, ring):
    if ring != 4:
        return jnp.concatenate([block] + [swapped(block, by, ring) for by in range(1, ring)], axis=0)
    half = block.shape[0] // 2
    one, two = swapped(block, 1, ring), swapped(block, 2, ring)
    low, high = swapped(two[:half], 1, ring), swapped(one[half:], 2, ring)
    return jnp.concatenate([block, one, two, low, high], axis=0)


def scattered(terms, ring, wait_first=None, wait_second=None):
    rows = terms.shape[0] // ring
    parts = [terms[by * rows : (by + 1) * rows] for by in range(ring)]
    total = parts[0].astype(F32)
    if ring != 4:
        for by in range(1, ring):
            total = total + swapped(parts[by], by, ring).astype(F32)
        return total if wait_first is None else (total, wait_first, wait_second)
    half = rows // 2
    low, high = swapped(parts[3][:half], 1, ring), swapped(parts[3][half:], 2, ring)
    if wait_first is not None:
        low, high, wait_first = lax.optimization_barrier((low, high, wait_first))
    two = jnp.concatenate([added(parts[2][:half], low), parts[2][half:]], axis=0)
    one = jnp.concatenate([parts[1][:half], added(parts[1][half:], high)], axis=0)
    one, two = swapped(one, 1, ring), swapped(two, 2, ring)
    if wait_first is not None:
        one, two, wait_second = lax.optimization_barrier((one, two, wait_second))
    total = total + one.astype(F32) + two.astype(F32)
    return total if wait_first is None else (total, wait_first, wait_second)


def added(left, right):
    return (left.astype(F32) + right.astype(F32)).astype(BF16)


def flipped(block, axis, by):
    return lax.ppermute(block, axis, [(i, i ^ by) for i in range(lax.axis_size(axis))])


def doubled(block, axis):
    by, mine = 1, lax.axis_index(axis)
    while by < lax.axis_size(axis):
        other = flipped(block, axis, by)
        first = (mine & by) == 0
        block = jnp.concatenate(
            [jnp.where(first, block, other), jnp.where(first, other, block)], axis=0
        )
        by *= 2
    return block


def halved(block, axis):
    by, mine = lax.axis_size(axis) // 2, lax.axis_index(axis)
    while by:
        low, high = jnp.split(block, 2, axis=0)
        first = (mine & by) == 0
        block = jnp.where(first, low, high) + flipped(jnp.where(first, high, low), axis, by)
        by //= 2
    return block


def core_halves(array, lines, axis):
    size = array.shape[axis] // lines
    even, odd = (
        jnp.concatenate(
            [
                lax.slice_in_dim(array, line * size, (line + 1) * size, axis=axis)
                for line in range(which, lines, 2)
            ],
            axis=axis,
        )
        for which in range(2)
    )
    first = lax.axis_index("batch") % 2 == 0
    return jnp.where(first, even, odd), jnp.where(first, odd, even)


def core_sum(features, grads, lines, fill=()):
    if (features.shape[1] // lines) % 128:
        mine, others = core_halves(dot_tn(features, grads).astype(BF16), lines, 0)
        return added(mine, flipped(others, "batch", 1))
    mine, others = core_halves(features, lines, 1)
    sent = flipped(dot_tn(others, grads).astype(BF16), "batch", 1)
    mine = after(mine, *fill) if fill else mine
    return (dot_tn(mine, grads) + sent.astype(F32)).astype(BF16)


def line_sum(terms, lines):
    groups = [list(range(core, lines, 2)) for core in range(2)]
    return lax.psum_scatter(
        terms, "batch", scatter_dimension=0, axis_index_groups=groups, tiled=True
    )


def after(value, *others):
    return lax.optimization_barrier((value,) + others)[0]


def exchanged(blocks, mine, ring):
    parts = [
        swapped(lax.dynamic_index_in_dim(blocks, mine ^ by, 0, keepdims=False), by, ring)
        if by
        else lax.dynamic_index_in_dim(blocks, mine, 0, keepdims=False)
        for by in range(ring)
    ]
    made = jnp.stack(parts)
    return jnp.concatenate(
        [lax.dynamic_index_in_dim(made, mine ^ j, 0, keepdims=True) for j in range(ring)], axis=0
    )


def local(
    layer_input,
    segments,
    mixer_gain,
    query_weight,
    key_weight,
    value_weight,
    squeeze,
    expand,
    forget_bias,
    swish_weight,
    head_gain,
    output_weight,
    feed_gain,
    gate_weight,
    up_weight,
    down_weight,
    cotangent,
):
    ring, lines = lax.axis_size("seq"), lax.axis_size("batch")
    devices = ring * lines
    mine = lax.axis_index("seq")
    rows, width = layer_input.shape[1], layer_input.shape[2]
    length = rows * ring
    own = width // devices
    head_size = width // HEADS
    copies = ring // HEADS
    part = width // ring
    head = mine // copies
    hidden_part = gate_weight.shape[1] // ring
    slots_all = HEADS * SLOTS

    def to_order(array):
        if copies == 1:
            return array
        blocks = array.reshape((ring, rows) + array.shape[1:])
        moved = [lax.dynamic_index_in_dim(blocks, mine ^ by, 0, keepdims=False) for by in range(ring)]
        return jnp.concatenate(moved, axis=0)

    def whole_head(array):
        if copies == 1:
            return array
        full = lax.all_gather(to_order(array), "seq", axis=1, tiled=True)
        return to_order(lax.dynamic_slice_in_dim(full, head * head_size, head_size, 1))

    def own_part(array):
        if copies == 1:
            return array
        return lax.dynamic_slice_in_dim(array, (mine % copies) * part, part, 1)

    params = jnp.concatenate(
        [
            mixer_gain,
            head_gain,
            feed_gain,
            forget_bias,
            expand.T.reshape(-1),
            squeeze.reshape(-1),
        ]
    )
    count = params.shape[0]
    params = jnp.concatenate([params, segments.reshape(rows).astype(BF16)])
    input_own = layer_input.reshape(rows, width)
    grad_own = cotangent.reshape(rows, width)

    def permuted(array):
        shape = array.shape[:-1]
        array = array.reshape(shape + (ring, lines, own))
        return jnp.swapaxes(array, -3, -2).reshape(shape + (width,))

    def restored(array):
        shape = array.shape[:-1]
        array = array.reshape(shape + (lines, ring, own))
        return jnp.swapaxes(array, -3, -2).reshape(shape + (width,))

    def columns(*arrays):
        blocks = [a.reshape(own, ring, a.shape[1] // ring) for a in arrays]
        return jnp.concatenate(blocks, axis=2).transpose(1, 0, 2)

    w_output = lax.all_gather(output_weight, "batch", axis=0, tiled=True)
    mixer_columns = exchanged(
        columns(query_weight, key_weight, value_weight, swish_weight), mine, ring
    )
    w_mixer = lax.all_gather(mixer_columns.reshape(ring * own, -1), "batch", axis=0, tiled=True)
    feed_columns = exchanged(columns(gate_weight, up_weight), mine, ring)
    w_feed = lax.all_gather(feed_columns.reshape(ring * own, -1), "batch", axis=0, tiled=True)
    w_down = lax.all_gather(after(down_weight, feed_columns), "batch", axis=0, tiled=True)
    if ring != 4:
        w_feed = w_feed.reshape(lines, ring, own, -1).transpose(1, 0, 2, 3).reshape(width, -1)

    inputs = after(gathered(permuted(input_own), ring), w_output)
    small = doubled(doubled(params[None], "batch"), "seq")
    grad_out = gathered(after(grad_own, inputs, w_mixer), ring)
    small = small.reshape(devices, -1)
    segment = lax.dynamic_index_in_dim(
        small.reshape(ring, lines, -1), lax.axis_index("batch"), 1, keepdims=False
    )[:, count : count + rows].reshape(length).astype(F32)
    cuts = np.cumsum([own, own, own, slots_all // devices, RANK * slots_all // devices])
    gain_one, gain_head, gain_two, bias_full, expand_t, w_squeeze = jnp.split(
        small[:, :count], cuts, axis=1
    )
    gain_one = permuted(gain_one.reshape(width)).astype(F32)
    gain_head = lax.dynamic_slice_in_dim(gain_head.reshape(width), head * head_size, head_size, 0)
    gain_head = gain_head.astype(F32)
    gain_two = gain_two.reshape(width).astype(F32)
    bias_head = lax.dynamic_slice_in_dim(bias_full.reshape(slots_all), head * SLOTS, SLOTS, 0)
    expand_head = lax.dynamic_slice_in_dim(
        expand_t.reshape(slots_all, RANK), head * SLOTS, SLOTS, 0
    )
    w_squeeze = permuted(w_squeeze.reshape(width, RANK).T)

    chunked = segment.reshape(-1, CHUNK)
    before = jnp.concatenate([jnp.full((1,), -1.0, F32), chunked[:-1, -1]])
    previous = jnp.concatenate([jnp.full((1,), -1.0, F32), segment[:-1]])
    mask_rows = jnp.stack(
        [
            segment,
            (chunked == before[:, None]).astype(F32).reshape(-1),
            (chunked == chunked[:, -1:]).astype(F32).reshape(-1),
            (segment == previous).astype(F32),
        ]
        + [jnp.zeros_like(segment)] * 4
    )

    inputs = inputs.astype(F32)
    scale_one = rms_scale(inputs)
    plain_one = inputs * scale_one
    normed = (plain_one * gain_one).astype(BF16)
    mixer_pre = dot_nn(normed, w_mixer)
    joined = mixer_pre.astype(BF16)
    if copies > 1:
        joined = jnp.concatenate(
            [whole_head(joined[:, at * part : (at + 1) * part]) for at in range(3)], axis=1
        )
    swish_pre = whole_head(mixer_pre[:, 3 * part :])
    reduced = dot_nt(normed, w_squeeze).astype(BF16)
    forget_logit = dot_nt(expand_head, reduced) + bias_head.astype(F32)[:, None]
    log_rate = jax.nn.log_sigmoid(forget_logit) / TAU_GATE
    rates = jnp.concatenate([log_rate, -jnp.expm1(log_rate)], axis=0)
    order = mine.reshape(1).astype(jnp.int32)
    mixed, choice, starts = mixer_forward(order, ring, head_size, joined, rates, mask_rows)
    head_factor = rms_scale(mixed)
    head_plain = mixed * head_factor
    head_normed = head_plain * gain_head
    swish_sig = jax.nn.sigmoid(swish_pre)
    swish_act = swish_pre * swish_sig
    gated = own_part((head_normed * swish_act).astype(BF16))
    terms = dot_nn(gated, w_output).astype(BF16)
    terms, grad_out = lax.optimization_barrier((terms, grad_out))
    if ring == 4:
        feed_in, hidden = fold(
            finish_forward,
            terms.reshape(ring, rows, width),
            (input_own, gain_two[None]),
            (jax.ShapeDtypeStruct((rows, width), F32),),
            "fold_forward",
        )
        feed_in = feed_in.reshape(length, width)
    else:
        hidden = input_own.astype(F32) + scattered(terms, ring)
        feed_in = gathered((hidden * rms_scale(hidden) * gain_two).astype(BF16), ring)

    feed_pre = dot_nn(feed_in, w_feed)
    gate_pre, up_pre = feed_pre[:, :hidden_part], feed_pre[:, hidden_part:]
    gate_sig = jax.nn.sigmoid(gate_pre)
    gate_act = gate_pre * gate_sig
    inner = (gate_act * up_pre).astype(BF16)

    term_down = dot_tn(inner, grad_out).astype(BF16)
    grad_inner = dot_nt(after(grad_out, term_down), w_down)
    grad_gatepre = grad_inner * up_pre * (gate_sig * (1.0 + gate_pre * (1.0 - gate_sig)))
    grad_feedpre = jnp.concatenate(
        [grad_gatepre.astype(BF16), (grad_inner * gate_act).astype(BF16)], axis=1
    )
    back_feedin = dot_nt(grad_feedpre, w_feed).astype(BF16)
    result_terms = dot_nn(after(inner, back_feedin), w_down).astype(BF16)
    feed_lines = feed_in if ring == 4 else permuted(feed_in)
    term_feedpre = core_sum(after(feed_lines, back_feedin), grad_feedpre, lines, (result_terms,))
    down_share = lax.psum_scatter(term_down, "batch", scatter_dimension=0, tiled=True)
    feed_sum = line_sum(after(term_feedpre, down_share), lines)
    if ring == 4:
        grad_branch, grad_hidden, term_feed = fold(
            finish_backward,
            after(back_feedin, term_feedpre).reshape(ring, rows, width),
            (grad_own, hidden, gain_two[None]),
            (
                jax.ShapeDtypeStruct((rows, width), F32),
                jax.ShapeDtypeStruct((1, width), F32),
            ),
            "fold_backward",
        )
        grad_branch, term_feed = grad_branch.reshape(length, width), term_feed[0]
    else:
        grad_feedin = scattered(back_feedin, ring)
        scale_two = rms_scale(hidden)
        term_feed = jnp.sum(grad_feedin * hidden * scale_two, axis=0)
        scaled_two = grad_feedin * gain_two
        grad_hidden = (
            grad_own.astype(F32)
            + scale_two * scaled_two
            - hidden * scale_two**3 * jnp.mean(scaled_two * hidden, axis=-1, keepdims=True)
        )
        grad_branch = gathered(grad_hidden.astype(BF16), ring)

    grad_gated = whole_head(dot_nt(grad_branch, w_output))

    slope = swish_sig * (1.0 + swish_pre * (1.0 - swish_sig))
    grad_swishpre = own_part((grad_gated * head_normed * slope).astype(BF16))
    grad_normed_head = grad_gated * swish_act
    term_head = jnp.sum(grad_normed_head * head_plain, axis=0) / copies
    scaled_head = grad_normed_head * gain_head
    grad_mixed = head_factor * scaled_head - mixed * head_factor**3 * jnp.mean(
        scaled_head * mixed, axis=-1, keepdims=True
    )
    result, grad_mixed, normed_late = scattered(
        after(result_terms, grad_branch), ring, grad_mixed.astype(BF16), normed
    )
    layer_output = (hidden + result).astype(BF16).reshape(1, rows, width)
    term_output = core_sum(after(gated, grad_mixed), grad_branch, lines)
    output_share = line_sum(after(term_output, feed_sum), lines)
    grad_mixed = after(grad_mixed, term_output)
    grad_pre, grad_rate = mixer_backward(
        order, ring, joined, grad_mixed, rates, mask_rows, choice, starts
    )
    grad_logit = (grad_rate * jax.nn.sigmoid(-forget_logit) / TAU_GATE).astype(BF16)
    term_bias = jnp.sum(grad_logit.astype(F32), axis=1) / copies
    term_expand = dot_nn(grad_logit, reduced) / copies
    grad_reduced = (dot_tn(grad_logit, expand_head) / copies).astype(BF16)
    if copies > 1:
        grad_pre = jnp.concatenate(
            [own_part(grad_pre[:, at * head_size : (at + 1) * head_size]) for at in range(3)], axis=1
        )
    grad_pre = jnp.concatenate([grad_pre, grad_swishpre], axis=1)
    term_pre = dot_tn(normed_late, grad_pre).astype(BF16)
    pre_sum = lax.psum_scatter(
        after(term_pre, output_share), "batch", scatter_dimension=0, tiled=True
    )
    grad_normed = dot_nt(after(grad_pre, term_pre), w_mixer) + dot_nn(grad_reduced, w_squeeze)
    grad_normed = dot_nt(after(grad_pre, term_pre), w_mixer) + dot_nn(grad_reduced, w_squeeze)
    term_mixer = restored(jnp.sum(grad_normed * plain_one, axis=0))
    term_squeeze = restored(dot_tn(grad_reduced, normed))
    feed_share = exchanged(after(feed_sum, term_pre).reshape(ring, own, 2 * hidden_part), mine, ring)
    grad_normed, (feed_share, term_mixer, term_squeeze), _ = scattered(
        grad_normed.astype(BF16), ring, (feed_share, term_mixer, term_squeeze), term_bias
    )
    grad_normed = restored(grad_normed)
    inputs_own = input_own.astype(F32)
    scale_own = rms_scale(inputs_own)
    scaled_one = grad_normed * restored(gain_one)
    grad_input = (
        grad_hidden
        + scale_own * scaled_one
        - inputs_own * scale_own**3 * jnp.mean(scaled_one * inputs_own, axis=-1, keepdims=True)
    ).astype(BF16)
    pre_share = exchanged(pre_sum.reshape(ring, own, 4 * part), mine, ring)

    def joined_columns(blocks, first, size):
        return jnp.concatenate(
            [blocks[at, :, first : first + size] for at in range(ring)], axis=1
        ).astype(F32)

    query_share, key_share, value_share, swish_share = (
        joined_columns(pre_share, at * part, part) for at in range(4)
    )
    gate_share = joined_columns(feed_share, 0, hidden_part)
    up_share = joined_columns(feed_share, hidden_part, hidden_part)

    def placed(array, size):
        full = jnp.zeros((HEADS, size) + array.shape[1:], F32)
        return lax.dynamic_update_slice_in_dim(full, array[None], head, 0)

    terms = jnp.concatenate(
        [
            term_mixer.reshape(devices, -1),
            placed(term_head, head_size).reshape(devices, -1),
            term_feed.reshape(devices, -1),
            placed(term_bias, SLOTS).reshape(devices, -1),
            placed(term_expand, SLOTS).reshape(devices, -1),
            term_squeeze.T.reshape(devices, -1),
        ],
        axis=1,
    )
    share = halved(halved(terms, "seq"), "batch")[0]
    mixer_share, head_share, feedgain_share, bias_share, expand_share, squeeze_share = jnp.split(
        share, cuts
    )
    return (
        layer_output,
        grad_input.reshape(1, rows, width),
        mixer_share,
        query_share,
        key_share,
        value_share,
        squeeze_share.reshape(own, RANK),
        expand_share.reshape(-1, RANK).T,
        bias_share,
        swish_share,
        head_share,
        output_share.astype(F32),
        feedgain_share,
        gate_share,
        up_share,
        down_share.astype(F32),
    )


def solution(mesh):
    rows = P(BOTH, None)
    spread = P(BOTH)
    in_specs = (
        P("batch", "seq", None),
        P("batch", "seq"),
        spread,
        rows,
        rows,
        rows,
        rows,
        P(None, BOTH),
        spread,
        rows,
        spread,
        rows,
        spread,
        rows,
        rows,
        rows,
        P("batch", "seq", None),
    )
    out_specs = (
        P("batch", "seq", None),
        P("batch", "seq", None),
        spread,
        rows,
        rows,
        rows,
        rows,
        P(None, BOTH),
        spread,
        rows,
        spread,
        rows,
        spread,
        rows,
        rows,
        rows,
    )
    return jax.shard_map(local, mesh=mesh, in_specs=in_specs, out_specs=out_specs, check_vma=False)
```
